32 devices in a mesh: dp: 8 (over y, x, core), tensor: 4 (over z).
Axes of the slice: x: 2, y: 2, z: 4, core: 2. Of those that a mesh axis runs over, the one named last changes fastest.
Arguments:
- tokens: bfloat16 [16384, 1024], P(('dp', 'tensor')), may hold values from -6 to 6
- lengths: int32 [8], P('dp'), may hold values from 120 to 2048, as said below
- ln1_gain: float32 [1024], replicated, may hold values from 0.1 to 1.9
- ln1_bias: float32 [1024], replicated, may hold values from -3 to 3
- w_query: bfloat16 [1024, 1024], P(None, 'tensor'), may hold values from -0.25 to 0.25
- w_key: bfloat16 [1024, 1024], P(None, 'tensor'), may hold values from -0.25 to 0.25
- w_value: bfloat16 [1024, 1024], P(None, 'tensor'), may hold values from -0.1875 to 0.1875
- w_out: bfloat16 [1024, 1024], P('tensor'), may hold values from -0.75 to 0.75
- ln2_gain: float32 [1024], replicated, may hold values from 0.1 to 1.9
- ln2_bias: float32 [1024], replicated, may hold values from -3 to 3
- w_gate: bfloat16 [1024, 4096], P(None, 'tensor'), may hold values from -0.1875 to 0.1875
- w_up: bfloat16 [1024, 4096], P(None, 'tensor'), may hold values from -0.1875 to 0.1875
- down_weight: bfloat16 [4096, 1024], P('tensor'), may hold values from -0.125 to 0.125
- cotangent: bfloat16 [16384, 1024], P(('dp', 'tensor')), may hold values from -6 to 6
Outputs:
- output: bfloat16 [16384, 1024], P(('dp', 'tensor'))
- input_grad: float32 [16384, 1024], P(('dp', 'tensor'))
- ln1_gain_grad: float32 [1024], replicated
- ln1_bias_grad: float32 [1024], replicated
- query_grad: float32 [1024, 1024], P(None, 'tensor')
- key_grad: float32 [1024, 1024], P(None, 'tensor')
- value_grad: float32 [1024, 1024], P(None, 'tensor')
- out_grad: float32 [1024, 1024], P('tensor')
- ln2_gain_grad: float32 [1024], replicated
- ln2_bias_grad: float32 [1024], replicated
- gate_grad: float32 [1024, 4096], P(None, 'tensor')
- up_grad: float32 [1024, 4096], P(None, 'tensor')
- down_grad: float32 [4096, 1024], P('tensor')
The draws below stay inside these ranges and needn't reach their ends.
Inputs may be any that keep to these rules, and one draw needn't show every extreme that they name: `lengths`: real tokens of each window; every draw has a window of exactly 2048 and one of exactly 120.
All inputs are finite; a program needn't handle non-finite values.
Results may differ from the reference program's by a relative error of at most 0.023.
The reference program's roundings to bfloat16 on the way count: a program that leaves them out, or rounds other values in their place, can miss the bound.
Values may be sent and summed in bfloat16 or wider, within the bound.
A program may use at most 192 MiB of HBM per device.

```python
import math
import jax
import jax.numpy as jnp
from jax import lax

D = 1024
HD = 64
FF = 4096
LEN = 2048
SHORTEST = 120
SEQS = 8
TOKENS = 16384
N_TENSOR = 4


def draw_lengths(key, part):
    first_key, second_key, third_key, fourth_key = jax.random.split(key, 4)
    spread = LEN - SHORTEST + 1
    first = jax.random.randint(first_key, (SEQS,), 0, spread)
    second = jax.random.randint(second_key, (SEQS,), 0, spread)
    picked = SHORTEST + jnp.maximum(first, second)
    longest_at = jax.random.randint(third_key, (), 0, SEQS)
    shortest_at = (longest_at + 1 + jax.random.randint(fourth_key, (), 0, SEQS - 1)) % SEQS
    places = jnp.arange(SEQS)
    picked = jnp.where(places == longest_at, LEN, jnp.where(places == shortest_at, SHORTEST, picked))
    return picked.astype(jnp.int32)


def block_levels(key, dims, cuts, low, top_value):
    level = 1.0
    for axis_at, shards_of in cuts:
        steps = jax.random.uniform(jax.random.fold_in(jax.random.fold_in(key, 6), axis_at), (shards_of,), jnp.float32, low / len(cuts), top_value / len(cuts))
        level = level * jnp.repeat(jnp.exp(steps), dims[axis_at] // shards_of).reshape((-1,) + (1,) * (len(dims) - 1 - axis_at))
    return level


def scatter_about(stream_key, dims, deviation, most, cuts=(), kind=jnp.bfloat16):
    loudness = block_levels(stream_key, dims, cuts, -0.22, 0.18) if cuts else 1.0
    values = jax.random.normal(stream_key, dims, jnp.float32) * deviation * loudness
    return jnp.minimum(jnp.maximum(values, -most), most).astype(kind)


def setup_inputs(seed: int = 0) -> dict:
    seeds = jax.random.split(jax.random.key(seed), 15)
    return {
        "tokens": scatter_about(seeds[0], (TOKENS, D), 1.0, 6.0, ((0, 32),)),
        "lengths": draw_lengths(jax.random.fold_in(seeds[14], 71), 0),
        "ln1_gain": jnp.clip(1.0 + 0.18 * jax.random.normal(seeds[2], (D,), jnp.float32), 0.1, 1.9),
        "ln1_bias": scatter_about(seeds[3], (D,), 0.5, 3.0, (), jnp.float32),
        "w_query": scatter_about(seeds[4], (D, D), (D // 2) ** -0.5, 0.25, ((1, 4),)),
        "w_key": scatter_about(seeds[5], (D, D), (D // 2) ** -0.5, 0.25, ((1, 4),)),
        "w_value": scatter_about(seeds[6], (D, D), D ** -0.5, 0.1875, ((1, 4),)),
        "w_out": scatter_about(seeds[7], (D, D), (D // 16) ** -0.5, 0.75, ((0, 4),)),
        "ln2_gain": jnp.clip(1.0 + 0.18 * jax.random.normal(seeds[8], (D,), jnp.float32), 0.1, 1.9),
        "ln2_bias": scatter_about(seeds[9], (D,), 0.5, 3.0, (), jnp.float32),
        "w_gate": scatter_about(seeds[10], (D, FF), D ** -0.5, 0.1875, ((1, 4),)),
        "w_up": scatter_about(seeds[11], (D, FF), D ** -0.5, 0.1875, ((1, 4),)),
        "down_weight": scatter_about(seeds[12], (FF, D), (FF // 2) ** -0.5, 0.125, ((0, 4),)),
        "cotangent": scatter_about(seeds[13], (TOKENS, D), 1.0, 6.0, ((0, 32),)),
    }


eps = 1e-05
highest_precision = lax.Precision.HIGHEST

@jax.custom_vjp
def low(v):
    return lax.optimization_barrier(v.astype(jnp.bfloat16)).astype(jnp.float32)

@jax.custom_vjp
def low_back(v):
    return v

def low_keep(v):
    return (low(v), None)

def low_pass(kept, grad):
    return (grad,)

def backward_retained(v):
    return (v, None)

def back_low(kept, grad):
    return (low(grad),)
low.defvjp(low_keep, low_pass)
low_back.defvjp(backward_retained, back_low)

def layer_norm(values, gain, shift):
    centre = lax.optimization_barrier(jnp.mean(values, axis=-1, keepdims=True))
    centred = values - centre
    inverse = lax.rsqrt(lax.optimization_barrier(jnp.mean(centred * centred, axis=-1, keepdims=True)) + eps)
    return centred * inverse * gain + shift

def angle_tables(length, width):
    half_width = width // 2
    freqs = 10000.0 ** (-(jnp.arange(half_width, dtype=jnp.float32) * 2.0 / width))
    angles = jnp.arange(length, dtype=jnp.float32)[:, None] * freqs[None, :]
    return (jnp.cos(angles), jnp.sin(angles))

def rotate(values, cosine, sine):
    half_width = values.shape[-1] // 2
    first = values[..., :half_width]
    second = values[..., half_width:]
    return jnp.concatenate([first * cosine - second * sine, second * cosine + first * sine], axis=-1)

def split_heads(stacked):
    shards, length, columns = stacked.shape
    per_shard = columns // HD
    return stacked.reshape(shards, length, per_shard, HD).transpose(0, 2, 1, 3).reshape(shards * per_shard, length, HD)

def join_heads(headed):
    heads, length, depth = headed.shape
    per_shard = heads // N_TENSOR
    return headed.reshape(N_TENSOR, per_shard, length, depth).transpose(0, 2, 1, 3).reshape(N_TENSOR, length, per_shard * depth)

def column_shards(weight):
    rows, columns = weight.shape
    return weight.reshape(rows, N_TENSOR, columns // N_TENSOR).transpose(1, 0, 2)

def row_partitions(weight):
    rows, columns = weight.shape
    return weight.reshape(N_TENSOR, rows // N_TENSOR, columns)

def grouped(rows_each, weight):
    return jnp.einsum('trd,tdc->trc', rows_each, column_shards(weight), precision=highest_precision)

def layer(inputs, limit, params):
    gain1, shift1, w_query, w_key, w_value, w_out, gain2, shift2, w_gate, w_up, down_weight = params
    length = inputs.shape[0]
    attn_in = low(layer_norm(inputs, gain1, shift1))
    attn_each = low_back(jnp.broadcast_to(attn_in[None], (N_TENSOR,) + attn_in.shape))
    query_raw = low_back(grouped(attn_each, w_query))
    key_raw = low_back(grouped(attn_each, w_key))
    value_raw = low_back(grouped(attn_each, w_value))
    cosine, sine = angle_tables(length, HD)
    query = low(rotate(split_heads(query_raw), cosine[None], sine[None]))
    keys = low(rotate(split_heads(key_raw), cosine[None], sine[None]))
    values = low(split_heads(value_raw))
    live = jnp.arange(length) < limit
    scores = jnp.einsum('hqe,hke->hqk', query, keys, precision=highest_precision) * (1.0 / math.sqrt(HD))
    scores = low_back(jnp.where(live[None, None, :], scores, -1e+30))
    probs = low(jax.nn.softmax(scores, axis=-1))
    context = low(low_back(jnp.einsum('hqk,hke->hqe', probs, values, precision=highest_precision)))
    attn_parts = jnp.einsum('trc,tcd->trd', join_heads(context), row_partitions(w_out), precision=highest_precision)
    middle = inputs + low_back(lax.optimization_barrier(jnp.sum(low(attn_parts), axis=0)))
    ffn_in = low(layer_norm(middle, gain2, shift2))
    ffn_each = low_back(jnp.broadcast_to(ffn_in[None], (N_TENSOR,) + ffn_in.shape))
    gate = low_back(grouped(ffn_each, w_gate))
    upper = low_back(grouped(ffn_each, w_up))
    hidden_activations = low(jax.nn.silu(gate) * upper)
    feedforward_pieces = jnp.einsum('yuh,yhb->yub', hidden_activations, row_partitions(down_weight), precision=highest_precision)
    result = middle + low_back(lax.optimization_barrier(jnp.sum(low(feedforward_pieces), axis=0)))
    return jnp.where(live[:, None], result, 0.0)

def reference(tokens, lengths, ln1_gain, ln1_bias, w_query, w_key, w_value, w_out, ln2_gain, ln2_bias, w_gate, w_up, down_weight, cotangent):
    params = tuple((weight.astype(jnp.float32) for weight in (ln1_gain, ln1_bias, w_query, w_key, w_value, w_out, ln2_gain, ln2_bias, w_gate, w_up, down_weight)))
    windows = lengths.shape[0]
    inputs = tokens.astype(jnp.float32).reshape(windows, LEN, D)
    upstream = cotangent.astype(jnp.float32).reshape(windows, LEN, D)

    def one_window(carry, item):
        window_input, window_ct, limit = item

        def apply_layer(rows, weights):
            return layer(rows, limit, weights)
        result, pullback = jax.vjp(apply_layer, window_input, params)
        input_grad, weight_grads = pullback(window_ct)
        return (tuple((total + grad for total, grad in zip(carry, weight_grads))), (result, input_grad))
    zeros = tuple((jnp.zeros_like(weight) for weight in params))
    totals, (results, input_grads) = lax.scan(one_window, zeros, (inputs, upstream, lengths))
    return (results.reshape(TOKENS, D).astype(jnp.bfloat16), input_grads.reshape(TOKENS, D), totals[0], totals[1], totals[2], totals[3], totals[4], totals[5], totals[6], totals[7], totals[8], totals[9], totals[10])
```

```python
import functools
import math

import jax
import jax.numpy as jnp
from jax import lax
from jax.experimental import pallas as pl
from jax.experimental.pallas import tpu as pltpu
from jax.sharding import PartitionSpec as P

HD = 64
WIDE = 256
EPS = 1e-05
LOG2E = math.log2(math.e)
SCALE = 1.0 / math.sqrt(HD)
F32 = jnp.float32
BF = jnp.bfloat16
NT = (((1,), (1,)), ((), ()))
NN = (((1,), (0,)), ((), ()))
TN = (((0,), (0,)), ((), ()))
MESH = pl.DeviceIdType.MESH


def dot(a, b, dims=NN):
    return lax.dot_general(a, b, dims, preferred_element_type=F32)


def lanes(shape):
    return lax.broadcasted_iota(jnp.int32, shape, 1)


def split3(x):
    hi = x.astype(BF).astype(F32)
    mid = (x - hi).astype(BF).astype(F32)
    return hi, mid, x - hi - mid


def partner(x):
    width = x.shape[1]
    first = lanes(x.shape) % HD < HD // 2
    return jnp.where(first, pltpu.roll(x, width - HD // 2, 1), pltpu.roll(x, HD // 2, 1))


def angle_tables(length):
    half = HD // 2
    lane = lax.optimization_barrier(lax.iota(jnp.int32, 2 * HD))
    freqs = 10000.0 ** (-((lane % half).astype(F32) * 2.0 / HD))
    angles = lax.iota(F32, length)[:, None] * freqs[None, :]
    sign = jnp.where(lane % HD < half, -1.0, 1.0)
    return jnp.cos(angles), jnp.sin(angles) * sign[None, :]


def project_kernel(width, x_ref, wq_ref, wk_ref, wv_ref, cos_ref, sin_ref, q_ref, k_ref, v_ref):
    x = x_ref[...]
    cosine = jnp.tile(cos_ref[...], (1, width // (2 * HD)))
    sine = jnp.tile(sin_ref[...], (1, width // (2 * HD)))
    for w_ref, out_ref in ((wq_ref, q_ref), (wk_ref, k_ref)):
        raw = dot(x, w_ref[...])
        out_ref[...] = (raw * cosine + partner(raw) * sine).astype(BF)
    v_ref[...] = dot(x, wv_ref[...]).astype(BF)


def project(rows, w_query, w_key, w_value, cosine, sine, block=512):
    n, depth = rows.shape
    width = w_query.shape[1]
    whole = pl.BlockSpec((depth, width), lambda i: (0, 0))
    table = pl.BlockSpec((block, 2 * HD), lambda i: (i, 0))
    out = pl.BlockSpec((block, width), lambda i: (i, 0))
    return pl.pallas_call(
        functools.partial(project_kernel, width),
        out_shape=(jax.ShapeDtypeStruct((n, width), BF),) * 3,
        grid=(n // block,),
        in_specs=[pl.BlockSpec((block, depth), lambda i: (i, 0)), whole, whole, whole, table, table],
        out_specs=(out, out, out),
        compiler_params=pltpu.CompilerParams(vmem_limit_bytes=40 << 20),
        cost_estimate=pl.CostEstimate(
            flops=2 * n * depth * 3 * width, bytes_accessed=2 * (n * depth + 3 * n * width), transcendentals=0
        ),
        name="project",
    )(rows, w_query, w_key, w_value, cosine, sine)


def own_lanes(h, shape):
    lane = lanes(shape)
    off = lax.rem(lane - h * HD + shape[1], shape[1])
    return off < HD, off


def attend(q, k, v):
    scores = dot(q, k, NT)
    peak = jnp.max(scores, axis=1, keepdims=True)
    return dot(jnp.exp2(scores - peak).astype(BF), v), peak


def query_operand(h, q):
    own, off = own_lanes(h, q.shape)
    q = jnp.where(own, q.astype(F32), 0.0) * (LOG2E * SCALE)
    high = q.astype(BF).astype(F32)
    return high + pltpu.roll(q - high, HD, 1), own, off - 2 * HD


def differ(a, b, bits):
    return sum(lax.rem(a // (1 << k) + b // (1 << k), 2) * (1 << k) for k in range(bits))


def remote(src, dst, send, recv, **to):
    return pltpu.make_async_remote_copy(
        src_ref=src, dst_ref=dst, send_sem=send, recv_sem=recv, device_id=to, device_id_type=MESH
    )


def ring(n, step):
    return lax.rem(lax.axis_index("tensor") + step, n)


def same_core(s, chips):
    me = lax.axis_index("dp")
    return differ(me // 2, s, chips.bit_length() - 1) * 2 + lax.rem(me, 2)


def sibling():
    me = lax.axis_index("dp")
    return me + 1 - 2 * lax.rem(me, 2)


def greet(n, chips, both_cores=False):
    barrier = pltpu.get_barrier_semaphore()
    if both_cores:
        pl.semaphore_signal(barrier, inc=1, device_id={"dp": sibling()}, device_id_type=MESH)
    for step in range(1, n):
        pl.semaphore_signal(barrier, inc=1, device_id={"tensor": ring(n, step)}, device_id_type=MESH)
    for s in range(1, chips):
        pl.semaphore_signal(
            barrier, inc=1, device_id={"dp": same_core(s, chips)}, device_id_type=MESH
        )
    pl.semaphore_wait(barrier, n + chips - 2 + both_cores)


def att_fwd_kernel(
    n, chips, limit_ref, q_ref, k_ref, v_ref, gb_ref, wo_ref,
    ctx_ref, lse_ref, out_ref, gb_all, wo_z, wo_all, ka, va, send_sem, recv_sem, own_sem,
    gs_send, gs_recv, gr_send, gr_recv, wz_send, wz_recv, ws_send, ws_recv, wr_send, wr_recv, keep_sem,
):
    s = pl.program_id(0)
    h = pl.program_id(1)
    heads = pl.num_programs(1)
    rows = q_ref.shape[0] // n
    me = lax.axis_index("tensor")
    place = lax.axis_index("dp")
    core = lax.rem(place, 2)
    bits = chips.bit_length() - 1
    limit = limit_ref[0]

    def spread_gb(c):
        return remote(
            gb_ref, gb_all.at[place // 2, core], gs_send.at[c], gs_recv.at[c], dp=same_core(c, chips)
        )

    def relay_gb(c):
        there = gb_all.at[differ(place // 2, c, bits), core]
        return remote(
            there if c else gb_ref, there, gr_send.at[c], gr_recv.at[c], dp=sibling()
        )

    def wo_over(step):
        return remote(
            wo_ref, wo_z.at[me], wz_send.at[step], wz_recv.at[step], tensor=ring(n, step + 1)
        )

    def spread_wo(c):
        return remote(
            wo_z, wo_all.at[:, place], ws_send.at[c], ws_recv.at[c], dp=same_core(c, chips)
        )

    def relay_wo(c):
        there = wo_all.at[:, differ(place // 2, c, bits) * 2 + core]
        return remote(there if c else wo_z, there, wr_send.at[c], wr_recv.at[c], dp=sibling())

    keeps = [
        pltpu.make_async_copy(gb_ref, gb_all.at[place // 2, core], keep_sem.at[0]),
        pltpu.make_async_copy(wo_ref, wo_z.at[me], keep_sem.at[1]),
        pltpu.make_async_copy(wo_z, wo_all.at[:, place], keep_sem.at[2]),
    ]

    @pl.when((s == 0) & (h == 0))
    def _():
        greet(n, chips, True)
        for step in range(n - 1):
            wo_over(step).start()
        keeps[0].start()
        keeps[1].start()
        for c in range(1, chips):
            spread_gb(c).start()
        relay_gb(0).start()

    @pl.when((s == 1) & (h == 0))
    def _():
        for step in range(n - 1):
            wo_over(step).wait()
        keeps[1].wait()
        for c in range(1, chips):
            spread_wo(c).start()
        relay_wo(0).start()
        keeps[2].start()

    @pl.when((s == n - 2) & (h == 0))
    def _():
        for c in range(1, chips // 2 + 1):
            spread_gb(c).wait_recv()
            relay_gb(c).start()

    @pl.when((s == n - 1) & (h == 0))
    def _():
        for c in range(1, chips):
            spread_wo(c).wait_recv()
            relay_wo(c).start()
        for c in range(chips // 2 + 1, chips):
            spread_gb(c).wait_recv()
            relay_gb(c).start()

    @pl.when(s == 0)
    def _():
        own, off = own_lanes(h, k_ref.shape)
        k = jnp.where(own, k_ref[...].astype(F32), 0.0)
        row = lax.broadcasted_iota(jnp.int32, k.shape, 0)
        bias = jnp.where(row < limit, 0.0, -1e30)
        ka[h] = jnp.where(off == 2 * HD, bias, k + pltpu.roll(k, HD, 1)).astype(BF)
        v = jnp.where(own, v_ref[...].astype(F32), 0.0)
        va[h] = jnp.where(off == HD, 1.0, v).astype(BF)

    owner = ring(n, s + 1)
    block = pl.ds(pl.multiple_of(owner * rows, rows), rows)
    q, own, off = query_operand(h, q_ref[block, :])
    acc, peak = attend(jnp.where(off == 0, 1.0, q).astype(BF), ka[h], va[h])
    total = jnp.sum(jnp.where(off == -HD, acc, 0.0), axis=1, keepdims=True)
    out = (acc * (1.0 / total)).astype(BF)
    ctx_ref[block, :] = jnp.where(own, out, ctx_ref[block, :])
    lse_ref[block, :] = jnp.where(
        lanes((rows, 128)) == h, peak + jnp.log2(total), lse_ref[block, :]
    )

    def push(step):
        return pltpu.make_async_remote_copy(
            src_ref=ctx_ref.at[block],
            dst_ref=out_ref.at[me],
            send_sem=send_sem.at[step],
            recv_sem=recv_sem.at[step],
            device_id={"tensor": owner},
            device_id_type=MESH,
        )

    @pl.when((h == heads - 1) & (s < n - 1))
    def _():
        push(s).start()

    @pl.when((h == heads - 1) & (s == n - 1))
    def _():
        keep = pltpu.make_async_copy(ctx_ref.at[block], out_ref.at[me], own_sem)
        keep.start()
        for step in range(n - 1):
            push(step).wait()
        keep.wait()
        keeps[0].wait()
        keeps[2].wait()
        for c in range(chips):
            relay_gb(c).wait()
            relay_wo(c).wait()
            if c:
                spread_gb(c).wait_send()
                spread_wo(c).wait_send()


def att_fwd(q, k, v, grad_rows, w_out_piece, limit, heads, n, devices):
    total, width = q.shape
    rows = total // n
    depth = grad_rows.shape[1]
    share = w_out_piece.shape[0]
    chips = devices // 2
    hbm = pl.BlockSpec(memory_space=pl.ANY)

    def whole(d):
        return pl.BlockSpec((total, d), lambda *_: (0, 0), pipeline_mode=pl.Buffered(1))

    return pl.pallas_call(
        functools.partial(att_fwd_kernel, n, chips),
        out_shape=(
            jax.ShapeDtypeStruct((total, width), BF),
            jax.ShapeDtypeStruct((total, 128), F32),
            jax.ShapeDtypeStruct((n, rows, width), BF),
            jax.ShapeDtypeStruct((chips, 2, rows, depth), BF),
            jax.ShapeDtypeStruct((n, share, depth), BF),
            jax.ShapeDtypeStruct((n, devices, share, depth), BF),
        ),
        grid_spec=pltpu.PrefetchScalarGridSpec(
            num_scalar_prefetch=1,
            grid=(n, heads),
            in_specs=[whole(width)] * 3 + [hbm] * 2,
            out_specs=[whole(width), whole(128)] + [hbm] * 4,
            scratch_shapes=[pltpu.VMEM((heads, total, width), BF)] * 2
            + [pltpu.SemaphoreType.DMA((n - 1,))] * 2
            + [pltpu.SemaphoreType.DMA]
            + [pltpu.SemaphoreType.DMA((chips,))] * 4
            + [pltpu.SemaphoreType.DMA((n - 1,))] * 2
            + [pltpu.SemaphoreType.DMA((chips,))] * 4
            + [pltpu.SemaphoreType.DMA((3,))],
        ),
        compiler_params=pltpu.CompilerParams(
            vmem_limit_bytes=56 << 20, collective_id=1, has_side_effects=True
        ),
        cost_estimate=pl.CostEstimate(
            flops=4 * total * total * 256 * heads,
            bytes_accessed=10 * total * width,
            transcendentals=total * total * heads,
        ),
        name="att_fwd",
    )(limit, q, k, v, grad_rows, w_out_piece)


def att_bwd_kernel(
    n, bk, chips, heads, limit_ref, ga_ref, wo_ref, parts_ref, q_ref, k_ref, v_ref, ctx_ref, lse_ref,
    cos_ref, sin_ref, pk_ref, own_ref, sums_ref, do, gc, ka, va, dka, dva, dqs, dvs,
    send_sem, recv_sem, out_send, out_recv, pk_send, pk_recv, keep_sem,
):
    h = pl.program_id(0)
    t = pl.program_id(1)
    total, width = k_ref.shape
    rows = total // n
    me = lax.axis_index("tensor")
    limit = limit_ref[0]
    mine = pl.ds(pl.multiple_of(me * rows, rows), rows)
    to_first = lax.rem(width - h * HD, width)

    def push(step):
        return remote(
            gc.at[step], do.at[mine], send_sem.at[step], recv_sem.at[step], tensor=ring(n, step + 1)
        )

    def push_out(s):
        return remote(
            parts_ref.at[s], sums_ref.at[s - 1], out_send.at[s - 1], out_recv.at[s - 1],
            dp=same_core(s, chips),
        )

    def columns(slot):
        return pl.ds(pl.multiple_of(slot * 128, 128), 128)

    def push_pack(slot, step):
        owner = ring(n, step + 1)
        return remote(
            pk_ref.at[pl.ds(pl.multiple_of(owner * rows, rows), rows), columns(slot)],
            own_ref.at[me, :, columns(slot)],
            pk_send.at[slot, step], pk_recv.at[slot, step], tensor=owner,
        )

    def keep(slot):
        return pltpu.make_async_copy(
            pk_ref.at[mine, columns(slot)], own_ref.at[me, :, columns(slot)], keep_sem.at[slot]
        )

    def send_pack(slot):
        for step in range(n - 1):
            push_pack(slot, step).start()
        keep(slot).start()

    @pl.when((h == 0) & (t == 0))
    def _():
        greet(n, chips)
        for s in range(1, chips):
            push_out(s).start()

        def send(step, carry):
            gc[step] = dot(ga_ref[...], wo_ref[ring(n, step + 1)], NT).astype(BF)
            push(step).start()
            return carry

        lax.fori_loop(0, n - 1, send, 0)
        do[mine, :] = dot(ga_ref[...], wo_ref[me], NT).astype(BF)

    @pl.when((h == 0) & (t > 0))
    def _():
        push(t - 1).wait_recv()

    @pl.when(t == 0)
    def _():
        lane = lanes((total, width))
        row = lax.broadcasted_iota(jnp.int32, (total, width), 0)
        k = jnp.where(lane < HD, pltpu.roll(k_ref[...].astype(F32), to_first, 1), 0.0)
        k = jnp.where(
            lane == 2 * HD + 3, jnp.where(row < limit, 0.0, -1e30), k + pltpu.roll(k, HD, 1)
        )
        ones = (lane >= 2 * HD) & (lane < 2 * HD + 3)
        ka[...] = jnp.where(ones, 1.0, k).astype(BF)
        v = jnp.where(lane < HD, pltpu.roll(v_ref[...].astype(F32), to_first, 1), 0.0)
        va[...] = jnp.where(ones, 1.0, v).astype(BF)
        dka[...] = jnp.zeros_like(dka)
        dva[...] = jnp.zeros_like(dva)

    source = ring(n, n - t)
    block = pl.ds(pl.multiple_of(source * rows, rows), rows)
    off = lanes((rows, width)) - 2 * HD
    q = pltpu.roll(q_ref[block, :].astype(F32), to_first, 1) * (LOG2E * SCALE)
    q = jnp.where(off < -HD, q, 0.0)
    high = q.astype(BF).astype(F32)
    q = high + pltpu.roll(q - high, HD, 1)
    logsum = jnp.sum(
        jnp.where(lanes((rows, 128)) == h, lse_ref[block, :], 0.0), axis=1, keepdims=True
    )
    a, b, c = split3(-logsum)
    q = jnp.where(off == 0, a, jnp.where(off == 1, b, jnp.where(off == 2, c, q)))
    q = jnp.where(off == 3, 1.0, q).astype(BF)
    g = jnp.where(off < -HD, pltpu.roll(do[block, :].astype(F32), to_first, 1), 0.0)
    delta = jnp.sum(
        g * pltpu.roll(ctx_ref[block, :].astype(F32), to_first, 1), axis=1, keepdims=True
    )
    a, b, c = split3(-delta)
    g = jnp.where(off == 0, a, jnp.where(off == 1, b, jnp.where(off == 2, c, g))).astype(BF)
    acc = jnp.zeros((rows, width), F32)
    for j in range(total // bk):
        rk = pl.ds(j * bk, bk)
        kt = ka[rk, :]
        probs = jnp.exp2(dot(kt, q, NT))
        grad = (probs * dot(va[rk, :], g, NT)).astype(BF)
        dva[rk, :] += dot(probs.astype(BF), g)
        dka[rk, :] += dot(grad, q)
        acc = acc + dot(grad, kt, TN)
    dqs[block, :] = acc[:, :128] * SCALE

    @pl.when(t == n - 1)
    def _():
        first = lanes((total, 128)) < HD
        dk = dka[:, :128]
        grad = jnp.where(first, dqs[...], (dk + pltpu.roll(dk, HD, 1)) * (1.0 / LOG2E))
        grad = grad * cos_ref[...] - partner(grad) * sin_ref[...]
        pk_ref[:, columns(h)] = grad.astype(BF)
        send_pack(h)

        @pl.when(lax.rem(h, 2) == 0)
        def _():
            dvs[...] = dva[:, :128]

        @pl.when(lax.rem(h, 2) == 1)
        def _():
            both = jnp.where(first, dvs[...], pltpu.roll(dva[:, :128], HD, 1))
            pk_ref[:, columns(heads + h // 2)] = both.astype(BF)
            send_pack(heads + h // 2)

    @pl.when((t == n - 1) & (h == heads - 1))
    def _():
        for step in range(n - 1):
            push(step).wait_send()
        for s in range(1, chips):
            push_out(s).wait()
        for slot in range(heads + heads // 2):
            keep(slot).wait()
            for step in range(n - 1):
                push_pack(slot, step).wait()


def att_bwd(grad_attn, w_out, parts, q, k, v, ctx, lse, limit, cosine, sine, heads, n, bk=512):
    total, width = q.shape
    rows, depth = grad_attn.shape
    chips = parts.shape[0]
    slots = heads + heads // 2
    hbm = pl.BlockSpec(memory_space=pl.ANY)

    def whole(*shape):
        return pl.BlockSpec(shape, lambda *_: (0,) * len(shape), pipeline_mode=pl.Buffered(1))

    return pl.pallas_call(
        functools.partial(att_bwd_kernel, n, bk, chips, heads),
        out_shape=(
            jax.ShapeDtypeStruct((total, slots * 128), BF),
            jax.ShapeDtypeStruct((n, rows, slots * 128), BF),
            jax.ShapeDtypeStruct((chips - 1, rows, depth), BF),
        ),
        grid_spec=pltpu.PrefetchScalarGridSpec(
            num_scalar_prefetch=1,
            grid=(heads, n),
            in_specs=[whole(rows, depth), whole(n, width, depth), hbm]
            + [whole(total, width)] * 4
            + [whole(total, 128)] * 3,
            out_specs=[whole(total, slots * 128), hbm, hbm],
            scratch_shapes=[
                pltpu.VMEM((total, width), BF),
                pltpu.VMEM((n - 1, rows, width), BF),
                pltpu.VMEM((total, width), BF),
                pltpu.VMEM((total, width), BF),
                pltpu.VMEM((total, width), F32),
                pltpu.VMEM((total, width), F32),
                pltpu.VMEM((total, 128), F32),
                pltpu.VMEM((total, 128), F32),
            ]
            + [pltpu.SemaphoreType.DMA((n - 1,))] * 2
            + [pltpu.SemaphoreType.DMA((chips - 1,))] * 2
            + [pltpu.SemaphoreType.DMA((slots, n - 1))] * 2
            + [pltpu.SemaphoreType.DMA((slots,))],
        ),
        compiler_params=pltpu.CompilerParams(
            vmem_limit_bytes=56 << 20, collective_id=2, has_side_effects=True
        ),
        cost_estimate=pl.CostEstimate(
            flops=10 * total * total * 256 * heads,
            bytes_accessed=20 * total * width,
            transcendentals=total * total * heads,
        ),
        name="att_bwd",
    )(limit, grad_attn, w_out, parts, q, k, v, ctx, lse, cosine, sine)


def finish_kernel(
    chips, n, width, x_ref, pk_ref, own_ref, w_ref, tokens_ref, middle_ref, gain_ref, vec_ref,
    input_ref, q_ref, k_ref, v_ref, sums_ref,
    full, mate, sib, land, fin, every, vec_z, vec_dp, vec_me,
    sx_send, sx_recv, rs_send, rs_recv, ag_send, ag_recv, rl_send, rl_recv,
    vz_send, vz_recv, vd_send, vd_recv, own_sem,
):
    bits = chips.bit_length() - 1
    me = lax.axis_index("dp")
    place = lax.axis_index("tensor")
    core = lax.rem(me, 2)
    chip = me // 2
    other = 1 - core
    heads = width // HD
    piece = fin.shape[0]

    def swap(s):
        return remote(mate.at[s], sib.at[s], sx_send.at[s], sx_recv.at[s], dp=chip * 2 + other)

    def push(s):
        return remote(sib.at[s], land.at[s], rs_send.at[s], rs_recv.at[s], dp=same_core(s, chips))

    def spread(s):
        return remote(
            fin, every.at[chip, core], ag_send.at[s], ag_recv.at[s], dp=same_core(s, chips)
        )

    def relay(s):
        src = every.at[differ(chip, s, bits), core]
        return remote(src, src, rl_send.at[s], rl_recv.at[s], dp=chip * 2 + other)

    def vec_over(step):
        return remote(
            vec_me.at[0], vec_z.at[place], vz_send.at[step], vz_recv.at[step], tensor=ring(n, step + 1)
        )

    def vec_across(step):
        return remote(
            vec_me.at[1], vec_dp.at[me], vd_send.at[step], vd_recv.at[step],
            dp=lax.rem(me + step + 1, 2 * chips),
        )

    barrier = pltpu.get_barrier_semaphore()
    for step in range(n - 1):
        pl.semaphore_signal(barrier, inc=1, device_id={"tensor": ring(n, step + 1)}, device_id_type=MESH)
    for step in range(2 * chips - 1):
        to = lax.rem(me + step + 1, 2 * chips)
        pl.semaphore_signal(barrier, inc=1, device_id={"dp": to}, device_id_type=MESH)

    full[...] = dot(x_ref[...], pk_ref[...], TN)
    pl.semaphore_wait(barrier, n + 2 * chips - 2)

    def part(s, which):
        start = (differ(chip, s, bits) * 2 + which) * piece
        return full[pl.ds(pl.multiple_of(start, piece), piece), :]

    for s in range(chips):
        mate[s] = part(s, other).astype(BF)
        swap(s).start()

    grad = jnp.zeros(input_ref.shape, F32)
    for t in range(n):
        grad = grad + dot(own_ref[t], w_ref[t]).astype(BF).astype(F32)

    for s in range(1, chips):
        swap(s).wait_recv()
        sib[s] = (sib[s].astype(F32) + part(s, core)).astype(BF)
        push(s).start()
    swap(0).wait_recv()
    total = sib[0].astype(F32) + part(0, core)

    values = tokens_ref[...].astype(F32)
    values = values - jnp.mean(values, axis=1, keepdims=True)
    inverse = lax.rsqrt(jnp.mean(values * values, axis=1, keepdims=True) + EPS)
    scaled = values * inverse
    through = grad * gain_ref[...]
    inner = through - jnp.mean(through, axis=1, keepdims=True)
    inner = inner - scaled * jnp.mean(through * scaled, axis=1, keepdims=True)
    input_ref[...] = middle_ref[...] + inverse * inner
    vec_me[0, 0:1] = jnp.sum(grad * scaled, axis=0, keepdims=True)
    vec_me[0, 1:2] = jnp.sum(grad, axis=0, keepdims=True)
    vec_me[0, 2:4] = vec_ref[...]
    vec_me[0, 4:8] = jnp.zeros((4, vec_ref.shape[1]), F32)
    vec_z[place] = vec_me[0]
    for step in range(n - 1):
        vec_over(step).start()

    for s in range(1, chips):
        push(s).wait_recv()
        total = total + land[s].astype(F32)
    fin[...] = total.astype(BF)
    for s in range(1, chips):
        spread(s).start()
    mine = pltpu.make_async_copy(fin, every.at[chip, core], own_sem)
    mine.start()
    mine.wait()
    relay(0).start()

    for step in range(n - 1):
        vec_over(step).wait()
    vec = vec_z[0]
    for t in range(1, n):
        vec = vec + vec_z[t]
    vec_me[1] = vec
    vec_dp[me] = vec
    for step in range(2 * chips - 1):
        vec_across(step).start()
    for s in range(1, chips):
        spread(s).wait_recv()
        relay(s).start()
    for step in range(2 * chips - 1):
        vec_across(step).wait()
    vec = vec_dp[0]
    for t in range(1, 2 * chips):
        vec = vec + vec_dp[t]
    sums_ref[...] = vec
    for s in range(chips):
        relay(s).wait()
        swap(s).wait_send()
        if s > 0:
            spread(s).wait_send()
            push(s).wait_send()
    first = lanes((piece, 128)) < HD
    for d in range(2 * chips):
        rows = slice(d * piece, (d + 1) * piece)
        g = every[d // 2, d % 2].astype(F32)
        for pair in range(heads // 2):
            a = g[:, pair * 256 : pair * 256 + 128]
            b = g[:, pair * 256 + 128 : pair * 256 + 256]
            out = slice(pair * 128, pair * 128 + 128)
            q_ref[rows, out] = jnp.where(first, a, pltpu.roll(b, HD, 1))
            k_ref[rows, out] = jnp.where(first, pltpu.roll(a, HD, 1), b)
            v_ref[rows, out] = g[:, (heads + pair) * 128 : (heads + pair + 1) * 128]


def finish(rows_all, packed, own, w_all, tokens, middle, gain, vec, width, devices):
    n, rows, packs = own.shape
    depth = tokens.shape[1]
    chips = devices // 2
    piece = depth // devices
    vmem = pl.BlockSpec(memory_space=pltpu.VMEM)
    out = jax.ShapeDtypeStruct((depth, width), F32)
    return pl.pallas_call(
        functools.partial(finish_kernel, chips, n, width),
        out_shape=(
            jax.ShapeDtypeStruct((rows, depth), F32), out, out, out,
            jax.ShapeDtypeStruct((8, depth), F32),
        ),
        in_specs=[vmem] * 8,
        out_specs=[vmem] * 5,
        scratch_shapes=[
            pltpu.VMEM((depth, packs), F32),
            pltpu.VMEM((chips, piece, packs), BF),
            pltpu.VMEM((chips, piece, packs), BF),
            pltpu.VMEM((chips, piece, packs), BF),
            pltpu.VMEM((piece, packs), BF),
            pltpu.VMEM((chips, 2, piece, packs), BF),
            pltpu.VMEM((n, 8, depth), F32),
            pltpu.VMEM((devices, 8, depth), F32),
            pltpu.VMEM((2, 8, depth), F32),
        ]
        + [pltpu.SemaphoreType.DMA((chips,))] * 8
        + [pltpu.SemaphoreType.DMA((n - 1,))] * 2
        + [pltpu.SemaphoreType.DMA((devices - 1,))] * 2
        + [pltpu.SemaphoreType.DMA],
        compiler_params=pltpu.CompilerParams(
            vmem_limit_bytes=56 << 20, collective_id=4, has_side_effects=True
        ),
        cost_estimate=pl.CostEstimate(
            flops=4 * n * rows * depth * packs, bytes_accessed=20 << 20, transcendentals=0
        ),
        name="finish",
    )(rows_all, packed, own, w_all, tokens, middle, gain.reshape(1, depth), vec)


def ffn_kernel(
    chips, x_ref, gb_ref, w_ref, dx_ref, out_ref, dw_ref,
    rows_all, gb, hid, gate_g, up_g, own, sib, mate, acc,
    ag_send, ag_recv, rl_send, rl_recv, sx_send, sx_recv, rs_send, rs_recv, gb_sem, out_sem, dx_sem,
):
    bits = chips.bit_length() - 1
    me = lax.axis_index("dp")
    core = lax.rem(me, 2)
    chip = me // 2
    other = 1 - core
    rows, depth = x_ref.shape
    n = dw_ref.shape[0]
    share = dw_ref.shape[2]

    def spread(s):
        to = differ(chip, s, bits) * 2 + core
        return remote(x_ref, rows_all.at[chip, core], ag_send.at[s], ag_recv.at[s], dp=to)

    def relay(s):
        src = differ(chip, s, bits)
        return remote(
            rows_all.at[src, core], rows_all.at[src, core], rl_send.at[s], rl_recv.at[s],
            dp=chip * 2 + other,
        )

    def swap(s):
        return remote(
            mate.at[lax.rem(s, 2)], sib.at[s], sx_send.at[s], sx_recv.at[s], dp=chip * 2 + other
        )

    def push(s):
        to = differ(chip, s, bits) * 2 + core
        return remote(sib.at[s, 0], dx_ref.at[s], rs_send.at[s], rs_recv.at[s], dp=to)

    def fetch(s):
        slot = lax.rem(s, 2)
        return pltpu.make_async_copy(
            gb_ref.at[differ(chip, s, bits)], gb.at[slot], gb_sem.at[slot]
        )

    def keep(s):
        return pltpu.make_async_copy(sib.at[s, 1], out_ref.at[s], out_sem.at[s])

    fetch(0).start()
    barrier = pltpu.get_barrier_semaphore()
    pl.semaphore_signal(barrier, inc=1, device_id={"dp": chip * 2 + other}, device_id_type=MESH)
    for s in range(1, chips):
        to = differ(chip, s, bits) * 2 + core
        pl.semaphore_signal(barrier, inc=1, device_id={"dp": to}, device_id_type=MESH)
    pl.semaphore_wait(barrier, chips)
    for s in range(1, chips):
        spread(s).start()
    mine = pltpu.make_async_copy(x_ref, rows_all.at[chip, core], ag_send.at[0])
    mine.start()
    mine.wait()
    relay(0).start()
    acc[...] = jnp.zeros_like(acc)

    def shard(src, slot, which, put):
        x = rows_all[src, which]
        grad = gb[slot, which]
        gate = dot(x, w_ref[0], NT)
        upper = dot(x, w_ref[1], NT)
        grad_hidden = dot(grad, w_ref[2], NT)
        sigma = jax.nn.sigmoid(gate)
        act = gate * sigma
        part = pl.ds(pl.multiple_of(which * rows, rows), rows)
        hidden = (act * upper).astype(BF)
        grad_gate = (grad_hidden * upper * sigma * (1.0 + gate * (1.0 - sigma))).astype(BF)
        grad_upper = (grad_hidden * act).astype(BF)
        hid[part, :] = hidden
        gate_g[part, :] = grad_gate
        up_g[part, :] = grad_upper
        put[0] = (dot(grad_gate, w_ref[0]) + dot(grad_upper, w_ref[1])).astype(BF)
        put[1] = dot(hidden, w_ref[2]).astype(BF)

    def step(s, carry):
        src = differ(chip, s, bits)
        slot = lax.rem(s, 2)
        relay(s).wait_recv()
        fetch(s).wait()

        @pl.when(s < chips - 1)
        def _():
            fetch(s + 1).start()

        @pl.when(s >= 2)
        def _():
            swap(s - 2).wait_send()

        shard(src, slot, other, mate.at[slot])
        swap(s).start()
        shard(src, slot, core, own)
        swap(s).wait_recv()
        for k in range(2):
            sib[s, k] = (sib[s, k].astype(F32) + own[k].astype(F32)).astype(BF)

        @pl.when(s > 0)
        def _():
            push(s).start()

        keep(s).start()

        @pl.when(s < chips - 1)
        def _():
            spread(s + 1).wait_recv()
            relay(s + 1).start()

        x = rows_all[src].reshape(2 * rows, depth)
        acc[0] += dot(gate_g[...], x, TN)
        acc[1] += dot(up_g[...], x, TN)
        acc[2] += dot(hid[...], gb[slot].reshape(2 * rows, depth), TN)
        return carry

    lax.fori_loop(0, chips, step, 0)
    first = pltpu.make_async_copy(sib.at[0, 0], dx_ref.at[0], dx_sem)
    first.start()
    for t in range(n):
        for k in range(3):
            dw_ref[t, k] = acc[k, t * share : (t + 1) * share, :].astype(BF)
    first.wait()
    for s in range(chips):
        keep(s).wait()
        relay(s).wait_send()
        if s >= chips - 2:
            swap(s).wait_send()
        if s > 0:
            spread(s).wait_send()
            push(s).wait()


def ffn(x, grad_branch, weights, n, devices):
    rows, depth = x.shape
    chips = devices // 2
    hidden = weights.shape[1]
    share = hidden // n
    vmem = pl.BlockSpec(memory_space=pltpu.VMEM)
    hbm = pl.BlockSpec(memory_space=pl.ANY)
    return pl.pallas_call(
        functools.partial(ffn_kernel, chips),
        out_shape=(
            jax.ShapeDtypeStruct((chips, rows, depth), BF),
            jax.ShapeDtypeStruct((chips, rows, depth), BF),
            jax.ShapeDtypeStruct((n, 3, share, depth), BF),
        ),
        in_specs=[vmem, hbm, vmem],
        out_specs=[hbm, hbm, vmem],
        scratch_shapes=[
            pltpu.VMEM((chips, 2, rows, depth), BF),
            pltpu.VMEM((2, 2, rows, depth), BF),
        ]
        + [pltpu.VMEM((2 * rows, hidden), BF)] * 3
        + [
            pltpu.VMEM((2, rows, depth), BF),
            pltpu.VMEM((chips, 2, rows, depth), BF),
            pltpu.VMEM((2, 2, rows, depth), BF),
            pltpu.VMEM((3, hidden, depth), F32),
        ]
        + [pltpu.SemaphoreType.DMA((chips,))] * 8
        + [pltpu.SemaphoreType.DMA((2,)), pltpu.SemaphoreType.DMA((chips,)), pltpu.SemaphoreType.DMA],
        compiler_params=pltpu.CompilerParams(
            vmem_limit_bytes=60 << 20, collective_id=3, has_side_effects=True
        ),
        cost_estimate=pl.CostEstimate(
            flops=2 * 9 * devices * rows * depth * hidden, bytes_accessed=30 << 20, transcendentals=0
        ),
        name="ffn",
    )(x, grad_branch, weights)


def norm_parts(values):
    centre = jnp.mean(values, axis=-1, keepdims=True)
    centred = values - centre
    inverse = lax.rsqrt(jnp.mean(centred * centred, axis=-1, keepdims=True) + EPS)
    return centred * inverse, inverse


def norm_back(upstream, scaled, inverse, gain):
    through = upstream * gain
    inner = (
        through
        - jnp.mean(through, axis=-1, keepdims=True)
        - scaled * jnp.mean(through * scaled, axis=-1, keepdims=True)
    )
    return inverse * inner, jnp.sum(upstream * scaled, axis=0), jnp.sum(upstream, axis=0)


def pack_weights(w_query, w_key, w_value):
    depth, width = w_query.shape
    query, key = (w.T.reshape(width // HD, 1, HD, depth) for w in (w_query, w_key))
    both = jnp.concatenate([query, key], axis=1).reshape(2 * width, depth)
    return jnp.concatenate([both, w_value.T], axis=0)


def on_device(
    tokens, lengths, ln1_gain, ln1_bias, w_query, w_key, w_value, w_out,
    ln2_gain, ln2_bias, w_gate, w_up, down_weight, cotangent,
):
    n = lax.axis_size("tensor")
    local_rows, depth = tokens.shape
    length = local_rows * n
    width = w_query.shape[1]
    heads = width // HD
    row_ids = lax.axis_index("tensor") * local_rows + lax.iota(jnp.int32, local_rows)
    valid = (row_ids < lengths[0])[:, None]

    def gather(x):
        return lax.all_gather(x, "tensor", axis=0, tiled=True)

    def padded(x):
        return x if width >= WIDE else jnp.pad(x, ((0, 0), (0, WIDE - width)))

    inputs = tokens.astype(F32)
    scaled1, _ = norm_parts(inputs)
    attn_rows = gather((scaled1 * ln1_gain + ln1_bias).astype(BF))
    cosine, sine = angle_tables(length)
    grad_out = jnp.where(valid, cotangent.astype(F32), 0.0)
    devices = lax.axis_size("dp")
    place = lax.axis_index("dp")
    share = w_gate.shape[1] // devices

    def piece(x, axis):
        return lax.dynamic_slice_in_dim(x, place * share, share, axis)

    weights = jnp.stack([piece(w_gate, 1).T, piece(w_up, 1).T, piece(down_weight, 0)])
    weights = lax.all_gather(weights, "tensor", axis=1, tiled=True)
    q, k, v = project(attn_rows, w_query, w_key, w_value, cosine, sine)
    q, k, v = padded(q), padded(k), padded(v)
    context, logsum, context_own, grad_branch, _, w_out_all = att_fwd(
        q, k, v, grad_out.astype(BF),
        lax.dynamic_slice_in_dim(w_out, place * (width // devices), width // devices, 0),
        lengths, heads, n, devices,
    )
    w_out_all = w_out_all.reshape(n, width, depth)
    if width < WIDE:
        w_out_all = jnp.pad(w_out_all, ((0, 0), (0, WIDE - width), (0, 0)))
    attn_out = sum(dot(context_own[t], w_out_all[t]).astype(BF).astype(F32) for t in range(n))
    middle = inputs + attn_out
    scaled2, inverse2 = norm_parts(middle)
    ffn_in = (scaled2 * ln2_gain + ln2_bias).astype(BF)
    w_packed, ffn_in = lax.optimization_barrier(
        (pack_weights(w_query, w_key, w_value), ffn_in)
    )
    w_packed = lax.all_gather(w_packed, "tensor", axis=0)
    grad_parts, out_parts, ffn_grads = ffn(ffn_in, grad_branch, weights, n, devices)
    grad_ffn_in = sum(grad_parts[p].astype(F32) for p in range(devices // 2))
    grad_norm2, gain2_grad, shift2_grad = norm_back(
        grad_ffn_in, scaled2, inverse2, ln2_gain
    )
    grad_middle = grad_out + grad_norm2
    grad_attn = grad_middle.astype(BF)
    parts = jnp.stack([dot(context_own[t, :, :width], grad_attn, TN).astype(BF) for t in range(n)])
    parts = parts.reshape(n, devices, width // devices, depth).transpose(1, 0, 2, 3)
    parts = lax.psum_scatter(parts, "dp", scatter_dimension=0, tiled=True)[0]
    grads = jnp.concatenate([ffn_grads.reshape(n, 3 * share, depth), parts], axis=1)
    grads = lax.psum_scatter(grads, "tensor", scatter_dimension=0, tiled=True)[0]
    grads = lax.all_gather(grads, "dp", axis=0)
    gate_grad, up_grad, down_grad = (
        grads[:, k * share : (k + 1) * share].reshape(devices * share, depth).astype(F32)
        for k in range(3)
    )
    gate_grad, up_grad = gate_grad.T, up_grad.T
    out_grad = grads[:, 3 * share :].reshape(width, depth).astype(F32)
    packed, packed_own, out_sums = att_bwd(
        grad_attn, w_out_all, out_parts, q, k, v, context, logsum, lengths, cosine, sine, heads, n
    )
    ffn_out = sum(x.astype(F32) for x in (out_parts[0], *out_sums))
    output = jnp.where(valid, middle + ffn_out, 0.0).astype(BF)
    input_grad, query_grad, key_grad, value_grad, sums = finish(
        attn_rows, packed, packed_own, w_packed, tokens, grad_middle, ln1_gain,
        jnp.stack([gain2_grad, shift2_grad]), width, devices,
    )
    gain1_grad, shift1_grad, gain2_grad, shift2_grad = (sums[i] for i in range(4))
    return (
        output, input_grad, gain1_grad, shift1_grad, query_grad, key_grad, value_grad, out_grad,
        gain2_grad, shift2_grad, gate_grad, up_grad, down_grad,
    )


def solution(mesh):
    rows = P(("dp", "tensor"), None)
    columns = P(None, "tensor")
    parts = P("tensor", None)
    return jax.shard_map(
        on_device,
        mesh=mesh,
        in_specs=(
            rows, P("dp"), P(), P(), columns, columns, columns, parts,
            P(), P(), columns, columns, parts, rows,
        ),
        out_specs=(
            rows, rows, P(), P(), columns, columns, columns, parts,
            P(), P(), columns, columns, parts,
        ),
        check_vma=False,
    )
```

```python
import functools
import math

import jax
import jax.numpy as jnp
from jax import lax
from jax.experimental import pallas as pl
from jax.experimental.pallas import tpu as pltpu
from jax.sharding import PartitionSpec as P

HD = 64
EPS = 1e-05
SCALE = 1.0 / math.sqrt(HD)
F32 = jnp.float32
BF = jnp.bfloat16
NT = (((1,), (1,)), ((), ()))
NN = (((1,), (0,)), ((), ()))
TN = (((0,), (0,)), ((), ()))
MESH = pl.DeviceIdType.MESH


def dot(a, b, dims=NN):
    return lax.dot_general(a, b, dims, preferred_element_type=F32)


def lanes(shape):
    return lax.broadcasted_iota(jnp.int32, shape, 1)


def split3(x):
    hi = x.astype(BF).astype(F32)
    mid = (x - hi).astype(BF).astype(F32)
    return hi, mid, x - hi - mid


def partner(x):
    width = x.shape[1]
    first = lanes(x.shape) % HD < HD // 2
    return jnp.where(first, pltpu.roll(x, width - HD // 2, 1), pltpu.roll(x, HD // 2, 1))


def angle_tables(length):
    half = HD // 2
    lane = lax.optimization_barrier(lax.iota(jnp.int32, 2 * HD))
    freqs = 10000.0 ** (-((lane % half).astype(F32) * 2.0 / HD))
    angles = lax.iota(F32, length)[:, None] * freqs[None, :]
    sign = jnp.where(lane % HD < half, -1.0, 1.0)
    return jnp.cos(angles), jnp.sin(angles) * sign[None, :]


def project_kernel(
    limit_ref, x_ref, wq_ref, wk_ref, wv_ref, cos_ref, sin_ref, q_ref, k_ref, v_ref
):
    x = x_ref[...]
    block = x.shape[0]
    heads = q_ref.shape[0]
    width = heads * HD
    cosine = jnp.tile(cos_ref[...], (1, heads // 2))
    sine = jnp.tile(sin_ref[...], (1, heads // 2))
    lane = lanes((block, 128))
    row = pl.program_id(0) * block + lax.broadcasted_iota(jnp.int32, (block, 128), 0)
    ones = jnp.where(lane < HD + 3, 1.0, 0.0)
    bias = jnp.where(lane == HD + 3, jnp.where(row < limit_ref[0], 0.0, -1e30), ones)
    unit = jnp.where(lane == HD + 3, 1.0, 0.0)

    def turned(w_ref):
        raw = dot(x, w_ref[...])
        return raw * cosine + partner(raw) * sine

    def put(out_ref, values, extra):
        for h in range(heads):
            own = values[:, h // 2 * 128 : h // 2 * 128 + 128]
            own = pltpu.roll(own, HD, 1) if h % 2 else own
            out_ref[h] = jnp.where(lane < HD, own, extra).astype(BF)

    put(q_ref, turned(wq_ref).astype(BF).astype(F32) * SCALE, unit)
    put(k_ref, turned(wk_ref), bias)
    put(v_ref, dot(x, wv_ref[...]), ones)


def project(rows, w_query, w_key, w_value, cosine, sine, limit, block=512):
    n, depth = rows.shape
    width = w_query.shape[1]
    heads = width // HD
    whole = pl.BlockSpec((depth, width), lambda i, *_: (0, 0))
    table = pl.BlockSpec((block, 2 * HD), lambda i, *_: (i, 0))
    out = pl.BlockSpec((heads, block, 128), lambda i, *_: (0, i, 0))
    return pl.pallas_call(
        project_kernel,
        out_shape=(jax.ShapeDtypeStruct((heads, n, 128), BF),) * 3,
        grid_spec=pltpu.PrefetchScalarGridSpec(
            num_scalar_prefetch=1,
            grid=(n // block,),
            in_specs=[pl.BlockSpec((block, depth), lambda i, *_: (i, 0))]
            + [whole] * 3
            + [table] * 2,
            out_specs=(out, out, out),
        ),
        compiler_params=pltpu.CompilerParams(vmem_limit_bytes=40 << 20),
        cost_estimate=pl.CostEstimate(
            flops=2 * n * depth * 3 * width, bytes_accessed=2 * (n * depth + 6 * n * width), transcendentals=0
        ),
        name="project",
    )(limit, rows, w_query, w_key, w_value, cosine, sine)


def differ(a, b, bits):
    return sum(lax.rem(a // (1 << k) + b // (1 << k), 2) * (1 << k) for k in range(bits))


def remote(src, dst, send, recv, **to):
    return pltpu.make_async_remote_copy(
        src_ref=src, dst_ref=dst, send_sem=send, recv_sem=recv, device_id=to, device_id_type=MESH
    )


def ring(n, step):
    return lax.rem(lax.axis_index("tensor") + step, n)


def same_core(s, chips):
    me = lax.axis_index("dp")
    return differ(me // 2, s, chips.bit_length() - 1) * 2 + lax.rem(me, 2)


def sibling():
    me = lax.axis_index("dp")
    return me + 1 - 2 * lax.rem(me, 2)


def greet(n, chips, both_cores=False):
    barrier = pltpu.get_barrier_semaphore()
    if both_cores:
        pl.semaphore_signal(barrier, inc=1, device_id={"dp": sibling()}, device_id_type=MESH)
    for step in range(1, n):
        pl.semaphore_signal(barrier, inc=1, device_id={"tensor": ring(n, step)}, device_id_type=MESH)
    for s in range(1, chips):
        pl.semaphore_signal(
            barrier, inc=1, device_id={"dp": same_core(s, chips)}, device_id_type=MESH
        )
    pl.semaphore_wait(barrier, n + chips - 2 + both_cores)


def att_fwd_kernel(
    n, chips, q_ref, k_ref, v_ref, gb_ref, wo_ref,
    ctx_ref, lse_ref, out_ref, gb_all, wo_z, wo_all, send_sem, recv_sem, own_sem,
    gs_send, gs_recv, gr_send, gr_recv, wz_send, wz_recv, ws_send, ws_recv, wr_send, wr_recv, keep_sem,
):
    s = pl.program_id(0)
    h = pl.program_id(1)
    heads = pl.num_programs(1)
    rows = q_ref.shape[1] // n
    me = lax.axis_index("tensor")
    place = lax.axis_index("dp")
    core = lax.rem(place, 2)
    bits = chips.bit_length() - 1

    def spread_gb(c):
        return remote(
            gb_ref, gb_all.at[place // 2, core], gs_send.at[c], gs_recv.at[c], dp=same_core(c, chips)
        )

    def relay_gb(c):
        there = gb_all.at[differ(place // 2, c, bits), core]
        return remote(
            there if c else gb_ref, there, gr_send.at[c], gr_recv.at[c], dp=sibling()
        )

    def wo_over(step):
        return remote(
            wo_ref, wo_z.at[me], wz_send.at[step], wz_recv.at[step], tensor=ring(n, step + 1)
        )

    def spread_wo(c):
        return remote(
            wo_z, wo_all.at[:, place], ws_send.at[c], ws_recv.at[c], dp=same_core(c, chips)
        )

    def relay_wo(c):
        there = wo_all.at[:, differ(place // 2, c, bits) * 2 + core]
        return remote(there if c else wo_z, there, wr_send.at[c], wr_recv.at[c], dp=sibling())

    keeps = [
        pltpu.make_async_copy(gb_ref, gb_all.at[place // 2, core], keep_sem.at[0]),
        pltpu.make_async_copy(wo_ref, wo_z.at[me], keep_sem.at[1]),
        pltpu.make_async_copy(wo_z, wo_all.at[:, place], keep_sem.at[2]),
    ]

    @pl.when((s == 0) & (h == 0))
    def _():
        greet(n, chips, True)
        for step in range(n - 1):
            wo_over(step).start()
        keeps[0].start()
        keeps[1].start()
        for c in range(1, chips):
            spread_gb(c).start()
        relay_gb(0).start()

    @pl.when((s == 1) & (h == 0))
    def _():
        for step in range(n - 1):
            wo_over(step).wait()
        keeps[1].wait()
        for c in range(1, chips):
            spread_wo(c).start()
        relay_wo(0).start()
        keeps[2].start()

    @pl.when((s == n - 2) & (h == 0))
    def _():
        for c in range(1, chips // 2 + 1):
            spread_gb(c).wait_recv()
            relay_gb(c).start()

    @pl.when((s == n - 1) & (h == 0))
    def _():
        for c in range(1, chips):
            spread_wo(c).wait_recv()
            relay_wo(c).start()
        for c in range(chips // 2 + 1, chips):
            spread_gb(c).wait_recv()
            relay_gb(c).start()

    owner = ring(n, s + 1)
    block = pl.ds(pl.multiple_of(owner * rows, rows), rows)
    scores = dot(q_ref[h, block, :], k_ref[h], NT)
    peak = jnp.max(scores, axis=1, keepdims=True)
    acc = dot(jnp.exp(scores - peak).astype(BF), v_ref[h])
    lane = lanes((rows, 128))
    total = jnp.sum(jnp.where(lane == HD, acc, 0.0), axis=1, keepdims=True)
    out = acc * (1.0 / total)
    odd = lax.rem(h, 2)
    out = jnp.where(odd == 1, pltpu.roll(out, HD, 1), out).astype(BF)
    pair = pl.ds(pl.multiple_of(h // 2 * 128, 128), 128)
    ctx_ref[block, pair] = jnp.where((lane >= HD) == (odd == 1), out, ctx_ref[block, pair])
    lse_ref[block, :] = jnp.where(lane == h, peak + jnp.log(total), lse_ref[block, :])

    def push(step):
        return pltpu.make_async_remote_copy(
            src_ref=ctx_ref.at[block],
            dst_ref=out_ref.at[me],
            send_sem=send_sem.at[step],
            recv_sem=recv_sem.at[step],
            device_id={"tensor": owner},
            device_id_type=MESH,
        )

    @pl.when((h == heads - 1) & (s < n - 1))
    def _():
        push(s).start()

    @pl.when((h == heads - 1) & (s == n - 1))
    def _():
        keep = pltpu.make_async_copy(ctx_ref.at[block], out_ref.at[me], own_sem)
        keep.start()
        for step in range(n - 1):
            push(step).wait()
        keep.wait()
        keeps[0].wait()
        keeps[2].wait()
        for c in range(chips):
            relay_gb(c).wait()
            relay_wo(c).wait()
            if c:
                spread_gb(c).wait_send()
                spread_wo(c).wait_send()


def att_fwd(q, k, v, grad_rows, w_out_piece, n, devices):
    heads, total, _ = q.shape
    width = heads * HD
    rows = total // n
    depth = grad_rows.shape[1]
    share = w_out_piece.shape[0]
    chips = devices // 2
    hbm = pl.BlockSpec(memory_space=pl.ANY)

    def whole(*shape):
        return pl.BlockSpec(shape, lambda *_: (0,) * len(shape), pipeline_mode=pl.Buffered(1))

    return pl.pallas_call(
        functools.partial(att_fwd_kernel, n, chips),
        out_shape=(
            jax.ShapeDtypeStruct((total, width), BF),
            jax.ShapeDtypeStruct((total, 128), F32),
            jax.ShapeDtypeStruct((n, rows, width), BF),
            jax.ShapeDtypeStruct((chips, 2, rows, depth), BF),
            jax.ShapeDtypeStruct((n, share, depth), BF),
            jax.ShapeDtypeStruct((n, devices, share, depth), BF),
        ),
        grid_spec=pltpu.PrefetchScalarGridSpec(
            num_scalar_prefetch=0,
            grid=(n, heads),
            in_specs=[whole(heads, total, 128)] * 3 + [hbm] * 2,
            out_specs=[whole(total, width), whole(total, 128)] + [hbm] * 4,
            scratch_shapes=[pltpu.SemaphoreType.DMA((n - 1,))] * 2
            + [pltpu.SemaphoreType.DMA]
            + [pltpu.SemaphoreType.DMA((chips,))] * 4
            + [pltpu.SemaphoreType.DMA((n - 1,))] * 2
            + [pltpu.SemaphoreType.DMA((chips,))] * 4
            + [pltpu.SemaphoreType.DMA((3,))],
        ),
        compiler_params=pltpu.CompilerParams(
            vmem_limit_bytes=40 << 20, collective_id=1, has_side_effects=True
        ),
        cost_estimate=pl.CostEstimate(
            flops=4 * total * total * 256 * heads,
            bytes_accessed=10 * total * width,
            transcendentals=total * total * heads,
        ),
        name="att_fwd",
    )(q, k, v, grad_rows, w_out_piece)


def att_bwd_kernel(
    n, bk, chips, ga_ref, wo_ref, cown_ref, parts_ref, q_ref, k_ref, v_ref, ctx_ref, lse_ref,
    cos_ref, sin_ref, pk_ref, own_ref, sums_ref, og_ref, do, gc, dka, dva, dqs, dvs,
    og_full, og_own, og_mate, og_sib, og_land, og_piece, og_z,
    send_sem, recv_sem, out_send, out_recv, pk_send, pk_recv, keep_sem,
    om_send, om_recv, op_send, op_recv, oz_send, oz_recv,
):
    h = pl.program_id(0)
    t = pl.program_id(1)
    heads, total, _ = k_ref.shape
    rows = total // n
    me = lax.axis_index("tensor")
    place = lax.axis_index("dp")
    core = lax.rem(place, 2)
    bits = chips.bit_length() - 1
    share = og_ref.shape[0]
    mine = pl.ds(pl.multiple_of(me * rows, rows), rows)

    def push(step):
        return remote(
            gc.at[step], do.at[mine], send_sem.at[step], recv_sem.at[step], tensor=ring(n, step + 1)
        )

    def push_out(s):
        return remote(
            parts_ref.at[s], sums_ref.at[s - 1], out_send.at[s - 1], out_recv.at[s - 1],
            dp=same_core(s, chips),
        )

    def columns(slot):
        return pl.ds(pl.multiple_of(slot * 128, 128), 128)

    def push_pack(slot, step):
        owner = ring(n, step + 1)
        return remote(
            pk_ref.at[pl.ds(pl.multiple_of(owner * rows, rows), rows), columns(slot)],
            own_ref.at[me, :, columns(slot)],
            pk_send.at[slot, step], pk_recv.at[slot, step], tensor=owner,
        )

    def keep(slot):
        return pltpu.make_async_copy(
            pk_ref.at[mine, columns(slot)], own_ref.at[me, :, columns(slot)], keep_sem.at[slot]
        )

    def send_pack(slot):
        for step in range(n - 1):
            push_pack(slot, step).start()
        keep(slot).start()

    @pl.when((h == 0) & (t == 0))
    def _():
        greet(n, chips, True)
        for s in range(1, chips):
            push_out(s).start()

        def send(step, carry):
            gc[step] = dot(ga_ref[...], wo_ref[ring(n, step + 1)], NT).astype(BF)
            push(step).start()
            return carry

        lax.fori_loop(0, n - 1, send, 0)
        do[mine, :] = dot(ga_ref[...], wo_ref[me], NT).astype(BF)

    def og_swap():
        return remote(og_mate, og_sib, om_send, om_recv, dp=sibling())

    def og_push(s):
        return remote(og_sib.at[s], og_land.at[s], op_send.at[s], op_recv.at[s], dp=same_core(s, chips))

    def og_over(step):
        to = ring(n, step + 1)
        return remote(og_piece.at[to], og_z.at[me], oz_send.at[step], oz_recv.at[step], tensor=to)

    @pl.when((h == 0) & (t == 1))
    def _():
        def term(part, carry):
            og_full[...] = dot(cown_ref[part], ga_ref[...], TN)
            for s in range(chips):
                start = differ(place // 2, s, bits) * 2
                here = pl.ds(pl.multiple_of((start + core) * share, share), share)
                there = pl.ds(pl.multiple_of((start + 1 - core) * share, share), share)
                og_own[s, part] = og_full[here, :]
                og_mate[s, part] = og_full[there, :].astype(BF)
            return carry

        lax.fori_loop(0, n, term, 0)
        og_swap().start()

    @pl.when((h == 0) & (t == n - 1))
    def _():
        og_swap().wait_recv()
        for s in range(chips):
            og_sib[s] = (og_own[s] + og_sib[s].astype(F32)).astype(BF)
            if s:
                og_push(s).start()

    @pl.when((h == 1) & (t == 1))
    def _():
        joined = og_sib[0].astype(F32)
        for s in range(1, chips):
            og_push(s).wait_recv()
            joined = joined + og_land[s].astype(F32)
        og_piece[...] = joined.astype(BF)
        for step in range(n - 1):
            og_over(step).start()

    @pl.when((h == heads - 1) & (t == n - 1))
    def _():
        og_z[me] = og_piece[me]
        for step in range(n - 1):
            og_over(step).wait_recv()
        joined = og_z[0].astype(F32)
        for part in range(1, n):
            joined = joined + og_z[part].astype(F32)
        og_ref[...] = joined.astype(BF)

    @pl.when((h == 0) & (t > 0))
    def _():
        push(t - 1).wait_recv()

    @pl.when(t == 0)
    def _():
        dka[...] = jnp.zeros_like(dka)
        dva[...] = jnp.zeros_like(dva)

    source = ring(n, n - t)
    block = pl.ds(pl.multiple_of(source * rows, rows), rows)
    pair = columns(h // 2)
    odd = lax.rem(h, 2) == 1
    lane = lanes((rows, 128))
    off = lane - HD
    logsum = jnp.sum(jnp.where(lane == h, lse_ref[block, :], 0.0), axis=1, keepdims=True)
    a, b, c = split3(-logsum)
    q = q_ref[h, block, :].astype(F32)
    q = jnp.where(off == 0, a, jnp.where(off == 1, b, jnp.where(off == 2, c, q))).astype(BF)
    g = jnp.where((lane >= HD) == odd, do[block, pair].astype(F32), 0.0)
    delta = jnp.sum(g * ctx_ref[block, pair].astype(F32), axis=1, keepdims=True)
    a, b, c = split3(-delta)
    g = jnp.where(odd, pltpu.roll(g, HD, 1), g)
    g = jnp.where(off == 0, a, jnp.where(off == 1, b, jnp.where(off == 2, c, g))).astype(BF)
    acc = jnp.zeros((rows, 128), F32)
    for j in range(total // bk):
        rk = pl.ds(j * bk, bk)
        kt = k_ref[h, rk, :]
        probs = jnp.exp(dot(kt, q, NT))
        grad = (probs * dot(v_ref[h, rk, :], g, NT)).astype(BF)
        dva[rk, :] += dot(probs.astype(BF), g)
        dka[rk, :] += dot(grad, q)
        acc = acc + dot(grad, kt, TN)
    dqs[block, :] = acc * SCALE

    @pl.when(t == n - 1)
    def _():
        first = lanes((total, 128)) < HD
        grad = jnp.where(first, dqs[...], pltpu.roll(dka[...], HD, 1))
        grad = grad * cos_ref[...] - partner(grad) * sin_ref[...]
        pk_ref[:, columns(h)] = grad.astype(BF)
        send_pack(h)

        @pl.when(lax.rem(h, 2) == 0)
        def _():
            dvs[...] = dva[...]

        @pl.when(lax.rem(h, 2) == 1)
        def _():
            both = jnp.where(first, dvs[...], pltpu.roll(dva[...], HD, 1))
            pk_ref[:, columns(heads + h // 2)] = both.astype(BF)
            send_pack(heads + h // 2)

    @pl.when((t == n - 1) & (h == heads - 1))
    def _():
        for step in range(n - 1):
            push(step).wait_send()
        for s in range(1, chips):
            push_out(s).wait()
        og_swap().wait_send()
        for s in range(1, chips):
            og_push(s).wait_send()
        for step in range(n - 1):
            og_over(step).wait_send()
        for slot in range(heads + heads // 2):
            keep(slot).wait()
            for step in range(n - 1):
                push_pack(slot, step).wait()


def att_bwd(grad_attn, w_out, ctx_own, parts, q, k, v, ctx, lse, cosine, sine, n, bk=512):
    heads, total, _ = q.shape
    width = heads * HD
    rows, depth = grad_attn.shape
    chips = parts.shape[0]
    share = width // (2 * chips)
    slots = heads + heads // 2
    hbm = pl.BlockSpec(memory_space=pl.ANY)

    def whole(*shape):
        return pl.BlockSpec(shape, lambda *_: (0,) * len(shape), pipeline_mode=pl.Buffered(1))

    return pl.pallas_call(
        functools.partial(att_bwd_kernel, n, bk, chips),
        out_shape=(
            jax.ShapeDtypeStruct((total, slots * 128), BF),
            jax.ShapeDtypeStruct((n, rows, slots * 128), BF),
            jax.ShapeDtypeStruct((chips - 1, rows, depth), BF),
            jax.ShapeDtypeStruct((share, depth), BF),
        ),
        grid_spec=pltpu.PrefetchScalarGridSpec(
            num_scalar_prefetch=0,
            grid=(heads, n),
            in_specs=[whole(rows, depth), whole(n, width, depth), whole(n, rows, width), hbm]
            + [whole(heads, total, 128)] * 3
            + [whole(total, width)]
            + [whole(total, 128)] * 3,
            out_specs=[whole(total, slots * 128), hbm, hbm, whole(share, depth)],
            scratch_shapes=[
                pltpu.VMEM((total, width), BF),
                pltpu.VMEM((n - 1, rows, width), BF),
            ]
            + [pltpu.VMEM((total, 128), F32)] * 4
            + [
                pltpu.VMEM((width, depth), F32),
                pltpu.VMEM((chips, n, share, depth), F32),
                pltpu.VMEM((chips, n, share, depth), BF),
                pltpu.VMEM((chips, n, share, depth), BF),
                pltpu.VMEM((chips, n, share, depth), BF),
                pltpu.VMEM((n, share, depth), BF),
                pltpu.VMEM((n, share, depth), BF),
            ]
            + [pltpu.SemaphoreType.DMA((n - 1,))] * 2
            + [pltpu.SemaphoreType.DMA((chips - 1,))] * 2
            + [pltpu.SemaphoreType.DMA((slots, n - 1))] * 2
            + [pltpu.SemaphoreType.DMA((slots,))]
            + [pltpu.SemaphoreType.DMA] * 2
            + [pltpu.SemaphoreType.DMA((chips,))] * 2
            + [pltpu.SemaphoreType.DMA((n - 1,))] * 2,
        ),
        compiler_params=pltpu.CompilerParams(
            vmem_limit_bytes=56 << 20, collective_id=2, has_side_effects=True
        ),
        cost_estimate=pl.CostEstimate(
            flops=10 * total * total * 256 * heads,
            bytes_accessed=20 * total * width,
            transcendentals=total * total * heads,
        ),
        name="att_bwd",
    )(grad_attn, w_out, ctx_own, parts, q, k, v, ctx, lse, cosine, sine)


def finish_kernel(
    chips, n, width, x_ref, pk_ref, own_ref, w_ref, tokens_ref, middle_ref, gain_ref, vec_ref,
    input_ref, q_ref, k_ref, v_ref, sums_ref,
    full, mate, sib, land, fin, every, vec_z, vec_dp, vec_me,
    sx_send, sx_recv, rs_send, rs_recv, ag_send, ag_recv, rl_send, rl_recv,
    vz_send, vz_recv, vd_send, vd_recv, own_sem,
):
    bits = chips.bit_length() - 1
    me = lax.axis_index("dp")
    place = lax.axis_index("tensor")
    core = lax.rem(me, 2)
    chip = me // 2
    other = 1 - core
    heads = width // HD
    piece = fin.shape[0]

    def swap(s):
        return remote(mate.at[s], sib.at[s], sx_send.at[s], sx_recv.at[s], dp=chip * 2 + other)

    def push(s):
        return remote(sib.at[s], land.at[s], rs_send.at[s], rs_recv.at[s], dp=same_core(s, chips))

    def spread(s):
        return remote(
            fin, every.at[chip, core], ag_send.at[s], ag_recv.at[s], dp=same_core(s, chips)
        )

    def relay(s):
        src = every.at[differ(chip, s, bits), core]
        return remote(src, src, rl_send.at[s], rl_recv.at[s], dp=chip * 2 + other)

    def vec_over(step):
        return remote(
            vec_me.at[0], vec_z.at[place], vz_send.at[step], vz_recv.at[step], tensor=ring(n, step + 1)
        )

    def vec_across(step):
        return remote(
            vec_me.at[1], vec_dp.at[me], vd_send.at[step], vd_recv.at[step],
            dp=lax.rem(me + step + 1, 2 * chips),
        )

    barrier = pltpu.get_barrier_semaphore()
    for step in range(n - 1):
        pl.semaphore_signal(barrier, inc=1, device_id={"tensor": ring(n, step + 1)}, device_id_type=MESH)
    for step in range(2 * chips - 1):
        to = lax.rem(me + step + 1, 2 * chips)
        pl.semaphore_signal(barrier, inc=1, device_id={"dp": to}, device_id_type=MESH)

    full[...] = dot(x_ref[...], pk_ref[...], TN)
    pl.semaphore_wait(barrier, n + 2 * chips - 2)

    def part(s, which):
        start = (differ(chip, s, bits) * 2 + which) * piece
        return full[pl.ds(pl.multiple_of(start, piece), piece), :]

    for s in range(chips):
        mate[s] = part(s, other).astype(BF)
        swap(s).start()

    grad = jnp.zeros(input_ref.shape, F32)
    for t in range(n):
        grad = grad + dot(own_ref[t], w_ref[t]).astype(BF).astype(F32)

    for s in range(1, chips):
        swap(s).wait_recv()
        sib[s] = (sib[s].astype(F32) + part(s, core)).astype(BF)
        push(s).start()
    swap(0).wait_recv()
    total = sib[0].astype(F32) + part(0, core)

    values = tokens_ref[...].astype(F32)
    values = values - jnp.mean(values, axis=1, keepdims=True)
    inverse = lax.rsqrt(jnp.mean(values * values, axis=1, keepdims=True) + EPS)
    scaled = values * inverse
    through = grad * gain_ref[...]
    inner = through - jnp.mean(through, axis=1, keepdims=True)
    inner = inner - scaled * jnp.mean(through * scaled, axis=1, keepdims=True)
    input_ref[...] = middle_ref[...] + inverse * inner
    vec_me[0, 0:1] = jnp.sum(grad * scaled, axis=0, keepdims=True)
    vec_me[0, 1:2] = jnp.sum(grad, axis=0, keepdims=True)
    vec_me[0, 2:4] = vec_ref[...]
    vec_me[0, 4:8] = jnp.zeros((4, vec_ref.shape[1]), F32)
    vec_z[place] = vec_me[0]
    for step in range(n - 1):
        vec_over(step).start()

    for s in range(1, chips):
        push(s).wait_recv()
        total = total + land[s].astype(F32)
    fin[...] = total.astype(BF)
    for s in range(1, chips):
        spread(s).start()
    mine = pltpu.make_async_copy(fin, every.at[chip, core], own_sem)
    mine.start()
    mine.wait()
    relay(0).start()

    for step in range(n - 1):
        vec_over(step).wait()
    vec = vec_z[0]
    for t in range(1, n):
        vec = vec + vec_z[t]
    vec_me[1] = vec
    vec_dp[me] = vec
    for step in range(2 * chips - 1):
        vec_across(step).start()
    for s in range(1, chips):
        spread(s).wait_recv()
        relay(s).start()
    for step in range(2 * chips - 1):
        vec_across(step).wait()
    vec = vec_dp[0]
    for t in range(1, 2 * chips):
        vec = vec + vec_dp[t]
    sums_ref[...] = vec
    for s in range(chips):
        relay(s).wait()
        swap(s).wait_send()
        if s > 0:
            spread(s).wait_send()
            push(s).wait_send()
    first = lanes((piece, 128)) < HD
    for d in range(2 * chips):
        rows = slice(d * piece, (d + 1) * piece)
        g = every[d // 2, d % 2].astype(F32)
        for pair in range(heads // 2):
            a = g[:, pair * 256 : pair * 256 + 128]
            b = g[:, pair * 256 + 128 : pair * 256 + 256]
            out = slice(pair * 128, pair * 128 + 128)
            q_ref[rows, out] = jnp.where(first, a, pltpu.roll(b, HD, 1))
            k_ref[rows, out] = jnp.where(first, pltpu.roll(a, HD, 1), b)
            v_ref[rows, out] = g[:, (heads + pair) * 128 : (heads + pair + 1) * 128]


def finish(rows_all, packed, own, w_all, tokens, middle, gain, vec, width, devices):
    n, rows, packs = own.shape
    depth = tokens.shape[1]
    chips = devices // 2
    piece = depth // devices
    vmem = pl.BlockSpec(memory_space=pltpu.VMEM)
    out = jax.ShapeDtypeStruct((depth, width), F32)
    return pl.pallas_call(
        functools.partial(finish_kernel, chips, n, width),
        out_shape=(
            jax.ShapeDtypeStruct((rows, depth), F32), out, out, out,
            jax.ShapeDtypeStruct((8, depth), F32),
        ),
        in_specs=[vmem] * 8,
        out_specs=[vmem] * 5,
        scratch_shapes=[
            pltpu.VMEM((depth, packs), F32),
            pltpu.VMEM((chips, piece, packs), BF),
            pltpu.VMEM((chips, piece, packs), BF),
            pltpu.VMEM((chips, piece, packs), BF),
            pltpu.VMEM((piece, packs), BF),
            pltpu.VMEM((chips, 2, piece, packs), BF),
            pltpu.VMEM((n, 8, depth), F32),
            pltpu.VMEM((devices, 8, depth), F32),
            pltpu.VMEM((2, 8, depth), F32),
        ]
        + [pltpu.SemaphoreType.DMA((chips,))] * 8
        + [pltpu.SemaphoreType.DMA((n - 1,))] * 2
        + [pltpu.SemaphoreType.DMA((devices - 1,))] * 2
        + [pltpu.SemaphoreType.DMA],
        compiler_params=pltpu.CompilerParams(
            vmem_limit_bytes=56 << 20, collective_id=4, has_side_effects=True
        ),
        cost_estimate=pl.CostEstimate(
            flops=4 * n * rows * depth * packs, bytes_accessed=20 << 20, transcendentals=0
        ),
        name="finish",
    )(rows_all, packed, own, w_all, tokens, middle, gain.reshape(1, depth), vec)


def ffn_kernel(
    chips, x_ref, gb_ref, w_ref, dx_ref, out_ref, dw_ref,
    rows_all, gb, hid, gate_g, up_g, own, sib, mate, acc,
    ag_send, ag_recv, rl_send, rl_recv, sx_send, sx_recv, rs_send, rs_recv, gb_sem, out_sem, dx_sem,
):
    bits = chips.bit_length() - 1
    me = lax.axis_index("dp")
    core = lax.rem(me, 2)
    chip = me // 2
    other = 1 - core
    rows, depth = x_ref.shape
    n = dw_ref.shape[0]
    share = dw_ref.shape[2]

    def spread(s):
        to = differ(chip, s, bits) * 2 + core
        return remote(x_ref, rows_all.at[chip, core], ag_send.at[s], ag_recv.at[s], dp=to)

    def relay(s):
        src = differ(chip, s, bits)
        return remote(
            rows_all.at[src, core], rows_all.at[src, core], rl_send.at[s], rl_recv.at[s],
            dp=chip * 2 + other,
        )

    def swap(s):
        return remote(
            mate.at[lax.rem(s, 2)], sib.at[s], sx_send.at[s], sx_recv.at[s], dp=chip * 2 + other
        )

    def push(s):
        to = differ(chip, s, bits) * 2 + core
        return remote(sib.at[s, 0], dx_ref.at[s], rs_send.at[s], rs_recv.at[s], dp=to)

    def fetch(s):
        slot = lax.rem(s, 2)
        return pltpu.make_async_copy(
            gb_ref.at[differ(chip, s, bits)], gb.at[slot], gb_sem.at[slot]
        )

    def keep(s):
        return pltpu.make_async_copy(sib.at[s, 1], out_ref.at[s], out_sem.at[s])

    fetch(0).start()
    barrier = pltpu.get_barrier_semaphore()
    pl.semaphore_signal(barrier, inc=1, device_id={"dp": chip * 2 + other}, device_id_type=MESH)
    for s in range(1, chips):
        to = differ(chip, s, bits) * 2 + core
        pl.semaphore_signal(barrier, inc=1, device_id={"dp": to}, device_id_type=MESH)
    pl.semaphore_wait(barrier, chips)
    for s in range(1, chips):
        spread(s).start()
    mine = pltpu.make_async_copy(x_ref, rows_all.at[chip, core], ag_send.at[0])
    mine.start()
    mine.wait()
    relay(0).start()
    acc[...] = jnp.zeros_like(acc)

    def shard(src, slot, which, put):
        x = rows_all[src, which]
        grad = gb[slot, which]
        gate = dot(x, w_ref[0], NT)
        upper = dot(x, w_ref[1], NT)
        grad_hidden = dot(grad, w_ref[2], NT)
        sigma = jax.nn.sigmoid(gate)
        act = gate * sigma
        part = pl.ds(pl.multiple_of(which * rows, rows), rows)
        hidden = (act * upper).astype(BF)
        grad_gate = (grad_hidden * upper * sigma * (1.0 + gate * (1.0 - sigma))).astype(BF)
        grad_upper = (grad_hidden * act).astype(BF)
        hid[part, :] = hidden
        gate_g[part, :] = grad_gate
        up_g[part, :] = grad_upper
        put[0] = (dot(grad_gate, w_ref[0]) + dot(grad_upper, w_ref[1])).astype(BF)
        put[1] = dot(hidden, w_ref[2]).astype(BF)

    def step(s, carry):
        src = differ(chip, s, bits)
        slot = lax.rem(s, 2)
        relay(s).wait_recv()
        fetch(s).wait()

        @pl.when(s < chips - 1)
        def _():
            fetch(s + 1).start()

        @pl.when(s >= 2)
        def _():
            swap(s - 2).wait_send()

        shard(src, slot, other, mate.at[slot])
        swap(s).start()
        shard(src, slot, core, own)
        swap(s).wait_recv()
        for k in range(2):
            sib[s, k] = (sib[s, k].astype(F32) + own[k].astype(F32)).astype(BF)

        @pl.when(s > 0)
        def _():
            push(s).start()

        keep(s).start()

        @pl.when(s < chips - 1)
        def _():
            spread(s + 1).wait_recv()
            relay(s + 1).start()

        x = rows_all[src].reshape(2 * rows, depth)
        acc[0] += dot(gate_g[...], x, TN)
        acc[1] += dot(up_g[...], x, TN)
        acc[2] += dot(hid[...], gb[slot].reshape(2 * rows, depth), TN)
        return carry

    lax.fori_loop(0, chips, step, 0)
    first = pltpu.make_async_copy(sib.at[0, 0], dx_ref.at[0], dx_sem)
    first.start()
    for t in range(n):
        for k in range(3):
            dw_ref[t, k] = acc[k, t * share : (t + 1) * share, :].astype(BF)
    first.wait()
    for s in range(chips):
        keep(s).wait()
        relay(s).wait_send()
        if s >= chips - 2:
            swap(s).wait_send()
        if s > 0:
            spread(s).wait_send()
            push(s).wait()


def ffn(x, grad_branch, weights, n, devices):
    rows, depth = x.shape
    chips = devices // 2
    hidden = weights.shape[1]
    share = hidden // n
    vmem = pl.BlockSpec(memory_space=pltpu.VMEM)
    hbm = pl.BlockSpec(memory_space=pl.ANY)
    return pl.pallas_call(
        functools.partial(ffn_kernel, chips),
        out_shape=(
            jax.ShapeDtypeStruct((chips, rows, depth), BF),
            jax.ShapeDtypeStruct((chips, rows, depth), BF),
            jax.ShapeDtypeStruct((n, 3, share, depth), BF),
        ),
        in_specs=[vmem, hbm, vmem],
        out_specs=[hbm, hbm, vmem],
        scratch_shapes=[
            pltpu.VMEM((chips, 2, rows, depth), BF),
            pltpu.VMEM((2, 2, rows, depth), BF),
        ]
        + [pltpu.VMEM((2 * rows, hidden), BF)] * 3
        + [
            pltpu.VMEM((2, rows, depth), BF),
            pltpu.VMEM((chips, 2, rows, depth), BF),
            pltpu.VMEM((2, 2, rows, depth), BF),
            pltpu.VMEM((3, hidden, depth), F32),
        ]
        + [pltpu.SemaphoreType.DMA((chips,))] * 8
        + [pltpu.SemaphoreType.DMA((2,)), pltpu.SemaphoreType.DMA((chips,)), pltpu.SemaphoreType.DMA],
        compiler_params=pltpu.CompilerParams(
            vmem_limit_bytes=60 << 20, collective_id=3, has_side_effects=True
        ),
        cost_estimate=pl.CostEstimate(
            flops=2 * 9 * devices * rows * depth * hidden, bytes_accessed=30 << 20, transcendentals=0
        ),
        name="ffn",
    )(x, grad_branch, weights)


def norm_parts(values):
    centre = jnp.mean(values, axis=-1, keepdims=True)
    centred = values - centre
    inverse = lax.rsqrt(jnp.mean(centred * centred, axis=-1, keepdims=True) + EPS)
    return centred * inverse, inverse


def norm_back(upstream, scaled, inverse, gain):
    through = upstream * gain
    inner = (
        through
        - jnp.mean(through, axis=-1, keepdims=True)
        - scaled * jnp.mean(through * scaled, axis=-1, keepdims=True)
    )
    return inverse * inner, jnp.sum(upstream * scaled, axis=0), jnp.sum(upstream, axis=0)


def pack_weights(w_query, w_key, w_value):
    depth, width = w_query.shape
    query, key = (w.T.reshape(width // HD, 1, HD, depth) for w in (w_query, w_key))
    both = jnp.concatenate([query, key], axis=1).reshape(2 * width, depth)
    return jnp.concatenate([both, w_value.T], axis=0)


def on_device(
    tokens, lengths, ln1_gain, ln1_bias, w_query, w_key, w_value, w_out,
    ln2_gain, ln2_bias, w_gate, w_up, down_weight, cotangent,
):
    n = lax.axis_size("tensor")
    local_rows, depth = tokens.shape
    length = local_rows * n
    width = w_query.shape[1]
    row_ids = lax.axis_index("tensor") * local_rows + lax.iota(jnp.int32, local_rows)
    valid = (row_ids < lengths[0])[:, None]

    def gather(x):
        return lax.all_gather(x, "tensor", axis=0, tiled=True)

    inputs = tokens.astype(F32)
    scaled1, _ = norm_parts(inputs)
    attn_rows = gather((scaled1 * ln1_gain + ln1_bias).astype(BF))
    cosine, sine = angle_tables(length)
    grad_out = jnp.where(valid, cotangent.astype(F32), 0.0)
    devices = lax.axis_size("dp")
    place = lax.axis_index("dp")
    share = w_gate.shape[1] // devices

    def piece(x, axis):
        return lax.dynamic_slice_in_dim(x, place * share, share, axis)

    weights = jnp.stack([piece(w_gate, 1).T, piece(w_up, 1).T, piece(down_weight, 0)])
    weights = lax.all_gather(weights, "tensor", axis=1, tiled=True)
    q, k, v = project(attn_rows, w_query, w_key, w_value, cosine, sine, lengths)
    context, logsum, context_own, grad_branch, _, w_out_all = att_fwd(
        q, k, v, grad_out.astype(BF),
        lax.dynamic_slice_in_dim(w_out, place * (width // devices), width // devices, 0),
        n, devices,
    )
    w_out_all = w_out_all.reshape(n, width, depth)
    attn_out = sum(dot(context_own[t], w_out_all[t]).astype(BF).astype(F32) for t in range(n))
    middle = inputs + attn_out
    scaled2, inverse2 = norm_parts(middle)
    ffn_in = (scaled2 * ln2_gain + ln2_bias).astype(BF)
    w_packed, ffn_in = lax.optimization_barrier(
        (pack_weights(w_query, w_key, w_value), ffn_in)
    )
    w_packed = lax.all_gather(w_packed, "tensor", axis=0)
    grad_parts, out_parts, ffn_grads = ffn(ffn_in, grad_branch, weights, n, devices)
    grad_ffn_in = sum(grad_parts[p].astype(F32) for p in range(devices // 2))
    grad_norm2, gain2_grad, shift2_grad = norm_back(
        grad_ffn_in, scaled2, inverse2, ln2_gain
    )
    grad_middle = grad_out + grad_norm2
    grad_attn = grad_middle.astype(BF)
    ffn_grads = ffn_grads.reshape(n, 3 * share, depth)
    ffn_grads = lax.psum_scatter(ffn_grads, "tensor", scatter_dimension=0, tiled=True)[0]
    w_packed, grad_attn = lax.optimization_barrier((w_packed, grad_attn))
    packed, packed_own, out_sums, out_piece = att_bwd(
        grad_attn, w_out_all, context_own, out_parts, q, k, v, context, logsum, cosine, sine, n
    )
    ffn_grads, out_piece = lax.optimization_barrier((ffn_grads, out_piece))
    grads = lax.all_gather(jnp.concatenate([ffn_grads, out_piece]), "dp", axis=0)
    gate_grad, up_grad, down_grad = (
        grads[:, k * share : (k + 1) * share].reshape(devices * share, depth).astype(F32)
        for k in range(3)
    )
    gate_grad, up_grad = gate_grad.T, up_grad.T
    out_grad = grads[:, 3 * share :].reshape(width, depth).astype(F32)
    ffn_out = sum(x.astype(F32) for x in (out_parts[0], *out_sums))
    output = jnp.where(valid, middle + ffn_out, 0.0).astype(BF)
    input_grad, query_grad, key_grad, value_grad, sums = finish(
        attn_rows, packed, packed_own, w_packed, tokens, grad_middle, ln1_gain,
        jnp.stack([gain2_grad, shift2_grad]), width, devices,
    )
    gain1_grad, shift1_grad, gain2_grad, shift2_grad = (sums[i] for i in range(4))
    return (
        output, input_grad, gain1_grad, shift1_grad, query_grad, key_grad, value_grad, out_grad,
        gain2_grad, shift2_grad, gate_grad, up_grad, down_grad,
    )


def solution(mesh):
    rows = P(("dp", "tensor"), None)
    columns = P(None, "tensor")
    parts = P("tensor", None)
    return jax.shard_map(
        on_device,
        mesh=mesh,
        in_specs=(
            rows, P("dp"), P(), P(), columns, columns, columns, parts,
            P(), P(), columns, columns, parts, rows,
        ),
        out_specs=(
            rows, rows, P(), P(), columns, columns, columns, parts,
            P(), P(), columns, columns, parts,
        ),
        check_vma=False,
    )
```

```python
import functools
import math

import jax
import jax.numpy as jnp
from jax import lax
from jax.experimental import pallas as pl
from jax.experimental.pallas import tpu as pltpu
from jax.sharding import PartitionSpec as P

HD = 64
EPS = 1e-05
SCALE = 1.0 / math.sqrt(HD)
F32 = jnp.float32
BF = jnp.bfloat16
NT = (((1,), (1,)), ((), ()))
NN = (((1,), (0,)), ((), ()))
TN = (((0,), (0,)), ((), ()))
MESH = pl.DeviceIdType.MESH


def dot(a, b, dims=NN):
    return lax.dot_general(a, b, dims, preferred_element_type=F32)


def lanes(shape):
    return lax.broadcasted_iota(jnp.int32, shape, 1)


def split3(x):
    hi = x.astype(BF).astype(F32)
    mid = (x - hi).astype(BF).astype(F32)
    return hi, mid, x - hi - mid


def partner(x):
    width = x.shape[1]
    first = lanes(x.shape) % HD < HD // 2
    return jnp.where(first, pltpu.roll(x, width - HD // 2, 1), pltpu.roll(x, HD // 2, 1))


STEP = 64


def angle_tables(length):
    half = HD // 2
    lane = lax.optimization_barrier(lax.iota(jnp.int32, 2 * HD))
    freqs = 10000.0 ** (-((lane % half).astype(F32) * 2.0 / HD))
    sign = jnp.where(lane % HD < half, -1.0, 1.0)

    def table(positions):
        angles = positions[:, None] * freqs[None, :]
        return jnp.stack([jnp.cos(angles), jnp.sin(angles)])

    return table(lax.iota(F32, length // STEP) * STEP), table(lax.iota(F32, STEP)), sign[None, :]


def differ(a, b, bits):
    return sum(lax.rem(a // (1 << k) + b // (1 << k), 2) * (1 << k) for k in range(bits))


def remote(src, dst, send, recv, **to):
    return pltpu.make_async_remote_copy(
        src_ref=src, dst_ref=dst, send_sem=send, recv_sem=recv, device_id=to, device_id_type=MESH
    )


def ring(n, step):
    return lax.rem(lax.axis_index("tensor") + step, n)


def same_core(s, chips):
    me = lax.axis_index("dp")
    return differ(me // 2, s, chips.bit_length() - 1) * 2 + lax.rem(me, 2)


def sibling():
    me = lax.axis_index("dp")
    return me + 1 - 2 * lax.rem(me, 2)


def greet(n, chips, both_cores=False):
    barrier = pltpu.get_barrier_semaphore()
    if both_cores:
        pl.semaphore_signal(barrier, inc=1, device_id={"dp": sibling()}, device_id_type=MESH)
    for step in range(1, n):
        pl.semaphore_signal(barrier, inc=1, device_id={"tensor": ring(n, step)}, device_id_type=MESH)
    for s in range(1, chips):
        pl.semaphore_signal(
            barrier, inc=1, device_id={"dp": same_core(s, chips)}, device_id_type=MESH
        )
    pl.semaphore_wait(barrier, n + chips - 2 + both_cores)


def begin_kernel(
    n, chips, chunks, limit_ref, tokens_ref, ct_ref, gain_ref, shift_ref, wq_ref, wk_ref, wv_ref,
    coarse_ref, fine_ref, sign_ref,
    q_ref, k_ref, v_ref, cos_ref, sin_ref, rows_ref, gb_all, landed, gb,
    right_send, right_recv, left_send, left_recv, gs_send, gs_recv, gr_send, gr_recv, keep_sem, rows_sem,
):
    me = lax.axis_index("tensor")
    place = lax.axis_index("dp")
    core = lax.rem(place, 2)
    bits = chips.bit_length() - 1
    rows, depth = tokens_ref.shape
    heads = q_ref.shape[0]
    piece = rows // chunks
    limit = limit_ref[0]

    def over(shard, d, c, send, recv, to):
        part = landed.at[shard, pl.ds(c * piece, piece)]
        return remote(part, part, send.at[d, c], recv.at[d, c], tensor=to)

    def rightward(d, c):
        return over(me - d, d, c, right_send, right_recv, me + 1)

    def leftward(d, c):
        return over(me + d, d, c, left_send, left_recv, me - 1)

    def from_left(d, c):
        return over(me - d, d - 1, c, right_send, right_recv, me - 1)

    def from_right(d, c):
        return over(me + d, d - 1, c, left_send, left_recv, me + 1)

    def spread_gb(c):
        return remote(
            gb, gb_all.at[place // 2, core], gs_send.at[c], gs_recv.at[c], dp=same_core(c, chips)
        )

    def relay_gb(c):
        there = gb_all.at[differ(place // 2, c, bits), core]
        return remote(there if c else gb, there, gr_send.at[c], gr_recv.at[c], dp=sibling())

    barrier = pltpu.get_barrier_semaphore()
    pl.semaphore_signal(barrier, inc=1, device_id={"dp": sibling()}, device_id_type=MESH)
    for s in range(1, chips):
        to = same_core(s, chips)
        pl.semaphore_signal(barrier, inc=1, device_id={"dp": to}, device_id_type=MESH)

    @pl.when(me > 0)
    def _():
        pl.semaphore_signal(barrier, inc=1, device_id={"tensor": me - 1}, device_id_type=MESH)

    @pl.when(me < n - 1)
    def _():
        pl.semaphore_signal(barrier, inc=1, device_id={"tensor": me + 1}, device_id_type=MESH)

    values = tokens_ref[...].astype(F32)
    values = values - jnp.mean(values, axis=1, keepdims=True)
    inverse = lax.rsqrt(jnp.mean(values * values, axis=1, keepdims=True) + EPS)
    landed[me] = (values * inverse * gain_ref[...] + shift_ref[...]).astype(BF)

    pl.semaphore_wait(barrier, chips + jnp.minimum(me, 1) + jnp.minimum(n - 1 - me, 1))

    for c in range(chunks):

        @pl.when(me < n - 1)
        def _():
            rightward(0, c).start()

        @pl.when(me > 0)
        def _():
            leftward(0, c).start()

    row = me * rows + lax.broadcasted_iota(jnp.int32, (rows, depth), 0)
    gb[...] = jnp.where(row < limit, ct_ref[...].astype(F32), 0.0).astype(BF)
    for s in range(1, chips):
        spread_gb(s).start()
    relay_gb(0).start()
    keep = pltpu.make_async_copy(gb, gb_all.at[place // 2, core], keep_sem)
    keep.start()

    lane = lanes((rows, 128))
    ones = jnp.where(lane < HD + 3, 1.0, 0.0)
    unit = jnp.where(lane == HD + 3, 1.0, 0.0)

    def put(out_ref, here, values, extra):
        for h in range(heads):
            own = values[:, h // 2 * 128 : h // 2 * 128 + 128]
            own = pltpu.roll(own, HD, 1) if h % 2 else own
            out_ref[h, here, :] = jnp.where(lane < HD, own, extra).astype(BF)

    def project(shard):
        here = pl.ds(pl.multiple_of(shard * rows, rows), rows)
        for i in range(rows // STEP):
            part = pl.ds(pl.multiple_of(shard * rows + i * STEP, STEP), STEP)
            coarse = pl.ds(shard * (rows // STEP) + i, 1)
            c0, s0 = coarse_ref[0, coarse, :], coarse_ref[1, coarse, :]
            cos_ref[part, :] = c0 * fine_ref[0] - s0 * fine_ref[1]
            sin_ref[part, :] = (s0 * fine_ref[0] + c0 * fine_ref[1]) * sign_ref[...]
        cosine = jnp.tile(cos_ref[here, :], (1, heads // 2))
        sine = jnp.tile(sin_ref[here, :], (1, heads // 2))
        x = landed[shard]
        row = shard * rows + lax.broadcasted_iota(jnp.int32, (rows, 128), 0)
        bias = jnp.where(lane == HD + 3, jnp.where(row < limit, 0.0, -1e30), ones)
        raw = dot(x, wq_ref[...])
        turned = (raw * cosine + partner(raw) * sine).astype(BF).astype(F32)
        put(q_ref, here, turned * SCALE, unit)
        raw = dot(x, wk_ref[...])
        put(k_ref, here, raw * cosine + partner(raw) * sine, bias)
        put(v_ref, here, dot(x, wv_ref[...]), ones)

    def save(shard):
        return pltpu.make_async_copy(landed.at[shard], rows_ref.at[shard], rows_sem.at[shard])

    for d in range(1, n + 1):
        for c in range(chunks):
            if d < n:

                @pl.when(me >= d)
                def _():
                    from_left(d, c).wait_recv()

                @pl.when((me >= d) & (me < n - 1))
                def _():
                    rightward(d, c).start()

                @pl.when(me + d < n)
                def _():
                    from_right(d, c).wait_recv()

                @pl.when((me + d < n) & (me > 0))
                def _():
                    leftward(d, c).start()

            if c == 0:

                @pl.when(me >= d - 1)
                def _():
                    save(me - d + 1).start()
                    project(me - d + 1)

            if c == 1 and d > 1:

                @pl.when(me + d - 1 < n)
                def _():
                    save(me + d - 1).start()
                    project(me + d - 1)

            if c == chunks - 1 and d == 2:
                for s in range(1, chips // 2 + 1):
                    spread_gb(s).wait_recv()
                    relay_gb(s).start()

            if c == 0 and d == n:
                for s in range(chips // 2 + 1, chips):
                    spread_gb(s).wait_recv()
                    relay_gb(s).start()

    for d in range(n - 1):
        for c in range(chunks):

            @pl.when((me >= d) & (me < n - 1))
            def _():
                rightward(d, c).wait_send()

            @pl.when((me + d < n) & (me > 0))
            def _():
                leftward(d, c).wait_send()

    for s in range(chips):
        relay_gb(s).wait()
        if s:
            spread_gb(s).wait_send()
    keep.wait()
    for shard in range(n):
        save(shard).wait()


def begin(tokens, cotangent, gain, shift, w_query, w_key, w_value, tables, limit, n, devices):
    rows, depth = tokens.shape
    total = n * rows
    heads = w_query.shape[1] // HD
    chips = devices // 2
    chunks = 4
    vmem = pl.BlockSpec(memory_space=pltpu.VMEM)
    hbm = pl.BlockSpec(memory_space=pl.ANY)
    return pl.pallas_call(
        functools.partial(begin_kernel, n, chips, chunks),
        out_shape=(jax.ShapeDtypeStruct((heads, total, 128), BF),) * 3
        + (jax.ShapeDtypeStruct((total, 128), F32),) * 2
        + (
            jax.ShapeDtypeStruct((n, rows, depth), BF),
            jax.ShapeDtypeStruct((chips, 2, rows, depth), BF),
        ),
        in_specs=[pl.BlockSpec(memory_space=pltpu.SMEM)] + [vmem] * 10,
        out_specs=[vmem] * 5 + [hbm] * 2,
        scratch_shapes=[pltpu.VMEM((n, rows, depth), BF), pltpu.VMEM((rows, depth), BF)]
        + [pltpu.SemaphoreType.DMA((n - 1, chunks))] * 4
        + [pltpu.SemaphoreType.DMA((chips,))] * 4
        + [pltpu.SemaphoreType.DMA, pltpu.SemaphoreType.DMA((n,))],
        compiler_params=pltpu.CompilerParams(
            vmem_limit_bytes=44 << 20, collective_id=5, has_side_effects=True
        ),
        cost_estimate=pl.CostEstimate(
            flops=6 * total * depth * heads * HD * 10, bytes_accessed=30 << 20, transcendentals=0
        ),
        name="begin",
    )(
        limit, tokens, cotangent, gain.reshape(1, depth), shift.reshape(1, depth),
        w_query, w_key, w_value, *tables,
    )


def att_fwd_kernel(
    n, chips, q_ref, k_ref, v_ref, wo_ref,
    ctx_ref, lse_ref, out_ref, wo_z, wo_all, send_sem, recv_sem, own_sem,
    wz_send, wz_recv, ws_send, ws_recv, wr_send, wr_recv, keep_sem,
):
    s = pl.program_id(0)
    h = pl.program_id(1)
    heads = pl.num_programs(1)
    rows = q_ref.shape[1] // n
    me = lax.axis_index("tensor")
    place = lax.axis_index("dp")
    core = lax.rem(place, 2)
    bits = chips.bit_length() - 1

    def wo_over(step):
        return remote(
            wo_ref, wo_z.at[me], wz_send.at[step], wz_recv.at[step], tensor=ring(n, step + 1)
        )

    def spread_wo(c):
        return remote(
            wo_z, wo_all.at[:, place], ws_send.at[c], ws_recv.at[c], dp=same_core(c, chips)
        )

    def relay_wo(c):
        there = wo_all.at[:, differ(place // 2, c, bits) * 2 + core]
        return remote(there if c else wo_z, there, wr_send.at[c], wr_recv.at[c], dp=sibling())

    keeps = [
        pltpu.make_async_copy(wo_ref, wo_z.at[me], keep_sem.at[0]),
        pltpu.make_async_copy(wo_z, wo_all.at[:, place], keep_sem.at[1]),
    ]

    @pl.when((s == 0) & (h == 0))
    def _():
        greet(n, chips, True)
        for step in range(n - 1):
            wo_over(step).start()
        keeps[0].start()

    @pl.when((s == 1) & (h == 0))
    def _():
        for step in range(n - 1):
            wo_over(step).wait()
        keeps[0].wait()
        for c in range(1, chips):
            spread_wo(c).start()
        relay_wo(0).start()
        keeps[1].start()

    @pl.when((s == n - 1) & (h == 0))
    def _():
        for c in range(1, chips):
            spread_wo(c).wait_recv()
            relay_wo(c).start()

    owner = ring(n, s + 1)
    block = pl.ds(pl.multiple_of(owner * rows, rows), rows)
    scores = dot(q_ref[h, block, :], k_ref[h], NT)
    peak = jnp.max(scores, axis=1, keepdims=True)
    acc = dot(jnp.exp(scores - peak).astype(BF), v_ref[h])
    lane = lanes((rows, 128))
    total = jnp.sum(jnp.where(lane == HD, acc, 0.0), axis=1, keepdims=True)
    out = acc * (1.0 / total)
    odd = lax.rem(h, 2)
    out = jnp.where(odd == 1, pltpu.roll(out, HD, 1), out).astype(BF)
    pair = pl.ds(pl.multiple_of(h // 2 * 128, 128), 128)
    ctx_ref[block, pair] = jnp.where((lane >= HD) == (odd == 1), out, ctx_ref[block, pair])
    lse_ref[block, :] = jnp.where(lane == h, peak + jnp.log(total), lse_ref[block, :])

    def push(step):
        return pltpu.make_async_remote_copy(
            src_ref=ctx_ref.at[block],
            dst_ref=out_ref.at[me],
            send_sem=send_sem.at[step],
            recv_sem=recv_sem.at[step],
            device_id={"tensor": owner},
            device_id_type=MESH,
        )

    @pl.when((h == heads - 1) & (s < n - 1))
    def _():
        push(s).start()

    @pl.when((h == heads - 1) & (s == n - 1))
    def _():
        keep = pltpu.make_async_copy(ctx_ref.at[block], out_ref.at[me], own_sem)
        keep.start()
        for step in range(n - 1):
            push(step).wait()
        keep.wait()
        keeps[1].wait()
        for c in range(chips):
            relay_wo(c).wait()
            if c:
                spread_wo(c).wait_send()


def att_fwd(q, k, v, w_out_piece, n, devices):
    heads, total, _ = q.shape
    width = heads * HD
    rows = total // n
    share, depth = w_out_piece.shape
    chips = devices // 2
    hbm = pl.BlockSpec(memory_space=pl.ANY)

    def whole(*shape):
        return pl.BlockSpec(shape, lambda *_: (0,) * len(shape), pipeline_mode=pl.Buffered(1))

    return pl.pallas_call(
        functools.partial(att_fwd_kernel, n, chips),
        out_shape=(
            jax.ShapeDtypeStruct((total, width), BF),
            jax.ShapeDtypeStruct((total, 128), F32),
            jax.ShapeDtypeStruct((n, rows, width), BF),
            jax.ShapeDtypeStruct((n, share, depth), BF),
            jax.ShapeDtypeStruct((n, devices, share, depth), BF),
        ),
        grid_spec=pltpu.PrefetchScalarGridSpec(
            num_scalar_prefetch=0,
            grid=(n, heads),
            in_specs=[whole(heads, total, 128)] * 3 + [hbm],
            out_specs=[whole(total, width), whole(total, 128)] + [hbm] * 3,
            scratch_shapes=[pltpu.SemaphoreType.DMA((n - 1,))] * 2
            + [pltpu.SemaphoreType.DMA]
            + [pltpu.SemaphoreType.DMA((n - 1,))] * 2
            + [pltpu.SemaphoreType.DMA((chips,))] * 4
            + [pltpu.SemaphoreType.DMA((2,))],
        ),
        compiler_params=pltpu.CompilerParams(
            vmem_limit_bytes=40 << 20, collective_id=1, has_side_effects=True
        ),
        cost_estimate=pl.CostEstimate(
            flops=4 * total * total * 256 * heads,
            bytes_accessed=10 * total * width,
            transcendentals=total * total * heads,
        ),
        name="att_fwd",
    )(q, k, v, w_out_piece)


def att_bwd_kernel(
    n, bk, chips, ga_ref, wo_ref, cown_ref, parts_ref, q_ref, k_ref, v_ref, ctx_ref, lse_ref,
    cos_ref, sin_ref, pk_ref, own_ref, sums_ref, og_ref, do, gc, dka, dva, dqs, dvs,
    og_full, og_own, og_mate, og_sib, og_land, og_piece, og_z,
    send_sem, recv_sem, out_send, out_recv, pk_send, pk_recv, keep_sem,
    om_send, om_recv, op_send, op_recv, oz_send, oz_recv,
):
    h = pl.program_id(0)
    t = pl.program_id(1)
    heads, total, _ = k_ref.shape
    rows = total // n
    me = lax.axis_index("tensor")
    place = lax.axis_index("dp")
    core = lax.rem(place, 2)
    bits = chips.bit_length() - 1
    share = og_ref.shape[0]
    mine = pl.ds(pl.multiple_of(me * rows, rows), rows)

    def push(step):
        return remote(
            gc.at[step], do.at[mine], send_sem.at[step], recv_sem.at[step], tensor=ring(n, step + 1)
        )

    def push_out(s):
        return remote(
            parts_ref.at[s], sums_ref.at[s - 1], out_send.at[s - 1], out_recv.at[s - 1],
            dp=same_core(s, chips),
        )

    def columns(slot):
        return pl.ds(pl.multiple_of(slot * 128, 128), 128)

    def push_pack(slot, step):
        owner = ring(n, step + 1)
        return remote(
            pk_ref.at[pl.ds(pl.multiple_of(owner * rows, rows), rows), columns(slot)],
            own_ref.at[me, :, columns(slot)],
            pk_send.at[slot, step], pk_recv.at[slot, step], tensor=owner,
        )

    def keep(slot):
        return pltpu.make_async_copy(
            pk_ref.at[mine, columns(slot)], own_ref.at[me, :, columns(slot)], keep_sem.at[slot]
        )

    def send_pack(slot):
        for step in range(n - 1):
            push_pack(slot, step).start()
        keep(slot).start()

    @pl.when((h == 0) & (t == 0))
    def _():
        greet(n, chips, True)
        for s in range(1, chips):
            push_out(s).start()

        def send(step, carry):
            gc[step] = dot(ga_ref[...], wo_ref[ring(n, step + 1)], NT).astype(BF)
            push(step).start()
            return carry

        lax.fori_loop(0, n - 1, send, 0)
        do[mine, :] = dot(ga_ref[...], wo_ref[me], NT).astype(BF)

    def og_swap():
        return remote(og_mate, og_sib, om_send, om_recv, dp=sibling())

    def og_push(s):
        return remote(og_sib.at[s], og_land.at[s], op_send.at[s], op_recv.at[s], dp=same_core(s, chips))

    def og_over(step):
        to = ring(n, step + 1)
        return remote(og_piece.at[to], og_z.at[me], oz_send.at[step], oz_recv.at[step], tensor=to)

    @pl.when((h == 0) & (t == 1))
    def _():
        def term(part, carry):
            og_full[...] = dot(cown_ref[part], ga_ref[...], TN)
            for s in range(chips):
                start = differ(place // 2, s, bits) * 2
                here = pl.ds(pl.multiple_of((start + core) * share, share), share)
                there = pl.ds(pl.multiple_of((start + 1 - core) * share, share), share)
                og_own[s, part] = og_full[here, :]
                og_mate[s, part] = og_full[there, :].astype(BF)
            return carry

        lax.fori_loop(0, n, term, 0)
        og_swap().start()

    @pl.when((h == 0) & (t == n - 1))
    def _():
        og_swap().wait_recv()
        for s in range(chips):
            og_sib[s] = (og_own[s] + og_sib[s].astype(F32)).astype(BF)
            if s:
                og_push(s).start()

    @pl.when((h == 1) & (t == 1))
    def _():
        joined = og_sib[0].astype(F32)
        for s in range(1, chips):
            og_push(s).wait_recv()
            joined = joined + og_land[s].astype(F32)
        og_piece[...] = joined.astype(BF)
        for step in range(n - 1):
            og_over(step).start()

    @pl.when((h == heads - 1) & (t == n - 1))
    def _():
        og_z[me] = og_piece[me]
        for step in range(n - 1):
            og_over(step).wait_recv()
        joined = og_z[0].astype(F32)
        for part in range(1, n):
            joined = joined + og_z[part].astype(F32)
        og_ref[...] = joined.astype(BF)

    @pl.when((h == 0) & (t > 0))
    def _():
        push(t - 1).wait_recv()

    @pl.when(t == 0)
    def _():
        dka[...] = jnp.zeros_like(dka)
        dva[...] = jnp.zeros_like(dva)

    source = ring(n, n - t)
    block = pl.ds(pl.multiple_of(source * rows, rows), rows)
    pair = columns(h // 2)
    odd = lax.rem(h, 2) == 1
    lane = lanes((rows, 128))
    off = lane - HD
    logsum = jnp.sum(jnp.where(lane == h, lse_ref[block, :], 0.0), axis=1, keepdims=True)
    a, b, c = split3(-logsum)
    q = q_ref[h, block, :].astype(F32)
    q = jnp.where(off == 0, a, jnp.where(off == 1, b, jnp.where(off == 2, c, q))).astype(BF)
    g = jnp.where((lane >= HD) == odd, do[block, pair].astype(F32), 0.0)
    delta = jnp.sum(g * ctx_ref[block, pair].astype(F32), axis=1, keepdims=True)
    a, b, c = split3(-delta)
    g = jnp.where(odd, pltpu.roll(g, HD, 1), g)
    g = jnp.where(off == 0, a, jnp.where(off == 1, b, jnp.where(off == 2, c, g))).astype(BF)
    acc = jnp.zeros((rows, 128), F32)
    for j in range(total // bk):
        rk = pl.ds(j * bk, bk)
        kt = k_ref[h, rk, :]
        probs = jnp.exp(dot(kt, q, NT))
        grad = (probs * dot(v_ref[h, rk, :], g, NT)).astype(BF)
        dva[rk, :] += dot(probs.astype(BF), g)
        dka[rk, :] += dot(grad, q)
        acc = acc + dot(grad, kt, TN)
    dqs[block, :] = acc * SCALE

    @pl.when(t == n - 1)
    def _():
        first = lanes((total, 128)) < HD
        grad = jnp.where(first, dqs[...], pltpu.roll(dka[...], HD, 1))
        grad = grad * cos_ref[...] - partner(grad) * sin_ref[...]
        pk_ref[:, columns(h)] = grad.astype(BF)
        send_pack(h)

        @pl.when(lax.rem(h, 2) == 0)
        def _():
            dvs[...] = dva[...]

        @pl.when(lax.rem(h, 2) == 1)
        def _():
            both = jnp.where(first, dvs[...], pltpu.roll(dva[...], HD, 1))
            pk_ref[:, columns(heads + h // 2)] = both.astype(BF)
            send_pack(heads + h // 2)

    @pl.when((t == n - 1) & (h == heads - 1))
    def _():
        for step in range(n - 1):
            push(step).wait_send()
        for s in range(1, chips):
            push_out(s).wait()
        og_swap().wait_send()
        for s in range(1, chips):
            og_push(s).wait_send()
        for step in range(n - 1):
            og_over(step).wait_send()
        for slot in range(heads + heads // 2):
            keep(slot).wait()
            for step in range(n - 1):
                push_pack(slot, step).wait()


def att_bwd(grad_attn, w_out, ctx_own, parts, q, k, v, ctx, lse, cosine, sine, n, bk=512):
    heads, total, _ = q.shape
    width = heads * HD
    rows, depth = grad_attn.shape
    chips = parts.shape[0]
    share = width // (2 * chips)
    slots = heads + heads // 2
    hbm = pl.BlockSpec(memory_space=pl.ANY)

    def whole(*shape):
        return pl.BlockSpec(shape, lambda *_: (0,) * len(shape), pipeline_mode=pl.Buffered(1))

    return pl.pallas_call(
        functools.partial(att_bwd_kernel, n, bk, chips),
        out_shape=(
            jax.ShapeDtypeStruct((total, slots * 128), BF),
            jax.ShapeDtypeStruct((n, rows, slots * 128), BF),
            jax.ShapeDtypeStruct((chips - 1, rows, depth), BF),
            jax.ShapeDtypeStruct((share, depth), BF),
        ),
        grid_spec=pltpu.PrefetchScalarGridSpec(
            num_scalar_prefetch=0,
            grid=(heads, n),
            in_specs=[whole(rows, depth), whole(n, width, depth), whole(n, rows, width), hbm]
            + [whole(heads, total, 128)] * 3
            + [whole(total, width)]
            + [whole(total, 128)] * 3,
            out_specs=[whole(total, slots * 128), hbm, hbm, whole(share, depth)],
            scratch_shapes=[
                pltpu.VMEM((total, width), BF),
                pltpu.VMEM((n - 1, rows, width), BF),
            ]
            + [pltpu.VMEM((total, 128), F32)] * 4
            + [
                pltpu.VMEM((width, depth), F32),
                pltpu.VMEM((chips, n, share, depth), F32),
                pltpu.VMEM((chips, n, share, depth), BF),
                pltpu.VMEM((chips, n, share, depth), BF),
                pltpu.VMEM((chips, n, share, depth), BF),
                pltpu.VMEM((n, share, depth), BF),
                pltpu.VMEM((n, share, depth), BF),
            ]
            + [pltpu.SemaphoreType.DMA((n - 1,))] * 2
            + [pltpu.SemaphoreType.DMA((chips - 1,))] * 2
            + [pltpu.SemaphoreType.DMA((slots, n - 1))] * 2
            + [pltpu.SemaphoreType.DMA((slots,))]
            + [pltpu.SemaphoreType.DMA] * 2
            + [pltpu.SemaphoreType.DMA((chips,))] * 2
            + [pltpu.SemaphoreType.DMA((n - 1,))] * 2,
        ),
        compiler_params=pltpu.CompilerParams(
            vmem_limit_bytes=56 << 20, collective_id=2, has_side_effects=True
        ),
        cost_estimate=pl.CostEstimate(
            flops=10 * total * total * 256 * heads,
            bytes_accessed=20 * total * width,
            transcendentals=total * total * heads,
        ),
        name="att_bwd",
    )(grad_attn, w_out, ctx_own, parts, q, k, v, ctx, lse, cosine, sine)


def finish_kernel(
    chips, n, width, x_ref, pk_ref, own_ref, w_ref, tokens_ref, middle_ref, gain_ref, vec_ref,
    input_ref, q_ref, k_ref, v_ref, sums_ref,
    full, mate, sib, land, fin, every, vec_z, vec_dp, vec_me,
    sx_send, sx_recv, rs_send, rs_recv, ag_send, ag_recv, rl_send, rl_recv,
    vz_send, vz_recv, vd_send, vd_recv, own_sem,
):
    bits = chips.bit_length() - 1
    me = lax.axis_index("dp")
    place = lax.axis_index("tensor")
    core = lax.rem(me, 2)
    chip = me // 2
    other = 1 - core
    heads = width // HD
    piece = fin.shape[0]

    def swap(s):
        return remote(mate.at[s], sib.at[s], sx_send.at[s], sx_recv.at[s], dp=chip * 2 + other)

    def push(s):
        return remote(sib.at[s], land.at[s], rs_send.at[s], rs_recv.at[s], dp=same_core(s, chips))

    def spread(s):
        return remote(
            fin, every.at[chip, core], ag_send.at[s], ag_recv.at[s], dp=same_core(s, chips)
        )

    def relay(s):
        src = every.at[differ(chip, s, bits), core]
        return remote(src, src, rl_send.at[s], rl_recv.at[s], dp=chip * 2 + other)

    def vec_over(step):
        return remote(
            vec_me.at[0], vec_z.at[place], vz_send.at[step], vz_recv.at[step], tensor=ring(n, step + 1)
        )

    def vec_across(step):
        return remote(
            vec_me.at[1], vec_dp.at[me], vd_send.at[step], vd_recv.at[step],
            dp=lax.rem(me + step + 1, 2 * chips),
        )

    barrier = pltpu.get_barrier_semaphore()
    for step in range(n - 1):
        pl.semaphore_signal(barrier, inc=1, device_id={"tensor": ring(n, step + 1)}, device_id_type=MESH)
    for step in range(2 * chips - 1):
        to = lax.rem(me + step + 1, 2 * chips)
        pl.semaphore_signal(barrier, inc=1, device_id={"dp": to}, device_id_type=MESH)

    full[...] = dot(x_ref[...], pk_ref[...], TN)
    pl.semaphore_wait(barrier, n + 2 * chips - 2)

    def part(s, which):
        start = (differ(chip, s, bits) * 2 + which) * piece
        return full[pl.ds(pl.multiple_of(start, piece), piece), :]

    for s in range(chips):
        mate[s] = part(s, other).astype(BF)
        swap(s).start()

    grad = jnp.zeros(input_ref.shape, F32)
    for t in range(n):
        grad = grad + dot(own_ref[t], w_ref[t]).astype(BF).astype(F32)

    for s in range(1, chips):
        swap(s).wait_recv()
        sib[s] = (sib[s].astype(F32) + part(s, core)).astype(BF)
        push(s).start()
    swap(0).wait_recv()
    total = sib[0].astype(F32) + part(0, core)

    values = tokens_ref[...].astype(F32)
    values = values - jnp.mean(values, axis=1, keepdims=True)
    inverse = lax.rsqrt(jnp.mean(values * values, axis=1, keepdims=True) + EPS)
    scaled = values * inverse
    through = grad * gain_ref[...]
    inner = through - jnp.mean(through, axis=1, keepdims=True)
    inner = inner - scaled * jnp.mean(through * scaled, axis=1, keepdims=True)
    input_ref[...] = middle_ref[...] + inverse * inner
    vec_me[0, 0:1] = jnp.sum(grad * scaled, axis=0, keepdims=True)
    vec_me[0, 1:2] = jnp.sum(grad, axis=0, keepdims=True)
    vec_me[0, 2:4] = vec_ref[...]
    vec_me[0, 4:8] = jnp.zeros((4, vec_ref.shape[1]), F32)
    vec_z[place] = vec_me[0]
    for step in range(n - 1):
        vec_over(step).start()

    for s in range(1, chips):
        push(s).wait_recv()
        total = total + land[s].astype(F32)
    fin[...] = total.astype(BF)
    for s in range(1, chips):
        spread(s).start()
    mine = pltpu.make_async_copy(fin, every.at[chip, core], own_sem)
    mine.start()
    mine.wait()
    relay(0).start()

    for step in range(n - 1):
        vec_over(step).wait()
    vec = vec_z[0]
    for t in range(1, n):
        vec = vec + vec_z[t]
    vec_me[1] = vec
    vec_dp[me] = vec
    for step in range(2 * chips - 1):
        vec_across(step).start()
    for s in range(1, chips):
        spread(s).wait_recv()
        relay(s).start()
    for step in range(2 * chips - 1):
        vec_across(step).wait()
    vec = vec_dp[0]
    for t in range(1, 2 * chips):
        vec = vec + vec_dp[t]
    sums_ref[...] = vec
    for s in range(chips):
        relay(s).wait()
        swap(s).wait_send()
        if s > 0:
            spread(s).wait_send()
            push(s).wait_send()
    first = lanes((piece, 128)) < HD
    for d in range(2 * chips):
        rows = slice(d * piece, (d + 1) * piece)
        g = every[d // 2, d % 2].astype(F32)
        for pair in range(heads // 2):
            a = g[:, pair * 256 : pair * 256 + 128]
            b = g[:, pair * 256 + 128 : pair * 256 + 256]
            out = slice(pair * 128, pair * 128 + 128)
            q_ref[rows, out] = jnp.where(first, a, pltpu.roll(b, HD, 1))
            k_ref[rows, out] = jnp.where(first, pltpu.roll(a, HD, 1), b)
            v_ref[rows, out] = g[:, (heads + pair) * 128 : (heads + pair + 1) * 128]


def finish(rows_all, packed, own, w_all, tokens, middle, gain, vec, width, devices):
    n, rows, packs = own.shape
    depth = tokens.shape[1]
    chips = devices // 2
    piece = depth // devices
    vmem = pl.BlockSpec(memory_space=pltpu.VMEM)
    out = jax.ShapeDtypeStruct((depth, width), F32)
    return pl.pallas_call(
        functools.partial(finish_kernel, chips, n, width),
        out_shape=(
            jax.ShapeDtypeStruct((rows, depth), F32), out, out, out,
            jax.ShapeDtypeStruct((8, depth), F32),
        ),
        in_specs=[vmem] * 8,
        out_specs=[vmem] * 5,
        scratch_shapes=[
            pltpu.VMEM((depth, packs), F32),
            pltpu.VMEM((chips, piece, packs), BF),
            pltpu.VMEM((chips, piece, packs), BF),
            pltpu.VMEM((chips, piece, packs), BF),
            pltpu.VMEM((piece, packs), BF),
            pltpu.VMEM((chips, 2, piece, packs), BF),
            pltpu.VMEM((n, 8, depth), F32),
            pltpu.VMEM((devices, 8, depth), F32),
            pltpu.VMEM((2, 8, depth), F32),
        ]
        + [pltpu.SemaphoreType.DMA((chips,))] * 8
        + [pltpu.SemaphoreType.DMA((n - 1,))] * 2
        + [pltpu.SemaphoreType.DMA((devices - 1,))] * 2
        + [pltpu.SemaphoreType.DMA],
        compiler_params=pltpu.CompilerParams(
            vmem_limit_bytes=56 << 20, collective_id=4, has_side_effects=True
        ),
        cost_estimate=pl.CostEstimate(
            flops=4 * n * rows * depth * packs, bytes_accessed=20 << 20, transcendentals=0
        ),
        name="finish",
    )(rows_all, packed, own, w_all, tokens, middle, gain.reshape(1, depth), vec)


def ffn_kernel(
    chips, x_ref, gb_ref, w_ref, dx_ref, out_ref, dw_ref,
    rows_all, gb, hid, gate_g, up_g, own, sib, mate, acc,
    ag_send, ag_recv, rl_send, rl_recv, sx_send, sx_recv, rs_send, rs_recv, gb_sem, out_sem, dx_sem,
):
    bits = chips.bit_length() - 1
    me = lax.axis_index("dp")
    core = lax.rem(me, 2)
    chip = me // 2
    other = 1 - core
    rows, depth = x_ref.shape
    n = dw_ref.shape[0]
    share = dw_ref.shape[2]

    def spread(s):
        to = differ(chip, s, bits) * 2 + core
        return remote(x_ref, rows_all.at[chip, core], ag_send.at[s], ag_recv.at[s], dp=to)

    def relay(s):
        src = differ(chip, s, bits)
        return remote(
            rows_all.at[src, core], rows_all.at[src, core], rl_send.at[s], rl_recv.at[s],
            dp=chip * 2 + other,
        )

    def swap(s):
        return remote(
            mate.at[lax.rem(s, 2)], sib.at[s], sx_send.at[s], sx_recv.at[s], dp=chip * 2 + other
        )

    def push(s):
        to = differ(chip, s, bits) * 2 + core
        return remote(sib.at[s, 0], dx_ref.at[s], rs_send.at[s], rs_recv.at[s], dp=to)

    def fetch(s):
        slot = lax.rem(s, 2)
        return pltpu.make_async_copy(
            gb_ref.at[differ(chip, s, bits)], gb.at[slot], gb_sem.at[slot]
        )

    def keep(s):
        return pltpu.make_async_copy(sib.at[s, 1], out_ref.at[s], out_sem.at[s])

    fetch(0).start()
    barrier = pltpu.get_barrier_semaphore()
    pl.semaphore_signal(barrier, inc=1, device_id={"dp": chip * 2 + other}, device_id_type=MESH)
    for s in range(1, chips):
        to = differ(chip, s, bits) * 2 + core
        pl.semaphore_signal(barrier, inc=1, device_id={"dp": to}, device_id_type=MESH)
    pl.semaphore_wait(barrier, chips)
    for s in range(1, chips):
        spread(s).start()
    mine = pltpu.make_async_copy(x_ref, rows_all.at[chip, core], ag_send.at[0])
    mine.start()
    mine.wait()
    relay(0).start()
    acc[...] = jnp.zeros_like(acc)

    def shard(src, slot, which, put):
        x = rows_all[src, which]
        grad = gb[slot, which]
        gate = dot(x, w_ref[0], NT)
        upper = dot(x, w_ref[1], NT)
        grad_hidden = dot(grad, w_ref[2], NT)
        sigma = jax.nn.sigmoid(gate)
        act = gate * sigma
        part = pl.ds(pl.multiple_of(which * rows, rows), rows)
        hidden = (act * upper).astype(BF)
        grad_gate = (grad_hidden * upper * sigma * (1.0 + gate * (1.0 - sigma))).astype(BF)
        grad_upper = (grad_hidden * act).astype(BF)
        hid[part, :] = hidden
        gate_g[part, :] = grad_gate
        up_g[part, :] = grad_upper
        put[0] = (dot(grad_gate, w_ref[0]) + dot(grad_upper, w_ref[1])).astype(BF)
        put[1] = dot(hidden, w_ref[2]).astype(BF)

    def step(s, carry):
        src = differ(chip, s, bits)
        slot = lax.rem(s, 2)
        relay(s).wait_recv()
        fetch(s).wait()

        @pl.when(s < chips - 1)
        def _():
            fetch(s + 1).start()

        @pl.when(s >= 2)
        def _():
            swap(s - 2).wait_send()

        shard(src, slot, other, mate.at[slot])
        swap(s).start()
        shard(src, slot, core, own)
        swap(s).wait_recv()
        for k in range(2):
            sib[s, k] = (sib[s, k].astype(F32) + own[k].astype(F32)).astype(BF)

        @pl.when(s > 0)
        def _():
            push(s).start()

        keep(s).start()

        @pl.when(s < chips - 1)
        def _():
            spread(s + 1).wait_recv()
            relay(s + 1).start()

        x = rows_all[src].reshape(2 * rows, depth)
        acc[0] += dot(gate_g[...], x, TN)
        acc[1] += dot(up_g[...], x, TN)
        acc[2] += dot(hid[...], gb[slot].reshape(2 * rows, depth), TN)
        return carry

    lax.fori_loop(0, chips, step, 0)
    first = pltpu.make_async_copy(sib.at[0, 0], dx_ref.at[0], dx_sem)
    first.start()
    for t in range(n):
        for k in range(3):
            dw_ref[t, k] = acc[k, t * share : (t + 1) * share, :].astype(BF)
    first.wait()
    for s in range(chips):
        keep(s).wait()
        relay(s).wait_send()
        if s >= chips - 2:
            swap(s).wait_send()
        if s > 0:
            spread(s).wait_send()
            push(s).wait()


def ffn(x, grad_branch, weights, n, devices):
    rows, depth = x.shape
    chips = devices // 2
    hidden = weights.shape[1]
    share = hidden // n
    vmem = pl.BlockSpec(memory_space=pltpu.VMEM)
    hbm = pl.BlockSpec(memory_space=pl.ANY)
    return pl.pallas_call(
        functools.partial(ffn_kernel, chips),
        out_shape=(
            jax.ShapeDtypeStruct((chips, rows, depth), BF),
            jax.ShapeDtypeStruct((chips, rows, depth), BF),
            jax.ShapeDtypeStruct((n, 3, share, depth), BF),
        ),
        in_specs=[vmem, hbm, vmem],
        out_specs=[hbm, hbm, vmem],
        scratch_shapes=[
            pltpu.VMEM((chips, 2, rows, depth), BF),
            pltpu.VMEM((2, 2, rows, depth), BF),
        ]
        + [pltpu.VMEM((2 * rows, hidden), BF)] * 3
        + [
            pltpu.VMEM((2, rows, depth), BF),
            pltpu.VMEM((chips, 2, rows, depth), BF),
            pltpu.VMEM((2, 2, rows, depth), BF),
            pltpu.VMEM((3, hidden, depth), F32),
        ]
        + [pltpu.SemaphoreType.DMA((chips,))] * 8
        + [pltpu.SemaphoreType.DMA((2,)), pltpu.SemaphoreType.DMA((chips,)), pltpu.SemaphoreType.DMA],
        compiler_params=pltpu.CompilerParams(
            vmem_limit_bytes=60 << 20, collective_id=3, has_side_effects=True
        ),
        cost_estimate=pl.CostEstimate(
            flops=2 * 9 * devices * rows * depth * hidden, bytes_accessed=30 << 20, transcendentals=0
        ),
        name="ffn",
    )(x, grad_branch, weights)


def unpack_kernel(share, g_ref, gate_ref, up_ref, down_ref, out_ref):
    g = g_ref[0].astype(F32)
    gate_ref[...] = g[:share].T
    up_ref[...] = g[share : 2 * share].T
    down_ref[...] = g[2 * share : 3 * share]
    out_ref[...] = g[3 * share :]


def unpack(grads, share, width):
    devices, height, depth = grads.shape
    hidden = devices * share
    if share % 128:
        gate, up, down = (
            grads[:, k * share : (k + 1) * share].reshape(hidden, depth).astype(F32) for k in range(3)
        )
        return gate.T, up.T, down, grads[:, 3 * share :].reshape(width, depth).astype(F32)
    column = pl.BlockSpec((depth, share), lambda i: (0, i))
    return pl.pallas_call(
        functools.partial(unpack_kernel, share),
        out_shape=(
            jax.ShapeDtypeStruct((depth, hidden), F32),
            jax.ShapeDtypeStruct((depth, hidden), F32),
            jax.ShapeDtypeStruct((hidden, depth), F32),
            jax.ShapeDtypeStruct((width, depth), F32),
        ),
        grid=(devices,),
        in_specs=[pl.BlockSpec((1, height, depth), lambda i: (i, 0, 0))],
        out_specs=[
            column, column, pl.BlockSpec((share, depth), lambda i: (i, 0)),
            pl.BlockSpec((width // devices, depth), lambda i: (i, 0)),
        ],
        compiler_params=pltpu.CompilerParams(vmem_limit_bytes=40 << 20),
        name="unpack",
    )(grads)


def norm_parts(values):
    centre = jnp.mean(values, axis=-1, keepdims=True)
    centred = values - centre
    inverse = lax.rsqrt(jnp.mean(centred * centred, axis=-1, keepdims=True) + EPS)
    return centred * inverse, inverse


def norm_back(upstream, scaled, inverse, gain):
    through = upstream * gain
    inner = (
        through
        - jnp.mean(through, axis=-1, keepdims=True)
        - scaled * jnp.mean(through * scaled, axis=-1, keepdims=True)
    )
    return inverse * inner, jnp.sum(upstream * scaled, axis=0), jnp.sum(upstream, axis=0)


def pack_weights(w_query, w_key, w_value):
    depth, width = w_query.shape
    query, key = (w.T.reshape(width // HD, 1, HD, depth) for w in (w_query, w_key))
    both = jnp.concatenate([query, key], axis=1).reshape(2 * width, depth)
    return jnp.concatenate([both, w_value.T], axis=0)


def on_device(
    tokens, lengths, ln1_gain, ln1_bias, w_query, w_key, w_value, w_out,
    ln2_gain, ln2_bias, w_gate, w_up, down_weight, cotangent,
):
    n = lax.axis_size("tensor")
    local_rows, depth = tokens.shape
    length = local_rows * n
    width = w_query.shape[1]
    row_ids = lax.axis_index("tensor") * local_rows + lax.iota(jnp.int32, local_rows)
    valid = (row_ids < lengths[0])[:, None]

    inputs = tokens.astype(F32)
    grad_out = jnp.where(valid, cotangent.astype(F32), 0.0)
    devices = lax.axis_size("dp")
    place = lax.axis_index("dp")
    share = w_gate.shape[1] // devices

    def piece(x, axis):
        return lax.dynamic_slice_in_dim(x, place * share, share, axis)

    weights = jnp.stack([piece(w_gate, 1).T, piece(w_up, 1).T, piece(down_weight, 0)])
    q, k, v, cosine, sine, attn_rows, grad_branch = begin(
        tokens, cotangent, ln1_gain, ln1_bias, w_query, w_key, w_value, angle_tables(length),
        lengths, n, devices,
    )
    attn_rows = attn_rows.reshape(length, depth)
    weights, q = lax.optimization_barrier((weights, q))
    weights = lax.all_gather(weights, "tensor", axis=1, tiled=True)
    context, logsum, context_own, _, w_out_all = att_fwd(
        q, k, v,
        lax.dynamic_slice_in_dim(w_out, place * (width // devices), width // devices, 0),
        n, devices,
    )
    w_out_all = w_out_all.reshape(n, width, depth)
    attn_out = sum(dot(context_own[t], w_out_all[t]).astype(BF).astype(F32) for t in range(n))
    middle = inputs + attn_out
    scaled2, inverse2 = norm_parts(middle)
    ffn_in = (scaled2 * ln2_gain + ln2_bias).astype(BF)
    w_packed, ffn_in = lax.optimization_barrier(
        (pack_weights(w_query, w_key, w_value), ffn_in)
    )
    w_packed = lax.all_gather(w_packed, "tensor", axis=0)
    grad_parts, out_parts, ffn_grads = ffn(ffn_in, grad_branch, weights, n, devices)
    grad_ffn_in = sum(grad_parts[p].astype(F32) for p in range(devices // 2))
    grad_norm2, gain2_grad, shift2_grad = norm_back(
        grad_ffn_in, scaled2, inverse2, ln2_gain
    )
    grad_middle = grad_out + grad_norm2
    grad_attn = grad_middle.astype(BF)
    ffn_grads = ffn_grads.reshape(n, 3 * share, depth)
    ffn_grads = lax.psum_scatter(ffn_grads, "tensor", scatter_dimension=0, tiled=True)[0]
    w_packed, grad_attn = lax.optimization_barrier((w_packed, grad_attn))
    packed, packed_own, out_sums, out_piece = att_bwd(
        grad_attn, w_out_all, context_own, out_parts, q, k, v, context, logsum, cosine, sine, n
    )
    ffn_grads, out_piece = lax.optimization_barrier((ffn_grads, out_piece))
    grads = lax.all_gather(jnp.concatenate([ffn_grads, out_piece]), "dp", axis=0)
    gate_grad, up_grad, down_grad, out_grad = unpack(grads, share, width)
    ffn_out = sum(x.astype(F32) for x in (out_parts[0], *out_sums))
    output = jnp.where(valid, middle + ffn_out, 0.0).astype(BF)
    input_grad, query_grad, key_grad, value_grad, sums = finish(
        attn_rows, packed, packed_own, w_packed, tokens, grad_middle, ln1_gain,
        jnp.stack([gain2_grad, shift2_grad]), width, devices,
    )
    gain1_grad, shift1_grad, gain2_grad, shift2_grad = (sums[i] for i in range(4))
    return (
        output, input_grad, gain1_grad, shift1_grad, query_grad, key_grad, value_grad, out_grad,
        gain2_grad, shift2_grad, gate_grad, up_grad, down_grad,
    )


def solution(mesh):
    rows = P(("dp", "tensor"), None)
    columns = P(None, "tensor")
    parts = P("tensor", None)
    return jax.shard_map(
        on_device,
        mesh=mesh,
        in_specs=(
            rows, P("dp"), P(), P(), columns, columns, columns, parts,
            P(), P(), columns, columns, parts, rows,
        ),
        out_specs=(
            rows, rows, P(), P(), columns, columns, columns, parts,
            P(), P(), columns, columns, parts,
        ),
        check_vma=False,
    )
```

```python
import functools
import math

import jax
import jax.numpy as jnp
from jax import lax
from jax.experimental import pallas as pl
from jax.experimental.pallas import tpu as pltpu
from jax.sharding import PartitionSpec as P

HD = 64
EPS = 1e-05
SCALE = 1.0 / math.sqrt(HD)
F32 = jnp.float32
BF = jnp.bfloat16
NT = (((1,), (1,)), ((), ()))
NN = (((1,), (0,)), ((), ()))
TN = (((0,), (0,)), ((), ()))
MESH = pl.DeviceIdType.MESH


def dot(a, b, dims=NN):
    return lax.dot_general(a, b, dims, preferred_element_type=F32)


def lanes(shape):
    return lax.broadcasted_iota(jnp.int32, shape, 1)


def split3(x):
    hi = x.astype(BF).astype(F32)
    mid = (x - hi).astype(BF).astype(F32)
    return hi, mid, x - hi - mid


def partner(x):
    width = x.shape[1]
    first = lanes(x.shape) % HD < HD // 2
    return jnp.where(first, pltpu.roll(x, width - HD // 2, 1), pltpu.roll(x, HD // 2, 1))


STEP = 64


def angle_tables(length):
    half = HD // 2
    lane = lax.optimization_barrier(lax.iota(jnp.int32, 2 * HD))
    freqs = 10000.0 ** (-((lane % half).astype(F32) * 2.0 / HD))
    sign = jnp.where(lane % HD < half, -1.0, 1.0)

    def table(positions):
        angles = positions[:, None] * freqs[None, :]
        return jnp.stack([jnp.cos(angles), jnp.sin(angles)])

    return table(lax.iota(F32, length // STEP) * STEP), table(lax.iota(F32, STEP)), sign[None, :]


def differ(a, b, bits):
    return sum(lax.rem(a // (1 << k) + b // (1 << k), 2) * (1 << k) for k in range(bits))


def remote(src, dst, send, recv, **to):
    return pltpu.make_async_remote_copy(
        src_ref=src, dst_ref=dst, send_sem=send, recv_sem=recv, device_id=to, device_id_type=MESH
    )


def ring(n, step):
    return lax.rem(lax.axis_index("tensor") + step, n)


def same_core(s, chips):
    me = lax.axis_index("dp")
    return differ(me // 2, s, chips.bit_length() - 1) * 2 + lax.rem(me, 2)


def sibling():
    me = lax.axis_index("dp")
    return me + 1 - 2 * lax.rem(me, 2)


def greet(n, chips, both_cores=False):
    barrier = pltpu.get_barrier_semaphore()
    if both_cores:
        pl.semaphore_signal(barrier, inc=1, device_id={"dp": sibling()}, device_id_type=MESH)
    for step in range(1, n):
        pl.semaphore_signal(barrier, inc=1, device_id={"tensor": ring(n, step)}, device_id_type=MESH)
    for s in range(1, chips):
        pl.semaphore_signal(
            barrier, inc=1, device_id={"dp": same_core(s, chips)}, device_id_type=MESH
        )
    pl.semaphore_wait(barrier, n + chips - 2 + both_cores)


def begin_kernel(
    n, chips, chunks, limit_ref, tokens_ref, ct_ref, gain_ref, shift_ref, wq_ref, wk_ref, wv_ref,
    coarse_ref, fine_ref, sign_ref,
    q_ref, k_ref, v_ref, cos_ref, sin_ref, rows_ref, gb_all, landed, gb,
    right_send, right_recv, left_send, left_recv, gs_send, gs_recv, gr_send, gr_recv, keep_sem, rows_sem,
):
    me = lax.axis_index("tensor")
    place = lax.axis_index("dp")
    core = lax.rem(place, 2)
    bits = chips.bit_length() - 1
    rows, depth = tokens_ref.shape
    heads = q_ref.shape[0]
    piece = rows // chunks
    limit = limit_ref[0]

    def over(shard, d, c, send, recv, to):
        part = landed.at[shard, pl.ds(c * piece, piece)]
        return remote(part, part, send.at[d, c], recv.at[d, c], tensor=to)

    def rightward(d, c):
        return over(me - d, d, c, right_send, right_recv, me + 1)

    def leftward(d, c):
        return over(me + d, d, c, left_send, left_recv, me - 1)

    def from_left(d, c):
        return over(me - d, d - 1, c, right_send, right_recv, me - 1)

    def from_right(d, c):
        return over(me + d, d - 1, c, left_send, left_recv, me + 1)

    def spread_gb(c):
        return remote(
            gb, gb_all.at[place // 2, core], gs_send.at[c], gs_recv.at[c], dp=same_core(c, chips)
        )

    def relay_gb(c):
        there = gb_all.at[differ(place // 2, c, bits), core]
        return remote(there if c else gb, there, gr_send.at[c], gr_recv.at[c], dp=sibling())

    barrier = pltpu.get_barrier_semaphore()
    pl.semaphore_signal(barrier, inc=1, device_id={"dp": sibling()}, device_id_type=MESH)
    for s in range(1, chips):
        to = same_core(s, chips)
        pl.semaphore_signal(barrier, inc=1, device_id={"dp": to}, device_id_type=MESH)

    @pl.when(me > 0)
    def _():
        pl.semaphore_signal(barrier, inc=1, device_id={"tensor": me - 1}, device_id_type=MESH)

    @pl.when(me < n - 1)
    def _():
        pl.semaphore_signal(barrier, inc=1, device_id={"tensor": me + 1}, device_id_type=MESH)

    values = tokens_ref[...].astype(F32)
    values = values - jnp.mean(values, axis=1, keepdims=True)
    inverse = lax.rsqrt(jnp.mean(values * values, axis=1, keepdims=True) + EPS)
    landed[me] = (values * inverse * gain_ref[...] + shift_ref[...]).astype(BF)

    pl.semaphore_wait(barrier, chips + jnp.minimum(me, 1) + jnp.minimum(n - 1 - me, 1))

    for c in range(chunks):

        @pl.when(me < n - 1)
        def _():
            rightward(0, c).start()

        @pl.when(me > 0)
        def _():
            leftward(0, c).start()

    row = me * rows + lax.broadcasted_iota(jnp.int32, (rows, depth), 0)
    gb[...] = jnp.where(row < limit, ct_ref[...].astype(F32), 0.0).astype(BF)
    for s in range(1, chips):
        spread_gb(s).start()
    relay_gb(0).start()
    keep = pltpu.make_async_copy(gb, gb_all.at[place // 2, core], keep_sem)
    keep.start()

    lane = lanes((rows, 128))
    ones = jnp.where(lane < HD + 3, 1.0, 0.0)
    unit = jnp.where(lane == HD + 3, 1.0, 0.0)

    def put(out_ref, here, values, extra):
        for h in range(heads):
            own = values[:, h // 2 * 128 : h // 2 * 128 + 128]
            own = pltpu.roll(own, HD, 1) if h % 2 else own
            out_ref[h, here, :] = jnp.where(lane < HD, own, extra).astype(BF)

    def project(shard):
        here = pl.ds(pl.multiple_of(shard * rows, rows), rows)
        for i in range(rows // STEP):
            part = pl.ds(pl.multiple_of(shard * rows + i * STEP, STEP), STEP)
            coarse = pl.ds(shard * (rows // STEP) + i, 1)
            c0, s0 = coarse_ref[0, coarse, :], coarse_ref[1, coarse, :]
            cos_ref[part, :] = c0 * fine_ref[0] - s0 * fine_ref[1]
            sin_ref[part, :] = (s0 * fine_ref[0] + c0 * fine_ref[1]) * sign_ref[...]
        cosine = jnp.tile(cos_ref[here, :], (1, heads // 2))
        sine = jnp.tile(sin_ref[here, :], (1, heads // 2))
        x = landed[shard]
        row = shard * rows + lax.broadcasted_iota(jnp.int32, (rows, 128), 0)
        bias = jnp.where(lane == HD + 3, jnp.where(row < limit, 0.0, -1e30), ones)
        raw = dot(x, wq_ref[...])
        turned = (raw * cosine + partner(raw) * sine).astype(BF).astype(F32)
        put(q_ref, here, turned * SCALE, unit)
        raw = dot(x, wk_ref[...])
        put(k_ref, here, raw * cosine + partner(raw) * sine, bias)
        put(v_ref, here, dot(x, wv_ref[...]), ones)

    def save(shard):
        return pltpu.make_async_copy(landed.at[shard], rows_ref.at[shard], rows_sem.at[shard])

    for d in range(1, n + 1):
        for c in range(chunks):
            if d < n:

                @pl.when(me >= d)
                def _():
                    from_left(d, c).wait_recv()

                @pl.when((me >= d) & (me < n - 1))
                def _():
                    rightward(d, c).start()

                @pl.when(me + d < n)
                def _():
                    from_right(d, c).wait_recv()

                @pl.when((me + d < n) & (me > 0))
                def _():
                    leftward(d, c).start()

            if c == 0:

                @pl.when(me >= d - 1)
                def _():
                    save(me - d + 1).start()
                    project(me - d + 1)

            if c == 1 and d > 1:

                @pl.when(me + d - 1 < n)
                def _():
                    save(me + d - 1).start()
                    project(me + d - 1)

            if c == chunks - 1 and d == 2:
                for s in range(1, chips // 2 + 1):
                    spread_gb(s).wait_recv()
                    relay_gb(s).start()

            if c == 0 and d == n:
                for s in range(chips // 2 + 1, chips):
                    spread_gb(s).wait_recv()
                    relay_gb(s).start()

    for d in range(n - 1):
        for c in range(chunks):

            @pl.when((me >= d) & (me < n - 1))
            def _():
                rightward(d, c).wait_send()

            @pl.when((me + d < n) & (me > 0))
            def _():
                leftward(d, c).wait_send()

    for s in range(chips):
        relay_gb(s).wait()
        if s:
            spread_gb(s).wait_send()
    keep.wait()
    for shard in range(n):
        save(shard).wait()


def begin(tokens, cotangent, gain, shift, w_query, w_key, w_value, tables, limit, n, devices):
    rows, depth = tokens.shape
    total = n * rows
    heads = w_query.shape[1] // HD
    chips = devices // 2
    chunks = 4
    vmem = pl.BlockSpec(memory_space=pltpu.VMEM)
    hbm = pl.BlockSpec(memory_space=pl.ANY)
    return pl.pallas_call(
        functools.partial(begin_kernel, n, chips, chunks),
        out_shape=(jax.ShapeDtypeStruct((heads, total, 128), BF),) * 3
        + (jax.ShapeDtypeStruct((total, 128), F32),) * 2
        + (
            jax.ShapeDtypeStruct((n, rows, depth), BF),
            jax.ShapeDtypeStruct((chips, 2, rows, depth), BF),
        ),
        in_specs=[pl.BlockSpec(memory_space=pltpu.SMEM)] + [vmem] * 10,
        out_specs=[vmem] * 5 + [hbm] * 2,
        scratch_shapes=[pltpu.VMEM((n, rows, depth), BF), pltpu.VMEM((rows, depth), BF)]
        + [pltpu.SemaphoreType.DMA((n - 1, chunks))] * 4
        + [pltpu.SemaphoreType.DMA((chips,))] * 4
        + [pltpu.SemaphoreType.DMA, pltpu.SemaphoreType.DMA((n,))],
        compiler_params=pltpu.CompilerParams(
            vmem_limit_bytes=44 << 20, collective_id=5, has_side_effects=True
        ),
        cost_estimate=pl.CostEstimate(
            flops=6 * total * depth * heads * HD * 10, bytes_accessed=30 << 20, transcendentals=0
        ),
        name="begin",
    )(
        limit, tokens, cotangent, gain.reshape(1, depth), shift.reshape(1, depth),
        w_query, w_key, w_value, *tables,
    )


def att_fwd_kernel(
    n, chips, q_ref, k_ref, v_ref, wo_ref,
    ctx_ref, lse_ref, out_ref, wo_z, wo_all, send_sem, recv_sem, own_sem,
    wz_send, wz_recv, ws_send, ws_recv, wr_send, wr_recv, keep_sem,
):
    s = pl.program_id(0)
    h = pl.program_id(1)
    heads = pl.num_programs(1)
    rows = q_ref.shape[1] // n
    me = lax.axis_index("tensor")
    place = lax.axis_index("dp")
    core = lax.rem(place, 2)
    bits = chips.bit_length() - 1

    def wo_over(step):
        return remote(
            wo_ref, wo_z.at[me], wz_send.at[step], wz_recv.at[step], tensor=ring(n, step + 1)
        )

    def spread_wo(c):
        return remote(
            wo_z, wo_all.at[:, place], ws_send.at[c], ws_recv.at[c], dp=same_core(c, chips)
        )

    def relay_wo(c):
        there = wo_all.at[:, differ(place // 2, c, bits) * 2 + core]
        return remote(there if c else wo_z, there, wr_send.at[c], wr_recv.at[c], dp=sibling())

    keeps = [
        pltpu.make_async_copy(wo_ref, wo_z.at[me], keep_sem.at[0]),
        pltpu.make_async_copy(wo_z, wo_all.at[:, place], keep_sem.at[1]),
    ]

    @pl.when((s == 0) & (h == 0))
    def _():
        greet(n, chips, True)
        for step in range(n - 1):
            wo_over(step).start()
        keeps[0].start()

    @pl.when((s == 1) & (h == 0))
    def _():
        for step in range(n - 1):
            wo_over(step).wait()
        keeps[0].wait()
        for c in range(1, chips):
            spread_wo(c).start()
        relay_wo(0).start()
        keeps[1].start()

    @pl.when((s == n - 1) & (h == 0))
    def _():
        for c in range(1, chips):
            spread_wo(c).wait_recv()
            relay_wo(c).start()

    owner = ring(n, s + 1)
    block = pl.ds(pl.multiple_of(owner * rows, rows), rows)
    scores = dot(q_ref[h, block, :], k_ref[h], NT)
    peak = jnp.max(scores, axis=1, keepdims=True)
    acc = dot(jnp.exp(scores - peak).astype(BF), v_ref[h])
    lane = lanes((rows, 128))
    total = jnp.sum(jnp.where(lane == HD, acc, 0.0), axis=1, keepdims=True)
    out = acc * (1.0 / total)
    odd = lax.rem(h, 2)
    out = jnp.where(odd == 1, pltpu.roll(out, HD, 1), out).astype(BF)
    pair = pl.ds(pl.multiple_of(h // 2 * 128, 128), 128)
    ctx_ref[block, pair] = jnp.where((lane >= HD) == (odd == 1), out, ctx_ref[block, pair])
    lse_ref[block, :] = jnp.where(lane == h, peak + jnp.log(total), lse_ref[block, :])

    def push(step):
        return pltpu.make_async_remote_copy(
            src_ref=ctx_ref.at[block],
            dst_ref=out_ref.at[me],
            send_sem=send_sem.at[step],
            recv_sem=recv_sem.at[step],
            device_id={"tensor": owner},
            device_id_type=MESH,
        )

    @pl.when((h == heads - 1) & (s < n - 1))
    def _():
        push(s).start()

    @pl.when((h == heads - 1) & (s == n - 1))
    def _():
        keep = pltpu.make_async_copy(ctx_ref.at[block], out_ref.at[me], own_sem)
        keep.start()
        for step in range(n - 1):
            push(step).wait()
        keep.wait()
        keeps[1].wait()
        for c in range(chips):
            relay_wo(c).wait()
            if c:
                spread_wo(c).wait_send()


def att_fwd(q, k, v, w_out_piece, n, devices):
    heads, total, _ = q.shape
    width = heads * HD
    rows = total // n
    share, depth = w_out_piece.shape
    chips = devices // 2
    hbm = pl.BlockSpec(memory_space=pl.ANY)

    def whole(*shape):
        return pl.BlockSpec(shape, lambda *_: (0,) * len(shape), pipeline_mode=pl.Buffered(1))

    return pl.pallas_call(
        functools.partial(att_fwd_kernel, n, chips),
        out_shape=(
            jax.ShapeDtypeStruct((total, width), BF),
            jax.ShapeDtypeStruct((total, 128), F32),
            jax.ShapeDtypeStruct((n, rows, width), BF),
            jax.ShapeDtypeStruct((n, share, depth), BF),
            jax.ShapeDtypeStruct((n, devices, share, depth), BF),
        ),
        grid_spec=pltpu.PrefetchScalarGridSpec(
            num_scalar_prefetch=0,
            grid=(n, heads),
            in_specs=[whole(heads, total, 128)] * 3 + [hbm],
            out_specs=[whole(total, width), whole(total, 128)] + [hbm] * 3,
            scratch_shapes=[pltpu.SemaphoreType.DMA((n - 1,))] * 2
            + [pltpu.SemaphoreType.DMA]
            + [pltpu.SemaphoreType.DMA((n - 1,))] * 2
            + [pltpu.SemaphoreType.DMA((chips,))] * 4
            + [pltpu.SemaphoreType.DMA((2,))],
        ),
        compiler_params=pltpu.CompilerParams(
            vmem_limit_bytes=40 << 20, collective_id=1, has_side_effects=True
        ),
        cost_estimate=pl.CostEstimate(
            flops=4 * total * total * 256 * heads,
            bytes_accessed=10 * total * width,
            transcendentals=total * total * heads,
        ),
        name="att_fwd",
    )(q, k, v, w_out_piece)


def att_bwd_kernel(
    n, bk, chips, ga_ref, wo_ref, cown_ref, parts_ref, q_ref, k_ref, v_ref, ctx_ref, lse_ref,
    cos_ref, sin_ref, pk_ref, own_ref, sums_ref, og_ref, do, gc, dka, dva, dqs,
    og_full, og_own, og_mate, og_sib, og_land, og_piece, og_z,
    send_sem, recv_sem, out_send, out_recv, pk_send, pk_recv, keep_sem,
    om_send, om_recv, op_send, op_recv, oz_send, oz_recv,
):
    i = pl.program_id(0)
    heads, total, _ = k_ref.shape
    h = jnp.where(i < heads, i, (i - heads) // (n - 1))
    t = jnp.where(i < heads, 0, lax.rem(i - heads, n - 1) + 1)
    rows = total // n
    me = lax.axis_index("tensor")
    place = lax.axis_index("dp")
    core = lax.rem(place, 2)
    bits = chips.bit_length() - 1
    share = og_ref.shape[0]
    mine = pl.ds(pl.multiple_of(me * rows, rows), rows)

    def push(step):
        return remote(
            gc.at[step], do.at[mine], send_sem.at[step], recv_sem.at[step], tensor=ring(n, step + 1)
        )

    def push_out(s):
        return remote(
            parts_ref.at[s], sums_ref.at[s - 1], out_send.at[s - 1], out_recv.at[s - 1],
            dp=same_core(s, chips),
        )

    def columns(slot):
        return pl.ds(pl.multiple_of(slot * 128, 128), 128)

    def push_pack(slot, step):
        owner = ring(n, step + 1)
        return remote(
            pk_ref.at[pl.ds(pl.multiple_of(owner * rows, rows), rows), columns(slot)],
            own_ref.at[me, :, columns(slot)],
            pk_send.at[slot, step], pk_recv.at[slot, step], tensor=owner,
        )

    def keep(slot):
        return pltpu.make_async_copy(
            pk_ref.at[mine, columns(slot)], own_ref.at[me, :, columns(slot)], keep_sem.at[slot]
        )

    @pl.when(i == 0)
    def _():
        greet(n, chips, True)
        for s in range(1, chips):
            push_out(s).start()

        def send(step, carry):
            gc[step] = dot(ga_ref[...], wo_ref[ring(n, step + 1)], NT).astype(BF)
            push(step).start()
            return carry

        lax.fori_loop(0, n - 1, send, 0)
        do[mine, :] = dot(ga_ref[...], wo_ref[me], NT).astype(BF)

    def og_swap():
        return remote(og_mate, og_sib, om_send, om_recv, dp=sibling())

    def og_push(s):
        return remote(og_sib.at[s], og_land.at[s], op_send.at[s], op_recv.at[s], dp=same_core(s, chips))

    def og_over(step):
        to = ring(n, step + 1)
        return remote(og_piece.at[to], og_z.at[me], oz_send.at[step], oz_recv.at[step], tensor=to)

    @pl.when(i == 1)
    def _():
        def term(part, carry):
            og_full[...] = dot(cown_ref[part], ga_ref[...], TN)
            for s in range(chips):
                start = differ(place // 2, s, bits) * 2
                here = pl.ds(pl.multiple_of((start + core) * share, share), share)
                there = pl.ds(pl.multiple_of((start + 1 - core) * share, share), share)
                og_own[s, part] = og_full[here, :]
                og_mate[s, part] = og_full[there, :].astype(BF)
            return carry

        lax.fori_loop(0, n, term, 0)
        og_swap().start()

    @pl.when(i == 2)
    def _():
        og_swap().wait_recv()
        for s in range(chips):
            og_sib[s] = (og_own[s] + og_sib[s].astype(F32)).astype(BF)
            if s:
                og_push(s).start()

    @pl.when(i == heads + 2)
    def _():
        joined = og_sib[0].astype(F32)
        for s in range(1, chips):
            og_push(s).wait_recv()
            joined = joined + og_land[s].astype(F32)
        og_piece[...] = joined.astype(BF)
        for step in range(n - 1):
            og_over(step).start()

    @pl.when(i == heads * n - 1)
    def _():
        og_z[me] = og_piece[me]
        for step in range(n - 1):
            og_over(step).wait_recv()
        joined = og_z[0].astype(F32)
        for part in range(1, n):
            joined = joined + og_z[part].astype(F32)
        og_ref[...] = joined.astype(BF)

    @pl.when((h == 0) & (t > 0))
    def _():
        push(t - 1).wait_recv()

    source = ring(n, n - t)
    block = pl.ds(pl.multiple_of(source * rows, rows), rows)
    pair = columns(h // 2)
    odd = lax.rem(h, 2) == 1
    lane = lanes((rows, 128))
    off = lane - HD
    logsum = jnp.sum(jnp.where(lane == h, lse_ref[block, :], 0.0), axis=1, keepdims=True)
    a, b, c = split3(-logsum)
    q = q_ref[h, block, :].astype(F32)
    q = jnp.where(off == 0, a, jnp.where(off == 1, b, jnp.where(off == 2, c, q))).astype(BF)
    g = jnp.where((lane >= HD) == odd, do[block, pair].astype(F32), 0.0)
    delta = jnp.sum(g * ctx_ref[block, pair].astype(F32), axis=1, keepdims=True)
    a, b, c = split3(-delta)
    g = jnp.where(odd, pltpu.roll(g, HD, 1), g)
    g = jnp.where(off == 0, a, jnp.where(off == 1, b, jnp.where(off == 2, c, g))).astype(BF)
    acc = jnp.zeros((rows, 128), F32)
    for j in range(total // bk):
        rk = pl.ds(j * bk, bk)
        kt = k_ref[h, rk, :]
        probs = jnp.exp(dot(kt, q, NT))
        grad = (probs * dot(v_ref[h, rk, :], g, NT)).astype(BF)
        for sums, term in ((dva, dot(probs.astype(BF), g)), (dka, dot(grad, q))):
            before = jnp.where(t == 0, jnp.zeros_like(term), sums[h, rk, :])
            sums[h, rk, :] = before + term
        acc = acc + dot(grad, kt, TN)
    acc = acc * SCALE

    @pl.when(jnp.logical_not(odd))
    def _():
        dqs[block, :] = acc

    @pl.when(odd)
    def _():
        grad = jnp.where(lane < HD, dqs[block, :], pltpu.roll(acc, HD, 1))
        grad = grad * cos_ref[block, :] - partner(grad) * sin_ref[block, :]
        pk_ref[block, columns(heads + h // 2)] = grad.astype(BF)

    @pl.when(odd & (t == 0))
    def _():
        keep(heads + h // 2).start()

    @pl.when(odd & (t > 0))
    def _():
        push_pack(heads + h // 2, n - 1 - t).start()

    @pl.when(t == n - 1)
    def _():
        dk = dka[h]
        dk = dk * cos_ref[...] - partner(dk) * sin_ref[...]
        both = jnp.where(lanes((total, 128)) < HD, dk, pltpu.roll(dva[h], HD, 1))
        pk_ref[:, columns(h)] = both.astype(BF)
        for step in range(n - 1):
            push_pack(h, step).start()
        keep(h).start()

    @pl.when(i == heads * n - 1)
    def _():
        for step in range(n - 1):
            push(step).wait_send()
        for s in range(1, chips):
            push_out(s).wait()
        og_swap().wait_send()
        for s in range(1, chips):
            og_push(s).wait_send()
        for step in range(n - 1):
            og_over(step).wait_send()
        for slot in range(heads + heads // 2):
            keep(slot).wait()
            for step in range(n - 1):
                push_pack(slot, step).wait()


def att_bwd(grad_attn, w_out, ctx_own, parts, q, k, v, ctx, lse, cosine, sine, n, bk=512):
    heads, total, _ = q.shape
    width = heads * HD
    rows, depth = grad_attn.shape
    chips = parts.shape[0]
    share = width // (2 * chips)
    slots = heads + heads // 2
    hbm = pl.BlockSpec(memory_space=pl.ANY)

    def whole(*shape):
        return pl.BlockSpec(shape, lambda *_: (0,) * len(shape), pipeline_mode=pl.Buffered(1))

    return pl.pallas_call(
        functools.partial(att_bwd_kernel, n, bk, chips),
        out_shape=(
            jax.ShapeDtypeStruct((total, slots * 128), BF),
            jax.ShapeDtypeStruct((n, rows, slots * 128), BF),
            jax.ShapeDtypeStruct((chips - 1, rows, depth), BF),
            jax.ShapeDtypeStruct((share, depth), BF),
        ),
        grid_spec=pltpu.PrefetchScalarGridSpec(
            num_scalar_prefetch=0,
            grid=(heads * n,),
            in_specs=[whole(rows, depth), whole(n, width, depth), whole(n, rows, width), hbm]
            + [whole(heads, total, 128)] * 3
            + [whole(total, width)]
            + [whole(total, 128)] * 3,
            out_specs=[whole(total, slots * 128), hbm, hbm, whole(share, depth)],
            scratch_shapes=[
                pltpu.VMEM((total, width), BF),
                pltpu.VMEM((n - 1, rows, width), BF),
            ]
            + [pltpu.VMEM((heads, total, 128), F32)] * 2
            + [pltpu.VMEM((total, 128), F32)]
            + [
                pltpu.VMEM((width, depth), F32),
                pltpu.VMEM((chips, n, share, depth), F32),
                pltpu.VMEM((chips, n, share, depth), BF),
                pltpu.VMEM((chips, n, share, depth), BF),
                pltpu.VMEM((chips, n, share, depth), BF),
                pltpu.VMEM((n, share, depth), BF),
                pltpu.VMEM((n, share, depth), BF),
            ]
            + [pltpu.SemaphoreType.DMA((n - 1,))] * 2
            + [pltpu.SemaphoreType.DMA((chips - 1,))] * 2
            + [pltpu.SemaphoreType.DMA((slots, n - 1))] * 2
            + [pltpu.SemaphoreType.DMA((slots,))]
            + [pltpu.SemaphoreType.DMA] * 2
            + [pltpu.SemaphoreType.DMA((chips,))] * 2
            + [pltpu.SemaphoreType.DMA((n - 1,))] * 2,
        ),
        compiler_params=pltpu.CompilerParams(
            vmem_limit_bytes=56 << 20, collective_id=2, has_side_effects=True
        ),
        cost_estimate=pl.CostEstimate(
            flops=10 * total * total * 256 * heads,
            bytes_accessed=20 * total * width,
            transcendentals=total * total * heads,
        ),
        name="att_bwd",
    )(grad_attn, w_out, ctx_own, parts, q, k, v, ctx, lse, cosine, sine)


def finish_kernel(
    chips, n, width, x_ref, pk_ref, own_ref, w_ref, tokens_ref, middle_ref, gain_ref, vec_ref,
    input_ref, q_ref, k_ref, v_ref, sums_ref,
    full, mate, sib, land, fin, every, vec_z, vec_dp, vec_me,
    sx_send, sx_recv, rs_send, rs_recv, ag_send, ag_recv, rl_send, rl_recv,
    vz_send, vz_recv, vd_send, vd_recv, own_sem,
):
    bits = chips.bit_length() - 1
    me = lax.axis_index("dp")
    place = lax.axis_index("tensor")
    core = lax.rem(me, 2)
    chip = me // 2
    other = 1 - core
    heads = width // HD
    piece = fin.shape[0]

    def swap(s):
        return remote(mate.at[s], sib.at[s], sx_send.at[s], sx_recv.at[s], dp=chip * 2 + other)

    def push(s):
        return remote(sib.at[s], land.at[s], rs_send.at[s], rs_recv.at[s], dp=same_core(s, chips))

    def spread(s):
        return remote(
            fin, every.at[chip, core], ag_send.at[s], ag_recv.at[s], dp=same_core(s, chips)
        )

    def relay(s):
        src = every.at[differ(chip, s, bits), core]
        return remote(src, src, rl_send.at[s], rl_recv.at[s], dp=chip * 2 + other)

    def vec_over(step):
        return remote(
            vec_me.at[0], vec_z.at[place], vz_send.at[step], vz_recv.at[step], tensor=ring(n, step + 1)
        )

    def vec_across(step):
        return remote(
            vec_me.at[1], vec_dp.at[me], vd_send.at[step], vd_recv.at[step],
            dp=lax.rem(me + step + 1, 2 * chips),
        )

    barrier = pltpu.get_barrier_semaphore()
    for step in range(n - 1):
        pl.semaphore_signal(barrier, inc=1, device_id={"tensor": ring(n, step + 1)}, device_id_type=MESH)
    for step in range(2 * chips - 1):
        to = lax.rem(me + step + 1, 2 * chips)
        pl.semaphore_signal(barrier, inc=1, device_id={"dp": to}, device_id_type=MESH)

    full[...] = dot(x_ref[...], pk_ref[...], TN)
    pl.semaphore_wait(barrier, n + 2 * chips - 2)

    def part(s, which):
        start = (differ(chip, s, bits) * 2 + which) * piece
        return full[pl.ds(pl.multiple_of(start, piece), piece), :]

    for s in range(chips):
        mate[s] = part(s, other).astype(BF)
        swap(s).start()

    grad = jnp.zeros(input_ref.shape, F32)
    for t in range(n):
        w = w_ref[:, t].reshape(w_ref.shape[0] * w_ref.shape[2], w_ref.shape[3])
        grad = grad + dot(own_ref[t], w, NT).astype(BF).astype(F32)

    for s in range(1, chips):
        swap(s).wait_recv()
        sib[s] = (sib[s].astype(F32) + part(s, core)).astype(BF)
        push(s).start()
    swap(0).wait_recv()
    total = sib[0].astype(F32) + part(0, core)

    values = tokens_ref[...].astype(F32)
    values = values - jnp.mean(values, axis=1, keepdims=True)
    inverse = lax.rsqrt(jnp.mean(values * values, axis=1, keepdims=True) + EPS)
    scaled = values * inverse
    through = grad * gain_ref[...]
    inner = through - jnp.mean(through, axis=1, keepdims=True)
    inner = inner - scaled * jnp.mean(through * scaled, axis=1, keepdims=True)
    input_ref[...] = middle_ref[...] + inverse * inner
    vec_me[0, 0:1] = jnp.sum(grad * scaled, axis=0, keepdims=True)
    vec_me[0, 1:2] = jnp.sum(grad, axis=0, keepdims=True)
    vec_me[0, 2:4] = vec_ref[...]
    vec_me[0, 4:8] = jnp.zeros((4, vec_ref.shape[1]), F32)
    vec_z[place] = vec_me[0]
    for step in range(n - 1):
        vec_over(step).start()

    for s in range(1, chips):
        push(s).wait_recv()
        total = total + land[s].astype(F32)
    fin[...] = total.astype(BF)
    for s in range(1, chips):
        spread(s).start()
    mine = pltpu.make_async_copy(fin, every.at[chip, core], own_sem)
    mine.start()
    mine.wait()
    relay(0).start()

    for step in range(n - 1):
        vec_over(step).wait()
    vec = vec_z[0]
    for t in range(1, n):
        vec = vec + vec_z[t]
    vec_me[1] = vec
    vec_dp[me] = vec
    for step in range(2 * chips - 1):
        vec_across(step).start()
    for s in range(1, chips):
        spread(s).wait_recv()
        relay(s).start()
    for step in range(2 * chips - 1):
        vec_across(step).wait()
    vec = vec_dp[0]
    for t in range(1, 2 * chips):
        vec = vec + vec_dp[t]
    sums_ref[...] = vec
    for s in range(chips):
        relay(s).wait()
        swap(s).wait_send()
        if s > 0:
            spread(s).wait_send()
            push(s).wait_send()
    first = lanes((piece, 128)) < HD
    for d in range(2 * chips):
        rows = slice(d * piece, (d + 1) * piece)
        g = every[d // 2, d % 2].astype(F32)
        for pair in range(heads // 2):
            a = g[:, pair * 256 : pair * 256 + 128]
            b = g[:, pair * 256 + 128 : pair * 256 + 256]
            out = slice(pair * 128, pair * 128 + 128)
            q_ref[rows, out] = g[:, (heads + pair) * 128 : (heads + pair + 1) * 128]
            k_ref[rows, out] = jnp.where(first, a, pltpu.roll(b, HD, 1))
            v_ref[rows, out] = jnp.where(first, pltpu.roll(a, HD, 1), b)


def finish(rows_all, packed, own, w_all, tokens, middle, gain, vec, width, devices):
    n, rows, packs = own.shape
    depth = tokens.shape[1]
    chips = devices // 2
    piece = depth // devices
    vmem = pl.BlockSpec(memory_space=pltpu.VMEM)
    out = jax.ShapeDtypeStruct((depth, width), F32)
    return pl.pallas_call(
        functools.partial(finish_kernel, chips, n, width),
        out_shape=(
            jax.ShapeDtypeStruct((rows, depth), F32), out, out, out,
            jax.ShapeDtypeStruct((8, depth), F32),
        ),
        in_specs=[vmem] * 8,
        out_specs=[vmem] * 5,
        scratch_shapes=[
            pltpu.VMEM((depth, packs), F32),
            pltpu.VMEM((chips, piece, packs), BF),
            pltpu.VMEM((chips, piece, packs), BF),
            pltpu.VMEM((chips, piece, packs), BF),
            pltpu.VMEM((piece, packs), BF),
            pltpu.VMEM((chips, 2, piece, packs), BF),
            pltpu.VMEM((n, 8, depth), F32),
            pltpu.VMEM((devices, 8, depth), F32),
            pltpu.VMEM((2, 8, depth), F32),
        ]
        + [pltpu.SemaphoreType.DMA((chips,))] * 8
        + [pltpu.SemaphoreType.DMA((n - 1,))] * 2
        + [pltpu.SemaphoreType.DMA((devices - 1,))] * 2
        + [pltpu.SemaphoreType.DMA],
        compiler_params=pltpu.CompilerParams(
            vmem_limit_bytes=56 << 20, collective_id=4, has_side_effects=True
        ),
        cost_estimate=pl.CostEstimate(
            flops=4 * n * rows * depth * packs, bytes_accessed=20 << 20, transcendentals=0
        ),
        name="finish",
    )(rows_all, packed, own, w_all, tokens, middle, gain.reshape(1, depth), vec)


def ffn_kernel(
    chips, x_ref, gb_ref, w_ref, dx_ref, out_ref, dw_ref,
    rows_all, gb, hid, gate_g, up_g, own, sib, mate, acc,
    ag_send, ag_recv, rl_send, rl_recv, sx_send, sx_recv, rs_send, rs_recv, fw_send, fw_recv,
    gb_sem, out_sem, dx_sem,
):
    bits = chips.bit_length() - 1
    me = lax.axis_index("dp")
    core = lax.rem(me, 2)
    chip = me // 2
    other = 1 - core
    rows, depth = x_ref.shape
    n = dw_ref.shape[0]
    share = dw_ref.shape[2]

    def spread(s):
        to = differ(chip, s, bits) * 2 + core
        return remote(x_ref, rows_all.at[chip, core], ag_send.at[s], ag_recv.at[s], dp=to)

    square = chips == 4

    def hand_on(s):
        half = pl.ds((s - 1) * (rows // 2), rows // 2)
        part = rows_all.at[differ(chip, s, bits), core, half]
        to = differ(chip, 3 - s, bits) * 2 + core
        return remote(part, part, fw_send.at[s], fw_recv.at[s], dp=to)

    def handed(s):
        half = pl.ds((s - 1) * (rows // 2), rows // 2)
        part = rows_all.at[differ(chip, 3, bits), core, half]
        to = differ(chip, 3 - s, bits) * 2 + core
        return remote(part, part, fw_send.at[s], fw_recv.at[s], dp=to)

    def relay(s):
        src = differ(chip, s, bits)
        return remote(
            rows_all.at[src, core], rows_all.at[src, core], rl_send.at[s], rl_recv.at[s],
            dp=chip * 2 + other,
        )

    def swap(s):
        return remote(
            mate.at[lax.rem(s, 2)], sib.at[s], sx_send.at[s], sx_recv.at[s], dp=chip * 2 + other
        )

    def push(s):
        to = differ(chip, s, bits) * 2 + core
        return remote(sib.at[s, 0], dx_ref.at[s], rs_send.at[s], rs_recv.at[s], dp=to)

    def fetch(s):
        slot = lax.rem(s, 2)
        return pltpu.make_async_copy(
            gb_ref.at[differ(chip, s, bits)], gb.at[slot], gb_sem.at[slot]
        )

    def keep(s):
        return pltpu.make_async_copy(sib.at[s, 1], out_ref.at[s], out_sem.at[s])

    fetch(0).start()
    barrier = pltpu.get_barrier_semaphore()
    pl.semaphore_signal(barrier, inc=1, device_id={"dp": chip * 2 + other}, device_id_type=MESH)
    for s in range(1, chips):
        to = differ(chip, s, bits) * 2 + core
        pl.semaphore_signal(barrier, inc=1, device_id={"dp": to}, device_id_type=MESH)
    pl.semaphore_wait(barrier, chips)
    direct = range(1, 3) if square else range(1, chips)
    for s in direct:
        spread(s).start()
    mine = pltpu.make_async_copy(x_ref, rows_all.at[chip, core], ag_send.at[0])
    mine.start()
    mine.wait()
    relay(0).start()
    acc[...] = jnp.zeros_like(acc)

    def shard(src, slot, which, put):
        x = rows_all[src, which]
        grad = gb[slot, which]
        gate = dot(x, w_ref[0], NT)
        upper = dot(x, w_ref[1], NT)
        grad_hidden = dot(grad, w_ref[2], NT)
        sigma = jax.nn.sigmoid(gate)
        act = gate * sigma
        part = pl.ds(pl.multiple_of(which * rows, rows), rows)
        hidden = (act * upper).astype(BF)
        grad_gate = (grad_hidden * upper * sigma * (1.0 + gate * (1.0 - sigma))).astype(BF)
        grad_upper = (grad_hidden * act).astype(BF)
        hid[part, :] = hidden
        gate_g[part, :] = grad_gate
        up_g[part, :] = grad_upper
        put[0] = (dot(grad_gate, w_ref[0]) + dot(grad_upper, w_ref[1])).astype(BF)
        put[1] = dot(hidden, w_ref[2]).astype(BF)

    def step(s, carry):
        src = differ(chip, s, bits)
        slot = lax.rem(s, 2)
        relay(s).wait_recv()
        fetch(s).wait()

        @pl.when(s < chips - 1)
        def _():
            fetch(s + 1).start()

        @pl.when(s >= 2)
        def _():
            swap(s - 2).wait_send()

        shard(src, slot, other, mate.at[slot])
        swap(s).start()
        shard(src, slot, core, own)
        swap(s).wait_recv()
        for k in range(2):
            sib[s, k] = (sib[s, k].astype(F32) + own[k].astype(F32)).astype(BF)

        @pl.when(s > 0)
        def _():
            push(s).start()

        keep(s).start()

        if square:

            @pl.when(s == 0)
            def _():
                for near in (1, 2):
                    spread(near).wait_recv()
                    hand_on(near).start()
                    relay(near).start()

        else:

            @pl.when(s < chips - 1)
            def _():
                spread(s + 1).wait_recv()
                relay(s + 1).start()

        x = rows_all[src].reshape(2 * rows, depth)
        acc[0] += dot(gate_g[...], x, TN)
        acc[1] += dot(up_g[...], x, TN)
        acc[2] += dot(hid[...], gb[slot].reshape(2 * rows, depth), TN)

        if square:

            @pl.when(s == 1)
            def _():
                handed(1).wait_recv()
                handed(2).wait_recv()
                relay(3).start()

        return carry

    lax.fori_loop(0, chips, step, 0)
    first = pltpu.make_async_copy(sib.at[0, 0], dx_ref.at[0], dx_sem)
    first.start()
    for t in range(n):
        for k in range(3):
            dw_ref[t, k] = acc[k, t * share : (t + 1) * share, :].astype(BF)
    first.wait()
    for s in range(chips):
        keep(s).wait()
        relay(s).wait_send()
        if s >= chips - 2:
            swap(s).wait_send()
        if s in direct:
            spread(s).wait_send()
        if s > 0:
            push(s).wait()
    if square:
        hand_on(1).wait_send()
        hand_on(2).wait_send()


def ffn(x, grad_branch, weights, n, devices):
    rows, depth = x.shape
    chips = devices // 2
    hidden = weights.shape[1]
    share = hidden // n
    vmem = pl.BlockSpec(memory_space=pltpu.VMEM)
    hbm = pl.BlockSpec(memory_space=pl.ANY)
    return pl.pallas_call(
        functools.partial(ffn_kernel, chips),
        out_shape=(
            jax.ShapeDtypeStruct((chips, rows, depth), BF),
            jax.ShapeDtypeStruct((chips, rows, depth), BF),
            jax.ShapeDtypeStruct((n, 3, share, depth), BF),
        ),
        in_specs=[vmem, hbm, vmem],
        out_specs=[hbm, hbm, vmem],
        scratch_shapes=[
            pltpu.VMEM((chips, 2, rows, depth), BF),
            pltpu.VMEM((2, 2, rows, depth), BF),
        ]
        + [pltpu.VMEM((2 * rows, hidden), BF)] * 3
        + [
            pltpu.VMEM((2, rows, depth), BF),
            pltpu.VMEM((chips, 2, rows, depth), BF),
            pltpu.VMEM((2, 2, rows, depth), BF),
            pltpu.VMEM((3, hidden, depth), F32),
        ]
        + [pltpu.SemaphoreType.DMA((chips,))] * 8
        + [pltpu.SemaphoreType.DMA((3,))] * 2
        + [pltpu.SemaphoreType.DMA((2,)), pltpu.SemaphoreType.DMA((chips,)), pltpu.SemaphoreType.DMA],
        compiler_params=pltpu.CompilerParams(
            vmem_limit_bytes=60 << 20, collective_id=3, has_side_effects=True
        ),
        cost_estimate=pl.CostEstimate(
            flops=2 * 9 * devices * rows * depth * hidden, bytes_accessed=30 << 20, transcendentals=0
        ),
        name="ffn",
    )(x, grad_branch, weights)


def unpack_kernel(share, g_ref, gate_ref, up_ref, down_ref, out_ref):
    g = g_ref[0].astype(F32)
    gate_ref[...] = g[:share].T
    up_ref[...] = g[share : 2 * share].T
    down_ref[...] = g[2 * share : 3 * share]
    out_ref[...] = g[3 * share :]


def unpack(grads, share, width):
    devices, height, depth = grads.shape
    hidden = devices * share
    if share % 128:
        gate, up, down = (
            grads[:, k * share : (k + 1) * share].reshape(hidden, depth).astype(F32) for k in range(3)
        )
        return gate.T, up.T, down, grads[:, 3 * share :].reshape(width, depth).astype(F32)
    column = pl.BlockSpec((depth, share), lambda i: (0, i))
    return pl.pallas_call(
        functools.partial(unpack_kernel, share),
        out_shape=(
            jax.ShapeDtypeStruct((depth, hidden), F32),
            jax.ShapeDtypeStruct((depth, hidden), F32),
            jax.ShapeDtypeStruct((hidden, depth), F32),
            jax.ShapeDtypeStruct((width, depth), F32),
        ),
        grid=(devices,),
        in_specs=[pl.BlockSpec((1, height, depth), lambda i: (i, 0, 0))],
        out_specs=[
            column, column, pl.BlockSpec((share, depth), lambda i: (i, 0)),
            pl.BlockSpec((width // devices, depth), lambda i: (i, 0)),
        ],
        compiler_params=pltpu.CompilerParams(vmem_limit_bytes=40 << 20),
        name="unpack",
    )(grads)


def norm_parts(values):
    centre = jnp.mean(values, axis=-1, keepdims=True)
    centred = values - centre
    inverse = lax.rsqrt(jnp.mean(centred * centred, axis=-1, keepdims=True) + EPS)
    return centred * inverse, inverse


def norm_back(upstream, scaled, inverse, gain):
    through = upstream * gain
    inner = (
        through
        - jnp.mean(through, axis=-1, keepdims=True)
        - scaled * jnp.mean(through * scaled, axis=-1, keepdims=True)
    )
    return inverse * inner, jnp.sum(upstream * scaled, axis=0), jnp.sum(upstream, axis=0)


def pack_weights(w_query, w_key, w_value):
    depth, width = w_query.shape
    key, value = (w.reshape(depth, width // HD, 1, HD) for w in (w_key, w_value))
    both = jnp.concatenate([key, value], axis=2).reshape(depth, 2 * width)
    return jnp.concatenate([both, w_query], axis=1)


def on_device(
    tokens, lengths, ln1_gain, ln1_bias, w_query, w_key, w_value, w_out,
    ln2_gain, ln2_bias, w_gate, w_up, down_weight, cotangent,
):
    n = lax.axis_size("tensor")
    local_rows, depth = tokens.shape
    length = local_rows * n
    width = w_query.shape[1]
    row_ids = lax.axis_index("tensor") * local_rows + lax.iota(jnp.int32, local_rows)
    valid = (row_ids < lengths[0])[:, None]

    inputs = tokens.astype(F32)
    grad_out = jnp.where(valid, cotangent.astype(F32), 0.0)
    devices = lax.axis_size("dp")
    place = lax.axis_index("dp")
    share = w_gate.shape[1] // devices

    def piece(x, axis):
        return lax.dynamic_slice_in_dim(x, place * share, share, axis)

    weights = jnp.stack([piece(w_gate, 1).T, piece(w_up, 1).T, piece(down_weight, 0)])
    q, k, v, cosine, sine, attn_rows, grad_branch = begin(
        tokens, cotangent, ln1_gain, ln1_bias, w_query, w_key, w_value, angle_tables(length),
        lengths, n, devices,
    )
    attn_rows = attn_rows.reshape(length, depth)
    weights, q = lax.optimization_barrier((weights, q))
    weights = lax.all_gather(weights, "tensor", axis=1, tiled=True)

    def row_share(w):
        return lax.dynamic_slice_in_dim(w, place * (depth // devices), depth // devices, 0)

    w_packed = pack_weights(row_share(w_query), row_share(w_key), row_share(w_value))
    w_packed, weights = lax.optimization_barrier((w_packed, weights))
    w_packed = lax.all_gather(w_packed, "tensor", axis=0)
    context, logsum, context_own, _, w_out_all = att_fwd(
        q, k, v,
        lax.dynamic_slice_in_dim(w_out, place * (width // devices), width // devices, 0),
        n, devices,
    )
    w_out_all = w_out_all.reshape(n, width, depth)
    attn_out = sum(dot(context_own[t], w_out_all[t]).astype(BF).astype(F32) for t in range(n))
    middle = inputs + attn_out
    scaled2, inverse2 = norm_parts(middle)
    ffn_in = (scaled2 * ln2_gain + ln2_bias).astype(BF)
    grad_parts, out_parts, ffn_grads = ffn(ffn_in, grad_branch, weights, n, devices)
    grad_ffn_in = sum(grad_parts[p].astype(F32) for p in range(devices // 2))
    grad_norm2, gain2_grad, shift2_grad = norm_back(
        grad_ffn_in, scaled2, inverse2, ln2_gain
    )
    grad_middle = grad_out + grad_norm2
    grad_attn = grad_middle.astype(BF)
    ffn_grads = ffn_grads.reshape(n, 3 * share, depth)
    w_packed, grad_attn = lax.optimization_barrier((w_packed, grad_attn))
    ffn_grads = lax.psum_scatter(ffn_grads, "tensor", scatter_dimension=0, tiled=True)[0]
    w_packed = lax.all_gather(w_packed, "dp", axis=0)
    packed, packed_own, out_sums, out_piece = att_bwd(
        grad_attn, w_out_all, context_own, out_parts, q, k, v, context, logsum, cosine, sine, n
    )
    ffn_grads, out_piece = lax.optimization_barrier((ffn_grads, out_piece))
    grads = lax.all_gather(jnp.concatenate([ffn_grads, out_piece]), "dp", axis=0)
    gate_grad, up_grad, down_grad, out_grad = unpack(grads, share, width)
    ffn_out = sum(x.astype(F32) for x in (out_parts[0], *out_sums))
    output = jnp.where(valid, middle + ffn_out, 0.0).astype(BF)
    input_grad, query_grad, key_grad, value_grad, sums = finish(
        attn_rows, packed, packed_own, w_packed, tokens, grad_middle, ln1_gain,
        jnp.stack([gain2_grad, shift2_grad]), width, devices,
    )
    gain1_grad, shift1_grad, gain2_grad, shift2_grad = (sums[i] for i in range(4))
    return (
        output, input_grad, gain1_grad, shift1_grad, query_grad, key_grad, value_grad, out_grad,
        gain2_grad, shift2_grad, gate_grad, up_grad, down_grad,
    )


def solution(mesh):
    rows = P(("dp", "tensor"), None)
    columns = P(None, "tensor")
    parts = P("tensor", None)
    return jax.shard_map(
        on_device,
        mesh=mesh,
        in_specs=(
            rows, P("dp"), P(), P(), columns, columns, columns, parts,
            P(), P(), columns, columns, parts, rows,
        ),
        out_specs=(
            rows, rows, P(), P(), columns, columns, columns, parts,
            P(), P(), columns, columns, parts,
        ),
        check_vma=False,
    )
```

```python
import functools
import math

import jax
import jax.numpy as jnp
from jax import lax
from jax.experimental import pallas as pl
from jax.experimental.pallas import tpu as pltpu
from jax.sharding import PartitionSpec as P

HD = 64
EPS = 1e-05
SCALE = 1.0 / math.sqrt(HD)
F32 = jnp.float32
BF = jnp.bfloat16
NT = (((1,), (1,)), ((), ()))
NN = (((1,), (0,)), ((), ()))
TN = (((0,), (0,)), ((), ()))
MESH = pl.DeviceIdType.MESH


def dot(a, b, dims=NN):
    return lax.dot_general(a, b, dims, preferred_element_type=F32)


def lanes(shape):
    return lax.broadcasted_iota(jnp.int32, shape, 1)


def split3(x):
    hi = x.astype(BF).astype(F32)
    mid = (x - hi).astype(BF).astype(F32)
    return hi, mid, x - hi - mid


def partner(x):
    width = x.shape[1]
    first = lanes(x.shape) % HD < HD // 2
    return jnp.where(first, pltpu.roll(x, width - HD // 2, 1), pltpu.roll(x, HD // 2, 1))


STEP = 64


def angle_tables(length):
    half = HD // 2
    lane = lax.optimization_barrier(lax.iota(jnp.int32, 2 * HD))
    freqs = 10000.0 ** (-((lane % half).astype(F32) * 2.0 / HD))
    sign = jnp.where(lane % HD < half, -1.0, 1.0)

    def table(positions):
        angles = positions[:, None] * freqs[None, :]
        return jnp.stack([jnp.cos(angles), jnp.sin(angles)])

    return table(lax.iota(F32, length // STEP) * STEP), table(lax.iota(F32, STEP)), sign[None, :]


def differ(a, b, bits):
    return sum(lax.rem(a // (1 << k) + b // (1 << k), 2) * (1 << k) for k in range(bits))


def remote(src, dst, send, recv, **to):
    return pltpu.make_async_remote_copy(
        src_ref=src, dst_ref=dst, send_sem=send, recv_sem=recv, device_id=to, device_id_type=MESH
    )


def ring(n, step):
    return lax.rem(lax.axis_index("tensor") + step, n)


def same_core(s, chips):
    me = lax.axis_index("dp")
    return differ(me // 2, s, chips.bit_length() - 1) * 2 + lax.rem(me, 2)


def sibling():
    me = lax.axis_index("dp")
    return me + 1 - 2 * lax.rem(me, 2)


def greet(n, chips, both_cores=False):
    barrier = pltpu.get_barrier_semaphore()
    if both_cores:
        pl.semaphore_signal(barrier, inc=1, device_id={"dp": sibling()}, device_id_type=MESH)
    for step in range(1, n):
        pl.semaphore_signal(barrier, inc=1, device_id={"tensor": ring(n, step)}, device_id_type=MESH)
    for s in range(1, chips):
        pl.semaphore_signal(
            barrier, inc=1, device_id={"dp": same_core(s, chips)}, device_id_type=MESH
        )
    pl.semaphore_wait(barrier, n + chips - 2 + both_cores)


def begin_kernel(
    n, chips, chunks, limit_ref, tokens_ref, ct_ref, gain_ref, shift_ref, wq_ref, wk_ref, wv_ref,
    coarse_ref, fine_ref, sign_ref, gate_ref, up_ref, down_ref,
    q_ref, k_ref, v_ref, cos_ref, sin_ref, rows_ref, gb_all, share_ref, landed, gb, columns, w_sem,
    right_send, right_recv, left_send, left_recv, gs_send, gs_recv, gr_send, gr_recv, keep_sem, rows_sem,
):
    me = lax.axis_index("tensor")
    place = lax.axis_index("dp")
    core = lax.rem(place, 2)
    bits = chips.bit_length() - 1
    rows, depth = tokens_ref.shape
    heads = q_ref.shape[0]
    piece = rows // chunks
    limit = limit_ref[0]

    def over(shard, d, c, send, recv, to):
        part = landed.at[shard, pl.ds(c * piece, piece)]
        return remote(part, part, send.at[d, c], recv.at[d, c], tensor=to)

    def rightward(d, c):
        return over(me - d, d, c, right_send, right_recv, me + 1)

    def leftward(d, c):
        return over(me + d, d, c, left_send, left_recv, me - 1)

    def from_left(d, c):
        return over(me - d, d - 1, c, right_send, right_recv, me - 1)

    def from_right(d, c):
        return over(me + d, d - 1, c, left_send, left_recv, me + 1)

    def spread_gb(c):
        return remote(
            gb, gb_all.at[place // 2, core], gs_send.at[c], gs_recv.at[c], dp=same_core(c, chips)
        )

    def relay_gb(c):
        there = gb_all.at[differ(place // 2, c, bits), core]
        return remote(there if c else gb, there, gr_send.at[c], gr_recv.at[c], dp=sibling())

    barrier = pltpu.get_barrier_semaphore()
    pl.semaphore_signal(barrier, inc=1, device_id={"dp": sibling()}, device_id_type=MESH)
    for s in range(1, chips):
        to = same_core(s, chips)
        pl.semaphore_signal(barrier, inc=1, device_id={"dp": to}, device_id_type=MESH)

    @pl.when(me > 0)
    def _():
        pl.semaphore_signal(barrier, inc=1, device_id={"tensor": me - 1}, device_id_type=MESH)

    @pl.when(me < n - 1)
    def _():
        pl.semaphore_signal(barrier, inc=1, device_id={"tensor": me + 1}, device_id_type=MESH)

    values = tokens_ref[...].astype(F32)
    values = values - jnp.mean(values, axis=1, keepdims=True)
    inverse = lax.rsqrt(jnp.mean(values * values, axis=1, keepdims=True) + EPS)
    landed[me] = (values * inverse * gain_ref[...] + shift_ref[...]).astype(BF)

    pl.semaphore_wait(barrier, chips + jnp.minimum(me, 1) + jnp.minimum(n - 1 - me, 1))

    for c in range(chunks):

        @pl.when(me < n - 1)
        def _():
            rightward(0, c).start()

        @pl.when(me > 0)
        def _():
            leftward(0, c).start()

    row = me * rows + lax.broadcasted_iota(jnp.int32, (rows, depth), 0)
    gb[...] = jnp.where(row < limit, ct_ref[...].astype(F32), 0.0).astype(BF)
    for s in range(1, chips):
        spread_gb(s).start()
    relay_gb(0).start()
    keep = pltpu.make_async_copy(gb, gb_all.at[place // 2, core], keep_sem)
    keep.start()
    share = share_ref.shape[1]
    aligned = share % 128 == 0
    ours = pl.ds(pl.multiple_of(place * share, share), share)
    cuts = [pltpu.make_async_copy(down_ref.at[ours], share_ref.at[2], w_sem.at[2])]
    for k, ref in enumerate((gate_ref, up_ref)):
        src = ref.at[:, ours] if aligned else ref
        cuts.append(pltpu.make_async_copy(src, columns.at[k], w_sem.at[k]))
    for cut in cuts:
        cut.start()

    lane = lanes((rows, 128))
    ones = jnp.where(lane < HD + 3, 1.0, 0.0)
    unit = jnp.where(lane == HD + 3, 1.0, 0.0)

    def put(out_ref, here, values, extra):
        for h in range(heads):
            own = values[:, h // 2 * 128 : h // 2 * 128 + 128]
            own = pltpu.roll(own, HD, 1) if h % 2 else own
            out_ref[h, here, :] = jnp.where(lane < HD, own, extra).astype(BF)

    def project(shard):
        here = pl.ds(pl.multiple_of(shard * rows, rows), rows)
        for i in range(rows // STEP):
            part = pl.ds(pl.multiple_of(shard * rows + i * STEP, STEP), STEP)
            coarse = pl.ds(shard * (rows // STEP) + i, 1)
            c0, s0 = coarse_ref[0, coarse, :], coarse_ref[1, coarse, :]
            cos_ref[part, :] = c0 * fine_ref[0] - s0 * fine_ref[1]
            sin_ref[part, :] = (s0 * fine_ref[0] + c0 * fine_ref[1]) * sign_ref[...]
        cosine = jnp.tile(cos_ref[here, :], (1, heads // 2))
        sine = jnp.tile(sin_ref[here, :], (1, heads // 2))
        x = landed[shard]
        row = shard * rows + lax.broadcasted_iota(jnp.int32, (rows, 128), 0)
        bias = jnp.where(lane == HD + 3, jnp.where(row < limit, 0.0, -1e30), ones)
        raw = dot(x, wq_ref[...])
        turned = (raw * cosine + partner(raw) * sine).astype(BF).astype(F32)
        put(q_ref, here, turned * SCALE, unit)
        raw = dot(x, wk_ref[...])
        put(k_ref, here, raw * cosine + partner(raw) * sine, bias)
        put(v_ref, here, dot(x, wv_ref[...]), ones)

    def save(shard):
        return pltpu.make_async_copy(landed.at[shard], rows_ref.at[shard], rows_sem.at[shard])

    for d in range(1, n + 1):
        for c in range(chunks):
            if d < n:

                @pl.when(me >= d)
                def _():
                    from_left(d, c).wait_recv()

                @pl.when((me >= d) & (me < n - 1))
                def _():
                    rightward(d, c).start()

                @pl.when(me + d < n)
                def _():
                    from_right(d, c).wait_recv()

                @pl.when((me + d < n) & (me > 0))
                def _():
                    leftward(d, c).start()

            if c == 0:

                @pl.when(me >= d - 1)
                def _():
                    save(me - d + 1).start()
                    project(me - d + 1)

            if c == 2 and d == 1:
                for cut in cuts:
                    cut.wait()
                for k in range(2):
                    share_ref[k] = columns[k].astype(F32).T.astype(BF)

            if c == 1 and d > 1:

                @pl.when(me + d - 1 < n)
                def _():
                    save(me + d - 1).start()
                    project(me + d - 1)

            if c == chunks - 1 and d == 2:
                for s in range(1, chips // 2 + 1):
                    spread_gb(s).wait_recv()
                    relay_gb(s).start()

            if c == 0 and d == n:
                for s in range(chips // 2 + 1, chips):
                    spread_gb(s).wait_recv()
                    relay_gb(s).start()

    for d in range(n - 1):
        for c in range(chunks):

            @pl.when((me >= d) & (me < n - 1))
            def _():
                rightward(d, c).wait_send()

            @pl.when((me + d < n) & (me > 0))
            def _():
                leftward(d, c).wait_send()

    for s in range(chips):
        relay_gb(s).wait()
        if s:
            spread_gb(s).wait_send()
    keep.wait()
    for shard in range(n):
        save(shard).wait()


def begin(
    tokens, cotangent, gain, shift, w_query, w_key, w_value, tables, gate, up, down, limit, n, devices
):
    rows, depth = tokens.shape
    total = n * rows
    heads = w_query.shape[1] // HD
    chips = devices // 2
    chunks = 4
    share = down.shape[0] // devices
    if share % 128:
        place = lax.axis_index("dp")
        gate, up = (lax.dynamic_slice_in_dim(w, place * share, share, 1) for w in (gate, up))
    vmem = pl.BlockSpec(memory_space=pltpu.VMEM)
    hbm = pl.BlockSpec(memory_space=pl.ANY)
    return pl.pallas_call(
        functools.partial(begin_kernel, n, chips, chunks),
        out_shape=(jax.ShapeDtypeStruct((heads, total, 128), BF),) * 3
        + (jax.ShapeDtypeStruct((total, 128), F32),) * 2
        + (
            jax.ShapeDtypeStruct((n, rows, depth), BF),
            jax.ShapeDtypeStruct((chips, 2, rows, depth), BF),
            jax.ShapeDtypeStruct((3, share, depth), BF),
        ),
        in_specs=[pl.BlockSpec(memory_space=pltpu.SMEM)] + [vmem] * 10 + [hbm] * 3,
        out_specs=[vmem] * 5 + [hbm] * 2 + [vmem],
        scratch_shapes=[pltpu.VMEM((n, rows, depth), BF), pltpu.VMEM((rows, depth), BF)]
        + [pltpu.VMEM((2, depth, share), BF), pltpu.SemaphoreType.DMA((3,))]
        + [pltpu.SemaphoreType.DMA((n - 1, chunks))] * 4
        + [pltpu.SemaphoreType.DMA((chips,))] * 4
        + [pltpu.SemaphoreType.DMA, pltpu.SemaphoreType.DMA((n,))],
        compiler_params=pltpu.CompilerParams(
            vmem_limit_bytes=44 << 20, collective_id=5, has_side_effects=True
        ),
        cost_estimate=pl.CostEstimate(
            flops=6 * total * depth * heads * HD * 10, bytes_accessed=30 << 20, transcendentals=0
        ),
        name="begin",
    )(
        limit, tokens, cotangent, gain.reshape(1, depth), shift.reshape(1, depth),
        w_query, w_key, w_value, *tables, gate, up, down,
    )


def att_fwd_kernel(
    n, chips, q_ref, k_ref, v_ref, wo_ref,
    ctx_ref, lse_ref, out_ref, wo_z, wo_all, send_sem, recv_sem, own_sem,
    wz_send, wz_recv, ws_send, ws_recv, wr_send, wr_recv, keep_sem,
):
    s = pl.program_id(0)
    h = pl.program_id(1)
    heads = pl.num_programs(1)
    rows = q_ref.shape[1] // n
    me = lax.axis_index("tensor")
    place = lax.axis_index("dp")
    core = lax.rem(place, 2)
    bits = chips.bit_length() - 1

    def wo_over(step):
        return remote(
            wo_ref, wo_z.at[me], wz_send.at[step], wz_recv.at[step], tensor=ring(n, step + 1)
        )

    def spread_wo(c):
        return remote(
            wo_z, wo_all.at[:, place], ws_send.at[c], ws_recv.at[c], dp=same_core(c, chips)
        )

    def relay_wo(c):
        there = wo_all.at[:, differ(place // 2, c, bits) * 2 + core]
        return remote(there if c else wo_z, there, wr_send.at[c], wr_recv.at[c], dp=sibling())

    keeps = [
        pltpu.make_async_copy(wo_ref, wo_z.at[me], keep_sem.at[0]),
        pltpu.make_async_copy(wo_z, wo_all.at[:, place], keep_sem.at[1]),
    ]

    @pl.when((s == 0) & (h == 0))
    def _():
        greet(n, chips, True)
        for step in range(n - 1):
            wo_over(step).start()
        keeps[0].start()

    @pl.when((s == 1) & (h == 0))
    def _():
        for step in range(n - 1):
            wo_over(step).wait()
        keeps[0].wait()
        for c in range(1, chips):
            spread_wo(c).start()
        relay_wo(0).start()
        keeps[1].start()

    @pl.when((s == n - 1) & (h == 0))
    def _():
        for c in range(1, chips):
            spread_wo(c).wait_recv()
            relay_wo(c).start()

    owner = ring(n, s + 1)
    block = pl.ds(pl.multiple_of(owner * rows, rows), rows)
    scores = dot(q_ref[h, block, :], k_ref[h], NT)
    peak = jnp.max(scores, axis=1, keepdims=True)
    acc = dot(jnp.exp(scores - peak).astype(BF), v_ref[h])
    lane = lanes((rows, 128))
    total = jnp.sum(jnp.where(lane == HD, acc, 0.0), axis=1, keepdims=True)
    out = acc * (1.0 / total)
    odd = lax.rem(h, 2)
    out = jnp.where(odd == 1, pltpu.roll(out, HD, 1), out).astype(BF)
    pair = pl.ds(pl.multiple_of(h // 2 * 128, 128), 128)
    ctx_ref[block, pair] = jnp.where((lane >= HD) == (odd == 1), out, ctx_ref[block, pair])
    lse_ref[block, :] = jnp.where(lane == h, peak + jnp.log(total), lse_ref[block, :])

    def push(step):
        return pltpu.make_async_remote_copy(
            src_ref=ctx_ref.at[block],
            dst_ref=out_ref.at[me],
            send_sem=send_sem.at[step],
            recv_sem=recv_sem.at[step],
            device_id={"tensor": owner},
            device_id_type=MESH,
        )

    @pl.when((h == heads - 1) & (s < n - 1))
    def _():
        push(s).start()

    @pl.when((h == heads - 1) & (s == n - 1))
    def _():
        keep = pltpu.make_async_copy(ctx_ref.at[block], out_ref.at[me], own_sem)
        keep.start()
        for step in range(n - 1):
            push(step).wait()
        keep.wait()
        keeps[1].wait()
        for c in range(chips):
            relay_wo(c).wait()
            if c:
                spread_wo(c).wait_send()


def att_fwd(q, k, v, w_out_piece, n, devices):
    heads, total, _ = q.shape
    width = heads * HD
    rows = total // n
    share, depth = w_out_piece.shape
    chips = devices // 2
    hbm = pl.BlockSpec(memory_space=pl.ANY)

    def whole(*shape):
        return pl.BlockSpec(shape, lambda *_: (0,) * len(shape), pipeline_mode=pl.Buffered(1))

    return pl.pallas_call(
        functools.partial(att_fwd_kernel, n, chips),
        out_shape=(
            jax.ShapeDtypeStruct((total, width), BF),
            jax.ShapeDtypeStruct((total, 128), F32),
            jax.ShapeDtypeStruct((n, rows, width), BF),
            jax.ShapeDtypeStruct((n, share, depth), BF),
            jax.ShapeDtypeStruct((n, devices, share, depth), BF),
        ),
        grid_spec=pltpu.PrefetchScalarGridSpec(
            num_scalar_prefetch=0,
            grid=(n, heads),
            in_specs=[whole(heads, total, 128)] * 3 + [hbm],
            out_specs=[whole(total, width), whole(total, 128)] + [hbm] * 3,
            scratch_shapes=[pltpu.SemaphoreType.DMA((n - 1,))] * 2
            + [pltpu.SemaphoreType.DMA]
            + [pltpu.SemaphoreType.DMA((n - 1,))] * 2
            + [pltpu.SemaphoreType.DMA((chips,))] * 4
            + [pltpu.SemaphoreType.DMA((2,))],
        ),
        compiler_params=pltpu.CompilerParams(
            vmem_limit_bytes=40 << 20, collective_id=1, has_side_effects=True
        ),
        cost_estimate=pl.CostEstimate(
            flops=4 * total * total * 256 * heads,
            bytes_accessed=10 * total * width,
            transcendentals=total * total * heads,
        ),
        name="att_fwd",
    )(q, k, v, w_out_piece)


def att_bwd_kernel(
    n, bk, chips, ga_ref, wo_ref, cown_ref, parts_ref, q_ref, k_ref, v_ref, ctx_ref, lse_ref,
    cos_ref, sin_ref, pk_ref, own_ref, sums_ref, og_ref, do, gc, dka, dva, dqs,
    og_full, og_own, og_mate, og_sib, og_land, og_piece, og_z,
    send_sem, recv_sem, out_send, out_recv, pk_send, pk_recv, keep_sem,
    om_send, om_recv, op_send, op_recv, oz_send, oz_recv,
):
    i = pl.program_id(0)
    heads, total, _ = k_ref.shape
    h = jnp.where(i < heads, i, (i - heads) // (n - 1))
    t = jnp.where(i < heads, 0, lax.rem(i - heads, n - 1) + 1)
    rows = total // n
    me = lax.axis_index("tensor")
    place = lax.axis_index("dp")
    core = lax.rem(place, 2)
    bits = chips.bit_length() - 1
    share = og_ref.shape[0]
    mine = pl.ds(pl.multiple_of(me * rows, rows), rows)

    def push(step):
        return remote(
            gc.at[step], do.at[mine], send_sem.at[step], recv_sem.at[step], tensor=ring(n, step + 1)
        )

    def push_out(s):
        return remote(
            parts_ref.at[s], sums_ref.at[s - 1], out_send.at[s - 1], out_recv.at[s - 1],
            dp=same_core(s, chips),
        )

    def columns(slot):
        return pl.ds(pl.multiple_of(slot * 128, 128), 128)

    def push_pack(slot, step):
        owner = ring(n, step + 1)
        return remote(
            pk_ref.at[pl.ds(pl.multiple_of(owner * rows, rows), rows), columns(slot)],
            own_ref.at[me, :, columns(slot)],
            pk_send.at[slot, step], pk_recv.at[slot, step], tensor=owner,
        )

    def keep(slot):
        return pltpu.make_async_copy(
            pk_ref.at[mine, columns(slot)], own_ref.at[me, :, columns(slot)], keep_sem.at[slot]
        )

    @pl.when(i == 0)
    def _():
        greet(n, chips, True)

        def send(step, carry):
            gc[step] = dot(ga_ref[...], wo_ref[ring(n, step + 1)], NT).astype(BF)
            push(step).start()
            return carry

        lax.fori_loop(0, n - 1, send, 0)
        do[mine, :] = dot(ga_ref[...], wo_ref[me], NT).astype(BF)

    def og_swap():
        return remote(og_mate, og_sib, om_send, om_recv, dp=sibling())

    def og_push(s):
        return remote(og_sib.at[s], og_land.at[s], op_send.at[s], op_recv.at[s], dp=same_core(s, chips))

    def og_over(step):
        to = ring(n, step + 1)
        return remote(og_piece.at[to], og_z.at[me], oz_send.at[step], oz_recv.at[step], tensor=to)

    @pl.when(i == 1)
    def _():
        def term(part, carry):
            og_full[...] = dot(cown_ref[part], ga_ref[...], TN)
            for s in range(chips):
                start = differ(place // 2, s, bits) * 2
                here = pl.ds(pl.multiple_of((start + core) * share, share), share)
                there = pl.ds(pl.multiple_of((start + 1 - core) * share, share), share)
                og_own[s, part] = og_full[here, :]
                og_mate[s, part] = og_full[there, :].astype(BF)
            return carry

        lax.fori_loop(0, n, term, 0)
        og_swap().start()

    @pl.when(i == 2)
    def _():
        og_swap().wait_recv()
        for s in range(chips):
            og_sib[s] = (og_own[s] + og_sib[s].astype(F32)).astype(BF)
            if s:
                og_push(s).start()

    @pl.when(i == heads + 2)
    def _():
        joined = og_sib[0].astype(F32)
        for s in range(1, chips):
            og_push(s).wait_recv()
            joined = joined + og_land[s].astype(F32)
        og_piece[...] = joined.astype(BF)
        for step in range(n - 1):
            og_over(step).start()
        for s in range(1, chips):
            push_out(s).start()

    @pl.when(i == heads * n - 1)
    def _():
        og_z[me] = og_piece[me]
        for step in range(n - 1):
            og_over(step).wait_recv()
        joined = og_z[0].astype(F32)
        for part in range(1, n):
            joined = joined + og_z[part].astype(F32)
        og_ref[...] = joined.astype(BF)

    @pl.when((h == 0) & (t > 0))
    def _():
        push(t - 1).wait_recv()

    source = ring(n, n - t)
    block = pl.ds(pl.multiple_of(source * rows, rows), rows)
    pair = columns(h // 2)
    odd = lax.rem(h, 2) == 1
    lane = lanes((rows, 128))
    off = lane - HD
    logsum = jnp.sum(jnp.where(lane == h, lse_ref[block, :], 0.0), axis=1, keepdims=True)
    a, b, c = split3(-logsum)
    q = q_ref[h, block, :].astype(F32)
    q = jnp.where(off == 0, a, jnp.where(off == 1, b, jnp.where(off == 2, c, q))).astype(BF)
    g = jnp.where((lane >= HD) == odd, do[block, pair].astype(F32), 0.0)
    delta = jnp.sum(g * ctx_ref[block, pair].astype(F32), axis=1, keepdims=True)
    a, b, c = split3(-delta)
    g = jnp.where(odd, pltpu.roll(g, HD, 1), g)
    g = jnp.where(off == 0, a, jnp.where(off == 1, b, jnp.where(off == 2, c, g))).astype(BF)
    acc = jnp.zeros((rows, 128), F32)
    for j in range(total // bk):
        rk = pl.ds(j * bk, bk)
        kt = k_ref[h, rk, :]
        probs = jnp.exp(dot(kt, q, NT))
        grad = (probs * dot(v_ref[h, rk, :], g, NT)).astype(BF)
        for sums, term in ((dva, dot(probs.astype(BF), g)), (dka, dot(grad, q))):
            before = jnp.where(t == 0, jnp.zeros_like(term), sums[h, rk, :])
            sums[h, rk, :] = before + term
        acc = acc + dot(grad, kt, TN)
    acc = acc * SCALE

    @pl.when(jnp.logical_not(odd))
    def _():
        dqs[block, :] = acc

    @pl.when(odd)
    def _():
        grad = jnp.where(lane < HD, dqs[block, :], pltpu.roll(acc, HD, 1))
        grad = grad * cos_ref[block, :] - partner(grad) * sin_ref[block, :]
        pk_ref[block, columns(heads + h // 2)] = grad.astype(BF)

    @pl.when(odd & (t == 0))
    def _():
        keep(heads + h // 2).start()

    @pl.when(odd & (t > 0))
    def _():
        push_pack(heads + h // 2, n - 1 - t).start()

    @pl.when(t == n - 1)
    def _():
        dk = dka[h]
        dk = dk * cos_ref[...] - partner(dk) * sin_ref[...]
        both = jnp.where(lanes((total, 128)) < HD, dk, pltpu.roll(dva[h], HD, 1))
        pk_ref[:, columns(h)] = both.astype(BF)
        for step in range(n - 1):
            push_pack(h, step).start()
        keep(h).start()

    @pl.when(i == heads * n - 1)
    def _():
        for step in range(n - 1):
            push(step).wait_send()
        for s in range(1, chips):
            push_out(s).wait()
        og_swap().wait_send()
        for s in range(1, chips):
            og_push(s).wait_send()
        for step in range(n - 1):
            og_over(step).wait_send()
        for slot in range(heads + heads // 2):
            keep(slot).wait()
            for step in range(n - 1):
                push_pack(slot, step).wait()


def att_bwd(grad_attn, w_out, ctx_own, parts, q, k, v, ctx, lse, cosine, sine, n, bk=512):
    heads, total, _ = q.shape
    width = heads * HD
    rows, depth = grad_attn.shape
    chips = parts.shape[0]
    share = width // (2 * chips)
    slots = heads + heads // 2
    hbm = pl.BlockSpec(memory_space=pl.ANY)

    def whole(*shape):
        return pl.BlockSpec(shape, lambda *_: (0,) * len(shape), pipeline_mode=pl.Buffered(1))

    return pl.pallas_call(
        functools.partial(att_bwd_kernel, n, bk, chips),
        out_shape=(
            jax.ShapeDtypeStruct((total, slots * 128), BF),
            jax.ShapeDtypeStruct((n, rows, slots * 128), BF),
            jax.ShapeDtypeStruct((chips - 1, rows, depth), BF),
            jax.ShapeDtypeStruct((share, depth), BF),
        ),
        grid_spec=pltpu.PrefetchScalarGridSpec(
            num_scalar_prefetch=0,
            grid=(heads * n,),
            in_specs=[whole(rows, depth), whole(n, width, depth), whole(n, rows, width), hbm]
            + [whole(heads, total, 128)] * 3
            + [whole(total, width)]
            + [whole(total, 128)] * 3,
            out_specs=[whole(total, slots * 128), hbm, hbm, whole(share, depth)],
            scratch_shapes=[
                pltpu.VMEM((total, width), BF),
                pltpu.VMEM((n - 1, rows, width), BF),
            ]
            + [pltpu.VMEM((heads, total, 128), F32)] * 2
            + [pltpu.VMEM((total, 128), F32)]
            + [
                pltpu.VMEM((width, depth), F32),
                pltpu.VMEM((chips, n, share, depth), F32),
                pltpu.VMEM((chips, n, share, depth), BF),
                pltpu.VMEM((chips, n, share, depth), BF),
                pltpu.VMEM((chips, n, share, depth), BF),
                pltpu.VMEM((n, share, depth), BF),
                pltpu.VMEM((n, share, depth), BF),
            ]
            + [pltpu.SemaphoreType.DMA((n - 1,))] * 2
            + [pltpu.SemaphoreType.DMA((chips - 1,))] * 2
            + [pltpu.SemaphoreType.DMA((slots, n - 1))] * 2
            + [pltpu.SemaphoreType.DMA((slots,))]
            + [pltpu.SemaphoreType.DMA] * 2
            + [pltpu.SemaphoreType.DMA((chips,))] * 2
            + [pltpu.SemaphoreType.DMA((n - 1,))] * 2,
        ),
        compiler_params=pltpu.CompilerParams(
            vmem_limit_bytes=56 << 20, collective_id=2, has_side_effects=True
        ),
        cost_estimate=pl.CostEstimate(
            flops=10 * total * total * 256 * heads,
            bytes_accessed=20 * total * width,
            transcendentals=total * total * heads,
        ),
        name="att_bwd",
    )(grad_attn, w_out, ctx_own, parts, q, k, v, ctx, lse, cosine, sine)


def finish_kernel(
    chips, n, width, x_ref, pk_ref, own_ref, w_ref, tokens_ref, middle_ref, gain_ref, vec_ref,
    input_ref, q_ref, k_ref, v_ref, sums_ref,
    full, mate, sib, land, fin, every, vec_z, vec_dp, vec_me,
    sx_send, sx_recv, rs_send, rs_recv, ag_send, ag_recv, rl_send, rl_recv,
    vz_send, vz_recv, vd_send, vd_recv, own_sem,
):
    bits = chips.bit_length() - 1
    me = lax.axis_index("dp")
    place = lax.axis_index("tensor")
    core = lax.rem(me, 2)
    chip = me // 2
    other = 1 - core
    heads = width // HD
    piece = fin.shape[0]

    def swap(s):
        return remote(mate.at[s], sib.at[s], sx_send.at[s], sx_recv.at[s], dp=chip * 2 + other)

    def push(s):
        return remote(sib.at[s], land.at[s], rs_send.at[s], rs_recv.at[s], dp=same_core(s, chips))

    def spread(s):
        return remote(
            fin, every.at[chip, core], ag_send.at[s], ag_recv.at[s], dp=same_core(s, chips)
        )

    def relay(s):
        src = every.at[differ(chip, s, bits), core]
        return remote(src, src, rl_send.at[s], rl_recv.at[s], dp=chip * 2 + other)

    def vec_over(step):
        return remote(
            vec_me.at[0], vec_z.at[place], vz_send.at[step], vz_recv.at[step], tensor=ring(n, step + 1)
        )

    def vec_across(step):
        return remote(
            vec_me.at[1], vec_dp.at[me], vd_send.at[step], vd_recv.at[step],
            dp=lax.rem(me + step + 1, 2 * chips),
        )

    barrier = pltpu.get_barrier_semaphore()
    for step in range(n - 1):
        pl.semaphore_signal(barrier, inc=1, device_id={"tensor": ring(n, step + 1)}, device_id_type=MESH)
    for step in range(2 * chips - 1):
        to = lax.rem(me + step + 1, 2 * chips)
        pl.semaphore_signal(barrier, inc=1, device_id={"dp": to}, device_id_type=MESH)

    full[...] = dot(x_ref[...], pk_ref[...], TN)
    pl.semaphore_wait(barrier, n + 2 * chips - 2)

    def part(s, which):
        start = (differ(chip, s, bits) * 2 + which) * piece
        return full[pl.ds(pl.multiple_of(start, piece), piece), :]

    for s in range(chips):
        mate[s] = part(s, other).astype(BF)
        swap(s).start()

    grad = jnp.zeros(input_ref.shape, F32)
    for t in range(n):
        w = w_ref[:, t].reshape(w_ref.shape[0] * w_ref.shape[2], w_ref.shape[3])
        grad = grad + dot(own_ref[t], w, NT).astype(BF).astype(F32)

    for s in range(1, chips):
        swap(s).wait_recv()
        sib[s] = (sib[s].astype(F32) + part(s, core)).astype(BF)
        push(s).start()
    swap(0).wait_recv()
    total = sib[0].astype(F32) + part(0, core)

    values = tokens_ref[...].astype(F32)
    values = values - jnp.mean(values, axis=1, keepdims=True)
    inverse = lax.rsqrt(jnp.mean(values * values, axis=1, keepdims=True) + EPS)
    scaled = values * inverse
    through = grad * gain_ref[...]
    inner = through - jnp.mean(through, axis=1, keepdims=True)
    inner = inner - scaled * jnp.mean(through * scaled, axis=1, keepdims=True)
    input_ref[...] = middle_ref[...] + inverse * inner
    vec_me[0, 0:1] = jnp.sum(grad * scaled, axis=0, keepdims=True)
    vec_me[0, 1:2] = jnp.sum(grad, axis=0, keepdims=True)
    vec_me[0, 2:4] = vec_ref[...]
    vec_me[0, 4:8] = jnp.zeros((4, vec_ref.shape[1]), F32)
    vec_z[place] = vec_me[0]
    for step in range(n - 1):
        vec_over(step).start()

    for s in range(1, chips):
        push(s).wait_recv()
        total = total + land[s].astype(F32)
    fin[...] = total.astype(BF)
    for s in range(1, chips):
        spread(s).start()
    mine = pltpu.make_async_copy(fin, every.at[chip, core], own_sem)
    mine.start()
    mine.wait()
    relay(0).start()

    for step in range(n - 1):
        vec_over(step).wait()
    vec = vec_z[0]
    for t in range(1, n):
        vec = vec + vec_z[t]
    vec_me[1] = vec
    vec_dp[me] = vec
    for step in range(2 * chips - 1):
        vec_across(step).start()
    for s in range(1, chips):
        spread(s).wait_recv()
        relay(s).start()
    for step in range(2 * chips - 1):
        vec_across(step).wait()
    vec = vec_dp[0]
    for t in range(1, 2 * chips):
        vec = vec + vec_dp[t]
    sums_ref[...] = vec
    for s in range(chips):
        relay(s).wait()
        swap(s).wait_send()
        if s > 0:
            spread(s).wait_send()
            push(s).wait_send()
    first = lanes((piece, 128)) < HD
    for d in range(2 * chips):
        rows = slice(d * piece, (d + 1) * piece)
        g = every[d // 2, d % 2].astype(F32)
        for pair in range(heads // 2):
            a = g[:, pair * 256 : pair * 256 + 128]
            b = g[:, pair * 256 + 128 : pair * 256 + 256]
            out = slice(pair * 128, pair * 128 + 128)
            q_ref[rows, out] = g[:, (heads + pair) * 128 : (heads + pair + 1) * 128]
            k_ref[rows, out] = jnp.where(first, a, pltpu.roll(b, HD, 1))
            v_ref[rows, out] = jnp.where(first, pltpu.roll(a, HD, 1), b)


def finish(rows_all, packed, own, w_all, tokens, middle, gain, vec, width, devices):
    n, rows, packs = own.shape
    depth = tokens.shape[1]
    chips = devices // 2
    piece = depth // devices
    vmem = pl.BlockSpec(memory_space=pltpu.VMEM)
    out = jax.ShapeDtypeStruct((depth, width), F32)
    return pl.pallas_call(
        functools.partial(finish_kernel, chips, n, width),
        out_shape=(
            jax.ShapeDtypeStruct((rows, depth), F32), out, out, out,
            jax.ShapeDtypeStruct((8, depth), F32),
        ),
        in_specs=[vmem] * 8,
        out_specs=[vmem] * 5,
        scratch_shapes=[
            pltpu.VMEM((depth, packs), F32),
            pltpu.VMEM((chips, piece, packs), BF),
            pltpu.VMEM((chips, piece, packs), BF),
            pltpu.VMEM((chips, piece, packs), BF),
            pltpu.VMEM((piece, packs), BF),
            pltpu.VMEM((chips, 2, piece, packs), BF),
            pltpu.VMEM((n, 8, depth), F32),
            pltpu.VMEM((devices, 8, depth), F32),
            pltpu.VMEM((2, 8, depth), F32),
        ]
        + [pltpu.SemaphoreType.DMA((chips,))] * 8
        + [pltpu.SemaphoreType.DMA((n - 1,))] * 2
        + [pltpu.SemaphoreType.DMA((devices - 1,))] * 2
        + [pltpu.SemaphoreType.DMA],
        compiler_params=pltpu.CompilerParams(
            vmem_limit_bytes=56 << 20, collective_id=4, has_side_effects=True
        ),
        cost_estimate=pl.CostEstimate(
            flops=4 * n * rows * depth * packs, bytes_accessed=20 << 20, transcendentals=0
        ),
        name="finish",
    )(rows_all, packed, own, w_all, tokens, middle, gain.reshape(1, depth), vec)


def ffn_kernel(
    chips, x_ref, gb_ref, w_ref, wp_ref, dx_ref, out_ref, dw_ref, wp_z,
    rows_all, gb, hid, gate_g, up_g, own, sib, mate,
    ag_send, ag_recv, rl_send, rl_recv, sx_send, sx_recv, rs_send, rs_recv, fw_send, fw_recv,
    gb_sem, out_sem, dx_sem, wp_send, wp_recv, wp_sem,
):
    bits = chips.bit_length() - 1
    me = lax.axis_index("dp")
    core = lax.rem(me, 2)
    chip = me // 2
    other = 1 - core
    rows, depth = x_ref.shape
    n = dw_ref.shape[0]
    share = dw_ref.shape[2]

    def spread(s):
        to = differ(chip, s, bits) * 2 + core
        return remote(x_ref, rows_all.at[chip, core], ag_send.at[s], ag_recv.at[s], dp=to)

    square = chips == 4

    def hand_on(s):
        half = pl.ds((s - 1) * (rows // 2), rows // 2)
        part = rows_all.at[differ(chip, s, bits), core, half]
        to = differ(chip, 3 - s, bits) * 2 + core
        return remote(part, part, fw_send.at[s], fw_recv.at[s], dp=to)

    def handed(s):
        half = pl.ds((s - 1) * (rows // 2), rows // 2)
        part = rows_all.at[differ(chip, 3, bits), core, half]
        to = differ(chip, 3 - s, bits) * 2 + core
        return remote(part, part, fw_send.at[s], fw_recv.at[s], dp=to)

    def relay(s):
        src = differ(chip, s, bits)
        return remote(
            rows_all.at[src, core], rows_all.at[src, core], rl_send.at[s], rl_recv.at[s],
            dp=chip * 2 + other,
        )

    def swap(s):
        return remote(
            mate.at[lax.rem(s, 2)], sib.at[s], sx_send.at[s], sx_recv.at[s], dp=chip * 2 + other
        )

    def push(s):
        to = differ(chip, s, bits) * 2 + core
        return remote(sib.at[s, 0], dx_ref.at[s], rs_send.at[s], rs_recv.at[s], dp=to)

    def fetch(s):
        src = differ(chip, s, bits)
        return pltpu.make_async_copy(gb_ref.at[src], gb.at[src], gb_sem.at[s])

    part = lax.axis_index("tensor")

    def over(step):
        return remote(
            wp_ref, wp_z.at[part], wp_send.at[step], wp_recv.at[step], tensor=ring(n, step + 1)
        )

    def keep(s):
        return pltpu.make_async_copy(sib.at[s, 1], out_ref.at[s], out_sem.at[s])

    for s in range(chips):
        fetch(s).start()
    barrier = pltpu.get_barrier_semaphore()
    for step in range(1, n):
        pl.semaphore_signal(barrier, inc=1, device_id={"tensor": ring(n, step)}, device_id_type=MESH)
    pl.semaphore_signal(barrier, inc=1, device_id={"dp": chip * 2 + other}, device_id_type=MESH)
    for s in range(1, chips):
        to = differ(chip, s, bits) * 2 + core
        pl.semaphore_signal(barrier, inc=1, device_id={"dp": to}, device_id_type=MESH)
    pl.semaphore_wait(barrier, chips + n - 1)
    direct = range(1, 3) if square else range(1, chips)
    for s in direct:
        spread(s).start()
    mine = pltpu.make_async_copy(x_ref, rows_all.at[chip, core], ag_send.at[0])
    mine.start()
    mine.wait()
    relay(0).start()
    for step in range(n - 1):
        over(step).start()
    keep_wp = pltpu.make_async_copy(wp_ref, wp_z.at[part], wp_sem)
    keep_wp.start()

    def shard(src, which, put):
        x = rows_all[src, which]
        grad = gb[src, which]
        gate = dot(x, w_ref[0], NT)
        upper = dot(x, w_ref[1], NT)
        grad_hidden = dot(grad, w_ref[2], NT)
        sigma = jax.nn.sigmoid(gate)
        act = gate * sigma
        hidden = (act * upper).astype(BF)
        grad_gate = (grad_hidden * upper * sigma * (1.0 + gate * (1.0 - sigma))).astype(BF)
        grad_upper = (grad_hidden * act).astype(BF)
        hid[src, which] = hidden
        gate_g[src, which] = grad_gate
        up_g[src, which] = grad_upper
        put[0] = (dot(grad_gate, w_ref[0]) + dot(grad_upper, w_ref[1])).astype(BF)
        put[1] = dot(hidden, w_ref[2]).astype(BF)

    def step(s, carry):
        src = differ(chip, s, bits)
        slot = lax.rem(s, 2)
        relay(s).wait_recv()
        fetch(s).wait()

        @pl.when(s >= 2)
        def _():
            swap(s - 2).wait_send()

        shard(src, other, mate.at[slot])
        swap(s).start()
        shard(src, core, own)
        swap(s).wait_recv()
        for k in range(2):
            sib[s, k] = (sib[s, k].astype(F32) + own[k].astype(F32)).astype(BF)

        @pl.when(s > 0)
        def _():
            push(s).start()

        keep(s).start()

        if square:

            @pl.when(s == 0)
            def _():
                for near in (1, 2):
                    spread(near).wait_recv()
                    hand_on(near).start()
                    relay(near).start()

        else:

            @pl.when(s < chips - 1)
            def _():
                spread(s + 1).wait_recv()
                relay(s + 1).start()

        if square:

            @pl.when(s == 1)
            def _():
                handed(1).wait_recv()
                handed(2).wait_recv()
                relay(3).start()

        return carry

    lax.fori_loop(0, chips, step, 0)
    first = pltpu.make_async_copy(sib.at[0, 0], dx_ref.at[0], dx_sem)
    first.start()
    for k, (left, right) in enumerate(((gate_g, rows_all), (up_g, rows_all), (hid, gb))):
        left = left[...].reshape(-1, n * share)
        grad = dot(left, right[...].reshape(-1, depth), TN)
        for t in range(n):
            dw_ref[t, k] = grad[t * share : (t + 1) * share, :].astype(BF)
    first.wait()
    keep_wp.wait()
    for step in range(n - 1):
        over(step).wait()
    for s in range(chips):
        keep(s).wait()
        relay(s).wait_send()
        if s >= chips - 2:
            swap(s).wait_send()
        if s in direct:
            spread(s).wait_send()
        if s > 0:
            push(s).wait()
    if square:
        hand_on(1).wait_send()
        hand_on(2).wait_send()


def ffn(x, grad_branch, weights, w_packed, n, devices):
    rows, depth = x.shape
    chips = devices // 2
    hidden = weights.shape[1]
    share = hidden // n
    vmem = pl.BlockSpec(memory_space=pltpu.VMEM)
    hbm = pl.BlockSpec(memory_space=pl.ANY)
    return pl.pallas_call(
        functools.partial(ffn_kernel, chips),
        out_shape=(
            jax.ShapeDtypeStruct((chips, rows, depth), BF),
            jax.ShapeDtypeStruct((chips, rows, depth), BF),
            jax.ShapeDtypeStruct((n, 3, share, depth), BF),
            jax.ShapeDtypeStruct((n, *w_packed.shape), BF),
        ),
        in_specs=[vmem, hbm, vmem, hbm],
        out_specs=[hbm, hbm, vmem, hbm],
        scratch_shapes=[
            pltpu.VMEM((chips, 2, rows, depth), BF),
            pltpu.VMEM((chips, 2, rows, depth), BF),
        ]
        + [pltpu.VMEM((chips, 2, rows, hidden), BF)] * 3
        + [
            pltpu.VMEM((2, rows, depth), BF),
            pltpu.VMEM((chips, 2, rows, depth), BF),
            pltpu.VMEM((2, 2, rows, depth), BF),
        ]
        + [pltpu.SemaphoreType.DMA((chips,))] * 8
        + [pltpu.SemaphoreType.DMA((3,))] * 2
        + [pltpu.SemaphoreType.DMA((chips,))] * 2
        + [pltpu.SemaphoreType.DMA]
        + [pltpu.SemaphoreType.DMA((n - 1,))] * 2
        + [pltpu.SemaphoreType.DMA],
        compiler_params=pltpu.CompilerParams(
            vmem_limit_bytes=60 << 20, collective_id=3, has_side_effects=True
        ),
        cost_estimate=pl.CostEstimate(
            flops=2 * 9 * devices * rows * depth * hidden, bytes_accessed=30 << 20, transcendentals=0
        ),
        name="ffn",
    )(x, grad_branch, weights, w_packed)


def unpack_kernel(share, g_ref, gate_ref, up_ref, down_ref, out_ref):
    g = g_ref[0].astype(F32)
    gate_ref[...] = g[:share].T
    up_ref[...] = g[share : 2 * share].T
    down_ref[...] = g[2 * share : 3 * share]
    out_ref[...] = g[3 * share :]


def unpack(grads, share, width):
    devices, height, depth = grads.shape
    hidden = devices * share
    if share % 128:
        gate, up, down = (
            grads[:, k * share : (k + 1) * share].reshape(hidden, depth).astype(F32) for k in range(3)
        )
        return gate.T, up.T, down, grads[:, 3 * share :].reshape(width, depth).astype(F32)
    column = pl.BlockSpec((depth, share), lambda i: (0, i))
    return pl.pallas_call(
        functools.partial(unpack_kernel, share),
        out_shape=(
            jax.ShapeDtypeStruct((depth, hidden), F32),
            jax.ShapeDtypeStruct((depth, hidden), F32),
            jax.ShapeDtypeStruct((hidden, depth), F32),
            jax.ShapeDtypeStruct((width, depth), F32),
        ),
        grid=(devices,),
        in_specs=[pl.BlockSpec((1, height, depth), lambda i: (i, 0, 0))],
        out_specs=[
            column, column, pl.BlockSpec((share, depth), lambda i: (i, 0)),
            pl.BlockSpec((width // devices, depth), lambda i: (i, 0)),
        ],
        compiler_params=pltpu.CompilerParams(vmem_limit_bytes=40 << 20),
        name="unpack",
    )(grads)


def norm_parts(values):
    centre = jnp.mean(values, axis=-1, keepdims=True)
    centred = values - centre
    inverse = lax.rsqrt(jnp.mean(centred * centred, axis=-1, keepdims=True) + EPS)
    return centred * inverse, inverse


def norm_back(upstream, scaled, inverse, gain):
    through = upstream * gain
    inner = (
        through
        - jnp.mean(through, axis=-1, keepdims=True)
        - scaled * jnp.mean(through * scaled, axis=-1, keepdims=True)
    )
    return inverse * inner, jnp.sum(upstream * scaled, axis=0), jnp.sum(upstream, axis=0)


def pack_weights(w_query, w_key, w_value):
    depth, width = w_query.shape
    key, value = (w.reshape(depth, width // HD, 1, HD) for w in (w_key, w_value))
    both = jnp.concatenate([key, value], axis=2).reshape(depth, 2 * width)
    return jnp.concatenate([both, w_query], axis=1)


def on_device(
    tokens, lengths, ln1_gain, ln1_bias, w_query, w_key, w_value, w_out,
    ln2_gain, ln2_bias, w_gate, w_up, down_weight, cotangent,
):
    n = lax.axis_size("tensor")
    local_rows, depth = tokens.shape
    length = local_rows * n
    width = w_query.shape[1]
    row_ids = lax.axis_index("tensor") * local_rows + lax.iota(jnp.int32, local_rows)
    valid = (row_ids < lengths[0])[:, None]

    inputs = tokens.astype(F32)
    grad_out = jnp.where(valid, cotangent.astype(F32), 0.0)
    devices = lax.axis_size("dp")
    place = lax.axis_index("dp")
    share = w_gate.shape[1] // devices

    q, k, v, cosine, sine, attn_rows, grad_branch, weights = begin(
        tokens, cotangent, ln1_gain, ln1_bias, w_query, w_key, w_value, angle_tables(length),
        w_gate, w_up, down_weight, lengths, n, devices,
    )
    attn_rows = attn_rows.reshape(length, depth)
    weights = lax.all_gather(weights, "tensor", axis=1, tiled=True)

    def row_share(w):
        return lax.dynamic_slice_in_dim(w, place * (depth // devices), depth // devices, 0)

    w_packed = pack_weights(row_share(w_query), row_share(w_key), row_share(w_value))
    context, logsum, context_own, _, w_out_all = att_fwd(
        q, k, v,
        lax.dynamic_slice_in_dim(w_out, place * (width // devices), width // devices, 0),
        n, devices,
    )
    w_out_all = w_out_all.reshape(n, width, depth)
    attn_out = sum(dot(context_own[t], w_out_all[t]).astype(BF).astype(F32) for t in range(n))
    middle = inputs + attn_out
    scaled2, inverse2 = norm_parts(middle)
    ffn_in = (scaled2 * ln2_gain + ln2_bias).astype(BF)
    grad_parts, out_parts, ffn_grads, w_packed = ffn(
        ffn_in, grad_branch, weights, w_packed, n, devices
    )
    grad_ffn_in = sum(grad_parts[p].astype(F32) for p in range(devices // 2))
    grad_norm2, gain2_grad, shift2_grad = norm_back(
        grad_ffn_in, scaled2, inverse2, ln2_gain
    )
    grad_middle = grad_out + grad_norm2
    grad_attn = grad_middle.astype(BF)
    ffn_grads = ffn_grads.reshape(n, 3 * share, depth)
    w_packed = lax.all_gather(w_packed, "dp", axis=0)
    w_packed, ffn_grads = lax.optimization_barrier((w_packed, ffn_grads))
    ffn_grads = lax.psum_scatter(ffn_grads, "tensor", scatter_dimension=0, tiled=True)[0]
    packed, packed_own, out_sums, out_piece = att_bwd(
        grad_attn, w_out_all, context_own, out_parts, q, k, v, context, logsum, cosine, sine, n
    )
    ffn_grads, out_piece = lax.optimization_barrier((ffn_grads, out_piece))
    grads = lax.all_gather(jnp.concatenate([ffn_grads, out_piece]), "dp", axis=0)
    gate_grad, up_grad, down_grad, out_grad = unpack(grads, share, width)
    ffn_out = sum(x.astype(F32) for x in (out_parts[0], *out_sums))
    output = jnp.where(valid, middle + ffn_out, 0.0).astype(BF)
    input_grad, query_grad, key_grad, value_grad, sums = finish(
        attn_rows, packed, packed_own, w_packed, tokens, grad_middle, ln1_gain,
        jnp.stack([gain2_grad, shift2_grad]), width, devices,
    )
    gain1_grad, shift1_grad, gain2_grad, shift2_grad = (sums[i] for i in range(4))
    return (
        output, input_grad, gain1_grad, shift1_grad, query_grad, key_grad, value_grad, out_grad,
        gain2_grad, shift2_grad, gate_grad, up_grad, down_grad,
    )


def solution(mesh):
    rows = P(("dp", "tensor"), None)
    columns = P(None, "tensor")
    parts = P("tensor", None)
    return jax.shard_map(
        on_device,
        mesh=mesh,
        in_specs=(
            rows, P("dp"), P(), P(), columns, columns, columns, parts,
            P(), P(), columns, columns, parts, rows,
        ),
        out_specs=(
            rows, rows, P(), P(), columns, columns, columns, parts,
            P(), P(), columns, columns, parts,
        ),
        check_vma=False,
    )
```

```python
import functools
import math

import jax
import jax.numpy as jnp
from jax import lax
from jax.experimental import pallas as pl
from jax.experimental.pallas import tpu as pltpu
from jax.sharding import PartitionSpec as P

HD = 64
EPS = 1e-05
SCALE = 1.0 / math.sqrt(HD)
F32 = jnp.float32
BF = jnp.bfloat16
NT = (((1,), (1,)), ((), ()))
NN = (((1,), (0,)), ((), ()))
TN = (((0,), (0,)), ((), ()))
MESH = pl.DeviceIdType.MESH


def dot(a, b, dims=NN):
    return lax.dot_general(a, b, dims, preferred_element_type=F32)


def lanes(shape):
    return lax.broadcasted_iota(jnp.int32, shape, 1)


def split3(x):
    hi = x.astype(BF).astype(F32)
    mid = (x - hi).astype(BF).astype(F32)
    return hi, mid, x - hi - mid


def partner(x):
    width = x.shape[1]
    first = lanes(x.shape) % HD < HD // 2
    return jnp.where(first, pltpu.roll(x, width - HD // 2, 1), pltpu.roll(x, HD // 2, 1))


STEP = 64


def angle_tables(length):
    half = HD // 2
    lane = lax.optimization_barrier(lax.iota(jnp.int32, 2 * HD))
    freqs = 10000.0 ** (-((lane % half).astype(F32) * 2.0 / HD))
    sign = jnp.where(lane % HD < half, -1.0, 1.0)

    def table(positions):
        angles = positions[:, None] * freqs[None, :]
        return jnp.stack([jnp.cos(angles), jnp.sin(angles)])

    return table(lax.iota(F32, length // STEP) * STEP), table(lax.iota(F32, STEP)), sign[None, :]


def differ(a, b, bits):
    return sum(lax.rem(a // (1 << k) + b // (1 << k), 2) * (1 << k) for k in range(bits))


def remote(src, dst, send, recv, **to):
    return pltpu.make_async_remote_copy(
        src_ref=src, dst_ref=dst, send_sem=send, recv_sem=recv, device_id=to, device_id_type=MESH
    )


def ring(n, step):
    return lax.rem(lax.axis_index("tensor") + step, n)


def same_core(s, chips):
    me = lax.axis_index("dp")
    return differ(me // 2, s, chips.bit_length() - 1) * 2 + lax.rem(me, 2)


def sibling():
    me = lax.axis_index("dp")
    return me + 1 - 2 * lax.rem(me, 2)


def greet(n, chips, both_cores=False):
    barrier = pltpu.get_barrier_semaphore()
    if both_cores:
        pl.semaphore_signal(barrier, inc=1, device_id={"dp": sibling()}, device_id_type=MESH)
    for step in range(1, n):
        pl.semaphore_signal(barrier, inc=1, device_id={"tensor": ring(n, step)}, device_id_type=MESH)
    for s in range(1, chips):
        pl.semaphore_signal(
            barrier, inc=1, device_id={"dp": same_core(s, chips)}, device_id_type=MESH
        )
    pl.semaphore_wait(barrier, n + chips - 2 + both_cores)


def front_kernel(
    n, chips, chunks, limit_ref, tokens_ref, ct_ref, gain_ref, shift_ref, coarse_ref, fine_ref, sign_ref,
    wq_ref, wk_ref, wv_ref, gate_ref, up_ref, down_ref, wo_ref,
    ctx_ref, lse_ref, q_out, k_out, v_out, cos_out, sin_out, rows_ref, gb_all, w_all, out_ref, wo_z, wo_all,
    landed, gb, columns, own_w, wqkv, q_ref, k_ref, v_ref, cos_ref, sin_ref,
    right_send, right_recv, left_send, left_recv, gs_send, gs_recv, gr_send, gr_recv, rows_sem,
    wr_send, wr_recv, wl_send, wl_recv, send_sem, recv_sem, wz_send, wz_recv, ws_send, ws_recv,
    wx_send, wx_recv, cut_sem, load_sem, save_sem, keep_sem,
):
    i = pl.program_id(0)
    steps = pl.num_programs(0)
    me = lax.axis_index("tensor")
    place = lax.axis_index("dp")
    core = lax.rem(place, 2)
    bits = chips.bit_length() - 1
    rows, depth = tokens_ref.shape
    heads = q_ref.shape[0]
    piece = rows // chunks
    limit = limit_ref[0]
    s = i // heads
    h = lax.rem(i, heads)

    def over(shard, d, c, send, recv, to):
        part = landed.at[shard, pl.ds(c * piece, piece)]
        return remote(part, part, send.at[d, c], recv.at[d, c], tensor=to)

    def rightward(d, c):
        return over(me - d, d, c, right_send, right_recv, me + 1)

    def leftward(d, c):
        return over(me + d, d, c, left_send, left_recv, me - 1)

    def from_left(d, c):
        return over(me - d, d - 1, c, right_send, right_recv, me - 1)

    def from_right(d, c):
        return over(me + d, d - 1, c, left_send, left_recv, me + 1)

    def weights(shard, d, k, send, recv, to):
        there = w_all.at[k, shard]
        return remote(there if d else own_w.at[k], there, send.at[d, k], recv.at[d, k], tensor=to)

    def w_right(d, k):
        return weights(me - d, d, k, wr_send, wr_recv, me + 1)

    def w_left(d, k):
        return weights(me + d, d, k, wl_send, wl_recv, me - 1)

    def w_from_left(d, k):
        return weights(me - d, d - 1, k, wr_send, wr_recv, me - 1)

    def w_from_right(d, k):
        return weights(me + d, d - 1, k, wl_send, wl_recv, me + 1)

    def spread_gb(c):
        return remote(
            gb, gb_all.at[place // 2, core], gs_send.at[c], gs_recv.at[c], dp=same_core(c, chips)
        )

    def relay_gb(c):
        there = gb_all.at[differ(place // 2, c, bits), core]
        return remote(there if c else gb, there, gr_send.at[c], gr_recv.at[c], dp=sibling())

    def wo_over(step):
        return remote(
            wo_ref, wo_z.at[me], wz_send.at[step], wz_recv.at[step], tensor=ring(n, step + 1)
        )

    def spread_wo(c):
        return remote(
            wo_z, wo_all.at[:, place], ws_send.at[c], ws_recv.at[c], dp=same_core(c, chips)
        )

    def relay_wo(c):
        there = wo_all.at[:, differ(place // 2, c, bits) * 2 + core]
        return remote(there if c else wo_z, there, wx_send.at[c], wx_recv.at[c], dp=sibling())

    def push(step):
        owner = ring(n, step + 1)
        return remote(
            ctx_ref.at[pl.ds(pl.multiple_of(owner * rows, rows), rows)], out_ref.at[me],
            send_sem.at[step], recv_sem.at[step], tensor=owner,
        )

    def save(shard):
        return pltpu.make_async_copy(landed.at[shard], rows_ref.at[shard], rows_sem.at[shard])

    mine = pl.ds(pl.multiple_of(me * rows, rows), rows)
    keeps = [
        pltpu.make_async_copy(gb, gb_all.at[place // 2, core], keep_sem.at[0]),
        pltpu.make_async_copy(wo_ref, wo_z.at[me], keep_sem.at[1]),
        pltpu.make_async_copy(wo_z, wo_all.at[:, place], keep_sem.at[2]),
        pltpu.make_async_copy(ctx_ref.at[mine], out_ref.at[me], keep_sem.at[3]),
        pltpu.make_async_copy(own_w, w_all.at[:, me], keep_sem.at[4]),
    ]
    saves = [
        pltpu.make_async_copy(a, b, save_sem.at[j])
        for j, (a, b) in enumerate(
            ((q_ref, q_out), (k_ref, k_out), (v_ref, v_out), (cos_ref, cos_out), (sin_ref, sin_out))
        )
    ]

    @pl.when(i == 0)
    def _():
        loads = [
            pltpu.make_async_copy(ref, wqkv.at[j], load_sem.at[j])
            for j, ref in enumerate((wq_ref, wk_ref, wv_ref))
        ]
        share = own_w.shape[1]
        ours = pl.ds(pl.multiple_of(place * share, share), share)
        cuts = [pltpu.make_async_copy(down_ref.at[ours], own_w.at[2], cut_sem.at[2])]
        for k, ref in enumerate((gate_ref, up_ref)):
            src = ref if share % 128 else ref.at[:, ours]
            cuts.append(pltpu.make_async_copy(src, columns.at[k], cut_sem.at[k]))
        for copy in loads + cuts:
            copy.start()

        barrier = pltpu.get_barrier_semaphore()
        for step in range(1, n):
            to = ring(n, step)
            pl.semaphore_signal(barrier, inc=1, device_id={"tensor": to}, device_id_type=MESH)
        pl.semaphore_signal(barrier, inc=1, device_id={"dp": sibling()}, device_id_type=MESH)
        for c in range(1, chips):
            to = same_core(c, chips)
            pl.semaphore_signal(barrier, inc=1, device_id={"dp": to}, device_id_type=MESH)

        values = tokens_ref[...].astype(F32)
        values = values - jnp.mean(values, axis=1, keepdims=True)
        inverse = lax.rsqrt(jnp.mean(values * values, axis=1, keepdims=True) + EPS)
        landed[me] = (values * inverse * gain_ref[...] + shift_ref[...]).astype(BF)

        pl.semaphore_wait(barrier, n - 1 + chips)

        for c in range(chunks):

            @pl.when(me < n - 1)
            def _():
                rightward(0, c).start()

            @pl.when(me > 0)
            def _():
                leftward(0, c).start()

        row = me * rows + lax.broadcasted_iota(jnp.int32, (rows, depth), 0)
        gb[...] = jnp.where(row < limit, ct_ref[...].astype(F32), 0.0).astype(BF)
        for c in range(1, chips):
            spread_gb(c).start()
        relay_gb(0).start()
        keeps[0].start()
        keeps[1].start()
        for copy in loads:
            copy.wait()

        lane = lanes((rows, 128))
        ones = jnp.where(lane < HD + 3, 1.0, 0.0)
        unit = jnp.where(lane == HD + 3, 1.0, 0.0)

        def put(out, here, values, extra):
            for head in range(heads):
                own = values[:, head // 2 * 128 : head // 2 * 128 + 128]
                own = pltpu.roll(own, HD, 1) if head % 2 else own
                out[head, here, :] = jnp.where(lane < HD, own, extra).astype(BF)

        def project(shard):
            here = pl.ds(pl.multiple_of(shard * rows, rows), rows)
            for j in range(rows // STEP):
                part = pl.ds(pl.multiple_of(shard * rows + j * STEP, STEP), STEP)
                coarse = pl.ds(shard * (rows // STEP) + j, 1)
                c0, s0 = coarse_ref[0, coarse, :], coarse_ref[1, coarse, :]
                cos_ref[part, :] = c0 * fine_ref[0] - s0 * fine_ref[1]
                sin_ref[part, :] = (s0 * fine_ref[0] + c0 * fine_ref[1]) * sign_ref[...]
            cosine = jnp.tile(cos_ref[here, :], (1, heads // 2))
            sine = jnp.tile(sin_ref[here, :], (1, heads // 2))
            x = landed[shard]
            row = shard * rows + lax.broadcasted_iota(jnp.int32, (rows, 128), 0)
            bias = jnp.where(lane == HD + 3, jnp.where(row < limit, 0.0, -1e30), ones)
            raw = dot(x, wqkv[0])
            turned = (raw * cosine + partner(raw) * sine).astype(BF).astype(F32)
            put(q_ref, here, turned * SCALE, unit)
            raw = dot(x, wqkv[1])
            put(k_ref, here, raw * cosine + partner(raw) * sine, bias)
            put(v_ref, here, dot(x, wqkv[2]), ones)

        for d in range(1, n + 1):
            for c in range(chunks):
                if d < n:

                    @pl.when(me >= d)
                    def _():
                        from_left(d, c).wait_recv()

                    @pl.when((me >= d) & (me < n - 1))
                    def _():
                        rightward(d, c).start()

                    @pl.when(me + d < n)
                    def _():
                        from_right(d, c).wait_recv()

                    @pl.when((me + d < n) & (me > 0))
                    def _():
                        leftward(d, c).start()

                if c == 0:

                    @pl.when(me >= d - 1)
                    def _():
                        save(me - d + 1).start()
                        project(me - d + 1)

                if c == 1 and d > 1:

                    @pl.when(me + d - 1 < n)
                    def _():
                        save(me + d - 1).start()
                        project(me + d - 1)

                if c == 2 and d == 1:
                    for cut in cuts:
                        cut.wait()
                    for k in range(2):
                        own_w[k] = columns[k].astype(F32).T.astype(BF)
                    keeps[4].start()

                if c == chunks - 1 and d == 2:
                    for near in range(1, chips // 2 + 1):
                        spread_gb(near).wait_recv()
                        relay_gb(near).start()

            if d < n:

                @pl.when((me < n - 1) & (me + 1 == d))
                def _():
                    for k in range(3):
                        w_right(0, k).start()

                @pl.when((me > 0) & (n - me == d))
                def _():
                    for k in range(3):
                        w_left(0, k).start()

        for copy in saves:
            copy.start()
        for step in range(n - 1):
            wo_over(step).start()
        for far in range(chips // 2 + 1, chips):
            spread_gb(far).wait_recv()
            relay_gb(far).start()

    stride = max((heads * n - 2) // max(n - 2, 1), 1)
    for d in range(1, n - 1):

        @pl.when(i == 1 + (d - 1) * stride)
        def _():
            for k in range(3):

                @pl.when((me >= d) & (me < n - 1))
                def _():
                    w_from_left(d, k).wait_recv()
                    w_right(d, k).start()

                @pl.when((me + d < n) & (me > 0))
                def _():
                    w_from_right(d, k).wait_recv()
                    w_left(d, k).start()

    @pl.when(i == heads)
    def _():
        for step in range(n - 1):
            wo_over(step).wait()
        keeps[1].wait()
        for c in range(1, chips):
            spread_wo(c).start()
        relay_wo(0).start()
        keeps[2].start()

    @pl.when(i == (n - 1) * heads)
    def _():
        for c in range(1, chips):
            spread_wo(c).wait_recv()
            relay_wo(c).start()

    owner = ring(n, s + 1)
    block = pl.ds(pl.multiple_of(owner * rows, rows), rows)
    scores = dot(q_ref[h, block, :], k_ref[h], NT)
    peak = jnp.max(scores, axis=1, keepdims=True)
    acc = dot(jnp.exp(scores - peak).astype(BF), v_ref[h])
    lane = lanes((rows, 128))
    total = jnp.sum(jnp.where(lane == HD, acc, 0.0), axis=1, keepdims=True)
    out = acc * (1.0 / total)
    odd = lax.rem(h, 2)
    out = jnp.where(odd == 1, pltpu.roll(out, HD, 1), out).astype(BF)
    pair = pl.ds(pl.multiple_of(h // 2 * 128, 128), 128)
    ctx_ref[block, pair] = jnp.where((lane >= HD) == (odd == 1), out, ctx_ref[block, pair])
    lse_ref[block, :] = jnp.where(lane == h, peak + jnp.log(total), lse_ref[block, :])

    @pl.when((h == heads - 1) & (s < n - 1))
    def _():
        push(s).start()

    @pl.when(i == steps - 1)
    def _():
        keeps[3].start()
        for d in range(n - 1):
            for c in range(chunks):

                @pl.when((me >= d) & (me < n - 1))
                def _():
                    rightward(d, c).wait_send()

                @pl.when((me + d < n) & (me > 0))
                def _():
                    leftward(d, c).wait_send()

            for k in range(3):

                @pl.when((me >= d) & (me < n - 1))
                def _():
                    w_right(d, k).wait_send()

                @pl.when((me + d < n) & (me > 0))
                def _():
                    w_left(d, k).wait_send()

        for k in range(3):
            for d in range(1, n):

                @pl.when((me >= d) & ((me == n - 1) | (d == n - 1)))
                def _():
                    w_from_left(d, k).wait_recv()

                @pl.when((me + d < n) & ((me == 0) | (d == n - 1)))
                def _():
                    w_from_right(d, k).wait_recv()

        for c in range(chips):
            relay_gb(c).wait()
            relay_wo(c).wait()
            if c:
                spread_gb(c).wait_send()
                spread_wo(c).wait_send()
        for shard in range(n):
            save(shard).wait()
        for copy in saves:
            copy.wait()
        for step in range(n - 1):
            push(step).wait()
        for j in (0, 2, 3, 4):
            keeps[j].wait()


def front(
    tokens, cotangent, gain, shift, tables, w_query, w_key, w_value, gate, up, down, w_out, limit, n, devices
):
    rows, depth = tokens.shape
    total = n * rows
    width = w_query.shape[1]
    heads = width // HD
    chips = devices // 2
    chunks = 4
    place = lax.axis_index("dp")
    share = down.shape[0] // devices
    part = width // devices
    if share % 128:
        gate, up = (lax.dynamic_slice_in_dim(w, place * share, share, 1) for w in (gate, up))
    hbm = pl.BlockSpec(memory_space=pl.ANY)

    def whole(*shape):
        return pl.BlockSpec(shape, lambda *_: (0,) * len(shape), pipeline_mode=pl.Buffered(1))

    def dma(*shape):
        return pltpu.SemaphoreType.DMA(shape)

    head_array = jax.ShapeDtypeStruct((heads, total, 128), BF)
    table = jax.ShapeDtypeStruct((total, 128), F32)
    coarse, fine, sign = tables
    return pl.pallas_call(
        functools.partial(front_kernel, n, chips, chunks),
        out_shape=(
            jax.ShapeDtypeStruct((total, width), BF),
            table,
            head_array, head_array, head_array, table, table,
            jax.ShapeDtypeStruct((n, rows, depth), BF),
            jax.ShapeDtypeStruct((chips, 2, rows, depth), BF),
            jax.ShapeDtypeStruct((3, n, share, depth), BF),
            jax.ShapeDtypeStruct((n, rows, width), BF),
            jax.ShapeDtypeStruct((n, part, depth), BF),
            jax.ShapeDtypeStruct((n, devices, part, depth), BF),
        ),
        grid_spec=pltpu.PrefetchScalarGridSpec(
            num_scalar_prefetch=0,
            grid=(n * heads,),
            in_specs=[pl.BlockSpec(memory_space=pltpu.SMEM)]
            + [whole(rows, depth)] * 2
            + [whole(1, depth)] * 2
            + [whole(*coarse.shape), whole(*fine.shape), whole(*sign.shape)]
            + [hbm] * 7,
            out_specs=[whole(total, width), whole(total, 128)] + [hbm] * 11,
            scratch_shapes=[
                pltpu.VMEM((n, rows, depth), BF),
                pltpu.VMEM((rows, depth), BF),
                pltpu.VMEM((2, depth, share), BF),
                pltpu.VMEM((3, share, depth), BF),
                pltpu.VMEM((3, depth, width), BF),
            ]
            + [pltpu.VMEM((heads, total, 128), BF)] * 3
            + [pltpu.VMEM((total, 128), F32)] * 2
            + [dma(n - 1, chunks)] * 4
            + [dma(chips)] * 4
            + [dma(n)]
            + [dma(n - 1, 3)] * 4
            + [dma(n - 1)] * 4
            + [dma(chips)] * 4
            + [dma(3), dma(3), dma(5), dma(5)],
        ),
        compiler_params=pltpu.CompilerParams(
            vmem_limit_bytes=52 << 20, collective_id=1, has_side_effects=True
        ),
        cost_estimate=pl.CostEstimate(
            flops=4 * total * total * 256 * heads * 3, bytes_accessed=40 << 20, transcendentals=0
        ),
        name="front",
    )(
        limit, tokens, cotangent, gain.reshape(1, depth), shift.reshape(1, depth), coarse, fine, sign,
        w_query, w_key, w_value, gate, up, down,
        lax.dynamic_slice_in_dim(w_out, place * part, part, 0),
    )


def att_bwd_kernel(
    n, bk, chips, ga_ref, wo_ref, cown_ref, parts_ref, q_ref, k_ref, v_ref, ctx_ref, lse_ref,
    cos_ref, sin_ref, pk_ref, own_ref, sums_ref, og_ref, do, gc, dka, dva, dqs,
    og_full, og_own, og_mate, og_sib, og_land, og_piece, og_z,
    send_sem, recv_sem, out_send, out_recv, pk_send, pk_recv, keep_sem,
    om_send, om_recv, op_send, op_recv, oz_send, oz_recv,
):
    i = pl.program_id(0)
    heads, total, _ = k_ref.shape
    h = jnp.where(i < heads, i, (i - heads) // (n - 1))
    t = jnp.where(i < heads, 0, lax.rem(i - heads, n - 1) + 1)
    rows = total // n
    me = lax.axis_index("tensor")
    place = lax.axis_index("dp")
    core = lax.rem(place, 2)
    bits = chips.bit_length() - 1
    share = og_ref.shape[0]
    mine = pl.ds(pl.multiple_of(me * rows, rows), rows)

    def push(step):
        return remote(
            gc.at[step], do.at[mine], send_sem.at[step], recv_sem.at[step], tensor=ring(n, step + 1)
        )

    def push_out(s):
        return remote(
            parts_ref.at[s], sums_ref.at[s - 1], out_send.at[s - 1], out_recv.at[s - 1],
            dp=same_core(s, chips),
        )

    def columns(slot):
        return pl.ds(pl.multiple_of(slot * 128, 128), 128)

    def push_pack(slot, step):
        owner = ring(n, step + 1)
        return remote(
            pk_ref.at[pl.ds(pl.multiple_of(owner * rows, rows), rows), columns(slot)],
            own_ref.at[me, :, columns(slot)],
            pk_send.at[slot, step], pk_recv.at[slot, step], tensor=owner,
        )

    def keep(slot):
        return pltpu.make_async_copy(
            pk_ref.at[mine, columns(slot)], own_ref.at[me, :, columns(slot)], keep_sem.at[slot]
        )

    @pl.when(i == 0)
    def _():
        greet(n, chips, True)

        def send(step, carry):
            gc[step] = dot(ga_ref[...], wo_ref[ring(n, step + 1)], NT).astype(BF)
            push(step).start()
            return carry

        lax.fori_loop(0, n - 1, send, 0)
        do[mine, :] = dot(ga_ref[...], wo_ref[me], NT).astype(BF)

    def og_swap():
        return remote(og_mate, og_sib, om_send, om_recv, dp=sibling())

    def og_push(s):
        return remote(og_sib.at[s], og_land.at[s], op_send.at[s], op_recv.at[s], dp=same_core(s, chips))

    def og_over(step):
        to = ring(n, step + 1)
        return remote(og_piece.at[to], og_z.at[me], oz_send.at[step], oz_recv.at[step], tensor=to)

    @pl.when(i == 1)
    def _():
        def term(part, carry):
            og_full[...] = dot(cown_ref[part], ga_ref[...], TN)
            for s in range(chips):
                start = differ(place // 2, s, bits) * 2
                here = pl.ds(pl.multiple_of((start + core) * share, share), share)
                there = pl.ds(pl.multiple_of((start + 1 - core) * share, share), share)
                og_own[s, part] = og_full[here, :]
                og_mate[s, part] = og_full[there, :].astype(BF)
            return carry

        lax.fori_loop(0, n, term, 0)
        og_swap().start()

    @pl.when(i == 2)
    def _():
        og_swap().wait_recv()
        for s in range(chips):
            og_sib[s] = (og_own[s] + og_sib[s].astype(F32)).astype(BF)
            if s:
                og_push(s).start()

    @pl.when(i == heads + 2)
    def _():
        joined = og_sib[0].astype(F32)
        for s in range(1, chips):
            og_push(s).wait_recv()
            joined = joined + og_land[s].astype(F32)
        og_piece[...] = joined.astype(BF)
        for step in range(n - 1):
            og_over(step).start()
        for s in range(1, chips):
            push_out(s).start()

    @pl.when(i == heads * n - 1)
    def _():
        og_z[me] = og_piece[me]
        for step in range(n - 1):
            og_over(step).wait_recv()
        joined = og_z[0].astype(F32)
        for part in range(1, n):
            joined = joined + og_z[part].astype(F32)
        og_ref[...] = joined.astype(BF)

    @pl.when((h == 0) & (t > 0))
    def _():
        push(t - 1).wait_recv()

    source = ring(n, n - t)
    block = pl.ds(pl.multiple_of(source * rows, rows), rows)
    pair = columns(h // 2)
    odd = lax.rem(h, 2) == 1
    lane = lanes((rows, 128))
    off = lane - HD
    logsum = jnp.sum(jnp.where(lane == h, lse_ref[block, :], 0.0), axis=1, keepdims=True)
    a, b, c = split3(-logsum)
    q = q_ref[h, block, :].astype(F32)
    q = jnp.where(off == 0, a, jnp.where(off == 1, b, jnp.where(off == 2, c, q))).astype(BF)
    g = jnp.where((lane >= HD) == odd, do[block, pair].astype(F32), 0.0)
    delta = jnp.sum(g * ctx_ref[block, pair].astype(F32), axis=1, keepdims=True)
    a, b, c = split3(-delta)
    g = jnp.where(odd, pltpu.roll(g, HD, 1), g)
    g = jnp.where(off == 0, a, jnp.where(off == 1, b, jnp.where(off == 2, c, g))).astype(BF)
    acc = jnp.zeros((rows, 128), F32)
    for j in range(total // bk):
        rk = pl.ds(j * bk, bk)
        kt = k_ref[h, rk, :]
        probs = jnp.exp(dot(kt, q, NT))
        grad = (probs * dot(v_ref[h, rk, :], g, NT)).astype(BF)
        for sums, term in ((dva, dot(probs.astype(BF), g)), (dka, dot(grad, q))):
            before = jnp.where(t == 0, jnp.zeros_like(term), sums[h, rk, :])
            sums[h, rk, :] = before + term
        acc = acc + dot(grad, kt, TN)
    acc = acc * SCALE

    @pl.when(jnp.logical_not(odd))
    def _():
        dqs[block, :] = acc

    @pl.when(odd)
    def _():
        grad = jnp.where(lane < HD, dqs[block, :], pltpu.roll(acc, HD, 1))
        grad = grad * cos_ref[block, :] - partner(grad) * sin_ref[block, :]
        pk_ref[block, columns(heads + h // 2)] = grad.astype(BF)

    @pl.when(odd & (t == 0))
    def _():
        keep(heads + h // 2).start()

    @pl.when(odd & (t > 0))
    def _():
        push_pack(heads + h // 2, n - 1 - t).start()

    @pl.when(t == n - 1)
    def _():
        dk = dka[h]
        dk = dk * cos_ref[...] - partner(dk) * sin_ref[...]
        both = jnp.where(lanes((total, 128)) < HD, dk, pltpu.roll(dva[h], HD, 1))
        pk_ref[:, columns(h)] = both.astype(BF)
        for step in range(n - 1):
            push_pack(h, step).start()
        keep(h).start()

    @pl.when(i == heads * n - 1)
    def _():
        for step in range(n - 1):
            push(step).wait_send()
        for s in range(1, chips):
            push_out(s).wait()
        og_swap().wait_send()
        for s in range(1, chips):
            og_push(s).wait_send()
        for step in range(n - 1):
            og_over(step).wait_send()
        for slot in range(heads + heads // 2):
            keep(slot).wait()
            for step in range(n - 1):
                push_pack(slot, step).wait()


def att_bwd(grad_attn, w_out, ctx_own, parts, q, k, v, ctx, lse, cosine, sine, n, bk=512):
    heads, total, _ = q.shape
    width = heads * HD
    rows, depth = grad_attn.shape
    chips = parts.shape[0]
    share = width // (2 * chips)
    slots = heads + heads // 2
    hbm = pl.BlockSpec(memory_space=pl.ANY)

    def whole(*shape):
        return pl.BlockSpec(shape, lambda *_: (0,) * len(shape), pipeline_mode=pl.Buffered(1))

    return pl.pallas_call(
        functools.partial(att_bwd_kernel, n, bk, chips),
        out_shape=(
            jax.ShapeDtypeStruct((total, slots * 128), BF),
            jax.ShapeDtypeStruct((n, rows, slots * 128), BF),
            jax.ShapeDtypeStruct((chips - 1, rows, depth), BF),
            jax.ShapeDtypeStruct((share, depth), BF),
        ),
        grid_spec=pltpu.PrefetchScalarGridSpec(
            num_scalar_prefetch=0,
            grid=(heads * n,),
            in_specs=[whole(rows, depth), whole(n, width, depth), whole(n, rows, width), hbm]
            + [whole(heads, total, 128)] * 3
            + [whole(total, width)]
            + [whole(total, 128)] * 3,
            out_specs=[whole(total, slots * 128), hbm, hbm, whole(share, depth)],
            scratch_shapes=[
                pltpu.VMEM((total, width), BF),
                pltpu.VMEM((n - 1, rows, width), BF),
            ]
            + [pltpu.VMEM((heads, total, 128), F32)] * 2
            + [pltpu.VMEM((total, 128), F32)]
            + [
                pltpu.VMEM((width, depth), F32),
                pltpu.VMEM((chips, n, share, depth), F32),
                pltpu.VMEM((chips, n, share, depth), BF),
                pltpu.VMEM((chips, n, share, depth), BF),
                pltpu.VMEM((chips, n, share, depth), BF),
                pltpu.VMEM((n, share, depth), BF),
                pltpu.VMEM((n, share, depth), BF),
            ]
            + [pltpu.SemaphoreType.DMA((n - 1,))] * 2
            + [pltpu.SemaphoreType.DMA((chips - 1,))] * 2
            + [pltpu.SemaphoreType.DMA((slots, n - 1))] * 2
            + [pltpu.SemaphoreType.DMA((slots,))]
            + [pltpu.SemaphoreType.DMA] * 2
            + [pltpu.SemaphoreType.DMA((chips,))] * 2
            + [pltpu.SemaphoreType.DMA((n - 1,))] * 2,
        ),
        compiler_params=pltpu.CompilerParams(
            vmem_limit_bytes=56 << 20, collective_id=2, has_side_effects=True
        ),
        cost_estimate=pl.CostEstimate(
            flops=10 * total * total * 256 * heads,
            bytes_accessed=20 * total * width,
            transcendentals=total * total * heads,
        ),
        name="att_bwd",
    )(grad_attn, w_out, ctx_own, parts, q, k, v, ctx, lse, cosine, sine)


def finish_kernel(
    chips, n, width, x_ref, pk_ref, own_ref, w_ref, tokens_ref, middle_ref, gain_ref, vec_ref,
    input_ref, q_ref, k_ref, v_ref, sums_ref,
    full, mate, sib, land, fin, every, vec_z, vec_dp, vec_me,
    sx_send, sx_recv, rs_send, rs_recv, ag_send, ag_recv, rl_send, rl_recv,
    vz_send, vz_recv, vd_send, vd_recv, own_sem,
):
    bits = chips.bit_length() - 1
    me = lax.axis_index("dp")
    place = lax.axis_index("tensor")
    core = lax.rem(me, 2)
    chip = me // 2
    other = 1 - core
    heads = width // HD
    piece = fin.shape[0]

    def swap(s):
        return remote(mate.at[s], sib.at[s], sx_send.at[s], sx_recv.at[s], dp=chip * 2 + other)

    def push(s):
        return remote(sib.at[s], land.at[s], rs_send.at[s], rs_recv.at[s], dp=same_core(s, chips))

    def spread(s):
        return remote(
            fin, every.at[chip, core], ag_send.at[s], ag_recv.at[s], dp=same_core(s, chips)
        )

    def relay(s):
        src = every.at[differ(chip, s, bits), core]
        return remote(src, src, rl_send.at[s], rl_recv.at[s], dp=chip * 2 + other)

    def vec_over(step):
        return remote(
            vec_me.at[0], vec_z.at[place], vz_send.at[step], vz_recv.at[step], tensor=ring(n, step + 1)
        )

    def vec_across(step):
        return remote(
            vec_me.at[1], vec_dp.at[me], vd_send.at[step], vd_recv.at[step],
            dp=lax.rem(me + step + 1, 2 * chips),
        )

    barrier = pltpu.get_barrier_semaphore()
    for step in range(n - 1):
        pl.semaphore_signal(barrier, inc=1, device_id={"tensor": ring(n, step + 1)}, device_id_type=MESH)
    for step in range(2 * chips - 1):
        to = lax.rem(me + step + 1, 2 * chips)
        pl.semaphore_signal(barrier, inc=1, device_id={"dp": to}, device_id_type=MESH)

    full[...] = dot(x_ref[...], pk_ref[...], TN)
    pl.semaphore_wait(barrier, n + 2 * chips - 2)

    def part(s, which):
        start = (differ(chip, s, bits) * 2 + which) * piece
        return full[pl.ds(pl.multiple_of(start, piece), piece), :]

    for s in range(chips):
        mate[s] = part(s, other).astype(BF)
        swap(s).start()

    grad = jnp.zeros(input_ref.shape, F32)
    for t in range(n):
        w = w_ref[:, t].reshape(w_ref.shape[0] * w_ref.shape[2], w_ref.shape[3])
        grad = grad + dot(own_ref[t], w, NT).astype(BF).astype(F32)

    for s in range(1, chips):
        swap(s).wait_recv()
        sib[s] = (sib[s].astype(F32) + part(s, core)).astype(BF)
        push(s).start()
    swap(0).wait_recv()
    total = sib[0].astype(F32) + part(0, core)

    values = tokens_ref[...].astype(F32)
    values = values - jnp.mean(values, axis=1, keepdims=True)
    inverse = lax.rsqrt(jnp.mean(values * values, axis=1, keepdims=True) + EPS)
    scaled = values * inverse
    through = grad * gain_ref[...]
    inner = through - jnp.mean(through, axis=1, keepdims=True)
    inner = inner - scaled * jnp.mean(through * scaled, axis=1, keepdims=True)
    input_ref[...] = middle_ref[...] + inverse * inner
    vec_me[0, 0:1] = jnp.sum(grad * scaled, axis=0, keepdims=True)
    vec_me[0, 1:2] = jnp.sum(grad, axis=0, keepdims=True)
    vec_me[0, 2:4] = vec_ref[...]
    vec_me[0, 4:8] = jnp.zeros((4, vec_ref.shape[1]), F32)
    vec_z[place] = vec_me[0]
    for step in range(n - 1):
        vec_over(step).start()

    for s in range(1, chips):
        push(s).wait_recv()
        total = total + land[s].astype(F32)
    fin[...] = total.astype(BF)
    for s in range(1, chips):
        spread(s).start()
    mine = pltpu.make_async_copy(fin, every.at[chip, core], own_sem)
    mine.start()
    mine.wait()
    relay(0).start()

    for step in range(n - 1):
        vec_over(step).wait()
    vec = vec_z[0]
    for t in range(1, n):
        vec = vec + vec_z[t]
    vec_me[1] = vec
    vec_dp[me] = vec
    for step in range(2 * chips - 1):
        vec_across(step).start()
    for s in range(1, chips):
        spread(s).wait_recv()
        relay(s).start()
    for step in range(2 * chips - 1):
        vec_across(step).wait()
    vec = vec_dp[0]
    for t in range(1, 2 * chips):
        vec = vec + vec_dp[t]
    sums_ref[...] = vec
    for s in range(chips):
        relay(s).wait()
        swap(s).wait_send()
        if s > 0:
            spread(s).wait_send()
            push(s).wait_send()
    first = lanes((piece, 128)) < HD
    for d in range(2 * chips):
        rows = slice(d * piece, (d + 1) * piece)
        g = every[d // 2, d % 2].astype(F32)
        for pair in range(heads // 2):
            a = g[:, pair * 256 : pair * 256 + 128]
            b = g[:, pair * 256 + 128 : pair * 256 + 256]
            out = slice(pair * 128, pair * 128 + 128)
            q_ref[rows, out] = g[:, (heads + pair) * 128 : (heads + pair + 1) * 128]
            k_ref[rows, out] = jnp.where(first, a, pltpu.roll(b, HD, 1))
            v_ref[rows, out] = jnp.where(first, pltpu.roll(a, HD, 1), b)


def finish(rows_all, packed, own, w_all, tokens, middle, gain, vec, width, devices):
    n, rows, packs = own.shape
    depth = tokens.shape[1]
    chips = devices // 2
    piece = depth // devices
    vmem = pl.BlockSpec(memory_space=pltpu.VMEM)
    out = jax.ShapeDtypeStruct((depth, width), F32)
    return pl.pallas_call(
        functools.partial(finish_kernel, chips, n, width),
        out_shape=(
            jax.ShapeDtypeStruct((rows, depth), F32), out, out, out,
            jax.ShapeDtypeStruct((8, depth), F32),
        ),
        in_specs=[vmem] * 8,
        out_specs=[vmem] * 5,
        scratch_shapes=[
            pltpu.VMEM((depth, packs), F32),
            pltpu.VMEM((chips, piece, packs), BF),
            pltpu.VMEM((chips, piece, packs), BF),
            pltpu.VMEM((chips, piece, packs), BF),
            pltpu.VMEM((piece, packs), BF),
            pltpu.VMEM((chips, 2, piece, packs), BF),
            pltpu.VMEM((n, 8, depth), F32),
            pltpu.VMEM((devices, 8, depth), F32),
            pltpu.VMEM((2, 8, depth), F32),
        ]
        + [pltpu.SemaphoreType.DMA((chips,))] * 8
        + [pltpu.SemaphoreType.DMA((n - 1,))] * 2
        + [pltpu.SemaphoreType.DMA((devices - 1,))] * 2
        + [pltpu.SemaphoreType.DMA],
        compiler_params=pltpu.CompilerParams(
            vmem_limit_bytes=56 << 20, collective_id=4, has_side_effects=True
        ),
        cost_estimate=pl.CostEstimate(
            flops=4 * n * rows * depth * packs, bytes_accessed=20 << 20, transcendentals=0
        ),
        name="finish",
    )(rows_all, packed, own, w_all, tokens, middle, gain.reshape(1, depth), vec)


def ffn_kernel(
    chips, x_ref, gb_ref, w_ref, wp_ref, dx_ref, out_ref, dw_ref, wp_z,
    rows_all, gb, hid, gate_g, up_g, own, sib, mate,
    ag_send, ag_recv, rl_send, rl_recv, sx_send, sx_recv, rs_send, rs_recv, fw_send, fw_recv,
    gb_sem, out_sem, dx_sem, wp_send, wp_recv, wp_sem,
):
    bits = chips.bit_length() - 1
    me = lax.axis_index("dp")
    core = lax.rem(me, 2)
    chip = me // 2
    other = 1 - core
    rows, depth = x_ref.shape
    n = dw_ref.shape[0]
    share = dw_ref.shape[2]

    def spread(s):
        to = differ(chip, s, bits) * 2 + core
        return remote(x_ref, rows_all.at[chip, core], ag_send.at[s], ag_recv.at[s], dp=to)

    square = chips == 4

    def hand_on(s):
        half = pl.ds((s - 1) * (rows // 2), rows // 2)
        part = rows_all.at[differ(chip, s, bits), core, half]
        to = differ(chip, 3 - s, bits) * 2 + core
        return remote(part, part, fw_send.at[s], fw_recv.at[s], dp=to)

    def handed(s):
        half = pl.ds((s - 1) * (rows // 2), rows // 2)
        part = rows_all.at[differ(chip, 3, bits), core, half]
        to = differ(chip, 3 - s, bits) * 2 + core
        return remote(part, part, fw_send.at[s], fw_recv.at[s], dp=to)

    def relay(s):
        src = differ(chip, s, bits)
        return remote(
            rows_all.at[src, core], rows_all.at[src, core], rl_send.at[s], rl_recv.at[s],
            dp=chip * 2 + other,
        )

    def swap(s):
        return remote(
            mate.at[lax.rem(s, 2)], sib.at[s], sx_send.at[s], sx_recv.at[s], dp=chip * 2 + other
        )

    def push(s):
        to = differ(chip, s, bits) * 2 + core
        return remote(sib.at[s, 0], dx_ref.at[s], rs_send.at[s], rs_recv.at[s], dp=to)

    def fetch(s):
        src = differ(chip, s, bits)
        return pltpu.make_async_copy(gb_ref.at[src], gb.at[src], gb_sem.at[s])

    part = lax.axis_index("tensor")

    def over(step):
        return remote(
            wp_ref, wp_z.at[part], wp_send.at[step], wp_recv.at[step], tensor=ring(n, step + 1)
        )

    def keep(s):
        return pltpu.make_async_copy(sib.at[s, 1], out_ref.at[s], out_sem.at[s])

    for s in range(chips):
        fetch(s).start()
    barrier = pltpu.get_barrier_semaphore()
    for step in range(1, n):
        pl.semaphore_signal(barrier, inc=1, device_id={"tensor": ring(n, step)}, device_id_type=MESH)
    pl.semaphore_signal(barrier, inc=1, device_id={"dp": chip * 2 + other}, device_id_type=MESH)
    for s in range(1, chips):
        to = differ(chip, s, bits) * 2 + core
        pl.semaphore_signal(barrier, inc=1, device_id={"dp": to}, device_id_type=MESH)
    pl.semaphore_wait(barrier, chips + n - 1)
    direct = range(1, 3) if square else range(1, chips)
    for s in direct:
        spread(s).start()
    mine = pltpu.make_async_copy(x_ref, rows_all.at[chip, core], ag_send.at[0])
    mine.start()
    mine.wait()
    relay(0).start()
    for step in range(n - 1):
        over(step).start()
    keep_wp = pltpu.make_async_copy(wp_ref, wp_z.at[part], wp_sem)
    keep_wp.start()

    def shard(src, which, put):
        x = rows_all[src, which]
        grad = gb[src, which]
        gate = dot(x, w_ref[0], NT)
        upper = dot(x, w_ref[1], NT)
        grad_hidden = dot(grad, w_ref[2], NT)
        sigma = jax.nn.sigmoid(gate)
        act = gate * sigma
        hidden = (act * upper).astype(BF)
        grad_gate = (grad_hidden * upper * sigma * (1.0 + gate * (1.0 - sigma))).astype(BF)
        grad_upper = (grad_hidden * act).astype(BF)
        hid[src, which] = hidden
        gate_g[src, which] = grad_gate
        up_g[src, which] = grad_upper
        put[0] = (dot(grad_gate, w_ref[0]) + dot(grad_upper, w_ref[1])).astype(BF)
        put[1] = dot(hidden, w_ref[2]).astype(BF)

    def step(s, carry):
        src = differ(chip, s, bits)
        slot = lax.rem(s, 2)
        relay(s).wait_recv()
        fetch(s).wait()

        @pl.when(s >= 2)
        def _():
            swap(s - 2).wait_send()

        shard(src, other, mate.at[slot])
        swap(s).start()
        shard(src, core, own)
        swap(s).wait_recv()
        for k in range(2):
            sib[s, k] = (sib[s, k].astype(F32) + own[k].astype(F32)).astype(BF)

        @pl.when(s > 0)
        def _():
            push(s).start()

        keep(s).start()

        if square:

            @pl.when(s == 0)
            def _():
                for near in (1, 2):
                    spread(near).wait_recv()
                    hand_on(near).start()
                    relay(near).start()

        else:

            @pl.when(s < chips - 1)
            def _():
                spread(s + 1).wait_recv()
                relay(s + 1).start()

        if square:

            @pl.when(s == 1)
            def _():
                handed(1).wait_recv()
                handed(2).wait_recv()
                relay(3).start()

        return carry

    lax.fori_loop(0, chips, step, 0)
    first = pltpu.make_async_copy(sib.at[0, 0], dx_ref.at[0], dx_sem)
    first.start()
    for k, (left, right) in enumerate(((gate_g, rows_all), (up_g, rows_all), (hid, gb))):
        left = left[...].reshape(-1, n * share)
        grad = dot(left, right[...].reshape(-1, depth), TN)
        for t in range(n):
            dw_ref[t, k] = grad[t * share : (t + 1) * share, :].astype(BF)
    first.wait()
    keep_wp.wait()
    for step in range(n - 1):
        over(step).wait()
    for s in range(chips):
        keep(s).wait()
        relay(s).wait_send()
        if s >= chips - 2:
            swap(s).wait_send()
        if s in direct:
            spread(s).wait_send()
        if s > 0:
            push(s).wait()
    if square:
        hand_on(1).wait_send()
        hand_on(2).wait_send()


def ffn(x, grad_branch, weights, w_packed, n, devices):
    rows, depth = x.shape
    chips = devices // 2
    hidden = weights.shape[1]
    share = hidden // n
    vmem = pl.BlockSpec(memory_space=pltpu.VMEM)
    hbm = pl.BlockSpec(memory_space=pl.ANY)
    return pl.pallas_call(
        functools.partial(ffn_kernel, chips),
        out_shape=(
            jax.ShapeDtypeStruct((chips, rows, depth), BF),
            jax.ShapeDtypeStruct((chips, rows, depth), BF),
            jax.ShapeDtypeStruct((n, 3, share, depth), BF),
            jax.ShapeDtypeStruct((n, *w_packed.shape), BF),
        ),
        in_specs=[vmem, hbm, vmem, hbm],
        out_specs=[hbm, hbm, vmem, hbm],
        scratch_shapes=[
            pltpu.VMEM((chips, 2, rows, depth), BF),
            pltpu.VMEM((chips, 2, rows, depth), BF),
        ]
        + [pltpu.VMEM((chips, 2, rows, hidden), BF)] * 3
        + [
            pltpu.VMEM((2, rows, depth), BF),
            pltpu.VMEM((chips, 2, rows, depth), BF),
            pltpu.VMEM((2, 2, rows, depth), BF),
        ]
        + [pltpu.SemaphoreType.DMA((chips,))] * 8
        + [pltpu.SemaphoreType.DMA((3,))] * 2
        + [pltpu.SemaphoreType.DMA((chips,))] * 2
        + [pltpu.SemaphoreType.DMA]
        + [pltpu.SemaphoreType.DMA((n - 1,))] * 2
        + [pltpu.SemaphoreType.DMA],
        compiler_params=pltpu.CompilerParams(
            vmem_limit_bytes=60 << 20, collective_id=3, has_side_effects=True
        ),
        cost_estimate=pl.CostEstimate(
            flops=2 * 9 * devices * rows * depth * hidden, bytes_accessed=30 << 20, transcendentals=0
        ),
        name="ffn",
    )(x, grad_branch, weights, w_packed)


def unpack_kernel(share, g_ref, gate_ref, up_ref, down_ref, out_ref):
    g = g_ref[0].astype(F32)
    gate_ref[...] = g[:share].T
    up_ref[...] = g[share : 2 * share].T
    down_ref[...] = g[2 * share : 3 * share]
    out_ref[...] = g[3 * share :]


def unpack(grads, share, width):
    devices, height, depth = grads.shape
    hidden = devices * share
    if share % 128:
        gate, up, down = (
            grads[:, k * share : (k + 1) * share].reshape(hidden, depth).astype(F32) for k in range(3)
        )
        return gate.T, up.T, down, grads[:, 3 * share :].reshape(width, depth).astype(F32)
    column = pl.BlockSpec((depth, share), lambda i: (0, i))
    return pl.pallas_call(
        functools.partial(unpack_kernel, share),
        out_shape=(
            jax.ShapeDtypeStruct((depth, hidden), F32),
            jax.ShapeDtypeStruct((depth, hidden), F32),
            jax.ShapeDtypeStruct((hidden, depth), F32),
            jax.ShapeDtypeStruct((width, depth), F32),
        ),
        grid=(devices,),
        in_specs=[pl.BlockSpec((1, height, depth), lambda i: (i, 0, 0))],
        out_specs=[
            column, column, pl.BlockSpec((share, depth), lambda i: (i, 0)),
            pl.BlockSpec((width // devices, depth), lambda i: (i, 0)),
        ],
        compiler_params=pltpu.CompilerParams(vmem_limit_bytes=40 << 20),
        name="unpack",
    )(grads)


def norm_parts(values):
    centre = jnp.mean(values, axis=-1, keepdims=True)
    centred = values - centre
    inverse = lax.rsqrt(jnp.mean(centred * centred, axis=-1, keepdims=True) + EPS)
    return centred * inverse, inverse


def norm_back(upstream, scaled, inverse, gain):
    through = upstream * gain
    inner = (
        through
        - jnp.mean(through, axis=-1, keepdims=True)
        - scaled * jnp.mean(through * scaled, axis=-1, keepdims=True)
    )
    return inverse * inner, jnp.sum(upstream * scaled, axis=0), jnp.sum(upstream, axis=0)


def pack_weights(w_query, w_key, w_value):
    depth, width = w_query.shape
    key, value = (w.reshape(depth, width // HD, 1, HD) for w in (w_key, w_value))
    both = jnp.concatenate([key, value], axis=2).reshape(depth, 2 * width)
    return jnp.concatenate([both, w_query], axis=1)


def on_device(
    tokens, lengths, ln1_gain, ln1_bias, w_query, w_key, w_value, w_out,
    ln2_gain, ln2_bias, w_gate, w_up, down_weight, cotangent,
):
    n = lax.axis_size("tensor")
    local_rows, depth = tokens.shape
    length = local_rows * n
    width = w_query.shape[1]
    row_ids = lax.axis_index("tensor") * local_rows + lax.iota(jnp.int32, local_rows)
    valid = (row_ids < lengths[0])[:, None]

    inputs = tokens.astype(F32)
    grad_out = jnp.where(valid, cotangent.astype(F32), 0.0)
    devices = lax.axis_size("dp")
    place = lax.axis_index("dp")
    share = w_gate.shape[1] // devices

    (
        context, logsum, q, k, v, cosine, sine, attn_rows, grad_branch, weights, context_own, _, w_out_all,
    ) = front(
        tokens, cotangent, ln1_gain, ln1_bias, angle_tables(length), w_query, w_key, w_value,
        w_gate, w_up, down_weight, w_out, lengths, n, devices,
    )
    attn_rows = attn_rows.reshape(length, depth)
    weights = weights.reshape(3, n * share, depth)

    def row_share(w):
        return lax.dynamic_slice_in_dim(w, place * (depth // devices), depth // devices, 0)

    w_packed = pack_weights(row_share(w_query), row_share(w_key), row_share(w_value))
    w_out_all = w_out_all.reshape(n, width, depth)
    attn_out = sum(dot(context_own[t], w_out_all[t]).astype(BF).astype(F32) for t in range(n))
    middle = inputs + attn_out
    scaled2, inverse2 = norm_parts(middle)
    ffn_in = (scaled2 * ln2_gain + ln2_bias).astype(BF)
    grad_parts, out_parts, ffn_grads, w_packed = ffn(
        ffn_in, grad_branch, weights, w_packed, n, devices
    )
    grad_ffn_in = sum(grad_parts[p].astype(F32) for p in range(devices // 2))
    grad_norm2, gain2_grad, shift2_grad = norm_back(
        grad_ffn_in, scaled2, inverse2, ln2_gain
    )
    grad_middle = grad_out + grad_norm2
    grad_attn = grad_middle.astype(BF)
    ffn_grads = ffn_grads.reshape(n, 3 * share, depth)
    w_packed = lax.all_gather(w_packed, "dp", axis=0)
    ffn_grads = lax.psum_scatter(ffn_grads, "tensor", scatter_dimension=0, tiled=True)[0]
    packed, packed_own, out_sums, out_piece = att_bwd(
        grad_attn, w_out_all, context_own, out_parts, q, k, v, context, logsum, cosine, sine, n
    )
    ffn_grads, out_piece = lax.optimization_barrier((ffn_grads, out_piece))
    grads = lax.all_gather(jnp.concatenate([ffn_grads, out_piece]), "dp", axis=0)
    gate_grad, up_grad, down_grad, out_grad = unpack(grads, share, width)
    ffn_out = sum(x.astype(F32) for x in (out_parts[0], *out_sums))
    output = jnp.where(valid, middle + ffn_out, 0.0).astype(BF)
    input_grad, query_grad, key_grad, value_grad, sums = finish(
        attn_rows, packed, packed_own, w_packed, tokens, grad_middle, ln1_gain,
        jnp.stack([gain2_grad, shift2_grad]), width, devices,
    )
    gain1_grad, shift1_grad, gain2_grad, shift2_grad = (sums[i] for i in range(4))
    return (
        output, input_grad, gain1_grad, shift1_grad, query_grad, key_grad, value_grad, out_grad,
        gain2_grad, shift2_grad, gate_grad, up_grad, down_grad,
    )


def solution(mesh):
    rows = P(("dp", "tensor"), None)
    columns = P(None, "tensor")
    parts = P("tensor", None)
    return jax.shard_map(
        on_device,
        mesh=mesh,
        in_specs=(
            rows, P("dp"), P(), P(), columns, columns, columns, parts,
            P(), P(), columns, columns, parts, rows,
        ),
        out_specs=(
            rows, rows, P(), P(), columns, columns, columns, parts,
            P(), P(), columns, columns, parts,
        ),
        check_vma=False,
    )
```

```python
import functools
import math

import jax
import jax.numpy as jnp
from jax import lax
from jax.experimental import pallas as pl
from jax.experimental.pallas import tpu as pltpu
from jax.sharding import PartitionSpec as P

HD = 64
EPS = 1e-05
SCALE = 1.0 / math.sqrt(HD)
F32 = jnp.float32
BF = jnp.bfloat16
NT = (((1,), (1,)), ((), ()))
NN = (((1,), (0,)), ((), ()))
TN = (((0,), (0,)), ((), ()))
MESH = pl.DeviceIdType.MESH


def dot(a, b, dims=NN):
    return lax.dot_general(a, b, dims, preferred_element_type=F32)


def lanes(shape):
    return lax.broadcasted_iota(jnp.int32, shape, 1)


def split3(x):
    hi = x.astype(BF).astype(F32)
    mid = (x - hi).astype(BF).astype(F32)
    return hi, mid, x - hi - mid


def partner(x):
    width = x.shape[1]
    first = lanes(x.shape) % HD < HD // 2
    return jnp.where(first, pltpu.roll(x, width - HD // 2, 1), pltpu.roll(x, HD // 2, 1))


STEP = 64


def angle_tables(length):
    half = HD // 2
    lane = lax.optimization_barrier(lax.iota(jnp.int32, 2 * HD))
    freqs = 10000.0 ** (-((lane % half).astype(F32) * 2.0 / HD))
    sign = jnp.where(lane % HD < half, -1.0, 1.0)

    def table(positions):
        angles = positions[:, None] * freqs[None, :]
        return jnp.stack([jnp.cos(angles), jnp.sin(angles)])

    return table(lax.iota(F32, length // STEP) * STEP), table(lax.iota(F32, STEP)), sign[None, :]


def differ(a, b, bits):
    return sum(lax.rem(a // (1 << k) + b // (1 << k), 2) * (1 << k) for k in range(bits))


def remote(src, dst, send, recv, **to):
    return pltpu.make_async_remote_copy(
        src_ref=src, dst_ref=dst, send_sem=send, recv_sem=recv, device_id=to, device_id_type=MESH
    )


def ring(n, step):
    return lax.rem(lax.axis_index("tensor") + step, n)


def same_core(s, chips):
    me = lax.axis_index("dp")
    return differ(me // 2, s, chips.bit_length() - 1) * 2 + lax.rem(me, 2)


def sibling():
    me = lax.axis_index("dp")
    return me + 1 - 2 * lax.rem(me, 2)


def greet(n, chips, both_cores=False):
    barrier = pltpu.get_barrier_semaphore()
    if both_cores:
        pl.semaphore_signal(barrier, inc=1, device_id={"dp": sibling()}, device_id_type=MESH)
    for step in range(1, n):
        pl.semaphore_signal(barrier, inc=1, device_id={"tensor": ring(n, step)}, device_id_type=MESH)
    for s in range(1, chips):
        pl.semaphore_signal(
            barrier, inc=1, device_id={"dp": same_core(s, chips)}, device_id_type=MESH
        )
    pl.semaphore_wait(barrier, n + chips - 2 + both_cores)


def front_kernel(
    n, chips, chunks, limit_ref, tokens_ref, ct_ref, gain_ref, shift_ref, coarse_ref, fine_ref, sign_ref,
    wq_ref, wk_ref, wv_ref, gate_ref, up_ref, down_ref, wo_ref,
    ctx_ref, lse_ref, wp_ref, q_out, k_out, v_out, cos_out, sin_out, rows_ref, gb_all, w_all, out_ref, wo_z, wo_all,
    landed, gb, columns, own_w, wqkv, q_ref, k_ref, v_ref, cos_ref, sin_ref,
    right_send, right_recv, left_send, left_recv, gs_send, gs_recv, gr_send, gr_recv, rows_sem,
    wr_send, wr_recv, wl_send, wl_recv, send_sem, recv_sem, wz_send, wz_recv, ws_send, ws_recv,
    wx_send, wx_recv, cut_sem, load_sem, save_sem, keep_sem,
):
    i = pl.program_id(0)
    steps = pl.num_programs(0)
    me = lax.axis_index("tensor")
    place = lax.axis_index("dp")
    core = lax.rem(place, 2)
    bits = chips.bit_length() - 1
    rows, depth = tokens_ref.shape
    heads = q_ref.shape[0]
    piece = rows // chunks
    limit = limit_ref[0]
    s = i // heads
    h = lax.rem(i, heads)

    def over(shard, d, c, send, recv, to):
        part = landed.at[shard, pl.ds(c * piece, piece)]
        return remote(part, part, send.at[d, c], recv.at[d, c], tensor=to)

    def rightward(d, c):
        return over(me - d, d, c, right_send, right_recv, me + 1)

    def leftward(d, c):
        return over(me + d, d, c, left_send, left_recv, me - 1)

    def from_left(d, c):
        return over(me - d, d - 1, c, right_send, right_recv, me - 1)

    def from_right(d, c):
        return over(me + d, d - 1, c, left_send, left_recv, me + 1)

    def weights(shard, d, k, send, recv, to):
        there = w_all.at[k, shard]
        return remote(there if d else own_w.at[k], there, send.at[d, k], recv.at[d, k], tensor=to)

    def w_right(d, k):
        return weights(me - d, d, k, wr_send, wr_recv, me + 1)

    def w_left(d, k):
        return weights(me + d, d, k, wl_send, wl_recv, me - 1)

    def w_from_left(d, k):
        return weights(me - d, d - 1, k, wr_send, wr_recv, me - 1)

    def w_from_right(d, k):
        return weights(me + d, d - 1, k, wl_send, wl_recv, me + 1)

    def spread_gb(c):
        return remote(
            gb, gb_all.at[place // 2, core], gs_send.at[c], gs_recv.at[c], dp=same_core(c, chips)
        )

    def relay_gb(c):
        there = gb_all.at[differ(place // 2, c, bits), core]
        return remote(there if c else gb, there, gr_send.at[c], gr_recv.at[c], dp=sibling())

    def wo_over(step):
        return remote(
            wo_ref, wo_z.at[me], wz_send.at[step], wz_recv.at[step], tensor=ring(n, step + 1)
        )

    def spread_wo(c):
        return remote(
            wo_z, wo_all.at[:, place], ws_send.at[c], ws_recv.at[c], dp=same_core(c, chips)
        )

    def relay_wo(c):
        there = wo_all.at[:, differ(place // 2, c, bits) * 2 + core]
        return remote(there if c else wo_z, there, wx_send.at[c], wx_recv.at[c], dp=sibling())

    def push(step):
        owner = ring(n, step + 1)
        return remote(
            ctx_ref.at[pl.ds(pl.multiple_of(owner * rows, rows), rows)], out_ref.at[me],
            send_sem.at[step], recv_sem.at[step], tensor=owner,
        )

    def save(shard):
        return pltpu.make_async_copy(landed.at[shard], rows_ref.at[shard], rows_sem.at[shard])

    mine = pl.ds(pl.multiple_of(me * rows, rows), rows)
    keeps = [
        pltpu.make_async_copy(gb, gb_all.at[place // 2, core], keep_sem.at[0]),
        pltpu.make_async_copy(wo_ref, wo_z.at[me], keep_sem.at[1]),
        pltpu.make_async_copy(wo_z, wo_all.at[:, place], keep_sem.at[2]),
        pltpu.make_async_copy(ctx_ref.at[mine], out_ref.at[me], keep_sem.at[3]),
        pltpu.make_async_copy(own_w, w_all.at[:, me], keep_sem.at[4]),
    ]
    saves = [
        pltpu.make_async_copy(a, b, save_sem.at[j])
        for j, (a, b) in enumerate(
            ((q_ref, q_out), (k_ref, k_out), (v_ref, v_out), (cos_ref, cos_out), (sin_ref, sin_out))
        )
    ]

    @pl.when(i == 0)
    def _():
        loads = [
            pltpu.make_async_copy(ref, wqkv.at[j], load_sem.at[j])
            for j, ref in enumerate((wq_ref, wk_ref, wv_ref))
        ]
        share = own_w.shape[1]
        ours = pl.ds(pl.multiple_of(place * share, share), share)
        cuts = [pltpu.make_async_copy(down_ref.at[ours], own_w.at[2], cut_sem.at[2])]
        for k, ref in enumerate((gate_ref, up_ref)):
            src = ref if share % 128 else ref.at[:, ours]
            cuts.append(pltpu.make_async_copy(src, columns.at[k], cut_sem.at[k]))
        for copy in loads + cuts:
            copy.start()

        barrier = pltpu.get_barrier_semaphore()
        for step in range(1, n):
            to = ring(n, step)
            pl.semaphore_signal(barrier, inc=1, device_id={"tensor": to}, device_id_type=MESH)
        pl.semaphore_signal(barrier, inc=1, device_id={"dp": sibling()}, device_id_type=MESH)
        for c in range(1, chips):
            to = same_core(c, chips)
            pl.semaphore_signal(barrier, inc=1, device_id={"dp": to}, device_id_type=MESH)

        values = tokens_ref[...].astype(F32)
        values = values - jnp.mean(values, axis=1, keepdims=True)
        inverse = lax.rsqrt(jnp.mean(values * values, axis=1, keepdims=True) + EPS)
        landed[me] = (values * inverse * gain_ref[...] + shift_ref[...]).astype(BF)

        pl.semaphore_wait(barrier, n - 1 + chips)

        for c in range(chunks):

            @pl.when(me < n - 1)
            def _():
                rightward(0, c).start()

            @pl.when(me > 0)
            def _():
                leftward(0, c).start()

        row = me * rows + lax.broadcasted_iota(jnp.int32, (rows, depth), 0)
        gb[...] = jnp.where(row < limit, ct_ref[...].astype(F32), 0.0).astype(BF)
        for c in range(1, chips):
            spread_gb(c).start()
        relay_gb(0).start()
        keeps[0].start()
        keeps[1].start()
        for copy in loads:
            copy.wait()

        cut = wp_ref.shape[0]
        here = pl.ds(pl.multiple_of(place * cut, cut), cut)
        first = lanes((cut, 128)) < HD
        for p in range(heads // 2):
            at = slice(p * 128, p * 128 + 128)
            query, key, value = (wqkv[j, here, at].astype(F32) for j in range(3))
            even = jnp.where(first, key, pltpu.roll(value, HD, 1))
            odd = jnp.where(first, pltpu.roll(key, HD, 1), value)
            for slot, values in ((2 * p, even), (2 * p + 1, odd), (heads + p, query)):
                wp_ref[:, slot * 128 : slot * 128 + 128] = values.astype(BF)

        lane = lanes((rows, 128))
        ones = jnp.where(lane < HD + 3, 1.0, 0.0)
        unit = jnp.where(lane == HD + 3, 1.0, 0.0)

        def put(out, here, values, extra):
            for head in range(heads):
                own = values[:, head // 2 * 128 : head // 2 * 128 + 128]
                own = pltpu.roll(own, HD, 1) if head % 2 else own
                out[head, here, :] = jnp.where(lane < HD, own, extra).astype(BF)

        def project(shard):
            here = pl.ds(pl.multiple_of(shard * rows, rows), rows)
            for j in range(rows // STEP):
                part = pl.ds(pl.multiple_of(shard * rows + j * STEP, STEP), STEP)
                coarse = pl.ds(shard * (rows // STEP) + j, 1)
                c0, s0 = coarse_ref[0, coarse, :], coarse_ref[1, coarse, :]
                cos_ref[part, :] = c0 * fine_ref[0] - s0 * fine_ref[1]
                sin_ref[part, :] = (s0 * fine_ref[0] + c0 * fine_ref[1]) * sign_ref[...]
            cosine = jnp.tile(cos_ref[here, :], (1, heads // 2))
            sine = jnp.tile(sin_ref[here, :], (1, heads // 2))
            x = landed[shard]
            row = shard * rows + lax.broadcasted_iota(jnp.int32, (rows, 128), 0)
            bias = jnp.where(lane == HD + 3, jnp.where(row < limit, 0.0, -1e30), ones)
            raw = dot(x, wqkv[0])
            turned = (raw * cosine + partner(raw) * sine).astype(BF).astype(F32)
            put(q_ref, here, turned * SCALE, unit)
            raw = dot(x, wqkv[1])
            put(k_ref, here, raw * cosine + partner(raw) * sine, bias)
            put(v_ref, here, dot(x, wqkv[2]), ones)

        for d in range(1, n + 1):
            for c in range(chunks):
                if d < n:

                    @pl.when(me >= d)
                    def _():
                        from_left(d, c).wait_recv()

                    @pl.when((me >= d) & (me < n - 1))
                    def _():
                        rightward(d, c).start()

                    @pl.when(me + d < n)
                    def _():
                        from_right(d, c).wait_recv()

                    @pl.when((me + d < n) & (me > 0))
                    def _():
                        leftward(d, c).start()

                if c == 0:

                    @pl.when(me >= d - 1)
                    def _():
                        save(me - d + 1).start()
                        project(me - d + 1)

                if c == 1 and d > 1:

                    @pl.when(me + d - 1 < n)
                    def _():
                        save(me + d - 1).start()
                        project(me + d - 1)

                if c == 2 and d == 1:
                    for cut in cuts:
                        cut.wait()
                    for k in range(2):
                        own_w[k] = columns[k].astype(F32).T.astype(BF)
                    keeps[4].start()

                if c == chunks - 1 and d == 2:
                    for near in range(1, chips // 2 + 1):
                        spread_gb(near).wait_recv()
                        relay_gb(near).start()

            if d < n:

                @pl.when((me < n - 1) & (me + 1 == d))
                def _():
                    for k in range(3):
                        w_right(0, k).start()

                @pl.when((me > 0) & (n - me == d))
                def _():
                    for k in range(3):
                        w_left(0, k).start()

        for copy in saves:
            copy.start()
        for step in range(n - 1):
            wo_over(step).start()
        for far in range(chips // 2 + 1, chips):
            spread_gb(far).wait_recv()
            relay_gb(far).start()

    stride = max((heads * n - 2) // max(n - 2, 1), 1)
    for d in range(1, n - 1):

        @pl.when(i == 1 + (d - 1) * stride)
        def _():
            for k in range(3):

                @pl.when((me >= d) & (me < n - 1))
                def _():
                    w_from_left(d, k).wait_recv()
                    w_right(d, k).start()

                @pl.when((me + d < n) & (me > 0))
                def _():
                    w_from_right(d, k).wait_recv()
                    w_left(d, k).start()

    @pl.when(i == heads)
    def _():
        for step in range(n - 1):
            wo_over(step).wait()
        keeps[1].wait()
        for c in range(1, chips):
            spread_wo(c).start()
        relay_wo(0).start()
        keeps[2].start()

    @pl.when(i == (n - 1) * heads)
    def _():
        for c in range(1, chips):
            spread_wo(c).wait_recv()
            relay_wo(c).start()

    owner = ring(n, s + 1)
    block = pl.ds(pl.multiple_of(owner * rows, rows), rows)
    scores = dot(q_ref[h, block, :], k_ref[h], NT)
    peak = jnp.max(scores, axis=1, keepdims=True)
    acc = dot(jnp.exp(scores - peak).astype(BF), v_ref[h])
    lane = lanes((rows, 128))
    total = jnp.sum(jnp.where(lane == HD, acc, 0.0), axis=1, keepdims=True)
    out = acc * (1.0 / total)
    odd = lax.rem(h, 2)
    out = jnp.where(odd == 1, pltpu.roll(out, HD, 1), out).astype(BF)
    pair = pl.ds(pl.multiple_of(h // 2 * 128, 128), 128)
    ctx_ref[block, pair] = jnp.where((lane >= HD) == (odd == 1), out, ctx_ref[block, pair])
    lse_ref[block, :] = jnp.where(lane == h, peak + jnp.log(total), lse_ref[block, :])

    @pl.when((h == heads - 1) & (s < n - 1))
    def _():
        push(s).start()

    @pl.when(i == steps - 1)
    def _():
        keeps[3].start()
        for d in range(n - 1):
            for c in range(chunks):

                @pl.when((me >= d) & (me < n - 1))
                def _():
                    rightward(d, c).wait_send()

                @pl.when((me + d < n) & (me > 0))
                def _():
                    leftward(d, c).wait_send()

            for k in range(3):

                @pl.when((me >= d) & (me < n - 1))
                def _():
                    w_right(d, k).wait_send()

                @pl.when((me + d < n) & (me > 0))
                def _():
                    w_left(d, k).wait_send()

        for k in range(3):
            for d in range(1, n):

                @pl.when((me >= d) & ((me == n - 1) | (d == n - 1)))
                def _():
                    w_from_left(d, k).wait_recv()

                @pl.when((me + d < n) & ((me == 0) | (d == n - 1)))
                def _():
                    w_from_right(d, k).wait_recv()

        for c in range(chips):
            relay_gb(c).wait()
            relay_wo(c).wait()
            if c:
                spread_gb(c).wait_send()
                spread_wo(c).wait_send()
        for shard in range(n):
            save(shard).wait()
        for copy in saves:
            copy.wait()
        for step in range(n - 1):
            push(step).wait()
        for j in (0, 2, 3, 4):
            keeps[j].wait()


def front(
    tokens, cotangent, gain, shift, tables, w_query, w_key, w_value, gate, up, down, w_out, limit, n, devices
):
    rows, depth = tokens.shape
    total = n * rows
    width = w_query.shape[1]
    heads = width // HD
    chips = devices // 2
    chunks = 4
    place = lax.axis_index("dp")
    share = down.shape[0] // devices
    part = width // devices
    if share % 128:
        gate, up = (lax.dynamic_slice_in_dim(w, place * share, share, 1) for w in (gate, up))
    hbm = pl.BlockSpec(memory_space=pl.ANY)

    def whole(*shape):
        return pl.BlockSpec(shape, lambda *_: (0,) * len(shape), pipeline_mode=pl.Buffered(1))

    def dma(*shape):
        return pltpu.SemaphoreType.DMA(shape)

    head_array = jax.ShapeDtypeStruct((heads, total, 128), BF)
    table = jax.ShapeDtypeStruct((total, 128), F32)
    coarse, fine, sign = tables
    return pl.pallas_call(
        functools.partial(front_kernel, n, chips, chunks),
        out_shape=(
            jax.ShapeDtypeStruct((total, width), BF),
            table,
            jax.ShapeDtypeStruct((depth // devices, 3 * width), BF),
            head_array, head_array, head_array, table, table,
            jax.ShapeDtypeStruct((n, rows, depth), BF),
            jax.ShapeDtypeStruct((chips, 2, rows, depth), BF),
            jax.ShapeDtypeStruct((3, n, share, depth), BF),
            jax.ShapeDtypeStruct((n, rows, width), BF),
            jax.ShapeDtypeStruct((n, part, depth), BF),
            jax.ShapeDtypeStruct((n, devices, part, depth), BF),
        ),
        grid_spec=pltpu.PrefetchScalarGridSpec(
            num_scalar_prefetch=0,
            grid=(n * heads,),
            in_specs=[pl.BlockSpec(memory_space=pltpu.SMEM)]
            + [whole(rows, depth)] * 2
            + [whole(1, depth)] * 2
            + [whole(*coarse.shape), whole(*fine.shape), whole(*sign.shape)]
            + [hbm] * 7,
            out_specs=[whole(total, width), whole(total, 128), whole(depth // devices, 3 * width)]
            + [hbm] * 11,
            scratch_shapes=[
                pltpu.VMEM((n, rows, depth), BF),
                pltpu.VMEM((rows, depth), BF),
                pltpu.VMEM((2, depth, share), BF),
                pltpu.VMEM((3, share, depth), BF),
                pltpu.VMEM((3, depth, width), BF),
            ]
            + [pltpu.VMEM((heads, total, 128), BF)] * 3
            + [pltpu.VMEM((total, 128), F32)] * 2
            + [dma(n - 1, chunks)] * 4
            + [dma(chips)] * 4
            + [dma(n)]
            + [dma(n - 1, 3)] * 4
            + [dma(n - 1)] * 4
            + [dma(chips)] * 4
            + [dma(3), dma(3), dma(5), dma(5)],
        ),
        compiler_params=pltpu.CompilerParams(
            vmem_limit_bytes=60 << 20, collective_id=1, has_side_effects=True
        ),
        cost_estimate=pl.CostEstimate(
            flops=4 * total * total * 256 * heads * 3, bytes_accessed=40 << 20, transcendentals=0
        ),
        name="front",
    )(
        limit, tokens, cotangent, gain.reshape(1, depth), shift.reshape(1, depth), coarse, fine, sign,
        w_query, w_key, w_value, gate, up, down,
        lax.dynamic_slice_in_dim(w_out, place * part, part, 0),
    )


def att_bwd_kernel(
    n, bk, chips, ga_ref, wo_ref, cown_ref, parts_ref, q_ref, k_ref, v_ref, ctx_ref, lse_ref,
    cos_ref, sin_ref, pk_ref, own_ref, sums_ref, og_ref, do, gc, dka, dva, dqs,
    og_full, og_own, og_mate, og_sib, og_land, og_piece, og_z,
    send_sem, recv_sem, out_send, out_recv, pk_send, pk_recv, keep_sem,
    om_send, om_recv, op_send, op_recv, oz_send, oz_recv,
):
    i = pl.program_id(0)
    heads, total, _ = k_ref.shape
    h = jnp.where(i < heads, i, (i - heads) // (n - 1))
    t = jnp.where(i < heads, 0, lax.rem(i - heads, n - 1) + 1)
    rows = total // n
    me = lax.axis_index("tensor")
    place = lax.axis_index("dp")
    core = lax.rem(place, 2)
    bits = chips.bit_length() - 1
    share = og_ref.shape[0]
    mine = pl.ds(pl.multiple_of(me * rows, rows), rows)

    def push(step):
        return remote(
            gc.at[step], do.at[mine], send_sem.at[step], recv_sem.at[step], tensor=ring(n, step + 1)
        )

    def push_out(s):
        return remote(
            parts_ref.at[s], sums_ref.at[s - 1], out_send.at[s - 1], out_recv.at[s - 1],
            dp=same_core(s, chips),
        )

    def columns(slot):
        return pl.ds(pl.multiple_of(slot * 128, 128), 128)

    def push_pack(slot, step):
        owner = ring(n, step + 1)
        return remote(
            pk_ref.at[pl.ds(pl.multiple_of(owner * rows, rows), rows), columns(slot)],
            own_ref.at[me, :, columns(slot)],
            pk_send.at[slot, step], pk_recv.at[slot, step], tensor=owner,
        )

    def keep(slot):
        return pltpu.make_async_copy(
            pk_ref.at[mine, columns(slot)], own_ref.at[me, :, columns(slot)], keep_sem.at[slot]
        )

    @pl.when(i == 0)
    def _():
        greet(n, chips, True)

        def send(step, carry):
            gc[step] = dot(ga_ref[...], wo_ref[ring(n, step + 1)], NT).astype(BF)
            push(step).start()
            return carry

        lax.fori_loop(0, n - 1, send, 0)
        do[mine, :] = dot(ga_ref[...], wo_ref[me], NT).astype(BF)

    def og_swap():
        return remote(og_mate, og_sib, om_send, om_recv, dp=sibling())

    def og_push(s):
        return remote(og_sib.at[s], og_land.at[s], op_send.at[s], op_recv.at[s], dp=same_core(s, chips))

    def og_over(step):
        to = ring(n, step + 1)
        return remote(og_piece.at[to], og_z.at[me], oz_send.at[step], oz_recv.at[step], tensor=to)

    @pl.when(i == 1)
    def _():
        def term(part, carry):
            og_full[...] = dot(cown_ref[part], ga_ref[...], TN)
            for s in range(chips):
                start = differ(place // 2, s, bits) * 2
                here = pl.ds(pl.multiple_of((start + core) * share, share), share)
                there = pl.ds(pl.multiple_of((start + 1 - core) * share, share), share)
                og_own[s, part] = og_full[here, :]
                og_mate[s, part] = og_full[there, :].astype(BF)
            return carry

        lax.fori_loop(0, n, term, 0)
        og_swap().start()

    @pl.when(i == 2)
    def _():
        og_swap().wait_recv()
        for s in range(chips):
            og_sib[s] = (og_own[s] + og_sib[s].astype(F32)).astype(BF)
            if s:
                og_push(s).start()

    @pl.when(i == heads + 2)
    def _():
        joined = og_sib[0].astype(F32)
        for s in range(1, chips):
            og_push(s).wait_recv()
            joined = joined + og_land[s].astype(F32)
        og_piece[...] = joined.astype(BF)
        for step in range(n - 1):
            og_over(step).start()
        for s in range(1, chips):
            push_out(s).start()

    @pl.when(i == heads * n - 1)
    def _():
        og_z[me] = og_piece[me]
        for step in range(n - 1):
            og_over(step).wait_recv()
        joined = og_z[0].astype(F32)
        for part in range(1, n):
            joined = joined + og_z[part].astype(F32)
        og_ref[...] = joined.astype(BF)

    @pl.when((h == 0) & (t > 0))
    def _():
        push(t - 1).wait_recv()

    source = ring(n, n - t)
    block = pl.ds(pl.multiple_of(source * rows, rows), rows)
    pair = columns(h // 2)
    odd = lax.rem(h, 2) == 1
    lane = lanes((rows, 128))
    off = lane - HD
    logsum = jnp.sum(jnp.where(lane == h, lse_ref[block, :], 0.0), axis=1, keepdims=True)
    a, b, c = split3(-logsum)
    q = q_ref[h, block, :].astype(F32)
    q = jnp.where(off == 0, a, jnp.where(off == 1, b, jnp.where(off == 2, c, q))).astype(BF)
    g = jnp.where((lane >= HD) == odd, do[block, pair].astype(F32), 0.0)
    delta = jnp.sum(g * ctx_ref[block, pair].astype(F32), axis=1, keepdims=True)
    a, b, c = split3(-delta)
    g = jnp.where(odd, pltpu.roll(g, HD, 1), g)
    g = jnp.where(off == 0, a, jnp.where(off == 1, b, jnp.where(off == 2, c, g))).astype(BF)
    acc = jnp.zeros((rows, 128), F32)
    for j in range(total // bk):
        rk = pl.ds(j * bk, bk)
        kt = k_ref[h, rk, :]
        probs = jnp.exp(dot(kt, q, NT))
        grad = (probs * dot(v_ref[h, rk, :], g, NT)).astype(BF)
        for sums, term in ((dva, dot(probs.astype(BF), g)), (dka, dot(grad, q))):
            before = jnp.where(t == 0, jnp.zeros_like(term), sums[h, rk, :])
            sums[h, rk, :] = before + term
        acc = acc + dot(grad, kt, TN)
    acc = acc * SCALE

    @pl.when(jnp.logical_not(odd))
    def _():
        dqs[block, :] = acc

    @pl.when(odd)
    def _():
        grad = jnp.where(lane < HD, dqs[block, :], pltpu.roll(acc, HD, 1))
        grad = grad * cos_ref[block, :] - partner(grad) * sin_ref[block, :]
        pk_ref[block, columns(heads + h // 2)] = grad.astype(BF)

    @pl.when(odd & (t == 0))
    def _():
        keep(heads + h // 2).start()

    @pl.when(odd & (t > 0))
    def _():
        push_pack(heads + h // 2, n - 1 - t).start()

    @pl.when(t == n - 1)
    def _():
        dk = dka[h]
        dk = dk * cos_ref[...] - partner(dk) * sin_ref[...]
        both = jnp.where(lanes((total, 128)) < HD, dk, pltpu.roll(dva[h], HD, 1))
        pk_ref[:, columns(h)] = both.astype(BF)
        for step in range(n - 1):
            push_pack(h, step).start()
        keep(h).start()

    @pl.when(i == heads * n - 1)
    def _():
        for step in range(n - 1):
            push(step).wait_send()
        for s in range(1, chips):
            push_out(s).wait()
        og_swap().wait_send()
        for s in range(1, chips):
            og_push(s).wait_send()
        for step in range(n - 1):
            og_over(step).wait_send()
        for slot in range(heads + heads // 2):
            keep(slot).wait()
            for step in range(n - 1):
                push_pack(slot, step).wait()


def att_bwd(grad_attn, w_out, ctx_own, parts, q, k, v, ctx, lse, cosine, sine, n, bk=512):
    heads, total, _ = q.shape
    width = heads * HD
    rows, depth = grad_attn.shape
    chips = parts.shape[0]
    share = width // (2 * chips)
    slots = heads + heads // 2
    hbm = pl.BlockSpec(memory_space=pl.ANY)

    def whole(*shape):
        return pl.BlockSpec(shape, lambda *_: (0,) * len(shape), pipeline_mode=pl.Buffered(1))

    return pl.pallas_call(
        functools.partial(att_bwd_kernel, n, bk, chips),
        out_shape=(
            jax.ShapeDtypeStruct((total, slots * 128), BF),
            jax.ShapeDtypeStruct((n, rows, slots * 128), BF),
            jax.ShapeDtypeStruct((chips - 1, rows, depth), BF),
            jax.ShapeDtypeStruct((share, depth), BF),
        ),
        grid_spec=pltpu.PrefetchScalarGridSpec(
            num_scalar_prefetch=0,
            grid=(heads * n,),
            in_specs=[whole(rows, depth), whole(n, width, depth), whole(n, rows, width), hbm]
            + [whole(heads, total, 128)] * 3
            + [whole(total, width)]
            + [whole(total, 128)] * 3,
            out_specs=[whole(total, slots * 128), hbm, hbm, whole(share, depth)],
            scratch_shapes=[
                pltpu.VMEM((total, width), BF),
                pltpu.VMEM((n - 1, rows, width), BF),
            ]
            + [pltpu.VMEM((heads, total, 128), F32)] * 2
            + [pltpu.VMEM((total, 128), F32)]
            + [
                pltpu.VMEM((width, depth), F32),
                pltpu.VMEM((chips, n, share, depth), F32),
                pltpu.VMEM((chips, n, share, depth), BF),
                pltpu.VMEM((chips, n, share, depth), BF),
                pltpu.VMEM((chips, n, share, depth), BF),
                pltpu.VMEM((n, share, depth), BF),
                pltpu.VMEM((n, share, depth), BF),
            ]
            + [pltpu.SemaphoreType.DMA((n - 1,))] * 2
            + [pltpu.SemaphoreType.DMA((chips - 1,))] * 2
            + [pltpu.SemaphoreType.DMA((slots, n - 1))] * 2
            + [pltpu.SemaphoreType.DMA((slots,))]
            + [pltpu.SemaphoreType.DMA] * 2
            + [pltpu.SemaphoreType.DMA((chips,))] * 2
            + [pltpu.SemaphoreType.DMA((n - 1,))] * 2,
        ),
        compiler_params=pltpu.CompilerParams(
            vmem_limit_bytes=56 << 20, collective_id=2, has_side_effects=True
        ),
        cost_estimate=pl.CostEstimate(
            flops=10 * total * total * 256 * heads,
            bytes_accessed=20 * total * width,
            transcendentals=total * total * heads,
        ),
        name="att_bwd",
    )(grad_attn, w_out, ctx_own, parts, q, k, v, ctx, lse, cosine, sine)


def finish_kernel(
    chips, n, width, x_ref, pk_ref, own_ref, w_ref, tokens_ref, middle_ref, gain_ref, vec_ref,
    input_ref, q_ref, k_ref, v_ref, sums_ref,
    full, mate, sib, land, fin, every, vec_z, vec_dp, vec_me,
    sx_send, sx_recv, rs_send, rs_recv, ag_send, ag_recv, rl_send, rl_recv,
    vz_send, vz_recv, vd_send, vd_recv, own_sem,
):
    bits = chips.bit_length() - 1
    me = lax.axis_index("dp")
    place = lax.axis_index("tensor")
    core = lax.rem(me, 2)
    chip = me // 2
    other = 1 - core
    heads = width // HD
    piece = fin.shape[0]

    def swap(s):
        return remote(mate.at[s], sib.at[s], sx_send.at[s], sx_recv.at[s], dp=chip * 2 + other)

    def push(s):
        return remote(sib.at[s], land.at[s], rs_send.at[s], rs_recv.at[s], dp=same_core(s, chips))

    def spread(s):
        return remote(
            fin, every.at[chip, core], ag_send.at[s], ag_recv.at[s], dp=same_core(s, chips)
        )

    def relay(s):
        src = every.at[differ(chip, s, bits), core]
        return remote(src, src, rl_send.at[s], rl_recv.at[s], dp=chip * 2 + other)

    def vec_over(step):
        return remote(
            vec_me.at[0], vec_z.at[place], vz_send.at[step], vz_recv.at[step], tensor=ring(n, step + 1)
        )

    def vec_across(step):
        return remote(
            vec_me.at[1], vec_dp.at[me], vd_send.at[step], vd_recv.at[step],
            dp=lax.rem(me + step + 1, 2 * chips),
        )

    barrier = pltpu.get_barrier_semaphore()
    for step in range(n - 1):
        pl.semaphore_signal(barrier, inc=1, device_id={"tensor": ring(n, step + 1)}, device_id_type=MESH)
    for step in range(2 * chips - 1):
        to = lax.rem(me + step + 1, 2 * chips)
        pl.semaphore_signal(barrier, inc=1, device_id={"dp": to}, device_id_type=MESH)

    full[...] = dot(x_ref[...], pk_ref[...], TN)
    pl.semaphore_wait(barrier, n + 2 * chips - 2)

    def part(s, which):
        start = (differ(chip, s, bits) * 2 + which) * piece
        return full[pl.ds(pl.multiple_of(start, piece), piece), :]

    for s in range(chips):
        mate[s] = part(s, other).astype(BF)
        swap(s).start()

    grad = jnp.zeros(input_ref.shape, F32)
    for t in range(n):
        w = w_ref[:, t].reshape(w_ref.shape[0] * w_ref.shape[2], w_ref.shape[3])
        grad = grad + dot(own_ref[t], w, NT).astype(BF).astype(F32)

    for s in range(1, chips):
        swap(s).wait_recv()
        sib[s] = (sib[s].astype(F32) + part(s, core)).astype(BF)
        push(s).start()
    swap(0).wait_recv()
    total = sib[0].astype(F32) + part(0, core)

    values = tokens_ref[...].astype(F32)
    values = values - jnp.mean(values, axis=1, keepdims=True)
    inverse = lax.rsqrt(jnp.mean(values * values, axis=1, keepdims=True) + EPS)
    scaled = values * inverse
    through = grad * gain_ref[...]
    inner = through - jnp.mean(through, axis=1, keepdims=True)
    inner = inner - scaled * jnp.mean(through * scaled, axis=1, keepdims=True)
    input_ref[...] = middle_ref[...] + inverse * inner
    vec_me[0, 0:1] = jnp.sum(grad * scaled, axis=0, keepdims=True)
    vec_me[0, 1:2] = jnp.sum(grad, axis=0, keepdims=True)
    vec_me[0, 2:4] = vec_ref[...]
    vec_me[0, 4:8] = jnp.zeros((4, vec_ref.shape[1]), F32)
    vec_z[place] = vec_me[0]
    for step in range(n - 1):
        vec_over(step).start()

    for s in range(1, chips):
        push(s).wait_recv()
        total = total + land[s].astype(F32)
    fin[...] = total.astype(BF)
    for s in range(1, chips):
        spread(s).start()
    mine = pltpu.make_async_copy(fin, every.at[chip, core], own_sem)
    mine.start()
    mine.wait()
    relay(0).start()

    for step in range(n - 1):
        vec_over(step).wait()
    vec = vec_z[0]
    for t in range(1, n):
        vec = vec + vec_z[t]
    vec_me[1] = vec
    vec_dp[me] = vec
    for step in range(2 * chips - 1):
        vec_across(step).start()
    for s in range(1, chips):
        spread(s).wait_recv()
        relay(s).start()
    for step in range(2 * chips - 1):
        vec_across(step).wait()
    vec = vec_dp[0]
    for t in range(1, 2 * chips):
        vec = vec + vec_dp[t]
    sums_ref[...] = vec
    for s in range(chips):
        relay(s).wait()
        swap(s).wait_send()
        if s > 0:
            spread(s).wait_send()
            push(s).wait_send()
    first = lanes((piece, 128)) < HD
    for d in range(2 * chips):
        rows = slice(d * piece, (d + 1) * piece)
        g = every[d // 2, d % 2].astype(F32)
        for pair in range(heads // 2):
            a = g[:, pair * 256 : pair * 256 + 128]
            b = g[:, pair * 256 + 128 : pair * 256 + 256]
            out = slice(pair * 128, pair * 128 + 128)
            q_ref[rows, out] = g[:, (heads + pair) * 128 : (heads + pair + 1) * 128]
            k_ref[rows, out] = jnp.where(first, a, pltpu.roll(b, HD, 1))
            v_ref[rows, out] = jnp.where(first, pltpu.roll(a, HD, 1), b)


def finish(rows_all, packed, own, w_all, tokens, middle, gain, vec, width, devices):
    n, rows, packs = own.shape
    depth = tokens.shape[1]
    chips = devices // 2
    piece = depth // devices
    vmem = pl.BlockSpec(memory_space=pltpu.VMEM)
    out = jax.ShapeDtypeStruct((depth, width), F32)
    return pl.pallas_call(
        functools.partial(finish_kernel, chips, n, width),
        out_shape=(
            jax.ShapeDtypeStruct((rows, depth), F32), out, out, out,
            jax.ShapeDtypeStruct((8, depth), F32),
        ),
        in_specs=[vmem] * 8,
        out_specs=[vmem] * 5,
        scratch_shapes=[
            pltpu.VMEM((depth, packs), F32),
            pltpu.VMEM((chips, piece, packs), BF),
            pltpu.VMEM((chips, piece, packs), BF),
            pltpu.VMEM((chips, piece, packs), BF),
            pltpu.VMEM((piece, packs), BF),
            pltpu.VMEM((chips, 2, piece, packs), BF),
            pltpu.VMEM((n, 8, depth), F32),
            pltpu.VMEM((devices, 8, depth), F32),
            pltpu.VMEM((2, 8, depth), F32),
        ]
        + [pltpu.SemaphoreType.DMA((chips,))] * 8
        + [pltpu.SemaphoreType.DMA((n - 1,))] * 2
        + [pltpu.SemaphoreType.DMA((devices - 1,))] * 2
        + [pltpu.SemaphoreType.DMA],
        compiler_params=pltpu.CompilerParams(
            vmem_limit_bytes=56 << 20, collective_id=4, has_side_effects=True
        ),
        cost_estimate=pl.CostEstimate(
            flops=4 * n * rows * depth * packs, bytes_accessed=20 << 20, transcendentals=0
        ),
        name="finish",
    )(rows_all, packed, own, w_all, tokens, middle, gain.reshape(1, depth), vec)


def ffn_kernel(
    chips, x_ref, gb_ref, w_ref, wp_ref, dx_ref, out_ref, dw_ref, zs_ref, wp_z,
    rows_all, gb, hid, gate_g, up_g, own, sib, mate, partial, z_left, z_right,
    ag_send, ag_recv, rl_send, rl_recv, sx_send, sx_recv, rs_send, rs_recv, fw_send, fw_recv,
    gb_sem, out_sem, dx_sem, wp_send, wp_recv, wp_sem, zr_send, zr_recv, zl_send, zl_recv,
):
    bits = chips.bit_length() - 1
    me = lax.axis_index("dp")
    core = lax.rem(me, 2)
    chip = me // 2
    other = 1 - core
    rows, depth = x_ref.shape
    n, share, _ = dw_ref.shape

    def spread(s):
        to = differ(chip, s, bits) * 2 + core
        return remote(x_ref, rows_all.at[chip, core], ag_send.at[s], ag_recv.at[s], dp=to)

    square = chips == 4

    def hand_on(s):
        half = pl.ds((s - 1) * (rows // 2), rows // 2)
        part = rows_all.at[differ(chip, s, bits), core, half]
        to = differ(chip, 3 - s, bits) * 2 + core
        return remote(part, part, fw_send.at[s], fw_recv.at[s], dp=to)

    def handed(s):
        half = pl.ds((s - 1) * (rows // 2), rows // 2)
        part = rows_all.at[differ(chip, 3, bits), core, half]
        to = differ(chip, 3 - s, bits) * 2 + core
        return remote(part, part, fw_send.at[s], fw_recv.at[s], dp=to)

    def relay(s):
        src = differ(chip, s, bits)
        return remote(
            rows_all.at[src, core], rows_all.at[src, core], rl_send.at[s], rl_recv.at[s],
            dp=chip * 2 + other,
        )

    def swap(s):
        return remote(
            mate.at[lax.rem(s, 2)], sib.at[s], sx_send.at[s], sx_recv.at[s], dp=chip * 2 + other
        )

    def push(s):
        to = differ(chip, s, bits) * 2 + core
        return remote(sib.at[s, 0], dx_ref.at[s], rs_send.at[s], rs_recv.at[s], dp=to)

    def fetch(s):
        src = differ(chip, s, bits)
        return pltpu.make_async_copy(gb_ref.at[src], gb.at[src], gb_sem.at[s])

    part = lax.axis_index("tensor")

    def over(step):
        return remote(
            wp_ref, wp_z.at[part], wp_send.at[step], wp_recv.at[step], tensor=ring(n, step + 1)
        )

    def keep(s):
        return pltpu.make_async_copy(sib.at[s, 1], out_ref.at[s], out_sem.at[s])

    for s in range(chips):
        fetch(s).start()
    barrier = pltpu.get_barrier_semaphore()
    for step in range(1, n):
        pl.semaphore_signal(barrier, inc=1, device_id={"tensor": ring(n, step)}, device_id_type=MESH)
    pl.semaphore_signal(barrier, inc=1, device_id={"dp": chip * 2 + other}, device_id_type=MESH)
    for s in range(1, chips):
        to = differ(chip, s, bits) * 2 + core
        pl.semaphore_signal(barrier, inc=1, device_id={"dp": to}, device_id_type=MESH)
    pl.semaphore_wait(barrier, chips + n - 1)
    direct = range(1, 3) if square else range(1, chips)
    for s in direct:
        spread(s).start()
    mine = pltpu.make_async_copy(x_ref, rows_all.at[chip, core], ag_send.at[0])
    mine.start()
    mine.wait()
    relay(0).start()
    for step in range(n - 1):
        over(step).start()
    keep_wp = pltpu.make_async_copy(wp_ref, wp_z.at[part], wp_sem)
    keep_wp.start()

    def shard(src, which, put):
        x = rows_all[src, which]
        grad = gb[src, which]
        gate = dot(x, w_ref[0], NT)
        upper = dot(x, w_ref[1], NT)
        grad_hidden = dot(grad, w_ref[2], NT)
        sigma = jax.nn.sigmoid(gate)
        act = gate * sigma
        hidden = (act * upper).astype(BF)
        grad_gate = (grad_hidden * upper * sigma * (1.0 + gate * (1.0 - sigma))).astype(BF)
        grad_upper = (grad_hidden * act).astype(BF)
        hid[src, which] = hidden
        gate_g[src, which] = grad_gate
        up_g[src, which] = grad_upper
        put[0] = (dot(grad_gate, w_ref[0]) + dot(grad_upper, w_ref[1])).astype(BF)
        put[1] = dot(hidden, w_ref[2]).astype(BF)

    def step(s, carry):
        src = differ(chip, s, bits)
        slot = lax.rem(s, 2)
        relay(s).wait_recv()
        fetch(s).wait()

        @pl.when(s >= 2)
        def _():
            swap(s - 2).wait_send()

        shard(src, other, mate.at[slot])
        swap(s).start()
        shard(src, core, own)
        swap(s).wait_recv()
        for k in range(2):
            sib[s, k] = (sib[s, k].astype(F32) + own[k].astype(F32)).astype(BF)

        @pl.when(s > 0)
        def _():
            push(s).start()

        keep(s).start()

        if square:

            @pl.when(s == 0)
            def _():
                for near in (1, 2):
                    spread(near).wait_recv()
                    hand_on(near).start()
                    relay(near).start()

        else:

            @pl.when(s < chips - 1)
            def _():
                spread(s + 1).wait_recv()
                relay(s + 1).start()

        if square:

            @pl.when(s == 1)
            def _():
                handed(1).wait_recv()
                handed(2).wait_recv()
                relay(3).start()

        return carry

    lax.fori_loop(0, chips, step, 0)
    first = pltpu.make_async_copy(sib.at[0, 0], dx_ref.at[0], dx_sem)
    first.start()
    def zr(t, k, to):
        return remote(
            partial.at[t, k], z_left.at[t, k], zr_send.at[t, k], zr_recv.at[t, k], tensor=to
        )

    def zl(t, k, to):
        return remote(
            partial.at[t, k], z_right.at[t, k], zl_send.at[t, k], zl_recv.at[t, k], tensor=to
        )

    def join(t, k, more):
        partial[t, k] = (partial[t, k].astype(F32) + more[t, k].astype(F32)).astype(BF)

    def weight_grad(left, right):
        left = left[...].reshape(-1, n * share)
        return dot(left, right[...].reshape(-1, depth), TN)

    for k, left in enumerate((gate_g, up_g)):
        grad = weight_grad(left, rows_all)
        for t in range(n):
            partial[t, k] = grad[t * share : (t + 1) * share, :].astype(BF)

        for j in range(n - 1):

            @pl.when(part == 0)
            def _():
                zr(n - 1 - j, k, 1).start()

            @pl.when(part == n - 1)
            def _():
                zl(j, k, n - 2).start()

    grad = weight_grad(hid, gb)
    for t in range(n):
        dw_ref[t] = grad[t * share : (t + 1) * share, :].astype(BF)
    for k in range(2):
        for j in range(n - 1):
            t = n - 1 - j

            @pl.when((part > 0) & (part < t))
            def _():
                zr(t, k, part + 1).wait_recv()
                join(t, k, z_left)
                zr(t, k, part + 1).start()

            @pl.when((part < n - 1) & (part > j))
            def _():
                zl(j, k, part - 1).wait_recv()
                join(j, k, z_right)
                zl(j, k, part - 1).start()

        for t in range(n):

            @pl.when((part == t) & (part > 0))
            def _():
                zr(t, k, part - 1).wait_recv()
                join(t, k, z_left)

            @pl.when((part == t) & (part < n - 1))
            def _():
                zl(t, k, part + 1).wait_recv()
                join(t, k, z_right)

            @pl.when(part == t)
            def _():
                zs_ref[k] = partial[t, k]

            @pl.when(part < t)
            def _():
                zr(t, k, part + 1).wait_send()

            @pl.when(part > t)
            def _():
                zl(t, k, part - 1).wait_send()

    first.wait()
    keep_wp.wait()
    for step in range(n - 1):
        over(step).wait()
    for s in range(chips):
        keep(s).wait()
        relay(s).wait_send()
        if s >= chips - 2:
            swap(s).wait_send()
        if s in direct:
            spread(s).wait_send()
        if s > 0:
            push(s).wait()
    if square:
        hand_on(1).wait_send()
        hand_on(2).wait_send()


def ffn(x, grad_branch, weights, w_packed, n, devices):
    rows, depth = x.shape
    chips = devices // 2
    hidden = weights.shape[1]
    share = hidden // n
    vmem = pl.BlockSpec(memory_space=pltpu.VMEM)
    hbm = pl.BlockSpec(memory_space=pl.ANY)
    return pl.pallas_call(
        functools.partial(ffn_kernel, chips),
        out_shape=(
            jax.ShapeDtypeStruct((chips, rows, depth), BF),
            jax.ShapeDtypeStruct((chips, rows, depth), BF),
            jax.ShapeDtypeStruct((n, share, depth), BF),
            jax.ShapeDtypeStruct((2, share, depth), BF),
            jax.ShapeDtypeStruct((n, *w_packed.shape), BF),
        ),
        in_specs=[vmem, hbm, vmem, hbm],
        out_specs=[hbm, hbm, vmem, vmem, hbm],
        scratch_shapes=[
            pltpu.VMEM((chips, 2, rows, depth), BF),
            pltpu.VMEM((chips, 2, rows, depth), BF),
        ]
        + [pltpu.VMEM((chips, 2, rows, hidden), BF)] * 3
        + [
            pltpu.VMEM((2, rows, depth), BF),
            pltpu.VMEM((chips, 2, rows, depth), BF),
            pltpu.VMEM((2, 2, rows, depth), BF),
        ]
        + [pltpu.VMEM((n, 2, share, depth), BF)] * 3
        + [pltpu.SemaphoreType.DMA((chips,))] * 8
        + [pltpu.SemaphoreType.DMA((3,))] * 2
        + [pltpu.SemaphoreType.DMA((chips,))] * 2
        + [pltpu.SemaphoreType.DMA]
        + [pltpu.SemaphoreType.DMA((n - 1,))] * 2
        + [pltpu.SemaphoreType.DMA]
        + [pltpu.SemaphoreType.DMA((n, 2))] * 4,
        compiler_params=pltpu.CompilerParams(
            vmem_limit_bytes=62 << 20, collective_id=3, has_side_effects=True
        ),
        cost_estimate=pl.CostEstimate(
            flops=2 * 9 * devices * rows * depth * hidden, bytes_accessed=30 << 20, transcendentals=0
        ),
        name="ffn",
    )(x, grad_branch, weights, w_packed)


def unpack_kernel(g_ref, gate_ref, up_ref):
    gate_ref[...] = g_ref[0, 0].astype(F32).T
    up_ref[...] = g_ref[0, 1].astype(F32).T


def unpack(grads):
    devices, _, share, depth = grads.shape
    hidden = devices * share
    if share % 128:
        return tuple(grads[:, k].reshape(hidden, depth).astype(F32).T for k in range(2))
    column = pl.BlockSpec((depth, share), lambda i: (0, i))
    return pl.pallas_call(
        unpack_kernel,
        out_shape=(jax.ShapeDtypeStruct((depth, hidden), F32),) * 2,
        grid=(devices,),
        in_specs=[pl.BlockSpec((1, 2, share, depth), lambda i: (i, 0, 0, 0))],
        out_specs=[column, column],
        compiler_params=pltpu.CompilerParams(vmem_limit_bytes=40 << 20),
        name="unpack",
    )(grads)


def norm_parts(values):
    centre = jnp.mean(values, axis=-1, keepdims=True)
    centred = values - centre
    inverse = lax.rsqrt(jnp.mean(centred * centred, axis=-1, keepdims=True) + EPS)
    return centred * inverse, inverse


def norm_back(upstream, scaled, inverse, gain):
    through = upstream * gain
    inner = (
        through
        - jnp.mean(through, axis=-1, keepdims=True)
        - scaled * jnp.mean(through * scaled, axis=-1, keepdims=True)
    )
    return inverse * inner, jnp.sum(upstream * scaled, axis=0), jnp.sum(upstream, axis=0)


def on_device(
    tokens, lengths, ln1_gain, ln1_bias, w_query, w_key, w_value, w_out,
    ln2_gain, ln2_bias, w_gate, w_up, down_weight, cotangent,
):
    n = lax.axis_size("tensor")
    local_rows, depth = tokens.shape
    length = local_rows * n
    width = w_query.shape[1]
    row_ids = lax.axis_index("tensor") * local_rows + lax.iota(jnp.int32, local_rows)
    valid = (row_ids < lengths[0])[:, None]

    inputs = tokens.astype(F32)
    grad_out = jnp.where(valid, cotangent.astype(F32), 0.0)
    devices = lax.axis_size("dp")
    place = lax.axis_index("dp")
    share = w_gate.shape[1] // devices

    (
        context, logsum, w_packed, q, k, v, cosine, sine, attn_rows, grad_branch, weights, context_own, _,
        w_out_all,
    ) = front(
        tokens, cotangent, ln1_gain, ln1_bias, angle_tables(length), w_query, w_key, w_value,
        w_gate, w_up, down_weight, w_out, lengths, n, devices,
    )
    attn_rows = attn_rows.reshape(length, depth)
    weights = weights.reshape(3, n * share, depth)

    w_out_all = w_out_all.reshape(n, width, depth)
    attn_out = sum(dot(context_own[t], w_out_all[t]).astype(BF).astype(F32) for t in range(n))
    middle = inputs + attn_out
    scaled2, inverse2 = norm_parts(middle)
    ffn_in = (scaled2 * ln2_gain + ln2_bias).astype(BF)
    grad_parts, out_parts, down_grad, pair_grads, w_packed = ffn(
        ffn_in, grad_branch, weights, w_packed, n, devices
    )
    grad_ffn_in = sum(grad_parts[p].astype(F32) for p in range(devices // 2))
    grad_norm2, gain2_grad, shift2_grad = norm_back(
        grad_ffn_in, scaled2, inverse2, ln2_gain
    )
    grad_middle = grad_out + grad_norm2
    grad_attn = grad_middle.astype(BF)
    w_packed = lax.all_gather(w_packed, "dp", axis=0)
    pair_grads = lax.all_gather(pair_grads, "dp", axis=0)
    down_grad = lax.psum_scatter(down_grad, "tensor", scatter_dimension=0, tiled=True)[0]
    packed, packed_own, out_sums, out_piece = att_bwd(
        grad_attn, w_out_all, context_own, out_parts, q, k, v, context, logsum, cosine, sine, n
    )
    down_grad, out_piece = lax.optimization_barrier((down_grad, out_piece))
    grads = lax.all_gather(jnp.concatenate([down_grad, out_piece]), "dp", axis=0)
    gate_grad, up_grad = unpack(pair_grads)
    down_grad = grads[:, :share].reshape(devices * share, depth).astype(F32)
    out_grad = grads[:, share:].reshape(width, depth).astype(F32)
    ffn_out = sum(x.astype(F32) for x in (out_parts[0], *out_sums))
    output = jnp.where(valid, middle + ffn_out, 0.0).astype(BF)
    input_grad, query_grad, key_grad, value_grad, sums = finish(
        attn_rows, packed, packed_own, w_packed, tokens, grad_middle, ln1_gain,
        jnp.stack([gain2_grad, shift2_grad]), width, devices,
    )
    gain1_grad, shift1_grad, gain2_grad, shift2_grad = (sums[i] for i in range(4))
    return (
        output, input_grad, gain1_grad, shift1_grad, query_grad, key_grad, value_grad, out_grad,
        gain2_grad, shift2_grad, gate_grad, up_grad, down_grad,
    )


def solution(mesh):
    rows = P(("dp", "tensor"), None)
    columns = P(None, "tensor")
    parts = P("tensor", None)
    return jax.shard_map(
        on_device,
        mesh=mesh,
        in_specs=(
            rows, P("dp"), P(), P(), columns, columns, columns, parts,
            P(), P(), columns, columns, parts, rows,
        ),
        out_specs=(
            rows, rows, P(), P(), columns, columns, columns, parts,
            P(), P(), columns, columns, parts,
        ),
        check_vma=False,
    )
```

```python
import functools
import math

import jax
import jax.numpy as jnp
from jax import lax
from jax.experimental import pallas as pl
from jax.experimental.pallas import tpu as pltpu
from jax.sharding import PartitionSpec as P

HD = 64
EPS = 1e-05
SCALE = 1.0 / math.sqrt(HD)
F32 = jnp.float32
BF = jnp.bfloat16
NT = (((1,), (1,)), ((), ()))
NN = (((1,), (0,)), ((), ()))
TN = (((0,), (0,)), ((), ()))
MESH = pl.DeviceIdType.MESH


def dot(a, b, dims=NN):
    return lax.dot_general(a, b, dims, preferred_element_type=F32)


def lanes(shape):
    return lax.broadcasted_iota(jnp.int32, shape, 1)


def split3(x):
    hi = x.astype(BF).astype(F32)
    mid = (x - hi).astype(BF).astype(F32)
    return hi, mid, x - hi - mid


def partner(x):
    width = x.shape[1]
    first = lanes(x.shape) % HD < HD // 2
    return jnp.where(first, pltpu.roll(x, width - HD // 2, 1), pltpu.roll(x, HD // 2, 1))


STEP = 64


def angle_tables(length):
    half = HD // 2
    lane = lax.optimization_barrier(lax.iota(jnp.int32, 2 * HD))
    freqs = 10000.0 ** (-((lane % half).astype(F32) * 2.0 / HD))
    sign = jnp.where(lane % HD < half, -1.0, 1.0)

    def table(positions):
        angles = positions[:, None] * freqs[None, :]
        return jnp.stack([jnp.cos(angles), jnp.sin(angles)])

    return table(lax.iota(F32, length // STEP) * STEP), table(lax.iota(F32, STEP)), sign[None, :]


def differ(a, b, bits):
    return sum(lax.rem(a // (1 << k) + b // (1 << k), 2) * (1 << k) for k in range(bits))


def remote(src, dst, send, recv, **to):
    return pltpu.make_async_remote_copy(
        src_ref=src, dst_ref=dst, send_sem=send, recv_sem=recv, device_id=to, device_id_type=MESH
    )


def ring(n, step):
    return lax.rem(lax.axis_index("tensor") + step, n)


def same_core(s, chips):
    me = lax.axis_index("dp")
    return differ(me // 2, s, chips.bit_length() - 1) * 2 + lax.rem(me, 2)


def sibling():
    me = lax.axis_index("dp")
    return me + 1 - 2 * lax.rem(me, 2)


def greet(n, chips, both_cores=False):
    barrier = pltpu.get_barrier_semaphore()
    if both_cores:
        pl.semaphore_signal(barrier, inc=1, device_id={"dp": sibling()}, device_id_type=MESH)
    for step in range(1, n):
        pl.semaphore_signal(barrier, inc=1, device_id={"tensor": ring(n, step)}, device_id_type=MESH)
    for s in range(1, chips):
        pl.semaphore_signal(
            barrier, inc=1, device_id={"dp": same_core(s, chips)}, device_id_type=MESH
        )
    pl.semaphore_wait(barrier, n + chips - 2 + both_cores)


def front_kernel(
    n, chips, chunks, limit_ref, tokens_ref, ct_ref, gain_ref, shift_ref, coarse_ref, fine_ref, sign_ref,
    wq_ref, wk_ref, wv_ref, gate_ref, up_ref, down_ref, wo_ref,
    ctx_ref, lse_ref, wp_ref, q_out, k_out, v_out, cos_out, sin_out, rows_ref, gb_all, w_all, out_ref, wo_z, wo_all,
    landed, gb, columns, own_w, wqkv, q_ref, k_ref, v_ref, cos_ref, sin_ref,
    right_send, right_recv, left_send, left_recv, gs_send, gs_recv, gr_send, gr_recv, rows_sem,
    wr_send, wr_recv, wl_send, wl_recv, send_sem, recv_sem, wz_send, wz_recv, ws_send, ws_recv,
    wx_send, wx_recv, cut_sem, load_sem, save_sem, keep_sem,
):
    i = pl.program_id(0)
    steps = pl.num_programs(0)
    me = lax.axis_index("tensor")
    place = lax.axis_index("dp")
    core = lax.rem(place, 2)
    bits = chips.bit_length() - 1
    rows, depth = tokens_ref.shape
    heads = q_ref.shape[0]
    piece = rows // chunks
    limit = limit_ref[0]
    s = i // heads
    h = lax.rem(i, heads)

    def over(shard, d, c, send, recv, to):
        part = landed.at[shard, pl.ds(c * piece, piece)]
        return remote(part, part, send.at[d, c], recv.at[d, c], tensor=to)

    def rightward(d, c):
        return over(me - d, d, c, right_send, right_recv, me + 1)

    def leftward(d, c):
        return over(me + d, d, c, left_send, left_recv, me - 1)

    def from_left(d, c):
        return over(me - d, d - 1, c, right_send, right_recv, me - 1)

    def from_right(d, c):
        return over(me + d, d - 1, c, left_send, left_recv, me + 1)

    def weights(shard, d, k, send, recv, to):
        there = w_all.at[k, shard]
        return remote(there if d else own_w.at[k], there, send.at[d, k], recv.at[d, k], tensor=to)

    def w_right(d, k):
        return weights(me - d, d, k, wr_send, wr_recv, me + 1)

    def w_left(d, k):
        return weights(me + d, d, k, wl_send, wl_recv, me - 1)

    def w_from_left(d, k):
        return weights(me - d, d - 1, k, wr_send, wr_recv, me - 1)

    def w_from_right(d, k):
        return weights(me + d, d - 1, k, wl_send, wl_recv, me + 1)

    def spread_gb(c):
        return remote(
            gb, gb_all.at[place // 2, core], gs_send.at[c], gs_recv.at[c], dp=same_core(c, chips)
        )

    def relay_gb(c):
        there = gb_all.at[differ(place // 2, c, bits), core]
        return remote(there if c else gb, there, gr_send.at[c], gr_recv.at[c], dp=sibling())

    def wo_over(step):
        return remote(
            wo_ref, wo_z.at[me], wz_send.at[step], wz_recv.at[step], tensor=ring(n, step + 1)
        )

    def spread_wo(c):
        return remote(
            wo_z, wo_all.at[:, place], ws_send.at[c], ws_recv.at[c], dp=same_core(c, chips)
        )

    def relay_wo(c):
        there = wo_all.at[:, differ(place // 2, c, bits) * 2 + core]
        return remote(there if c else wo_z, there, wx_send.at[c], wx_recv.at[c], dp=sibling())

    def push(step):
        owner = ring(n, step + 1)
        return remote(
            ctx_ref.at[pl.ds(pl.multiple_of(owner * rows, rows), rows)], out_ref.at[me],
            send_sem.at[step], recv_sem.at[step], tensor=owner,
        )

    def save(shard):
        return pltpu.make_async_copy(landed.at[shard], rows_ref.at[shard], rows_sem.at[shard])

    mine = pl.ds(pl.multiple_of(me * rows, rows), rows)
    keeps = [
        pltpu.make_async_copy(gb, gb_all.at[place // 2, core], keep_sem.at[0]),
        pltpu.make_async_copy(wo_ref, wo_z.at[me], keep_sem.at[1]),
        pltpu.make_async_copy(wo_z, wo_all.at[:, place], keep_sem.at[2]),
        pltpu.make_async_copy(ctx_ref.at[mine], out_ref.at[me], keep_sem.at[3]),
        pltpu.make_async_copy(own_w, w_all.at[:, me], keep_sem.at[4]),
    ]
    saves = [
        pltpu.make_async_copy(a, b, save_sem.at[j])
        for j, (a, b) in enumerate(
            ((q_ref, q_out), (k_ref, k_out), (v_ref, v_out), (cos_ref, cos_out), (sin_ref, sin_out))
        )
    ]

    @pl.when(i == 0)
    def _():
        loads = [
            pltpu.make_async_copy(ref, wqkv.at[j], load_sem.at[j])
            for j, ref in enumerate((wq_ref, wk_ref, wv_ref))
        ]
        share = own_w.shape[1]
        ours = pl.ds(pl.multiple_of(place * share, share), share)
        cuts = [pltpu.make_async_copy(down_ref.at[ours], own_w.at[2], cut_sem.at[2])]
        for k, ref in enumerate((gate_ref, up_ref)):
            src = ref if share % 128 else ref.at[:, ours]
            cuts.append(pltpu.make_async_copy(src, columns.at[k], cut_sem.at[k]))
        for copy in loads + cuts:
            copy.start()

        barrier = pltpu.get_barrier_semaphore()
        for step in range(1, n):
            to = ring(n, step)
            pl.semaphore_signal(barrier, inc=1, device_id={"tensor": to}, device_id_type=MESH)
        pl.semaphore_signal(barrier, inc=1, device_id={"dp": sibling()}, device_id_type=MESH)
        for c in range(1, chips):
            to = same_core(c, chips)
            pl.semaphore_signal(barrier, inc=1, device_id={"dp": to}, device_id_type=MESH)

        values = tokens_ref[...].astype(F32)
        values = values - jnp.mean(values, axis=1, keepdims=True)
        inverse = lax.rsqrt(jnp.mean(values * values, axis=1, keepdims=True) + EPS)
        landed[me] = (values * inverse * gain_ref[...] + shift_ref[...]).astype(BF)

        pl.semaphore_wait(barrier, n - 1 + chips)

        for c in range(chunks):

            @pl.when(me < n - 1)
            def _():
                rightward(0, c).start()

            @pl.when(me > 0)
            def _():
                leftward(0, c).start()

        row = me * rows + lax.broadcasted_iota(jnp.int32, (rows, depth), 0)
        gb[...] = jnp.where(row < limit, ct_ref[...].astype(F32), 0.0).astype(BF)
        for c in range(1, chips):
            spread_gb(c).start()
        relay_gb(0).start()
        keeps[0].start()
        keeps[1].start()
        for copy in loads:
            copy.wait()

        cut = wp_ref.shape[0]
        here = pl.ds(pl.multiple_of(place * cut, cut), cut)
        first = lanes((cut, 128)) < HD
        for p in range(heads // 2):
            at = slice(p * 128, p * 128 + 128)
            query, key, value = (wqkv[j, here, at].astype(F32) for j in range(3))
            even = jnp.where(first, key, pltpu.roll(value, HD, 1))
            odd = jnp.where(first, pltpu.roll(key, HD, 1), value)
            for slot, values in ((2 * p, even), (2 * p + 1, odd), (heads + p, query)):
                wp_ref[:, slot * 128 : slot * 128 + 128] = values.astype(BF)

        lane = lanes((rows, 128))
        ones = jnp.where(lane < HD + 3, 1.0, 0.0)
        unit = jnp.where(lane == HD + 3, 1.0, 0.0)

        def put(out, here, values, extra):
            for head in range(heads):
                own = values[:, head // 2 * 128 : head // 2 * 128 + 128]
                own = pltpu.roll(own, HD, 1) if head % 2 else own
                out[head, here, :] = jnp.where(lane < HD, own, extra).astype(BF)

        def project(shard):
            here = pl.ds(pl.multiple_of(shard * rows, rows), rows)
            for j in range(rows // STEP):
                part = pl.ds(pl.multiple_of(shard * rows + j * STEP, STEP), STEP)
                coarse = pl.ds(shard * (rows // STEP) + j, 1)
                c0, s0 = coarse_ref[0, coarse, :], coarse_ref[1, coarse, :]
                cos_ref[part, :] = c0 * fine_ref[0] - s0 * fine_ref[1]
                sin_ref[part, :] = (s0 * fine_ref[0] + c0 * fine_ref[1]) * sign_ref[...]
            cosine = jnp.tile(cos_ref[here, :], (1, heads // 2))
            sine = jnp.tile(sin_ref[here, :], (1, heads // 2))
            x = landed[shard]
            row = shard * rows + lax.broadcasted_iota(jnp.int32, (rows, 128), 0)
            bias = jnp.where(lane == HD + 3, jnp.where(row < limit, 0.0, -1e30), ones)
            raw = dot(x, wqkv[0])
            turned = (raw * cosine + partner(raw) * sine).astype(BF).astype(F32)
            put(q_ref, here, turned * SCALE, unit)
            raw = dot(x, wqkv[1])
            put(k_ref, here, raw * cosine + partner(raw) * sine, bias)
            put(v_ref, here, dot(x, wqkv[2]), ones)

        for d in range(1, n + 1):
            for c in range(chunks):
                if d < n:

                    @pl.when(me >= d)
                    def _():
                        from_left(d, c).wait_recv()

                    @pl.when((me >= d) & (me < n - 1))
                    def _():
                        rightward(d, c).start()

                    @pl.when(me + d < n)
                    def _():
                        from_right(d, c).wait_recv()

                    @pl.when((me + d < n) & (me > 0))
                    def _():
                        leftward(d, c).start()

                if c == 0:

                    @pl.when(me >= d - 1)
                    def _():
                        save(me - d + 1).start()
                        project(me - d + 1)

                if c == 1 and d > 1:

                    @pl.when(me + d - 1 < n)
                    def _():
                        save(me + d - 1).start()
                        project(me + d - 1)

                if c == 2 and d == 1:
                    for cut in cuts:
                        cut.wait()
                    for k in range(2):
                        own_w[k] = columns[k].astype(F32).T.astype(BF)
                    keeps[4].start()

                if c == chunks - 1 and d == 2:
                    for near in range(1, chips // 2 + 1):
                        spread_gb(near).wait_recv()
                        relay_gb(near).start()

            if d < n:

                @pl.when((me < n - 1) & (me + 1 == d))
                def _():
                    for k in range(3):
                        w_right(0, k).start()

                @pl.when((me > 0) & (n - me == d))
                def _():
                    for k in range(3):
                        w_left(0, k).start()

        for copy in saves:
            copy.start()
        for step in range(n - 1):
            wo_over(step).start()
        for far in range(chips // 2 + 1, chips):
            spread_gb(far).wait_recv()
            relay_gb(far).start()

    stride = max((heads * n - 2) // max(n - 2, 1), 1)
    for d in range(1, n - 1):

        @pl.when(i == 1 + (d - 1) * stride)
        def _():
            for k in range(3):

                @pl.when((me >= d) & (me < n - 1))
                def _():
                    w_from_left(d, k).wait_recv()
                    w_right(d, k).start()

                @pl.when((me + d < n) & (me > 0))
                def _():
                    w_from_right(d, k).wait_recv()
                    w_left(d, k).start()

    @pl.when(i == heads)
    def _():
        for step in range(n - 1):
            wo_over(step).wait()
        keeps[1].wait()
        for c in range(1, chips):
            spread_wo(c).start()
        relay_wo(0).start()
        keeps[2].start()

    @pl.when(i == (n - 1) * heads)
    def _():
        for c in range(1, chips):
            spread_wo(c).wait_recv()
            relay_wo(c).start()

    owner = ring(n, s + 1)
    block = pl.ds(pl.multiple_of(owner * rows, rows), rows)
    scores = dot(q_ref[h, block, :], k_ref[h], NT)
    peak = jnp.max(scores, axis=1, keepdims=True)
    acc = dot(jnp.exp(scores - peak).astype(BF), v_ref[h])
    lane = lanes((rows, 128))
    total = jnp.sum(jnp.where(lane == HD, acc, 0.0), axis=1, keepdims=True)
    out = acc * (1.0 / total)
    odd = lax.rem(h, 2)
    out = jnp.where(odd == 1, pltpu.roll(out, HD, 1), out).astype(BF)
    pair = pl.ds(pl.multiple_of(h // 2 * 128, 128), 128)
    ctx_ref[block, pair] = jnp.where((lane >= HD) == (odd == 1), out, ctx_ref[block, pair])
    lse_ref[block, :] = jnp.where(lane == h, peak + jnp.log(total), lse_ref[block, :])

    @pl.when((h == heads - 1) & (s < n - 1))
    def _():
        push(s).start()

    @pl.when(i == steps - 1)
    def _():
        keeps[3].start()
        for d in range(n - 1):
            for c in range(chunks):

                @pl.when((me >= d) & (me < n - 1))
                def _():
                    rightward(d, c).wait_send()

                @pl.when((me + d < n) & (me > 0))
                def _():
                    leftward(d, c).wait_send()

            for k in range(3):

                @pl.when((me >= d) & (me < n - 1))
                def _():
                    w_right(d, k).wait_send()

                @pl.when((me + d < n) & (me > 0))
                def _():
                    w_left(d, k).wait_send()

        for k in range(3):
            for d in range(1, n):

                @pl.when((me >= d) & ((me == n - 1) | (d == n - 1)))
                def _():
                    w_from_left(d, k).wait_recv()

                @pl.when((me + d < n) & ((me == 0) | (d == n - 1)))
                def _():
                    w_from_right(d, k).wait_recv()

        for c in range(chips):
            relay_gb(c).wait()
            relay_wo(c).wait()
            if c:
                spread_gb(c).wait_send()
                spread_wo(c).wait_send()
        for shard in range(n):
            save(shard).wait()
        for copy in saves:
            copy.wait()
        for step in range(n - 1):
            push(step).wait()
        for j in (0, 2, 3, 4):
            keeps[j].wait()


def front(
    tokens, cotangent, gain, shift, tables, w_query, w_key, w_value, gate, up, down, w_out, limit, n, devices
):
    rows, depth = tokens.shape
    total = n * rows
    width = w_query.shape[1]
    heads = width // HD
    chips = devices // 2
    chunks = 4
    place = lax.axis_index("dp")
    share = down.shape[0] // devices
    part = width // devices
    if share % 128:
        gate, up = (lax.dynamic_slice_in_dim(w, place * share, share, 1) for w in (gate, up))
    hbm = pl.BlockSpec(memory_space=pl.ANY)

    def whole(*shape):
        return pl.BlockSpec(shape, lambda *_: (0,) * len(shape), pipeline_mode=pl.Buffered(1))

    def dma(*shape):
        return pltpu.SemaphoreType.DMA(shape)

    head_array = jax.ShapeDtypeStruct((heads, total, 128), BF)
    table = jax.ShapeDtypeStruct((total, 128), F32)
    coarse, fine, sign = tables
    return pl.pallas_call(
        functools.partial(front_kernel, n, chips, chunks),
        out_shape=(
            jax.ShapeDtypeStruct((total, width), BF),
            table,
            jax.ShapeDtypeStruct((depth // devices, 3 * width), BF),
            head_array, head_array, head_array, table, table,
            jax.ShapeDtypeStruct((n, rows, depth), BF),
            jax.ShapeDtypeStruct((chips, 2, rows, depth), BF),
            jax.ShapeDtypeStruct((3, n, share, depth), BF),
            jax.ShapeDtypeStruct((n, rows, width), BF),
            jax.ShapeDtypeStruct((n, part, depth), BF),
            jax.ShapeDtypeStruct((n, devices, part, depth), BF),
        ),
        grid_spec=pltpu.PrefetchScalarGridSpec(
            num_scalar_prefetch=0,
            grid=(n * heads,),
            in_specs=[pl.BlockSpec(memory_space=pltpu.SMEM)]
            + [whole(rows, depth)] * 2
            + [whole(1, depth)] * 2
            + [whole(*coarse.shape), whole(*fine.shape), whole(*sign.shape)]
            + [hbm] * 7,
            out_specs=[whole(total, width), whole(total, 128), whole(depth // devices, 3 * width)]
            + [hbm] * 11,
            scratch_shapes=[
                pltpu.VMEM((n, rows, depth), BF),
                pltpu.VMEM((rows, depth), BF),
                pltpu.VMEM((2, depth, share), BF),
                pltpu.VMEM((3, share, depth), BF),
                pltpu.VMEM((3, depth, width), BF),
            ]
            + [pltpu.VMEM((heads, total, 128), BF)] * 3
            + [pltpu.VMEM((total, 128), F32)] * 2
            + [dma(n - 1, chunks)] * 4
            + [dma(chips)] * 4
            + [dma(n)]
            + [dma(n - 1, 3)] * 4
            + [dma(n - 1)] * 4
            + [dma(chips)] * 4
            + [dma(3), dma(3), dma(5), dma(5)],
        ),
        compiler_params=pltpu.CompilerParams(
            vmem_limit_bytes=60 << 20, collective_id=1, has_side_effects=True
        ),
        cost_estimate=pl.CostEstimate(
            flops=4 * total * total * 256 * heads * 3, bytes_accessed=40 << 20, transcendentals=0
        ),
        name="front",
    )(
        limit, tokens, cotangent, gain.reshape(1, depth), shift.reshape(1, depth), coarse, fine, sign,
        w_query, w_key, w_value, gate, up, down,
        lax.dynamic_slice_in_dim(w_out, place * part, part, 0),
    )


def att_bwd_kernel(
    n, bk, chips, ga_ref, wo_ref, cown_ref, parts_ref, pg_ref, q_ref, k_ref, v_ref, ctx_ref, lse_ref,
    cos_ref, sin_ref, pk_ref, own_ref, sums_ref, og_ref, pg_all, do, gc, dka, dva, dqs,
    og_full, og_own, og_mate, og_sib, og_land, og_piece, og_z,
    send_sem, recv_sem, out_send, out_recv, pk_send, pk_recv, keep_sem,
    om_send, om_recv, op_send, op_recv, oz_send, oz_recv, gs_send, gs_recv, gr_send, gr_recv, pg_sem,
):
    i = pl.program_id(0)
    heads, total, _ = k_ref.shape
    h = jnp.where(i < heads, i, (i - heads) // (n - 1))
    t = jnp.where(i < heads, 0, lax.rem(i - heads, n - 1) + 1)
    rows = total // n
    me = lax.axis_index("tensor")
    place = lax.axis_index("dp")
    core = lax.rem(place, 2)
    bits = chips.bit_length() - 1
    share = og_ref.shape[0]
    mine = pl.ds(pl.multiple_of(me * rows, rows), rows)

    def push(step):
        return remote(
            gc.at[step], do.at[mine], send_sem.at[step], recv_sem.at[step], tensor=ring(n, step + 1)
        )

    def push_out(s):
        return remote(
            parts_ref.at[s], sums_ref.at[s - 1], out_send.at[s - 1], out_recv.at[s - 1],
            dp=same_core(s, chips),
        )

    def columns(slot):
        return pl.ds(pl.multiple_of(slot * 128, 128), 128)

    def push_pack(slot, step):
        owner = ring(n, step + 1)
        return remote(
            pk_ref.at[pl.ds(pl.multiple_of(owner * rows, rows), rows), columns(slot)],
            own_ref.at[me, :, columns(slot)],
            pk_send.at[slot, step], pk_recv.at[slot, step], tensor=owner,
        )

    def keep(slot):
        return pltpu.make_async_copy(
            pk_ref.at[mine, columns(slot)], own_ref.at[me, :, columns(slot)], keep_sem.at[slot]
        )

    @pl.when(i == 0)
    def _():
        greet(n, chips, True)

        def send(step, carry):
            gc[step] = dot(ga_ref[...], wo_ref[ring(n, step + 1)], NT).astype(BF)
            push(step).start()
            return carry

        lax.fori_loop(0, n - 1, send, 0)
        do[mine, :] = dot(ga_ref[...], wo_ref[me], NT).astype(BF)

    def pg_spread(s):
        return remote(pg_ref, pg_all.at[place], gs_send.at[s], gs_recv.at[s], dp=same_core(s, chips))

    def pg_relay(s):
        there = pg_all.at[differ(place // 2, s, bits) * 2 + core]
        return remote(there if s else pg_ref, there, gr_send.at[s], gr_recv.at[s], dp=sibling())

    def pg_keep():
        return pltpu.make_async_copy(pg_ref, pg_all.at[place], pg_sem)

    @pl.when(i == 1)
    def _():
        for s in range(1, chips):
            pg_spread(s).start()
        pg_relay(0).start()
        pg_keep().start()

    @pl.when(i == heads * n - 2)
    def _():
        for s in range(1, chips):
            pg_spread(s).wait_recv()
            pg_relay(s).start()

    def og_swap():
        return remote(og_mate, og_sib, om_send, om_recv, dp=sibling())

    def og_push(s):
        return remote(og_sib.at[s], og_land.at[s], op_send.at[s], op_recv.at[s], dp=same_core(s, chips))

    def og_over(step):
        to = ring(n, step + 1)
        return remote(og_piece.at[to], og_z.at[me], oz_send.at[step], oz_recv.at[step], tensor=to)

    @pl.when(i == 1)
    def _():
        def term(part, carry):
            og_full[...] = dot(cown_ref[part], ga_ref[...], TN)
            for s in range(chips):
                start = differ(place // 2, s, bits) * 2
                here = pl.ds(pl.multiple_of((start + core) * share, share), share)
                there = pl.ds(pl.multiple_of((start + 1 - core) * share, share), share)
                og_own[s, part] = og_full[here, :]
                og_mate[s, part] = og_full[there, :].astype(BF)
            return carry

        lax.fori_loop(0, n, term, 0)
        og_swap().start()

    @pl.when(i == 2)
    def _():
        og_swap().wait_recv()
        for s in range(chips):
            og_sib[s] = (og_own[s] + og_sib[s].astype(F32)).astype(BF)
            if s:
                og_push(s).start()

    @pl.when(i == heads + 2)
    def _():
        joined = og_sib[0].astype(F32)
        for s in range(1, chips):
            og_push(s).wait_recv()
            joined = joined + og_land[s].astype(F32)
        og_piece[...] = joined.astype(BF)
        for step in range(n - 1):
            og_over(step).start()
        for s in range(1, chips):
            push_out(s).start()

    @pl.when(i == heads * n - 1)
    def _():
        og_z[me] = og_piece[me]
        for step in range(n - 1):
            og_over(step).wait_recv()
        joined = og_z[0].astype(F32)
        for part in range(1, n):
            joined = joined + og_z[part].astype(F32)
        og_ref[...] = joined.astype(BF)

    @pl.when((h == 0) & (t > 0))
    def _():
        push(t - 1).wait_recv()

    source = ring(n, n - t)
    block = pl.ds(pl.multiple_of(source * rows, rows), rows)
    pair = columns(h // 2)
    odd = lax.rem(h, 2) == 1
    lane = lanes((rows, 128))
    off = lane - HD
    logsum = jnp.sum(jnp.where(lane == h, lse_ref[block, :], 0.0), axis=1, keepdims=True)
    a, b, c = split3(-logsum)
    q = q_ref[h, block, :].astype(F32)
    q = jnp.where(off == 0, a, jnp.where(off == 1, b, jnp.where(off == 2, c, q))).astype(BF)
    g = jnp.where((lane >= HD) == odd, do[block, pair].astype(F32), 0.0)
    delta = jnp.sum(g * ctx_ref[block, pair].astype(F32), axis=1, keepdims=True)
    a, b, c = split3(-delta)
    g = jnp.where(odd, pltpu.roll(g, HD, 1), g)
    g = jnp.where(off == 0, a, jnp.where(off == 1, b, jnp.where(off == 2, c, g))).astype(BF)
    acc = jnp.zeros((rows, 128), F32)
    for j in range(total // bk):
        rk = pl.ds(j * bk, bk)
        kt = k_ref[h, rk, :]
        probs = jnp.exp(dot(kt, q, NT))
        grad = (probs * dot(v_ref[h, rk, :], g, NT)).astype(BF)
        for sums, term in ((dva, dot(probs.astype(BF), g)), (dka, dot(grad, q))):
            before = jnp.where(t == 0, jnp.zeros_like(term), sums[h, rk, :])
            sums[h, rk, :] = before + term
        acc = acc + dot(grad, kt, TN)
    acc = acc * SCALE

    @pl.when(jnp.logical_not(odd))
    def _():
        dqs[block, :] = acc

    @pl.when(odd)
    def _():
        grad = jnp.where(lane < HD, dqs[block, :], pltpu.roll(acc, HD, 1))
        grad = grad * cos_ref[block, :] - partner(grad) * sin_ref[block, :]
        pk_ref[block, columns(heads + h // 2)] = grad.astype(BF)

    @pl.when(odd & (t == 0))
    def _():
        keep(heads + h // 2).start()

    @pl.when(odd & (t > 0))
    def _():
        push_pack(heads + h // 2, n - 1 - t).start()

    @pl.when(t == n - 1)
    def _():
        dk = dka[h]
        dk = dk * cos_ref[...] - partner(dk) * sin_ref[...]
        both = jnp.where(lanes((total, 128)) < HD, dk, pltpu.roll(dva[h], HD, 1))
        pk_ref[:, columns(h)] = both.astype(BF)
        for step in range(n - 1):
            push_pack(h, step).start()
        keep(h).start()

    @pl.when(i == heads * n - 1)
    def _():
        for step in range(n - 1):
            push(step).wait_send()
        for s in range(1, chips):
            push_out(s).wait()
        og_swap().wait_send()
        pg_keep().wait()
        for s in range(chips):
            pg_relay(s).wait()
            if s:
                pg_spread(s).wait_send()
        for s in range(1, chips):
            og_push(s).wait_send()
        for step in range(n - 1):
            og_over(step).wait_send()
        for slot in range(heads + heads // 2):
            keep(slot).wait()
            for step in range(n - 1):
                push_pack(slot, step).wait()


def att_bwd(
    grad_attn, w_out, ctx_own, parts, pair_grads, q, k, v, ctx, lse, cosine, sine, n, bk=512
):
    heads, total, _ = q.shape
    width = heads * HD
    rows, depth = grad_attn.shape
    chips = parts.shape[0]
    share = width // (2 * chips)
    slots = heads + heads // 2
    hbm = pl.BlockSpec(memory_space=pl.ANY)

    def whole(*shape):
        return pl.BlockSpec(shape, lambda *_: (0,) * len(shape), pipeline_mode=pl.Buffered(1))

    return pl.pallas_call(
        functools.partial(att_bwd_kernel, n, bk, chips),
        out_shape=(
            jax.ShapeDtypeStruct((total, slots * 128), BF),
            jax.ShapeDtypeStruct((n, rows, slots * 128), BF),
            jax.ShapeDtypeStruct((chips - 1, rows, depth), BF),
            jax.ShapeDtypeStruct((share, depth), BF),
            jax.ShapeDtypeStruct((2 * chips, *pair_grads.shape), BF),
        ),
        grid_spec=pltpu.PrefetchScalarGridSpec(
            num_scalar_prefetch=0,
            grid=(heads * n,),
            in_specs=[whole(rows, depth), whole(n, width, depth), whole(n, rows, width), hbm, hbm]
            + [whole(heads, total, 128)] * 3
            + [whole(total, width)]
            + [whole(total, 128)] * 3,
            out_specs=[whole(total, slots * 128), hbm, hbm, whole(share, depth), hbm],
            scratch_shapes=[
                pltpu.VMEM((total, width), BF),
                pltpu.VMEM((n - 1, rows, width), BF),
            ]
            + [pltpu.VMEM((heads, total, 128), F32)] * 2
            + [pltpu.VMEM((total, 128), F32)]
            + [
                pltpu.VMEM((width, depth), F32),
                pltpu.VMEM((chips, n, share, depth), F32),
                pltpu.VMEM((chips, n, share, depth), BF),
                pltpu.VMEM((chips, n, share, depth), BF),
                pltpu.VMEM((chips, n, share, depth), BF),
                pltpu.VMEM((n, share, depth), BF),
                pltpu.VMEM((n, share, depth), BF),
            ]
            + [pltpu.SemaphoreType.DMA((n - 1,))] * 2
            + [pltpu.SemaphoreType.DMA((chips - 1,))] * 2
            + [pltpu.SemaphoreType.DMA((slots, n - 1))] * 2
            + [pltpu.SemaphoreType.DMA((slots,))]
            + [pltpu.SemaphoreType.DMA] * 2
            + [pltpu.SemaphoreType.DMA((chips,))] * 2
            + [pltpu.SemaphoreType.DMA((n - 1,))] * 2
            + [pltpu.SemaphoreType.DMA((chips,))] * 4
            + [pltpu.SemaphoreType.DMA],
        ),
        compiler_params=pltpu.CompilerParams(
            vmem_limit_bytes=60 << 20, collective_id=2, has_side_effects=True
        ),
        cost_estimate=pl.CostEstimate(
            flops=10 * total * total * 256 * heads,
            bytes_accessed=20 * total * width,
            transcendentals=total * total * heads,
        ),
        name="att_bwd",
    )(grad_attn, w_out, ctx_own, parts, pair_grads, q, k, v, ctx, lse, cosine, sine)


def finish_kernel(
    chips, n, width, x_ref, pk_ref, own_ref, w_ref, tokens_ref, middle_ref, gain_ref, vec_ref,
    input_ref, q_ref, k_ref, v_ref, sums_ref,
    full, mate, sib, land, fin, every, vec_z, vec_dp, vec_me,
    sx_send, sx_recv, rs_send, rs_recv, ag_send, ag_recv, rl_send, rl_recv,
    vz_send, vz_recv, vd_send, vd_recv, own_sem,
):
    bits = chips.bit_length() - 1
    me = lax.axis_index("dp")
    place = lax.axis_index("tensor")
    core = lax.rem(me, 2)
    chip = me // 2
    other = 1 - core
    heads = width // HD
    piece = fin.shape[0]

    def swap(s):
        return remote(mate.at[s], sib.at[s], sx_send.at[s], sx_recv.at[s], dp=chip * 2 + other)

    def push(s):
        return remote(sib.at[s], land.at[s], rs_send.at[s], rs_recv.at[s], dp=same_core(s, chips))

    def spread(s):
        return remote(
            fin, every.at[chip, core], ag_send.at[s], ag_recv.at[s], dp=same_core(s, chips)
        )

    def relay(s):
        src = every.at[differ(chip, s, bits), core]
        return remote(src, src, rl_send.at[s], rl_recv.at[s], dp=chip * 2 + other)

    def vec_over(step):
        return remote(
            vec_me.at[0], vec_z.at[place], vz_send.at[step], vz_recv.at[step], tensor=ring(n, step + 1)
        )

    def vec_across(step):
        return remote(
            vec_me.at[1], vec_dp.at[me], vd_send.at[step], vd_recv.at[step],
            dp=lax.rem(me + step + 1, 2 * chips),
        )

    barrier = pltpu.get_barrier_semaphore()
    for step in range(n - 1):
        pl.semaphore_signal(barrier, inc=1, device_id={"tensor": ring(n, step + 1)}, device_id_type=MESH)
    for step in range(2 * chips - 1):
        to = lax.rem(me + step + 1, 2 * chips)
        pl.semaphore_signal(barrier, inc=1, device_id={"dp": to}, device_id_type=MESH)

    full[...] = dot(x_ref[...], pk_ref[...], TN)
    pl.semaphore_wait(barrier, n + 2 * chips - 2)

    def part(s, which):
        start = (differ(chip, s, bits) * 2 + which) * piece
        return full[pl.ds(pl.multiple_of(start, piece), piece), :]

    for s in range(chips):
        mate[s] = part(s, other).astype(BF)
        swap(s).start()

    grad = jnp.zeros(input_ref.shape, F32)
    for t in range(n):
        w = w_ref[:, t].reshape(w_ref.shape[0] * w_ref.shape[2], w_ref.shape[3])
        grad = grad + dot(own_ref[t], w, NT).astype(BF).astype(F32)

    for s in range(1, chips):
        swap(s).wait_recv()
        sib[s] = (sib[s].astype(F32) + part(s, core)).astype(BF)
        push(s).start()
    swap(0).wait_recv()
    total = sib[0].astype(F32) + part(0, core)

    values = tokens_ref[...].astype(F32)
    values = values - jnp.mean(values, axis=1, keepdims=True)
    inverse = lax.rsqrt(jnp.mean(values * values, axis=1, keepdims=True) + EPS)
    scaled = values * inverse
    through = grad * gain_ref[...]
    inner = through - jnp.mean(through, axis=1, keepdims=True)
    inner = inner - scaled * jnp.mean(through * scaled, axis=1, keepdims=True)
    input_ref[...] = middle_ref[...] + inverse * inner
    vec_me[0, 0:1] = jnp.sum(grad * scaled, axis=0, keepdims=True)
    vec_me[0, 1:2] = jnp.sum(grad, axis=0, keepdims=True)
    vec_me[0, 2:4] = vec_ref[...]
    vec_me[0, 4:8] = jnp.zeros((4, vec_ref.shape[1]), F32)
    vec_z[place] = vec_me[0]
    for step in range(n - 1):
        vec_over(step).start()

    for s in range(1, chips):
        push(s).wait_recv()
        total = total + land[s].astype(F32)
    fin[...] = total.astype(BF)
    for s in range(1, chips):
        spread(s).start()
    mine = pltpu.make_async_copy(fin, every.at[chip, core], own_sem)
    mine.start()
    mine.wait()
    relay(0).start()

    for step in range(n - 1):
        vec_over(step).wait()
    vec = vec_z[0]
    for t in range(1, n):
        vec = vec + vec_z[t]
    vec_me[1] = vec
    vec_dp[me] = vec
    for step in range(2 * chips - 1):
        vec_across(step).start()
    for s in range(1, chips):
        spread(s).wait_recv()
        relay(s).start()
    for step in range(2 * chips - 1):
        vec_across(step).wait()
    vec = vec_dp[0]
    for t in range(1, 2 * chips):
        vec = vec + vec_dp[t]
    sums_ref[...] = vec
    for s in range(chips):
        relay(s).wait()
        swap(s).wait_send()
        if s > 0:
            spread(s).wait_send()
            push(s).wait_send()
    first = lanes((piece, 128)) < HD
    for d in range(2 * chips):
        rows = slice(d * piece, (d + 1) * piece)
        g = every[d // 2, d % 2].astype(F32)
        for pair in range(heads // 2):
            a = g[:, pair * 256 : pair * 256 + 128]
            b = g[:, pair * 256 + 128 : pair * 256 + 256]
            out = slice(pair * 128, pair * 128 + 128)
            q_ref[rows, out] = g[:, (heads + pair) * 128 : (heads + pair + 1) * 128]
            k_ref[rows, out] = jnp.where(first, a, pltpu.roll(b, HD, 1))
            v_ref[rows, out] = jnp.where(first, pltpu.roll(a, HD, 1), b)


def finish(rows_all, packed, own, w_all, tokens, middle, gain, vec, width, devices):
    n, rows, packs = own.shape
    depth = tokens.shape[1]
    chips = devices // 2
    piece = depth // devices
    vmem = pl.BlockSpec(memory_space=pltpu.VMEM)
    out = jax.ShapeDtypeStruct((depth, width), F32)
    return pl.pallas_call(
        functools.partial(finish_kernel, chips, n, width),
        out_shape=(
            jax.ShapeDtypeStruct((rows, depth), F32), out, out, out,
            jax.ShapeDtypeStruct((8, depth), F32),
        ),
        in_specs=[vmem] * 8,
        out_specs=[vmem] * 5,
        scratch_shapes=[
            pltpu.VMEM((depth, packs), F32),
            pltpu.VMEM((chips, piece, packs), BF),
            pltpu.VMEM((chips, piece, packs), BF),
            pltpu.VMEM((chips, piece, packs), BF),
            pltpu.VMEM((piece, packs), BF),
            pltpu.VMEM((chips, 2, piece, packs), BF),
            pltpu.VMEM((n, 8, depth), F32),
            pltpu.VMEM((devices, 8, depth), F32),
            pltpu.VMEM((2, 8, depth), F32),
        ]
        + [pltpu.SemaphoreType.DMA((chips,))] * 8
        + [pltpu.SemaphoreType.DMA((n - 1,))] * 2
        + [pltpu.SemaphoreType.DMA((devices - 1,))] * 2
        + [pltpu.SemaphoreType.DMA],
        compiler_params=pltpu.CompilerParams(
            vmem_limit_bytes=56 << 20, collective_id=4, has_side_effects=True
        ),
        cost_estimate=pl.CostEstimate(
            flops=4 * n * rows * depth * packs, bytes_accessed=20 << 20, transcendentals=0
        ),
        name="finish",
    )(rows_all, packed, own, w_all, tokens, middle, gain.reshape(1, depth), vec)


def ffn_kernel(
    chips, x_ref, gb_ref, w_ref, wp_ref, dx_ref, out_ref, dw_ref, zs_ref, wp_z,
    rows_all, gb, hid, gate_g, up_g, own, sib, mate, partial, z_left, z_right,
    ag_send, ag_recv, rl_send, rl_recv, sx_send, sx_recv, rs_send, rs_recv, fw_send, fw_recv,
    gb_sem, out_sem, dx_sem, wp_send, wp_recv, wp_sem, zr_send, zr_recv, zl_send, zl_recv,
):
    bits = chips.bit_length() - 1
    me = lax.axis_index("dp")
    core = lax.rem(me, 2)
    chip = me // 2
    other = 1 - core
    rows, depth = x_ref.shape
    n, share, _ = dw_ref.shape

    def spread(s):
        to = differ(chip, s, bits) * 2 + core
        return remote(x_ref, rows_all.at[chip, core], ag_send.at[s], ag_recv.at[s], dp=to)

    square = chips == 4

    def hand_on(s):
        half = pl.ds((s - 1) * (rows // 2), rows // 2)
        part = rows_all.at[differ(chip, s, bits), core, half]
        to = differ(chip, 3 - s, bits) * 2 + core
        return remote(part, part, fw_send.at[s], fw_recv.at[s], dp=to)

    def handed(s):
        half = pl.ds((s - 1) * (rows // 2), rows // 2)
        part = rows_all.at[differ(chip, 3, bits), core, half]
        to = differ(chip, 3 - s, bits) * 2 + core
        return remote(part, part, fw_send.at[s], fw_recv.at[s], dp=to)

    def relay(s):
        src = differ(chip, s, bits)
        return remote(
            rows_all.at[src, core], rows_all.at[src, core], rl_send.at[s], rl_recv.at[s],
            dp=chip * 2 + other,
        )

    def swap(s):
        return remote(
            mate.at[lax.rem(s, 2)], sib.at[s], sx_send.at[s], sx_recv.at[s], dp=chip * 2 + other
        )

    def push(s):
        to = differ(chip, s, bits) * 2 + core
        return remote(sib.at[s, 0], dx_ref.at[s], rs_send.at[s], rs_recv.at[s], dp=to)

    def fetch(s):
        src = differ(chip, s, bits)
        return pltpu.make_async_copy(gb_ref.at[src], gb.at[src], gb_sem.at[s])

    part = lax.axis_index("tensor")

    def over(step):
        return remote(
            wp_ref, wp_z.at[part], wp_send.at[step], wp_recv.at[step], tensor=ring(n, step + 1)
        )

    def keep(s):
        return pltpu.make_async_copy(sib.at[s, 1], out_ref.at[s], out_sem.at[s])

    for s in range(chips):
        fetch(s).start()
    barrier = pltpu.get_barrier_semaphore()
    for step in range(1, n):
        pl.semaphore_signal(barrier, inc=1, device_id={"tensor": ring(n, step)}, device_id_type=MESH)
    pl.semaphore_signal(barrier, inc=1, device_id={"dp": chip * 2 + other}, device_id_type=MESH)
    for s in range(1, chips):
        to = differ(chip, s, bits) * 2 + core
        pl.semaphore_signal(barrier, inc=1, device_id={"dp": to}, device_id_type=MESH)
    pl.semaphore_wait(barrier, chips + n - 1)
    direct = range(1, 3) if square else range(1, chips)
    for s in direct:
        spread(s).start()
    mine = pltpu.make_async_copy(x_ref, rows_all.at[chip, core], ag_send.at[0])
    mine.start()
    mine.wait()
    relay(0).start()
    for step in range(n - 1):
        over(step).start()
    keep_wp = pltpu.make_async_copy(wp_ref, wp_z.at[part], wp_sem)
    keep_wp.start()

    def shard(src, which, put):
        x = rows_all[src, which]
        grad = gb[src, which]
        gate = dot(x, w_ref[0], NT)
        upper = dot(x, w_ref[1], NT)
        grad_hidden = dot(grad, w_ref[2], NT)
        sigma = jax.nn.sigmoid(gate)
        act = gate * sigma
        hidden = (act * upper).astype(BF)
        grad_gate = (grad_hidden * upper * sigma * (1.0 + gate * (1.0 - sigma))).astype(BF)
        grad_upper = (grad_hidden * act).astype(BF)
        hid[src, which] = hidden
        gate_g[src, which] = grad_gate
        up_g[src, which] = grad_upper
        put[0] = (dot(grad_gate, w_ref[0]) + dot(grad_upper, w_ref[1])).astype(BF)
        put[1] = dot(hidden, w_ref[2]).astype(BF)

    def step(s, carry):
        src = differ(chip, s, bits)
        slot = lax.rem(s, 2)
        relay(s).wait_recv()
        fetch(s).wait()

        @pl.when(s >= 2)
        def _():
            swap(s - 2).wait_send()

        shard(src, other, mate.at[slot])
        swap(s).start()
        shard(src, core, own)
        swap(s).wait_recv()
        for k in range(2):
            sib[s, k] = (sib[s, k].astype(F32) + own[k].astype(F32)).astype(BF)

        @pl.when(s > 0)
        def _():
            push(s).start()

        keep(s).start()

        if square:

            @pl.when(s == 0)
            def _():
                for near in (1, 2):
                    spread(near).wait_recv()
                    hand_on(near).start()
                    relay(near).start()

        else:

            @pl.when(s < chips - 1)
            def _():
                spread(s + 1).wait_recv()
                relay(s + 1).start()

        if square:

            @pl.when(s == 1)
            def _():
                handed(1).wait_recv()
                handed(2).wait_recv()
                relay(3).start()

        return carry

    lax.fori_loop(0, chips, step, 0)
    first = pltpu.make_async_copy(sib.at[0, 0], dx_ref.at[0], dx_sem)
    first.start()
    def zr(t, k, to):
        return remote(
            partial.at[t, k], z_left.at[t, k], zr_send.at[t, k], zr_recv.at[t, k], tensor=to
        )

    def zl(t, k, to):
        return remote(
            partial.at[t, k], z_right.at[t, k], zl_send.at[t, k], zl_recv.at[t, k], tensor=to
        )

    def join(t, k, more):
        partial[t, k] = (partial[t, k].astype(F32) + more[t, k].astype(F32)).astype(BF)

    def weight_grad(left, right):
        left = left[...].reshape(-1, n * share)
        return dot(left, right[...].reshape(-1, depth), TN)

    for k, left in enumerate((gate_g, up_g)):
        grad = weight_grad(left, rows_all)
        for t in range(n):
            partial[t, k] = grad[t * share : (t + 1) * share, :].astype(BF)

        for j in range(n - 1):

            @pl.when(part == 0)
            def _():
                zr(n - 1 - j, k, 1).start()

            @pl.when(part == n - 1)
            def _():
                zl(j, k, n - 2).start()

    grad = weight_grad(hid, gb)
    for t in range(n):
        dw_ref[t] = grad[t * share : (t + 1) * share, :].astype(BF)
    for k in range(2):
        for j in range(n - 1):
            t = n - 1 - j

            @pl.when((part > 0) & (part < t))
            def _():
                zr(t, k, part + 1).wait_recv()
                join(t, k, z_left)
                zr(t, k, part + 1).start()

            @pl.when((part < n - 1) & (part > j))
            def _():
                zl(j, k, part - 1).wait_recv()
                join(j, k, z_right)
                zl(j, k, part - 1).start()

        for t in range(n):

            @pl.when((part == t) & (part > 0))
            def _():
                zr(t, k, part - 1).wait_recv()
                join(t, k, z_left)

            @pl.when((part == t) & (part < n - 1))
            def _():
                zl(t, k, part + 1).wait_recv()
                join(t, k, z_right)

            @pl.when(part == t)
            def _():
                zs_ref[k] = partial[t, k]

            @pl.when(part < t)
            def _():
                zr(t, k, part + 1).wait_send()

            @pl.when(part > t)
            def _():
                zl(t, k, part - 1).wait_send()

    first.wait()
    keep_wp.wait()
    for step in range(n - 1):
        over(step).wait()
    for s in range(chips):
        keep(s).wait()
        relay(s).wait_send()
        if s >= chips - 2:
            swap(s).wait_send()
        if s in direct:
            spread(s).wait_send()
        if s > 0:
            push(s).wait()
    if square:
        hand_on(1).wait_send()
        hand_on(2).wait_send()


def ffn(x, grad_branch, weights, w_packed, n, devices):
    rows, depth = x.shape
    chips = devices // 2
    hidden = weights.shape[1]
    share = hidden // n
    vmem = pl.BlockSpec(memory_space=pltpu.VMEM)
    hbm = pl.BlockSpec(memory_space=pl.ANY)
    return pl.pallas_call(
        functools.partial(ffn_kernel, chips),
        out_shape=(
            jax.ShapeDtypeStruct((chips, rows, depth), BF),
            jax.ShapeDtypeStruct((chips, rows, depth), BF),
            jax.ShapeDtypeStruct((n, share, depth), BF),
            jax.ShapeDtypeStruct((2, share, depth), BF),
            jax.ShapeDtypeStruct((n, *w_packed.shape), BF),
        ),
        in_specs=[vmem, hbm, vmem, hbm],
        out_specs=[hbm, hbm, vmem, vmem, hbm],
        scratch_shapes=[
            pltpu.VMEM((chips, 2, rows, depth), BF),
            pltpu.VMEM((chips, 2, rows, depth), BF),
        ]
        + [pltpu.VMEM((chips, 2, rows, hidden), BF)] * 3
        + [
            pltpu.VMEM((2, rows, depth), BF),
            pltpu.VMEM((chips, 2, rows, depth), BF),
            pltpu.VMEM((2, 2, rows, depth), BF),
        ]
        + [pltpu.VMEM((n, 2, share, depth), BF)] * 3
        + [pltpu.SemaphoreType.DMA((chips,))] * 8
        + [pltpu.SemaphoreType.DMA((3,))] * 2
        + [pltpu.SemaphoreType.DMA((chips,))] * 2
        + [pltpu.SemaphoreType.DMA]
        + [pltpu.SemaphoreType.DMA((n - 1,))] * 2
        + [pltpu.SemaphoreType.DMA]
        + [pltpu.SemaphoreType.DMA((n, 2))] * 4,
        compiler_params=pltpu.CompilerParams(
            vmem_limit_bytes=62 << 20, collective_id=3, has_side_effects=True
        ),
        cost_estimate=pl.CostEstimate(
            flops=2 * 9 * devices * rows * depth * hidden, bytes_accessed=30 << 20, transcendentals=0
        ),
        name="ffn",
    )(x, grad_branch, weights, w_packed)


def unpack_kernel(g_ref, gate_ref, up_ref):
    gate_ref[...] = g_ref[0, 0].astype(F32).T
    up_ref[...] = g_ref[0, 1].astype(F32).T


def unpack(grads):
    devices, _, share, depth = grads.shape
    hidden = devices * share
    if share % 128:
        return tuple(grads[:, k].reshape(hidden, depth).astype(F32).T for k in range(2))
    column = pl.BlockSpec((depth, share), lambda i: (0, i))
    return pl.pallas_call(
        unpack_kernel,
        out_shape=(jax.ShapeDtypeStruct((depth, hidden), F32),) * 2,
        grid=(devices,),
        in_specs=[pl.BlockSpec((1, 2, share, depth), lambda i: (i, 0, 0, 0))],
        out_specs=[column, column],
        compiler_params=pltpu.CompilerParams(vmem_limit_bytes=40 << 20),
        name="unpack",
    )(grads)


def norm_parts(values):
    centre = jnp.mean(values, axis=-1, keepdims=True)
    centred = values - centre
    inverse = lax.rsqrt(jnp.mean(centred * centred, axis=-1, keepdims=True) + EPS)
    return centred * inverse, inverse


def norm_back(upstream, scaled, inverse, gain):
    through = upstream * gain
    inner = (
        through
        - jnp.mean(through, axis=-1, keepdims=True)
        - scaled * jnp.mean(through * scaled, axis=-1, keepdims=True)
    )
    return inverse * inner, jnp.sum(upstream * scaled, axis=0), jnp.sum(upstream, axis=0)


def on_device(
    tokens, lengths, ln1_gain, ln1_bias, w_query, w_key, w_value, w_out,
    ln2_gain, ln2_bias, w_gate, w_up, down_weight, cotangent,
):
    n = lax.axis_size("tensor")
    local_rows, depth = tokens.shape
    length = local_rows * n
    width = w_query.shape[1]
    row_ids = lax.axis_index("tensor") * local_rows + lax.iota(jnp.int32, local_rows)
    valid = (row_ids < lengths[0])[:, None]

    inputs = tokens.astype(F32)
    grad_out = jnp.where(valid, cotangent.astype(F32), 0.0)
    devices = lax.axis_size("dp")
    place = lax.axis_index("dp")
    share = w_gate.shape[1] // devices

    (
        context, logsum, w_packed, q, k, v, cosine, sine, attn_rows, grad_branch, weights, context_own, _,
        w_out_all,
    ) = front(
        tokens, cotangent, ln1_gain, ln1_bias, angle_tables(length), w_query, w_key, w_value,
        w_gate, w_up, down_weight, w_out, lengths, n, devices,
    )
    attn_rows = attn_rows.reshape(length, depth)
    weights = weights.reshape(3, n * share, depth)

    w_out_all = w_out_all.reshape(n, width, depth)
    attn_out = sum(dot(context_own[t], w_out_all[t]).astype(BF).astype(F32) for t in range(n))
    middle = inputs + attn_out
    scaled2, inverse2 = norm_parts(middle)
    ffn_in = (scaled2 * ln2_gain + ln2_bias).astype(BF)
    grad_parts, out_parts, down_grad, pair_grads, w_packed = ffn(
        ffn_in, grad_branch, weights, w_packed, n, devices
    )
    grad_ffn_in = sum(grad_parts[p].astype(F32) for p in range(devices // 2))
    grad_norm2, gain2_grad, shift2_grad = norm_back(
        grad_ffn_in, scaled2, inverse2, ln2_gain
    )
    grad_middle = grad_out + grad_norm2
    grad_attn = grad_middle.astype(BF)
    w_packed = lax.all_gather(w_packed, "dp", axis=0)
    down_grad = lax.psum_scatter(down_grad, "tensor", scatter_dimension=0, tiled=True)[0]
    packed, packed_own, out_sums, out_piece, pair_grads = att_bwd(
        grad_attn, w_out_all, context_own, out_parts, pair_grads, q, k, v, context, logsum, cosine, sine, n
    )
    down_grad, out_piece, w_packed = lax.optimization_barrier((down_grad, out_piece, w_packed))
    grads = lax.all_gather(jnp.concatenate([down_grad, out_piece]), "dp", axis=0)
    gate_grad, up_grad = unpack(pair_grads)
    down_grad = grads[:, :share].reshape(devices * share, depth).astype(F32)
    out_grad = grads[:, share:].reshape(width, depth).astype(F32)
    ffn_out = sum(x.astype(F32) for x in (out_parts[0], *out_sums))
    output = jnp.where(valid, middle + ffn_out, 0.0).astype(BF)
    input_grad, query_grad, key_grad, value_grad, sums = finish(
        attn_rows, packed, packed_own, w_packed, tokens, grad_middle, ln1_gain,
        jnp.stack([gain2_grad, shift2_grad]), width, devices,
    )
    gain1_grad, shift1_grad, gain2_grad, shift2_grad = (sums[i] for i in range(4))
    return (
        output, input_grad, gain1_grad, shift1_grad, query_grad, key_grad, value_grad, out_grad,
        gain2_grad, shift2_grad, gate_grad, up_grad, down_grad,
    )


def solution(mesh):
    rows = P(("dp", "tensor"), None)
    columns = P(None, "tensor")
    parts = P("tensor", None)
    return jax.shard_map(
        on_device,
        mesh=mesh,
        in_specs=(
            rows, P("dp"), P(), P(), columns, columns, columns, parts,
            P(), P(), columns, columns, parts, rows,
        ),
        out_specs=(
            rows, rows, P(), P(), columns, columns, columns, parts,
            P(), P(), columns, columns, parts,
        ),
        check_vma=False,
    )
```

```python
import functools
import math

import jax
import jax.numpy as jnp
from jax import lax
from jax.experimental import pallas as pl
from jax.experimental.pallas import tpu as pltpu
from jax.sharding import PartitionSpec as P

HD = 64
EPS = 1e-05
SCALE = 1.0 / math.sqrt(HD)
F32 = jnp.float32
BF = jnp.bfloat16
NT = (((1,), (1,)), ((), ()))
NN = (((1,), (0,)), ((), ()))
TN = (((0,), (0,)), ((), ()))
MESH = pl.DeviceIdType.MESH


def dot(a, b, dims=NN):
    return lax.dot_general(a, b, dims, preferred_element_type=F32)


def lanes(shape):
    return lax.broadcasted_iota(jnp.int32, shape, 1)


def split3(x):
    hi = x.astype(BF).astype(F32)
    mid = (x - hi).astype(BF).astype(F32)
    return hi, mid, x - hi - mid


def partner(x):
    width = x.shape[1]
    first = lanes(x.shape) % HD < HD // 2
    return jnp.where(first, pltpu.roll(x, width - HD // 2, 1), pltpu.roll(x, HD // 2, 1))


STEP = 64


def angle_tables(length):
    half = HD // 2
    lane = lax.optimization_barrier(lax.iota(jnp.int32, 2 * HD))
    freqs = 10000.0 ** (-((lane % half).astype(F32) * 2.0 / HD))
    sign = jnp.where(lane % HD < half, -1.0, 1.0)

    def table(positions):
        angles = positions[:, None] * freqs[None, :]
        return jnp.stack([jnp.cos(angles), jnp.sin(angles)])

    return table(lax.iota(F32, length // STEP) * STEP), table(lax.iota(F32, STEP)), sign[None, :]


def differ(a, b, bits):
    return sum(lax.rem(a // (1 << k) + b // (1 << k), 2) * (1 << k) for k in range(bits))


def remote(src, dst, send, recv, **to):
    return pltpu.make_async_remote_copy(
        src_ref=src, dst_ref=dst, send_sem=send, recv_sem=recv, device_id=to, device_id_type=MESH
    )


def ring(n, step):
    return lax.rem(lax.axis_index("tensor") + step, n)


def same_core(s, chips):
    me = lax.axis_index("dp")
    return differ(me // 2, s, chips.bit_length() - 1) * 2 + lax.rem(me, 2)


def sibling():
    me = lax.axis_index("dp")
    return me + 1 - 2 * lax.rem(me, 2)


def greet(n, chips, both_cores=False):
    barrier = pltpu.get_barrier_semaphore()
    if both_cores:
        pl.semaphore_signal(barrier, inc=1, device_id={"dp": sibling()}, device_id_type=MESH)
    for step in range(1, n):
        pl.semaphore_signal(barrier, inc=1, device_id={"tensor": ring(n, step)}, device_id_type=MESH)
    for s in range(1, chips):
        pl.semaphore_signal(
            barrier, inc=1, device_id={"dp": same_core(s, chips)}, device_id_type=MESH
        )
    pl.semaphore_wait(barrier, n + chips - 2 + both_cores)


def front_kernel(
    n, chips, chunks, limit_ref, tokens_ref, ct_ref, gain_ref, shift_ref, coarse_ref, fine_ref, sign_ref,
    wq_ref, wk_ref, wv_ref, gate_ref, up_ref, down_ref, wo_ref,
    ctx_ref, lse_ref, wp_ref, q_out, k_out, v_out, cos_out, sin_out, rows_ref, gb_all, w_all, out_ref, wo_z, wo_all,
    landed, gb, columns, own_w, wqkv, q_ref, k_ref, v_ref, cos_ref, sin_ref,
    right_send, right_recv, left_send, left_recv, gs_send, gs_recv, gr_send, gr_recv, rows_sem,
    wr_send, wr_recv, wl_send, wl_recv, send_sem, recv_sem, wz_send, wz_recv, ws_send, ws_recv,
    wx_send, wx_recv, cut_sem, load_sem, save_sem, keep_sem,
):
    i = pl.program_id(0)
    steps = pl.num_programs(0)
    me = lax.axis_index("tensor")
    place = lax.axis_index("dp")
    core = lax.rem(place, 2)
    bits = chips.bit_length() - 1
    rows, depth = tokens_ref.shape
    heads = q_ref.shape[0]
    piece = rows // chunks
    limit = limit_ref[0]
    s = i // heads
    h = lax.rem(i, heads)

    def over(shard, d, c, send, recv, to):
        part = landed.at[shard, pl.ds(c * piece, piece)]
        return remote(part, part, send.at[d, c], recv.at[d, c], tensor=to)

    def rightward(d, c):
        return over(me - d, d, c, right_send, right_recv, me + 1)

    def leftward(d, c):
        return over(me + d, d, c, left_send, left_recv, me - 1)

    def from_left(d, c):
        return over(me - d, d - 1, c, right_send, right_recv, me - 1)

    def from_right(d, c):
        return over(me + d, d - 1, c, left_send, left_recv, me + 1)

    def weights(shard, d, k, send, recv, to):
        there = w_all.at[k, shard]
        return remote(there if d else own_w.at[k], there, send.at[d, k], recv.at[d, k], tensor=to)

    def w_right(d, k):
        return weights(me - d, d, k, wr_send, wr_recv, me + 1)

    def w_left(d, k):
        return weights(me + d, d, k, wl_send, wl_recv, me - 1)

    def w_from_left(d, k):
        return weights(me - d, d - 1, k, wr_send, wr_recv, me - 1)

    def w_from_right(d, k):
        return weights(me + d, d - 1, k, wl_send, wl_recv, me + 1)

    def spread_gb(c):
        return remote(
            gb, gb_all.at[place // 2, core], gs_send.at[c], gs_recv.at[c], dp=same_core(c, chips)
        )

    def relay_gb(c):
        there = gb_all.at[differ(place // 2, c, bits), core]
        return remote(there if c else gb, there, gr_send.at[c], gr_recv.at[c], dp=sibling())

    def wo_over(step):
        return remote(
            wo_ref, wo_z.at[me], wz_send.at[step], wz_recv.at[step], tensor=ring(n, step + 1)
        )

    def spread_wo(c):
        return remote(
            wo_z, wo_all.at[:, place], ws_send.at[c], ws_recv.at[c], dp=same_core(c, chips)
        )

    def relay_wo(c):
        there = wo_all.at[:, differ(place // 2, c, bits) * 2 + core]
        return remote(there if c else wo_z, there, wx_send.at[c], wx_recv.at[c], dp=sibling())

    def push(step):
        owner = ring(n, step + 1)
        return remote(
            ctx_ref.at[pl.ds(pl.multiple_of(owner * rows, rows), rows)], out_ref.at[me],
            send_sem.at[step], recv_sem.at[step], tensor=owner,
        )

    def save(shard):
        return pltpu.make_async_copy(landed.at[shard], rows_ref.at[shard], rows_sem.at[shard])

    mine = pl.ds(pl.multiple_of(me * rows, rows), rows)
    keeps = [
        pltpu.make_async_copy(gb, gb_all.at[place // 2, core], keep_sem.at[0]),
        pltpu.make_async_copy(wo_ref, wo_z.at[me], keep_sem.at[1]),
        pltpu.make_async_copy(wo_z, wo_all.at[:, place], keep_sem.at[2]),
        pltpu.make_async_copy(ctx_ref.at[mine], out_ref.at[me], keep_sem.at[3]),
        pltpu.make_async_copy(own_w, w_all.at[:, me], keep_sem.at[4]),
    ]
    saves = [
        pltpu.make_async_copy(a, b, save_sem.at[j])
        for j, (a, b) in enumerate(
            ((q_ref, q_out), (k_ref, k_out), (v_ref, v_out), (cos_ref, cos_out), (sin_ref, sin_out))
        )
    ]

    @pl.when(i == 0)
    def _():
        loads = [
            pltpu.make_async_copy(ref, wqkv.at[j], load_sem.at[j])
            for j, ref in enumerate((wq_ref, wk_ref, wv_ref))
        ]
        share = own_w.shape[1]
        ours = pl.ds(pl.multiple_of(place * share, share), share)
        cuts = [pltpu.make_async_copy(down_ref.at[ours], own_w.at[2], cut_sem.at[2])]
        for k, ref in enumerate((gate_ref, up_ref)):
            src = ref if share % 128 else ref.at[:, ours]
            cuts.append(pltpu.make_async_copy(src, columns.at[k], cut_sem.at[k]))
        for copy in loads + cuts:
            copy.start()

        barrier = pltpu.get_barrier_semaphore()
        for step in range(1, n):
            to = ring(n, step)
            pl.semaphore_signal(barrier, inc=1, device_id={"tensor": to}, device_id_type=MESH)
        pl.semaphore_signal(barrier, inc=1, device_id={"dp": sibling()}, device_id_type=MESH)
        for c in range(1, chips):
            to = same_core(c, chips)
            pl.semaphore_signal(barrier, inc=1, device_id={"dp": to}, device_id_type=MESH)

        values = tokens_ref[...].astype(F32)
        values = values - jnp.mean(values, axis=1, keepdims=True)
        inverse = lax.rsqrt(jnp.mean(values * values, axis=1, keepdims=True) + EPS)
        landed[me] = (values * inverse * gain_ref[...] + shift_ref[...]).astype(BF)

        pl.semaphore_wait(barrier, n - 1 + chips)

        for c in range(chunks):

            @pl.when(me < n - 1)
            def _():
                rightward(0, c).start()

            @pl.when(me > 0)
            def _():
                leftward(0, c).start()

        row = me * rows + lax.broadcasted_iota(jnp.int32, (rows, depth), 0)
        gb[...] = jnp.where(row < limit, ct_ref[...].astype(F32), 0.0).astype(BF)
        for c in range(1, chips):
            spread_gb(c).start()
        relay_gb(0).start()
        keeps[0].start()
        keeps[1].start()
        for copy in loads:
            copy.wait()

        cut = wp_ref.shape[0]
        here = pl.ds(pl.multiple_of(place * cut, cut), cut)
        first = lanes((cut, 128)) < HD
        for p in range(heads // 2):
            at = slice(p * 128, p * 128 + 128)
            query, key, value = (wqkv[j, here, at].astype(F32) for j in range(3))
            even = jnp.where(first, key, pltpu.roll(value, HD, 1))
            odd = jnp.where(first, pltpu.roll(key, HD, 1), value)
            for slot, values in ((2 * p, even), (2 * p + 1, odd), (heads + p, query)):
                wp_ref[:, slot * 128 : slot * 128 + 128] = values.astype(BF)

        lane = lanes((rows, 128))
        ones = jnp.where(lane < HD + 3, 1.0, 0.0)
        unit = jnp.where(lane == HD + 3, 1.0, 0.0)

        def put(out, here, values, extra):
            for head in range(heads):
                own = values[:, head // 2 * 128 : head // 2 * 128 + 128]
                own = pltpu.roll(own, HD, 1) if head % 2 else own
                out[head, here, :] = jnp.where(lane < HD, own, extra).astype(BF)

        def project(shard):
            here = pl.ds(pl.multiple_of(shard * rows, rows), rows)
            for j in range(rows // STEP):
                part = pl.ds(pl.multiple_of(shard * rows + j * STEP, STEP), STEP)
                coarse = pl.ds(shard * (rows // STEP) + j, 1)
                c0, s0 = coarse_ref[0, coarse, :], coarse_ref[1, coarse, :]
                cos_ref[part, :] = c0 * fine_ref[0] - s0 * fine_ref[1]
                sin_ref[part, :] = (s0 * fine_ref[0] + c0 * fine_ref[1]) * sign_ref[...]
            cosine = jnp.tile(cos_ref[here, :], (1, heads // 2))
            sine = jnp.tile(sin_ref[here, :], (1, heads // 2))
            x = landed[shard]
            row = shard * rows + lax.broadcasted_iota(jnp.int32, (rows, 128), 0)
            bias = jnp.where(lane == HD + 3, jnp.where(row < limit, 0.0, -1e30), ones)
            raw = dot(x, wqkv[0])
            turned = (raw * cosine + partner(raw) * sine).astype(BF).astype(F32)
            put(q_ref, here, turned * SCALE, unit)
            raw = dot(x, wqkv[1])
            put(k_ref, here, raw * cosine + partner(raw) * sine, bias)
            put(v_ref, here, dot(x, wqkv[2]), ones)

        for d in range(1, n + 1):
            for c in range(chunks):
                if d < n:

                    @pl.when(me >= d)
                    def _():
                        from_left(d, c).wait_recv()

                    @pl.when((me >= d) & (me < n - 1))
                    def _():
                        rightward(d, c).start()

                    @pl.when(me + d < n)
                    def _():
                        from_right(d, c).wait_recv()

                    @pl.when((me + d < n) & (me > 0))
                    def _():
                        leftward(d, c).start()

                if c == 0:

                    @pl.when(me >= d - 1)
                    def _():
                        save(me - d + 1).start()
                        project(me - d + 1)

                if c == 1 and d > 1:

                    @pl.when(me + d - 1 < n)
                    def _():
                        save(me + d - 1).start()
                        project(me + d - 1)

                if c == 2 and d == 1:
                    for cut in cuts:
                        cut.wait()
                    for k in range(2):
                        own_w[k] = columns[k].astype(F32).T.astype(BF)
                    keeps[4].start()

                if c == chunks - 1 and d == 2:
                    for near in range(1, chips // 2 + 1):
                        spread_gb(near).wait_recv()
                        relay_gb(near).start()

            if d < n:

                @pl.when((me < n - 1) & (me + 1 == d))
                def _():
                    for k in range(3):
                        w_right(0, k).start()

                @pl.when((me > 0) & (n - me == d))
                def _():
                    for k in range(3):
                        w_left(0, k).start()

        for copy in saves:
            copy.start()
        for step in range(n - 1):
            wo_over(step).start()
        for far in range(chips // 2 + 1, chips):
            spread_gb(far).wait_recv()
            relay_gb(far).start()

    stride = max((heads * n - 2) // max(n - 2, 1), 1)
    for d in range(1, n - 1):

        @pl.when(i == 1 + (d - 1) * stride)
        def _():
            for k in range(3):

                @pl.when((me >= d) & (me < n - 1))
                def _():
                    w_from_left(d, k).wait_recv()
                    w_right(d, k).start()

                @pl.when((me + d < n) & (me > 0))
                def _():
                    w_from_right(d, k).wait_recv()
                    w_left(d, k).start()

    @pl.when(i == heads)
    def _():
        for step in range(n - 1):
            wo_over(step).wait()
        keeps[1].wait()
        for c in range(1, chips):
            spread_wo(c).start()
        relay_wo(0).start()
        keeps[2].start()

    @pl.when(i == (n - 1) * heads)
    def _():
        for c in range(1, chips):
            spread_wo(c).wait_recv()
            relay_wo(c).start()

    owner = ring(n, s + 1)
    block = pl.ds(pl.multiple_of(owner * rows, rows), rows)
    scores = dot(q_ref[h, block, :], k_ref[h], NT)
    peak = jnp.max(scores, axis=1, keepdims=True)
    acc = dot(jnp.exp(scores - peak).astype(BF), v_ref[h])
    lane = lanes((rows, 128))
    total = jnp.sum(jnp.where(lane == HD, acc, 0.0), axis=1, keepdims=True)
    out = acc * (1.0 / total)
    odd = lax.rem(h, 2)
    out = jnp.where(odd == 1, pltpu.roll(out, HD, 1), out).astype(BF)
    pair = pl.ds(pl.multiple_of(h // 2 * 128, 128), 128)
    ctx_ref[block, pair] = jnp.where((lane >= HD) == (odd == 1), out, ctx_ref[block, pair])
    lse_ref[block, :] = jnp.where(lane == h, peak + jnp.log(total), lse_ref[block, :])

    @pl.when((h == heads - 1) & (s < n - 1))
    def _():
        push(s).start()

    @pl.when(i == steps - 1)
    def _():
        keeps[3].start()
        for d in range(n - 1):
            for c in range(chunks):

                @pl.when((me >= d) & (me < n - 1))
                def _():
                    rightward(d, c).wait_send()

                @pl.when((me + d < n) & (me > 0))
                def _():
                    leftward(d, c).wait_send()

            for k in range(3):

                @pl.when((me >= d) & (me < n - 1))
                def _():
                    w_right(d, k).wait_send()

                @pl.when((me + d < n) & (me > 0))
                def _():
                    w_left(d, k).wait_send()

        for k in range(3):
            for d in range(1, n):

                @pl.when((me >= d) & ((me == n - 1) | (d == n - 1)))
                def _():
                    w_from_left(d, k).wait_recv()

                @pl.when((me + d < n) & ((me == 0) | (d == n - 1)))
                def _():
                    w_from_right(d, k).wait_recv()

        for c in range(chips):
            relay_gb(c).wait()
            relay_wo(c).wait()
            if c:
                spread_gb(c).wait_send()
                spread_wo(c).wait_send()
        for shard in range(n):
            save(shard).wait()
        for copy in saves:
            copy.wait()
        for step in range(n - 1):
            push(step).wait()
        for j in (0, 2, 3, 4):
            keeps[j].wait()


def front(
    tokens, cotangent, gain, shift, tables, w_query, w_key, w_value, gate, up, down, w_out, limit, n, devices
):
    rows, depth = tokens.shape
    total = n * rows
    width = w_query.shape[1]
    heads = width // HD
    chips = devices // 2
    chunks = 4
    place = lax.axis_index("dp")
    share = down.shape[0] // devices
    part = width // devices
    if share % 128:
        gate, up = (lax.dynamic_slice_in_dim(w, place * share, share, 1) for w in (gate, up))
    hbm = pl.BlockSpec(memory_space=pl.ANY)

    def whole(*shape):
        return pl.BlockSpec(shape, lambda *_: (0,) * len(shape), pipeline_mode=pl.Buffered(1))

    def dma(*shape):
        return pltpu.SemaphoreType.DMA(shape)

    head_array = jax.ShapeDtypeStruct((heads, total, 128), BF)
    table = jax.ShapeDtypeStruct((total, 128), F32)
    coarse, fine, sign = tables
    return pl.pallas_call(
        functools.partial(front_kernel, n, chips, chunks),
        out_shape=(
            jax.ShapeDtypeStruct((total, width), BF),
            table,
            jax.ShapeDtypeStruct((depth // devices, 3 * width), BF),
            head_array, head_array, head_array, table, table,
            jax.ShapeDtypeStruct((n, rows, depth), BF),
            jax.ShapeDtypeStruct((chips, 2, rows, depth), BF),
            jax.ShapeDtypeStruct((3, n, share, depth), BF),
            jax.ShapeDtypeStruct((n, rows, width), BF),
            jax.ShapeDtypeStruct((n, part, depth), BF),
            jax.ShapeDtypeStruct((n, devices, part, depth), BF),
        ),
        grid_spec=pltpu.PrefetchScalarGridSpec(
            num_scalar_prefetch=0,
            grid=(n * heads,),
            in_specs=[pl.BlockSpec(memory_space=pltpu.SMEM)]
            + [whole(rows, depth)] * 2
            + [whole(1, depth)] * 2
            + [whole(*coarse.shape), whole(*fine.shape), whole(*sign.shape)]
            + [hbm] * 7,
            out_specs=[whole(total, width), whole(total, 128), whole(depth // devices, 3 * width)]
            + [hbm] * 11,
            scratch_shapes=[
                pltpu.VMEM((n, rows, depth), BF),
                pltpu.VMEM((rows, depth), BF),
                pltpu.VMEM((2, depth, share), BF),
                pltpu.VMEM((3, share, depth), BF),
                pltpu.VMEM((3, depth, width), BF),
            ]
            + [pltpu.VMEM((heads, total, 128), BF)] * 3
            + [pltpu.VMEM((total, 128), F32)] * 2
            + [dma(n - 1, chunks)] * 4
            + [dma(chips)] * 4
            + [dma(n)]
            + [dma(n - 1, 3)] * 4
            + [dma(n - 1)] * 4
            + [dma(chips)] * 4
            + [dma(3), dma(3), dma(5), dma(5)],
        ),
        compiler_params=pltpu.CompilerParams(
            vmem_limit_bytes=60 << 20, collective_id=1, has_side_effects=True
        ),
        cost_estimate=pl.CostEstimate(
            flops=4 * total * total * 256 * heads * 3, bytes_accessed=40 << 20, transcendentals=0
        ),
        name="front",
    )(
        limit, tokens, cotangent, gain.reshape(1, depth), shift.reshape(1, depth), coarse, fine, sign,
        w_query, w_key, w_value, gate, up, down,
        lax.dynamic_slice_in_dim(w_out, place * part, part, 0),
    )


def att_bwd_kernel(
    n, bk, chips, ga_ref, wo_ref, cown_ref, parts_ref, q_ref, k_ref, v_ref, ctx_ref, lse_ref,
    cos_ref, sin_ref, pk_ref, own_ref, sums_ref, og_ref, do, gc, dka, dva, dqs,
    og_full, og_own, og_mate, og_sib, og_land, og_piece, og_z,
    send_sem, recv_sem, out_send, out_recv, pk_send, pk_recv, keep_sem,
    om_send, om_recv, op_send, op_recv, oz_send, oz_recv,
):
    i = pl.program_id(0)
    heads, total, _ = k_ref.shape
    h = jnp.where(i < heads, i, (i - heads) // (n - 1))
    t = jnp.where(i < heads, 0, lax.rem(i - heads, n - 1) + 1)
    rows = total // n
    me = lax.axis_index("tensor")
    place = lax.axis_index("dp")
    core = lax.rem(place, 2)
    bits = chips.bit_length() - 1
    share = og_ref.shape[0]
    mine = pl.ds(pl.multiple_of(me * rows, rows), rows)

    def push(step):
        return remote(
            gc.at[step], do.at[mine], send_sem.at[step], recv_sem.at[step], tensor=ring(n, step + 1)
        )

    def push_out(s):
        return remote(
            parts_ref.at[s], sums_ref.at[s - 1], out_send.at[s - 1], out_recv.at[s - 1],
            dp=same_core(s, chips),
        )

    def columns(slot):
        return pl.ds(pl.multiple_of(slot * 128, 128), 128)

    def push_pack(slot, step):
        owner = ring(n, step + 1)
        return remote(
            pk_ref.at[pl.ds(pl.multiple_of(owner * rows, rows), rows), columns(slot)],
            own_ref.at[me, :, columns(slot)],
            pk_send.at[slot, step], pk_recv.at[slot, step], tensor=owner,
        )

    def keep(slot):
        return pltpu.make_async_copy(
            pk_ref.at[mine, columns(slot)], own_ref.at[me, :, columns(slot)], keep_sem.at[slot]
        )

    @pl.when(i == 0)
    def _():
        greet(n, chips, True)

        def send(step, carry):
            gc[step] = dot(ga_ref[...], wo_ref[ring(n, step + 1)], NT).astype(BF)
            push(step).start()
            return carry

        lax.fori_loop(0, n - 1, send, 0)
        do[mine, :] = dot(ga_ref[...], wo_ref[me], NT).astype(BF)

    def og_swap():
        return remote(og_mate, og_sib, om_send, om_recv, dp=sibling())

    def og_push(s):
        return remote(og_sib.at[s], og_land.at[s], op_send.at[s], op_recv.at[s], dp=same_core(s, chips))

    def og_over(step):
        to = ring(n, step + 1)
        return remote(og_piece.at[to], og_z.at[me], oz_send.at[step], oz_recv.at[step], tensor=to)

    @pl.when(i == 1)
    def _():
        def term(part, carry):
            og_full[...] = dot(cown_ref[part], ga_ref[...], TN)
            for s in range(chips):
                start = differ(place // 2, s, bits) * 2
                here = pl.ds(pl.multiple_of((start + core) * share, share), share)
                there = pl.ds(pl.multiple_of((start + 1 - core) * share, share), share)
                og_own[s, part] = og_full[here, :]
                og_mate[s, part] = og_full[there, :].astype(BF)
            return carry

        lax.fori_loop(0, n, term, 0)
        og_swap().start()

    @pl.when(i == 2)
    def _():
        og_swap().wait_recv()
        for s in range(chips):
            og_sib[s] = (og_own[s] + og_sib[s].astype(F32)).astype(BF)
            if s:
                og_push(s).start()

    @pl.when(i == heads * n - 6)
    def _():
        joined = og_sib[0].astype(F32)
        for s in range(1, chips):
            og_push(s).wait_recv()
            joined = joined + og_land[s].astype(F32)
        og_piece[...] = joined.astype(BF)
        for step in range(n - 1):
            og_over(step).start()

    @pl.when(i == heads + 1)
    def _():
        for s in range(1, chips):
            push_out(s).start()

    @pl.when(i == heads * n - 1)
    def _():
        og_z[me] = og_piece[me]
        for step in range(n - 1):
            og_over(step).wait_recv()
        joined = og_z[0].astype(F32)
        for part in range(1, n):
            joined = joined + og_z[part].astype(F32)
        og_ref[...] = joined.astype(BF)

    @pl.when((h == 0) & (t > 0))
    def _():
        push(t - 1).wait_recv()

    source = ring(n, n - t)
    block = pl.ds(pl.multiple_of(source * rows, rows), rows)
    pair = columns(h // 2)
    odd = lax.rem(h, 2) == 1
    lane = lanes((rows, 128))
    off = lane - HD
    logsum = jnp.sum(jnp.where(lane == h, lse_ref[block, :], 0.0), axis=1, keepdims=True)
    a, b, c = split3(-logsum)
    q = q_ref[h, block, :].astype(F32)
    q = jnp.where(off == 0, a, jnp.where(off == 1, b, jnp.where(off == 2, c, q))).astype(BF)
    g = jnp.where((lane >= HD) == odd, do[block, pair].astype(F32), 0.0)
    delta = jnp.sum(g * ctx_ref[block, pair].astype(F32), axis=1, keepdims=True)
    a, b, c = split3(-delta)
    g = jnp.where(odd, pltpu.roll(g, HD, 1), g)
    g = jnp.where(off == 0, a, jnp.where(off == 1, b, jnp.where(off == 2, c, g))).astype(BF)
    acc = jnp.zeros((rows, 128), F32)
    for j in range(total // bk):
        rk = pl.ds(j * bk, bk)
        kt = k_ref[h, rk, :]
        probs = jnp.exp(dot(kt, q, NT))
        grad = (probs * dot(v_ref[h, rk, :], g, NT)).astype(BF)
        for sums, term in ((dva, dot(probs.astype(BF), g)), (dka, dot(grad, q))):
            before = jnp.where(t == 0, jnp.zeros_like(term), sums[h, rk, :])
            sums[h, rk, :] = before + term
        acc = acc + dot(grad, kt, TN)
    acc = acc * SCALE

    @pl.when(jnp.logical_not(odd))
    def _():
        dqs[block, :] = acc

    @pl.when(odd)
    def _():
        grad = jnp.where(lane < HD, dqs[block, :], pltpu.roll(acc, HD, 1))
        grad = grad * cos_ref[block, :] - partner(grad) * sin_ref[block, :]
        pk_ref[block, columns(heads + h // 2)] = grad.astype(BF)

    @pl.when(odd & (t == 0))
    def _():
        keep(heads + h // 2).start()

    @pl.when(odd & (t > 0))
    def _():
        push_pack(heads + h // 2, n - 1 - t).start()

    @pl.when(t == n - 1)
    def _():
        dk = dka[h]
        dk = dk * cos_ref[...] - partner(dk) * sin_ref[...]
        both = jnp.where(lanes((total, 128)) < HD, dk, pltpu.roll(dva[h], HD, 1))
        pk_ref[:, columns(h)] = both.astype(BF)
        for step in range(n - 1):
            push_pack(h, step).start()
        keep(h).start()

    @pl.when(i == heads * n - 1)
    def _():
        for step in range(n - 1):
            push(step).wait_send()
        for s in range(1, chips):
            push_out(s).wait()
        og_swap().wait_send()
        for s in range(1, chips):
            og_push(s).wait_send()
        for step in range(n - 1):
            og_over(step).wait_send()
        for slot in range(heads + heads // 2):
            keep(slot).wait()
            for step in range(n - 1):
                push_pack(slot, step).wait()


def att_bwd(
    grad_attn, w_out, ctx_own, parts, q, k, v, ctx, lse, cosine, sine, n, bk=512
):
    heads, total, _ = q.shape
    width = heads * HD
    rows, depth = grad_attn.shape
    chips = parts.shape[0]
    share = width // (2 * chips)
    slots = heads + heads // 2
    hbm = pl.BlockSpec(memory_space=pl.ANY)

    def whole(*shape):
        return pl.BlockSpec(shape, lambda *_: (0,) * len(shape), pipeline_mode=pl.Buffered(1))

    return pl.pallas_call(
        functools.partial(att_bwd_kernel, n, bk, chips),
        out_shape=(
            jax.ShapeDtypeStruct((total, slots * 128), BF),
            jax.ShapeDtypeStruct((n, rows, slots * 128), BF),
            jax.ShapeDtypeStruct((chips - 1, rows, depth), BF),
            jax.ShapeDtypeStruct((share, depth), BF),
        ),
        grid_spec=pltpu.PrefetchScalarGridSpec(
            num_scalar_prefetch=0,
            grid=(heads * n,),
            in_specs=[whole(rows, depth), whole(n, width, depth), whole(n, rows, width), hbm]
            + [whole(heads, total, 128)] * 3
            + [whole(total, width)]
            + [whole(total, 128)] * 3,
            out_specs=[whole(total, slots * 128), hbm, hbm, whole(share, depth)],
            scratch_shapes=[
                pltpu.VMEM((total, width), BF),
                pltpu.VMEM((n - 1, rows, width), BF),
            ]
            + [pltpu.VMEM((heads, total, 128), F32)] * 2
            + [pltpu.VMEM((total, 128), F32)]
            + [
                pltpu.VMEM((width, depth), F32),
                pltpu.VMEM((chips, n, share, depth), F32),
                pltpu.VMEM((chips, n, share, depth), BF),
                pltpu.VMEM((chips, n, share, depth), BF),
                pltpu.VMEM((chips, n, share, depth), BF),
                pltpu.VMEM((n, share, depth), BF),
                pltpu.VMEM((n, share, depth), BF),
            ]
            + [pltpu.SemaphoreType.DMA((n - 1,))] * 2
            + [pltpu.SemaphoreType.DMA((chips - 1,))] * 2
            + [pltpu.SemaphoreType.DMA((slots, n - 1))] * 2
            + [pltpu.SemaphoreType.DMA((slots,))]
            + [pltpu.SemaphoreType.DMA] * 2
            + [pltpu.SemaphoreType.DMA((chips,))] * 2
            + [pltpu.SemaphoreType.DMA((n - 1,))] * 2,
        ),
        compiler_params=pltpu.CompilerParams(
            vmem_limit_bytes=60 << 20, collective_id=2, has_side_effects=True
        ),
        cost_estimate=pl.CostEstimate(
            flops=10 * total * total * 256 * heads,
            bytes_accessed=20 * total * width,
            transcendentals=total * total * heads,
        ),
        name="att_bwd",
    )(grad_attn, w_out, ctx_own, parts, q, k, v, ctx, lse, cosine, sine)


def finish_kernel(
    chips, n, width, x_ref, pk_ref, own_ref, w_ref, tokens_ref, middle_ref, gain_ref, vec_ref, pg_ref,
    input_ref, q_ref, k_ref, v_ref, sums_ref, pg_all,
    full, mate, sib, land, fin, every, vec_z, vec_dp, vec_me,
    sx_send, sx_recv, rs_send, rs_recv, ag_send, ag_recv, rl_send, rl_recv,
    vz_send, vz_recv, vd_send, vd_recv, own_sem, gs_send, gs_recv, gr_send, gr_recv, pg_sem,
):
    bits = chips.bit_length() - 1
    me = lax.axis_index("dp")
    place = lax.axis_index("tensor")
    core = lax.rem(me, 2)
    chip = me // 2
    other = 1 - core
    heads = width // HD
    piece = fin.shape[0]

    def swap(s):
        return remote(mate.at[s], sib.at[s], sx_send.at[s], sx_recv.at[s], dp=chip * 2 + other)

    def push(s):
        return remote(sib.at[s], land.at[s], rs_send.at[s], rs_recv.at[s], dp=same_core(s, chips))

    def spread(s):
        return remote(
            fin, every.at[chip, core], ag_send.at[s], ag_recv.at[s], dp=same_core(s, chips)
        )

    def relay(s):
        src = every.at[differ(chip, s, bits), core]
        return remote(src, src, rl_send.at[s], rl_recv.at[s], dp=chip * 2 + other)

    def vec_over(step):
        return remote(
            vec_me.at[0], vec_z.at[place], vz_send.at[step], vz_recv.at[step], tensor=ring(n, step + 1)
        )

    def vec_across(step):
        return remote(
            vec_me.at[1], vec_dp.at[me], vd_send.at[step], vd_recv.at[step],
            dp=lax.rem(me + step + 1, 2 * chips),
        )

    def pg_spread(s):
        return remote(pg_ref, pg_all.at[me], gs_send.at[s], gs_recv.at[s], dp=same_core(s, chips))

    def pg_relay(s):
        there = pg_all.at[differ(chip, s, bits) * 2 + core]
        return remote(there if s else pg_ref, there, gr_send.at[s], gr_recv.at[s], dp=sibling())

    pg_keep = pltpu.make_async_copy(pg_ref, pg_all.at[me], pg_sem)
    barrier = pltpu.get_barrier_semaphore()
    for step in range(n - 1):
        pl.semaphore_signal(barrier, inc=1, device_id={"tensor": ring(n, step + 1)}, device_id_type=MESH)
    for step in range(2 * chips - 1):
        to = lax.rem(me + step + 1, 2 * chips)
        pl.semaphore_signal(barrier, inc=1, device_id={"dp": to}, device_id_type=MESH)

    full[...] = dot(x_ref[...], pk_ref[...], TN)
    pl.semaphore_wait(barrier, n + 2 * chips - 2)

    def part(s, which):
        start = (differ(chip, s, bits) * 2 + which) * piece
        return full[pl.ds(pl.multiple_of(start, piece), piece), :]

    for s in range(chips):
        mate[s] = part(s, other).astype(BF)
        swap(s).start()

    grad = jnp.zeros(input_ref.shape, F32)
    for t in range(n):
        w = w_ref[:, t].reshape(w_ref.shape[0] * w_ref.shape[2], w_ref.shape[3])
        grad = grad + dot(own_ref[t], w, NT).astype(BF).astype(F32)

    for s in range(1, chips):
        swap(s).wait_recv()
        sib[s] = (sib[s].astype(F32) + part(s, core)).astype(BF)
        push(s).start()
    swap(0).wait_recv()
    total = sib[0].astype(F32) + part(0, core)

    values = tokens_ref[...].astype(F32)
    values = values - jnp.mean(values, axis=1, keepdims=True)
    inverse = lax.rsqrt(jnp.mean(values * values, axis=1, keepdims=True) + EPS)
    scaled = values * inverse
    through = grad * gain_ref[...]
    inner = through - jnp.mean(through, axis=1, keepdims=True)
    inner = inner - scaled * jnp.mean(through * scaled, axis=1, keepdims=True)
    input_ref[...] = middle_ref[...] + inverse * inner
    vec_me[0, 0:1] = jnp.sum(grad * scaled, axis=0, keepdims=True)
    vec_me[0, 1:2] = jnp.sum(grad, axis=0, keepdims=True)
    vec_me[0, 2:4] = vec_ref[...]
    vec_me[0, 4:8] = jnp.zeros((4, vec_ref.shape[1]), F32)
    vec_z[place] = vec_me[0]
    for step in range(n - 1):
        vec_over(step).start()

    for s in range(1, chips):
        pg_spread(s).start()
    pg_relay(0).start()
    pg_keep.start()
    for s in range(1, chips):
        push(s).wait_recv()
        total = total + land[s].astype(F32)
    fin[...] = total.astype(BF)
    for s in range(1, chips):
        spread(s).start()
    mine = pltpu.make_async_copy(fin, every.at[chip, core], own_sem)
    mine.start()
    mine.wait()
    relay(0).start()

    for step in range(n - 1):
        vec_over(step).wait()
    vec = vec_z[0]
    for t in range(1, n):
        vec = vec + vec_z[t]
    vec_me[1] = vec
    vec_dp[me] = vec
    for step in range(2 * chips - 1):
        vec_across(step).start()
    for s in range(1, chips):
        spread(s).wait_recv()
        relay(s).start()
    for step in range(2 * chips - 1):
        vec_across(step).wait()
    vec = vec_dp[0]
    for t in range(1, 2 * chips):
        vec = vec + vec_dp[t]
    sums_ref[...] = vec
    for s in range(1, chips):
        pg_spread(s).wait_recv()
        pg_relay(s).start()
    for s in range(chips):
        relay(s).wait()
        swap(s).wait_send()
        if s > 0:
            spread(s).wait_send()
            push(s).wait_send()
    first = lanes((piece, 128)) < HD
    for d in range(2 * chips):
        rows = slice(d * piece, (d + 1) * piece)
        g = every[d // 2, d % 2].astype(F32)
        for pair in range(heads // 2):
            a = g[:, pair * 256 : pair * 256 + 128]
            b = g[:, pair * 256 + 128 : pair * 256 + 256]
            out = slice(pair * 128, pair * 128 + 128)
            q_ref[rows, out] = g[:, (heads + pair) * 128 : (heads + pair + 1) * 128]
            k_ref[rows, out] = jnp.where(first, a, pltpu.roll(b, HD, 1))
            v_ref[rows, out] = jnp.where(first, pltpu.roll(a, HD, 1), b)
    pg_keep.wait()
    for s in range(chips):
        pg_relay(s).wait()
        if s:
            pg_spread(s).wait_send()


def finish(
    rows_all, packed, own, w_all, tokens, middle, gain, vec, pair_grads, width, devices
):
    n, rows, packs = own.shape
    depth = tokens.shape[1]
    chips = devices // 2
    piece = depth // devices
    vmem = pl.BlockSpec(memory_space=pltpu.VMEM)
    hbm = pl.BlockSpec(memory_space=pl.ANY)
    out = jax.ShapeDtypeStruct((depth, width), F32)
    return pl.pallas_call(
        functools.partial(finish_kernel, chips, n, width),
        out_shape=(
            jax.ShapeDtypeStruct((rows, depth), F32), out, out, out,
            jax.ShapeDtypeStruct((8, depth), F32),
            jax.ShapeDtypeStruct((devices, *pair_grads.shape), BF),
        ),
        in_specs=[vmem] * 8 + [hbm],
        out_specs=[vmem] * 5 + [hbm],
        scratch_shapes=[
            pltpu.VMEM((depth, packs), F32),
            pltpu.VMEM((chips, piece, packs), BF),
            pltpu.VMEM((chips, piece, packs), BF),
            pltpu.VMEM((chips, piece, packs), BF),
            pltpu.VMEM((piece, packs), BF),
            pltpu.VMEM((chips, 2, piece, packs), BF),
            pltpu.VMEM((n, 8, depth), F32),
            pltpu.VMEM((devices, 8, depth), F32),
            pltpu.VMEM((2, 8, depth), F32),
        ]
        + [pltpu.SemaphoreType.DMA((chips,))] * 8
        + [pltpu.SemaphoreType.DMA((n - 1,))] * 2
        + [pltpu.SemaphoreType.DMA((devices - 1,))] * 2
        + [pltpu.SemaphoreType.DMA]
        + [pltpu.SemaphoreType.DMA((chips,))] * 4
        + [pltpu.SemaphoreType.DMA],
        compiler_params=pltpu.CompilerParams(
            vmem_limit_bytes=56 << 20, collective_id=4, has_side_effects=True
        ),
        cost_estimate=pl.CostEstimate(
            flops=4 * n * rows * depth * packs, bytes_accessed=20 << 20, transcendentals=0
        ),
        name="finish",
    )(rows_all, packed, own, w_all, tokens, middle, gain.reshape(1, depth), vec, pair_grads)


def ffn_kernel(
    chips, x_ref, gb_ref, w_ref, wp_ref, dx_ref, out_ref, dw_ref, zs_ref, wp_z,
    rows_all, gb, hid, gate_g, up_g, own, sib, mate, partial, z_left, z_right,
    ag_send, ag_recv, rl_send, rl_recv, sx_send, sx_recv, rs_send, rs_recv, fw_send, fw_recv,
    gb_sem, out_sem, dx_sem, wp_send, wp_recv, wp_sem, zr_send, zr_recv, zl_send, zl_recv,
):
    bits = chips.bit_length() - 1
    me = lax.axis_index("dp")
    core = lax.rem(me, 2)
    chip = me // 2
    other = 1 - core
    rows, depth = x_ref.shape
    n, share, _ = dw_ref.shape

    def spread(s):
        to = differ(chip, s, bits) * 2 + core
        return remote(x_ref, rows_all.at[chip, core], ag_send.at[s], ag_recv.at[s], dp=to)

    square = chips == 4

    def hand_on(s):
        half = pl.ds((s - 1) * (rows // 2), rows // 2)
        part = rows_all.at[differ(chip, s, bits), core, half]
        to = differ(chip, 3 - s, bits) * 2 + core
        return remote(part, part, fw_send.at[s], fw_recv.at[s], dp=to)

    def handed(s):
        half = pl.ds((s - 1) * (rows // 2), rows // 2)
        part = rows_all.at[differ(chip, 3, bits), core, half]
        to = differ(chip, 3 - s, bits) * 2 + core
        return remote(part, part, fw_send.at[s], fw_recv.at[s], dp=to)

    def relay(s):
        src = differ(chip, s, bits)
        return remote(
            rows_all.at[src, core], rows_all.at[src, core], rl_send.at[s], rl_recv.at[s],
            dp=chip * 2 + other,
        )

    def swap(s):
        return remote(
            mate.at[lax.rem(s, 2)], sib.at[s], sx_send.at[s], sx_recv.at[s], dp=chip * 2 + other
        )

    def push(s):
        to = differ(chip, s, bits) * 2 + core
        return remote(sib.at[s, 0], dx_ref.at[s], rs_send.at[s], rs_recv.at[s], dp=to)

    def fetch(s):
        src = differ(chip, s, bits)
        return pltpu.make_async_copy(gb_ref.at[src], gb.at[src], gb_sem.at[s])

    part = lax.axis_index("tensor")

    def over(step):
        return remote(
            wp_ref, wp_z.at[part], wp_send.at[step], wp_recv.at[step], tensor=ring(n, step + 1)
        )

    def keep(s):
        return pltpu.make_async_copy(sib.at[s, 1], out_ref.at[s], out_sem.at[s])

    for s in range(chips):
        fetch(s).start()
    barrier = pltpu.get_barrier_semaphore()
    for step in range(1, n):
        pl.semaphore_signal(barrier, inc=1, device_id={"tensor": ring(n, step)}, device_id_type=MESH)
    pl.semaphore_signal(barrier, inc=1, device_id={"dp": chip * 2 + other}, device_id_type=MESH)
    for s in range(1, chips):
        to = differ(chip, s, bits) * 2 + core
        pl.semaphore_signal(barrier, inc=1, device_id={"dp": to}, device_id_type=MESH)
    pl.semaphore_wait(barrier, chips + n - 1)
    direct = range(1, 3) if square else range(1, chips)
    for s in direct:
        spread(s).start()
    mine = pltpu.make_async_copy(x_ref, rows_all.at[chip, core], ag_send.at[0])
    mine.start()
    mine.wait()
    relay(0).start()
    for step in range(n - 1):
        over(step).start()
    keep_wp = pltpu.make_async_copy(wp_ref, wp_z.at[part], wp_sem)
    keep_wp.start()

    def shard(src, which, put):
        x = rows_all[src, which]
        grad = gb[src, which]
        gate = dot(x, w_ref[0], NT)
        upper = dot(x, w_ref[1], NT)
        grad_hidden = dot(grad, w_ref[2], NT)
        sigma = jax.nn.sigmoid(gate)
        act = gate * sigma
        hidden = (act * upper).astype(BF)
        grad_gate = (grad_hidden * upper * sigma * (1.0 + gate * (1.0 - sigma))).astype(BF)
        grad_upper = (grad_hidden * act).astype(BF)
        hid[src, which] = hidden
        gate_g[src, which] = grad_gate
        up_g[src, which] = grad_upper
        put[0] = (dot(grad_gate, w_ref[0]) + dot(grad_upper, w_ref[1])).astype(BF)
        put[1] = dot(hidden, w_ref[2]).astype(BF)

    def step(s, carry):
        src = differ(chip, s, bits)
        slot = lax.rem(s, 2)
        relay(s).wait_recv()
        fetch(s).wait()

        @pl.when(s >= 2)
        def _():
            swap(s - 2).wait_send()

        shard(src, other, mate.at[slot])
        swap(s).start()
        shard(src, core, own)
        swap(s).wait_recv()
        for k in range(2):
            sib[s, k] = (sib[s, k].astype(F32) + own[k].astype(F32)).astype(BF)

        @pl.when(s > 0)
        def _():
            push(s).start()

        keep(s).start()

        if square:

            @pl.when(s == 0)
            def _():
                for near in (1, 2):
                    spread(near).wait_recv()
                    hand_on(near).start()
                    relay(near).start()

        else:

            @pl.when(s < chips - 1)
            def _():
                spread(s + 1).wait_recv()
                relay(s + 1).start()

        if square:

            @pl.when(s == 1)
            def _():
                handed(1).wait_recv()
                handed(2).wait_recv()
                relay(3).start()

        return carry

    lax.fori_loop(0, chips, step, 0)
    first = pltpu.make_async_copy(sib.at[0, 0], dx_ref.at[0], dx_sem)
    first.start()
    def zr(t, k, to):
        return remote(
            partial.at[t, k], z_left.at[t, k], zr_send.at[t, k], zr_recv.at[t, k], tensor=to
        )

    def zl(t, k, to):
        return remote(
            partial.at[t, k], z_right.at[t, k], zl_send.at[t, k], zl_recv.at[t, k], tensor=to
        )

    def join(t, k, more):
        partial[t, k] = (partial[t, k].astype(F32) + more[t, k].astype(F32)).astype(BF)

    def weight_grad(left, right):
        left = left[...].reshape(-1, n * share)
        return dot(left, right[...].reshape(-1, depth), TN)

    for k, left in enumerate((gate_g, up_g)):
        grad = weight_grad(left, rows_all)
        for t in range(n):
            partial[t, k] = grad[t * share : (t + 1) * share, :].astype(BF)

        for j in range(n - 1):

            @pl.when(part == 0)
            def _():
                zr(n - 1 - j, k, 1).start()

            @pl.when(part == n - 1)
            def _():
                zl(j, k, n - 2).start()

    grad = weight_grad(hid, gb)
    for t in range(n):
        dw_ref[t] = grad[t * share : (t + 1) * share, :].astype(BF)
    for k in range(2):
        for j in range(n - 1):
            t = n - 1 - j

            @pl.when((part > 0) & (part < t))
            def _():
                zr(t, k, part + 1).wait_recv()
                join(t, k, z_left)
                zr(t, k, part + 1).start()

            @pl.when((part < n - 1) & (part > j))
            def _():
                zl(j, k, part - 1).wait_recv()
                join(j, k, z_right)
                zl(j, k, part - 1).start()

        for t in range(n):

            @pl.when((part == t) & (part > 0))
            def _():
                zr(t, k, part - 1).wait_recv()
                join(t, k, z_left)

            @pl.when((part == t) & (part < n - 1))
            def _():
                zl(t, k, part + 1).wait_recv()
                join(t, k, z_right)

            @pl.when(part == t)
            def _():
                zs_ref[k] = partial[t, k]

            @pl.when(part < t)
            def _():
                zr(t, k, part + 1).wait_send()

            @pl.when(part > t)
            def _():
                zl(t, k, part - 1).wait_send()

    first.wait()
    keep_wp.wait()
    for step in range(n - 1):
        over(step).wait()
    for s in range(chips):
        keep(s).wait()
        relay(s).wait_send()
        if s >= chips - 2:
            swap(s).wait_send()
        if s in direct:
            spread(s).wait_send()
        if s > 0:
            push(s).wait()
    if square:
        hand_on(1).wait_send()
        hand_on(2).wait_send()


def ffn(x, grad_branch, weights, w_packed, n, devices):
    rows, depth = x.shape
    chips = devices // 2
    hidden = weights.shape[1]
    share = hidden // n
    vmem = pl.BlockSpec(memory_space=pltpu.VMEM)
    hbm = pl.BlockSpec(memory_space=pl.ANY)
    return pl.pallas_call(
        functools.partial(ffn_kernel, chips),
        out_shape=(
            jax.ShapeDtypeStruct((chips, rows, depth), BF),
            jax.ShapeDtypeStruct((chips, rows, depth), BF),
            jax.ShapeDtypeStruct((n, share, depth), BF),
            jax.ShapeDtypeStruct((2, share, depth), BF),
            jax.ShapeDtypeStruct((n, *w_packed.shape), BF),
        ),
        in_specs=[vmem, hbm, vmem, hbm],
        out_specs=[hbm, hbm, vmem, vmem, hbm],
        scratch_shapes=[
            pltpu.VMEM((chips, 2, rows, depth), BF),
            pltpu.VMEM((chips, 2, rows, depth), BF),
        ]
        + [pltpu.VMEM((chips, 2, rows, hidden), BF)] * 3
        + [
            pltpu.VMEM((2, rows, depth), BF),
            pltpu.VMEM((chips, 2, rows, depth), BF),
            pltpu.VMEM((2, 2, rows, depth), BF),
        ]
        + [pltpu.VMEM((n, 2, share, depth), BF)] * 3
        + [pltpu.SemaphoreType.DMA((chips,))] * 8
        + [pltpu.SemaphoreType.DMA((3,))] * 2
        + [pltpu.SemaphoreType.DMA((chips,))] * 2
        + [pltpu.SemaphoreType.DMA]
        + [pltpu.SemaphoreType.DMA((n - 1,))] * 2
        + [pltpu.SemaphoreType.DMA]
        + [pltpu.SemaphoreType.DMA((n, 2))] * 4,
        compiler_params=pltpu.CompilerParams(
            vmem_limit_bytes=62 << 20, collective_id=3, has_side_effects=True
        ),
        cost_estimate=pl.CostEstimate(
            flops=2 * 9 * devices * rows * depth * hidden, bytes_accessed=30 << 20, transcendentals=0
        ),
        name="ffn",
    )(x, grad_branch, weights, w_packed)


def unpack_kernel(share, pair_ref, rest_ref, gate_ref, up_ref, down_ref, out_ref):
    gate_ref[...] = pair_ref[0, 0].astype(F32).T
    up_ref[...] = pair_ref[0, 1].astype(F32).T
    rest = rest_ref[0].astype(F32)
    down_ref[...] = rest[:share]
    out_ref[...] = rest[share:]


def unpack(pair, rest):
    devices, _, share, depth = pair.shape
    hidden = devices * share
    height = rest.shape[1]
    width = devices * (height - share)
    if share % 128:
        down = rest[:, :share].reshape(hidden, depth).astype(F32)
        gate, up = (pair[:, k].reshape(hidden, depth).astype(F32).T for k in range(2))
        return gate, up, down, rest[:, share:].reshape(width, depth).astype(F32)
    column = pl.BlockSpec((depth, share), lambda i: (0, i))
    return pl.pallas_call(
        functools.partial(unpack_kernel, share),
        out_shape=(jax.ShapeDtypeStruct((depth, hidden), F32),) * 2
        + (
            jax.ShapeDtypeStruct((hidden, depth), F32),
            jax.ShapeDtypeStruct((width, depth), F32),
        ),
        grid=(devices,),
        in_specs=[
            pl.BlockSpec((1, 2, share, depth), lambda i: (i, 0, 0, 0)),
            pl.BlockSpec((1, height, depth), lambda i: (i, 0, 0)),
        ],
        out_specs=[
            column, column, pl.BlockSpec((share, depth), lambda i: (i, 0)),
            pl.BlockSpec((height - share, depth), lambda i: (i, 0)),
        ],
        compiler_params=pltpu.CompilerParams(vmem_limit_bytes=40 << 20),
        name="unpack",
    )(pair, rest)


def norm_parts(values):
    centre = jnp.mean(values, axis=-1, keepdims=True)
    centred = values - centre
    inverse = lax.rsqrt(jnp.mean(centred * centred, axis=-1, keepdims=True) + EPS)
    return centred * inverse, inverse


def norm_back(upstream, scaled, inverse, gain):
    through = upstream * gain
    inner = (
        through
        - jnp.mean(through, axis=-1, keepdims=True)
        - scaled * jnp.mean(through * scaled, axis=-1, keepdims=True)
    )
    return inverse * inner, jnp.sum(upstream * scaled, axis=0), jnp.sum(upstream, axis=0)


def on_device(
    tokens, lengths, ln1_gain, ln1_bias, w_query, w_key, w_value, w_out,
    ln2_gain, ln2_bias, w_gate, w_up, down_weight, cotangent,
):
    n = lax.axis_size("tensor")
    local_rows, depth = tokens.shape
    length = local_rows * n
    width = w_query.shape[1]
    row_ids = lax.axis_index("tensor") * local_rows + lax.iota(jnp.int32, local_rows)
    valid = (row_ids < lengths[0])[:, None]

    inputs = tokens.astype(F32)
    grad_out = jnp.where(valid, cotangent.astype(F32), 0.0)
    devices = lax.axis_size("dp")
    place = lax.axis_index("dp")
    share = w_gate.shape[1] // devices

    (
        context, logsum, w_packed, q, k, v, cosine, sine, attn_rows, grad_branch, weights, context_own, _,
        w_out_all,
    ) = front(
        tokens, cotangent, ln1_gain, ln1_bias, angle_tables(length), w_query, w_key, w_value,
        w_gate, w_up, down_weight, w_out, lengths, n, devices,
    )
    attn_rows = attn_rows.reshape(length, depth)
    weights = weights.reshape(3, n * share, depth)

    w_out_all = w_out_all.reshape(n, width, depth)
    attn_out = sum(dot(context_own[t], w_out_all[t]).astype(BF).astype(F32) for t in range(n))
    middle = inputs + attn_out
    scaled2, inverse2 = norm_parts(middle)
    ffn_in = (scaled2 * ln2_gain + ln2_bias).astype(BF)
    grad_parts, out_parts, down_grad, pair_grads, w_packed = ffn(
        ffn_in, grad_branch, weights, w_packed, n, devices
    )
    grad_ffn_in = sum(grad_parts[p].astype(F32) for p in range(devices // 2))
    grad_norm2, gain2_grad, shift2_grad = norm_back(
        grad_ffn_in, scaled2, inverse2, ln2_gain
    )
    grad_middle = grad_out + grad_norm2
    grad_attn = grad_middle.astype(BF)
    w_packed = lax.all_gather(w_packed, "dp", axis=0)
    down_grad = lax.psum_scatter(down_grad, "tensor", scatter_dimension=0, tiled=True)[0]
    packed, packed_own, out_sums, out_piece = att_bwd(
        grad_attn, w_out_all, context_own, out_parts, q, k, v, context, logsum, cosine, sine, n
    )
    down_grad, out_piece, w_packed = lax.optimization_barrier((down_grad, out_piece, w_packed))
    grads = lax.all_gather(jnp.concatenate([down_grad, out_piece]), "dp", axis=0)
    ffn_out = sum(x.astype(F32) for x in (out_parts[0], *out_sums))
    output = jnp.where(valid, middle + ffn_out, 0.0).astype(BF)
    input_grad, query_grad, key_grad, value_grad, sums, pair_grads = finish(
        attn_rows, packed, packed_own, w_packed, tokens, grad_middle, ln1_gain,
        jnp.stack([gain2_grad, shift2_grad]), pair_grads, width, devices,
    )
    gate_grad, up_grad, down_grad, out_grad = unpack(pair_grads, grads)
    gain1_grad, shift1_grad, gain2_grad, shift2_grad = (sums[i] for i in range(4))
    return (
        output, input_grad, gain1_grad, shift1_grad, query_grad, key_grad, value_grad, out_grad,
        gain2_grad, shift2_grad, gate_grad, up_grad, down_grad,
    )


def solution(mesh):
    rows = P(("dp", "tensor"), None)
    columns = P(None, "tensor")
    parts = P("tensor", None)
    return jax.shard_map(
        on_device,
        mesh=mesh,
        in_specs=(
            rows, P("dp"), P(), P(), columns, columns, columns, parts,
            P(), P(), columns, columns, parts, rows,
        ),
        out_specs=(
            rows, rows, P(), P(), columns, columns, columns, parts,
            P(), P(), columns, columns, parts,
        ),
        check_vma=False,
    )
```

```python
import functools
import math

import jax
import jax.numpy as jnp
from jax import lax
from jax.experimental import pallas as pl
from jax.experimental.pallas import tpu as pltpu
from jax.sharding import PartitionSpec as P

HD = 64
EPS = 1e-05
SCALE = 1.0 / math.sqrt(HD)
F32 = jnp.float32
BF = jnp.bfloat16
NT = (((1,), (1,)), ((), ()))
NN = (((1,), (0,)), ((), ()))
TN = (((0,), (0,)), ((), ()))
MESH = pl.DeviceIdType.MESH


def dot(a, b, dims=NN):
    return lax.dot_general(a, b, dims, preferred_element_type=F32)


def lanes(shape):
    return lax.broadcasted_iota(jnp.int32, shape, 1)


def split3(x):
    hi = x.astype(BF).astype(F32)
    mid = (x - hi).astype(BF).astype(F32)
    return hi, mid, x - hi - mid


def partner(x):
    width = x.shape[1]
    first = lanes(x.shape) % HD < HD // 2
    return jnp.where(first, pltpu.roll(x, width - HD // 2, 1), pltpu.roll(x, HD // 2, 1))


STEP = 64


def angle_tables(length):
    half = HD // 2
    lane = lax.optimization_barrier(lax.iota(jnp.int32, 2 * HD))
    freqs = 10000.0 ** (-((lane % half).astype(F32) * 2.0 / HD))
    sign = jnp.where(lane % HD < half, -1.0, 1.0)

    def table(positions):
        angles = positions[:, None] * freqs[None, :]
        return jnp.stack([jnp.cos(angles), jnp.sin(angles)])

    return table(lax.iota(F32, length // STEP) * STEP), table(lax.iota(F32, STEP)), sign[None, :]


def differ(a, b, bits):
    return sum(lax.rem(a // (1 << k) + b // (1 << k), 2) * (1 << k) for k in range(bits))


def remote(src, dst, send, recv, **to):
    return pltpu.make_async_remote_copy(
        src_ref=src, dst_ref=dst, send_sem=send, recv_sem=recv, device_id=to, device_id_type=MESH
    )


def ring(n, step):
    return lax.rem(lax.axis_index("tensor") + step, n)


def same_core(s, chips):
    me = lax.axis_index("dp")
    return differ(me // 2, s, chips.bit_length() - 1) * 2 + lax.rem(me, 2)


def sibling():
    me = lax.axis_index("dp")
    return me + 1 - 2 * lax.rem(me, 2)


def greet(n, chips, both_cores=False):
    barrier = pltpu.get_barrier_semaphore()
    if both_cores:
        pl.semaphore_signal(barrier, inc=1, device_id={"dp": sibling()}, device_id_type=MESH)
    for step in range(1, n):
        pl.semaphore_signal(barrier, inc=1, device_id={"tensor": ring(n, step)}, device_id_type=MESH)
    for s in range(1, chips):
        pl.semaphore_signal(
            barrier, inc=1, device_id={"dp": same_core(s, chips)}, device_id_type=MESH
        )
    pl.semaphore_wait(barrier, n + chips - 2 + both_cores)


def front_kernel(
    n, chips, chunks, limit_ref, tokens_ref, ct_ref, gain_ref, shift_ref, coarse_ref, fine_ref, sign_ref,
    wq_ref, wk_ref, wv_ref, gate_ref, up_ref, down_ref, wo_ref,
    ctx_ref, lse_ref, wp_ref, q_out, k_out, v_out, cos_out, sin_out, rows_ref, gb_all, w_all, out_ref, wo_z, wo_all,
    landed, gb, columns, own_w, wqkv, q_ref, k_ref, v_ref, cos_ref, sin_ref,
    right_send, right_recv, left_send, left_recv, gs_send, gs_recv, gr_send, gr_recv, rows_sem,
    wr_send, wr_recv, wl_send, wl_recv, send_sem, recv_sem, wz_send, wz_recv, ws_send, ws_recv,
    wx_send, wx_recv, cut_sem, load_sem, save_sem, keep_sem,
):
    i = pl.program_id(0)
    steps = pl.num_programs(0)
    me = lax.axis_index("tensor")
    place = lax.axis_index("dp")
    core = lax.rem(place, 2)
    bits = chips.bit_length() - 1
    rows, depth = tokens_ref.shape
    heads = q_ref.shape[0]
    piece = rows // chunks
    limit = limit_ref[0]
    s = i // heads
    h = lax.rem(i, heads)

    def over(shard, d, c, send, recv, to):
        part = landed.at[shard, pl.ds(c * piece, piece)]
        return remote(part, part, send.at[d, c], recv.at[d, c], tensor=to)

    def rightward(d, c):
        return over(me - d, d, c, right_send, right_recv, me + 1)

    def leftward(d, c):
        return over(me + d, d, c, left_send, left_recv, me - 1)

    def from_left(d, c):
        return over(me - d, d - 1, c, right_send, right_recv, me - 1)

    def from_right(d, c):
        return over(me + d, d - 1, c, left_send, left_recv, me + 1)

    def weights(shard, d, k, send, recv, to):
        there = w_all.at[k, shard]
        return remote(there if d else own_w.at[k], there, send.at[d, k], recv.at[d, k], tensor=to)

    def w_right(d, k):
        return weights(me - d, d, k, wr_send, wr_recv, me + 1)

    def w_left(d, k):
        return weights(me + d, d, k, wl_send, wl_recv, me - 1)

    def w_from_left(d, k):
        return weights(me - d, d - 1, k, wr_send, wr_recv, me - 1)

    def w_from_right(d, k):
        return weights(me + d, d - 1, k, wl_send, wl_recv, me + 1)

    def spread_gb(c):
        return remote(
            gb, gb_all.at[place // 2, core], gs_send.at[c], gs_recv.at[c], dp=same_core(c, chips)
        )

    def relay_gb(c):
        there = gb_all.at[differ(place // 2, c, bits), core]
        return remote(there if c else gb, there, gr_send.at[c], gr_recv.at[c], dp=sibling())

    def wo_over(step):
        return remote(
            wo_ref, wo_z.at[me], wz_send.at[step], wz_recv.at[step], tensor=ring(n, step + 1)
        )

    def spread_wo(c):
        return remote(
            wo_z, wo_all.at[:, place], ws_send.at[c], ws_recv.at[c], dp=same_core(c, chips)
        )

    def relay_wo(c):
        there = wo_all.at[:, differ(place // 2, c, bits) * 2 + core]
        return remote(there if c else wo_z, there, wx_send.at[c], wx_recv.at[c], dp=sibling())

    def push(step):
        owner = ring(n, step + 1)
        return remote(
            ctx_ref.at[pl.ds(pl.multiple_of(owner * rows, rows), rows)], out_ref.at[me],
            send_sem.at[step], recv_sem.at[step], tensor=owner,
        )

    def save(shard):
        return pltpu.make_async_copy(landed.at[shard], rows_ref.at[shard], rows_sem.at[shard])

    mine = pl.ds(pl.multiple_of(me * rows, rows), rows)
    keeps = [
        pltpu.make_async_copy(gb, gb_all.at[place // 2, core], keep_sem.at[0]),
        pltpu.make_async_copy(wo_ref, wo_z.at[me], keep_sem.at[1]),
        pltpu.make_async_copy(wo_z, wo_all.at[:, place], keep_sem.at[2]),
        pltpu.make_async_copy(ctx_ref.at[mine], out_ref.at[me], keep_sem.at[3]),
        pltpu.make_async_copy(own_w, w_all.at[:, me], keep_sem.at[4]),
    ]
    saves = [
        pltpu.make_async_copy(a, b, save_sem.at[j])
        for j, (a, b) in enumerate(
            ((q_ref, q_out), (k_ref, k_out), (v_ref, v_out), (cos_ref, cos_out), (sin_ref, sin_out))
        )
    ]

    @pl.when(i == 0)
    def _():
        loads = [
            pltpu.make_async_copy(ref, wqkv.at[j], load_sem.at[j])
            for j, ref in enumerate((wq_ref, wk_ref, wv_ref))
        ]
        share = own_w.shape[1]
        ours = pl.ds(pl.multiple_of(place * share, share), share)
        cuts = [pltpu.make_async_copy(down_ref.at[ours], own_w.at[2], cut_sem.at[2])]
        for k, ref in enumerate((gate_ref, up_ref)):
            src = ref if share % 128 else ref.at[:, ours]
            cuts.append(pltpu.make_async_copy(src, columns.at[k], cut_sem.at[k]))
        for copy in loads + cuts:
            copy.start()

        barrier = pltpu.get_barrier_semaphore()
        for step in range(1, n):
            to = ring(n, step)
            pl.semaphore_signal(barrier, inc=1, device_id={"tensor": to}, device_id_type=MESH)
        pl.semaphore_signal(barrier, inc=1, device_id={"dp": sibling()}, device_id_type=MESH)
        for c in range(1, chips):
            to = same_core(c, chips)
            pl.semaphore_signal(barrier, inc=1, device_id={"dp": to}, device_id_type=MESH)

        values = tokens_ref[...].astype(F32)
        values = values - jnp.mean(values, axis=1, keepdims=True)
        inverse = lax.rsqrt(jnp.mean(values * values, axis=1, keepdims=True) + EPS)
        landed[me] = (values * inverse * gain_ref[...] + shift_ref[...]).astype(BF)

        pl.semaphore_wait(barrier, n - 1 + chips)

        for c in range(chunks):

            @pl.when(me < n - 1)
            def _():
                rightward(0, c).start()

            @pl.when(me > 0)
            def _():
                leftward(0, c).start()

        row = me * rows + lax.broadcasted_iota(jnp.int32, (rows, depth), 0)
        gb[...] = jnp.where(row < limit, ct_ref[...].astype(F32), 0.0).astype(BF)
        for c in range(1, chips):
            spread_gb(c).start()
        relay_gb(0).start()
        keeps[0].start()
        keeps[1].start()
        for copy in loads:
            copy.wait()

        cut = wp_ref.shape[0]
        here = pl.ds(pl.multiple_of(place * cut, cut), cut)
        first = lanes((cut, 128)) < HD
        for p in range(heads // 2):
            at = slice(p * 128, p * 128 + 128)
            query, key, value = (wqkv[j, here, at].astype(F32) for j in range(3))
            even = jnp.where(first, key, pltpu.roll(value, HD, 1))
            odd = jnp.where(first, pltpu.roll(key, HD, 1), value)
            for slot, values in ((2 * p, even), (2 * p + 1, odd), (heads + p, query)):
                wp_ref[:, slot * 128 : slot * 128 + 128] = values.astype(BF)

        lane = lanes((rows, 128))
        ones = jnp.where(lane < HD + 3, 1.0, 0.0)
        unit = jnp.where(lane == HD + 3, 1.0, 0.0)

        def put(out, here, values, extra):
            for head in range(heads):
                own = values[:, head // 2 * 128 : head // 2 * 128 + 128]
                own = pltpu.roll(own, HD, 1) if head % 2 else own
                out[head, here, :] = jnp.where(lane < HD, own, extra).astype(BF)

        def project(shard):
            here = pl.ds(pl.multiple_of(shard * rows, rows), rows)
            for j in range(rows // STEP):
                part = pl.ds(pl.multiple_of(shard * rows + j * STEP, STEP), STEP)
                coarse = pl.ds(shard * (rows // STEP) + j, 1)
                c0, s0 = coarse_ref[0, coarse, :], coarse_ref[1, coarse, :]
                cos_ref[part, :] = c0 * fine_ref[0] - s0 * fine_ref[1]
                sin_ref[part, :] = (s0 * fine_ref[0] + c0 * fine_ref[1]) * sign_ref[...]
            cosine = jnp.tile(cos_ref[here, :], (1, heads // 2))
            sine = jnp.tile(sin_ref[here, :], (1, heads // 2))
            x = landed[shard]
            row = shard * rows + lax.broadcasted_iota(jnp.int32, (rows, 128), 0)
            bias = jnp.where(lane == HD + 3, jnp.where(row < limit, 0.0, -1e30), ones)
            raw = dot(x, wqkv[0])
            turned = (raw * cosine + partner(raw) * sine).astype(BF).astype(F32)
            put(q_ref, here, turned * SCALE, unit)
            raw = dot(x, wqkv[1])
            put(k_ref, here, raw * cosine + partner(raw) * sine, bias)
            put(v_ref, here, dot(x, wqkv[2]), ones)

        for d in range(1, n + 1):
            for c in range(chunks):
                if d < n:

                    @pl.when(me >= d)
                    def _():
                        from_left(d, c).wait_recv()

                    @pl.when((me >= d) & (me < n - 1))
                    def _():
                        rightward(d, c).start()

                    @pl.when(me + d < n)
                    def _():
                        from_right(d, c).wait_recv()

                    @pl.when((me + d < n) & (me > 0))
                    def _():
                        leftward(d, c).start()

                if c == 0:

                    @pl.when(me >= d - 1)
                    def _():
                        save(me - d + 1).start()
                        project(me - d + 1)

                if c == 1 and d > 1:

                    @pl.when(me + d - 1 < n)
                    def _():
                        save(me + d - 1).start()
                        project(me + d - 1)

                if c == 2 and d == 1:
                    for cut in cuts:
                        cut.wait()
                    for k in range(2):
                        own_w[k] = columns[k].astype(F32).T.astype(BF)
                    keeps[4].start()

                if c == chunks - 1 and d == 2:
                    for near in range(1, chips // 2 + 1):
                        spread_gb(near).wait_recv()
                        relay_gb(near).start()

            if d < n:

                @pl.when((me < n - 1) & (me + 1 == d))
                def _():
                    for k in range(3):
                        w_right(0, k).start()

                @pl.when((me > 0) & (n - me == d))
                def _():
                    for k in range(3):
                        w_left(0, k).start()

        for copy in saves:
            copy.start()
        for step in range(n - 1):
            wo_over(step).start()
        for far in range(chips // 2 + 1, chips):
            spread_gb(far).wait_recv()
            relay_gb(far).start()

    stride = max((heads * n - 2) // max(n - 2, 1), 1)
    for d in range(1, n - 1):

        @pl.when(i == 1 + (d - 1) * stride)
        def _():
            for k in range(3):

                @pl.when((me >= d) & (me < n - 1))
                def _():
                    w_from_left(d, k).wait_recv()
                    w_right(d, k).start()

                @pl.when((me + d < n) & (me > 0))
                def _():
                    w_from_right(d, k).wait_recv()
                    w_left(d, k).start()

    @pl.when(i == heads)
    def _():
        for step in range(n - 1):
            wo_over(step).wait()
        keeps[1].wait()
        for c in range(1, chips):
            spread_wo(c).start()
        relay_wo(0).start()
        keeps[2].start()

    @pl.when(i == (n - 1) * heads)
    def _():
        for c in range(1, chips):
            spread_wo(c).wait_recv()
            relay_wo(c).start()

    owner = ring(n, s + 1)
    block = pl.ds(pl.multiple_of(owner * rows, rows), rows)
    scores = dot(q_ref[h, block, :], k_ref[h], NT)
    peak = jnp.max(scores, axis=1, keepdims=True)
    acc = dot(jnp.exp(scores - peak).astype(BF), v_ref[h])
    lane = lanes((rows, 128))
    total = jnp.sum(jnp.where(lane == HD, acc, 0.0), axis=1, keepdims=True)
    out = acc * (1.0 / total)
    odd = lax.rem(h, 2)
    out = jnp.where(odd == 1, pltpu.roll(out, HD, 1), out).astype(BF)
    pair = pl.ds(pl.multiple_of(h // 2 * 128, 128), 128)
    ctx_ref[block, pair] = jnp.where((lane >= HD) == (odd == 1), out, ctx_ref[block, pair])
    lse_ref[block, :] = jnp.where(lane == h, peak + jnp.log(total), lse_ref[block, :])

    @pl.when((h == heads - 1) & (s < n - 1))
    def _():
        push(s).start()

    @pl.when(i == steps - 1)
    def _():
        keeps[3].start()
        for d in range(n - 1):
            for c in range(chunks):

                @pl.when((me >= d) & (me < n - 1))
                def _():
                    rightward(d, c).wait_send()

                @pl.when((me + d < n) & (me > 0))
                def _():
                    leftward(d, c).wait_send()

            for k in range(3):

                @pl.when((me >= d) & (me < n - 1))
                def _():
                    w_right(d, k).wait_send()

                @pl.when((me + d < n) & (me > 0))
                def _():
                    w_left(d, k).wait_send()

        for k in range(3):
            for d in range(1, n):

                @pl.when((me >= d) & ((me == n - 1) | (d == n - 1)))
                def _():
                    w_from_left(d, k).wait_recv()

                @pl.when((me + d < n) & ((me == 0) | (d == n - 1)))
                def _():
                    w_from_right(d, k).wait_recv()

        for c in range(chips):
            relay_gb(c).wait()
            relay_wo(c).wait()
            if c:
                spread_gb(c).wait_send()
                spread_wo(c).wait_send()
        for shard in range(n):
            save(shard).wait()
        for copy in saves:
            copy.wait()
        for step in range(n - 1):
            push(step).wait()
        for j in (0, 2, 3, 4):
            keeps[j].wait()


def front(
    tokens, cotangent, gain, shift, tables, w_query, w_key, w_value, gate, up, down, w_out, limit, n, devices
):
    rows, depth = tokens.shape
    total = n * rows
    width = w_query.shape[1]
    heads = width // HD
    chips = devices // 2
    chunks = 4
    place = lax.axis_index("dp")
    share = down.shape[0] // devices
    part = width // devices
    if share % 128:
        gate, up = (lax.dynamic_slice_in_dim(w, place * share, share, 1) for w in (gate, up))
    hbm = pl.BlockSpec(memory_space=pl.ANY)

    def whole(*shape):
        return pl.BlockSpec(shape, lambda *_: (0,) * len(shape), pipeline_mode=pl.Buffered(1))

    def dma(*shape):
        return pltpu.SemaphoreType.DMA(shape)

    head_array = jax.ShapeDtypeStruct((heads, total, 128), BF)
    table = jax.ShapeDtypeStruct((total, 128), F32)
    coarse, fine, sign = tables
    return pl.pallas_call(
        functools.partial(front_kernel, n, chips, chunks),
        out_shape=(
            jax.ShapeDtypeStruct((total, width), BF),
            table,
            jax.ShapeDtypeStruct((depth // devices, 3 * width), BF),
            head_array, head_array, head_array, table, table,
            jax.ShapeDtypeStruct((n, rows, depth), BF),
            jax.ShapeDtypeStruct((chips, 2, rows, depth), BF),
            jax.ShapeDtypeStruct((3, n, share, depth), BF),
            jax.ShapeDtypeStruct((n, rows, width), BF),
            jax.ShapeDtypeStruct((n, part, depth), BF),
            jax.ShapeDtypeStruct((n, devices, part, depth), BF),
        ),
        grid_spec=pltpu.PrefetchScalarGridSpec(
            num_scalar_prefetch=0,
            grid=(n * heads,),
            in_specs=[pl.BlockSpec(memory_space=pltpu.SMEM)]
            + [whole(rows, depth)] * 2
            + [whole(1, depth)] * 2
            + [whole(*coarse.shape), whole(*fine.shape), whole(*sign.shape)]
            + [hbm] * 7,
            out_specs=[whole(total, width), whole(total, 128), whole(depth // devices, 3 * width)]
            + [hbm] * 11,
            scratch_shapes=[
                pltpu.VMEM((n, rows, depth), BF),
                pltpu.VMEM((rows, depth), BF),
                pltpu.VMEM((2, depth, share), BF),
                pltpu.VMEM((3, share, depth), BF),
                pltpu.VMEM((3, depth, width), BF),
            ]
            + [pltpu.VMEM((heads, total, 128), BF)] * 3
            + [pltpu.VMEM((total, 128), F32)] * 2
            + [dma(n - 1, chunks)] * 4
            + [dma(chips)] * 4
            + [dma(n)]
            + [dma(n - 1, 3)] * 4
            + [dma(n - 1)] * 4
            + [dma(chips)] * 4
            + [dma(3), dma(3), dma(5), dma(5)],
        ),
        compiler_params=pltpu.CompilerParams(
            vmem_limit_bytes=60 << 20, collective_id=1, has_side_effects=True
        ),
        cost_estimate=pl.CostEstimate(
            flops=4 * total * total * 256 * heads * 3, bytes_accessed=40 << 20, transcendentals=0
        ),
        name="front",
    )(
        limit, tokens, cotangent, gain.reshape(1, depth), shift.reshape(1, depth), coarse, fine, sign,
        w_query, w_key, w_value, gate, up, down,
        lax.dynamic_slice_in_dim(w_out, place * part, part, 0),
    )


def att_bwd_kernel(
    n, bk, chips, ga_ref, wo_ref, cown_ref, parts_ref, pg_ref, q_ref, k_ref, v_ref, ctx_ref, lse_ref,
    cos_ref, sin_ref, pk_ref, own_ref, sums_ref, og_ref, pg_all, do, gc, dka, dva, dqs,
    og_full, og_own, og_mate, og_sib, og_land, og_piece, og_z,
    send_sem, recv_sem, out_send, out_recv, pk_send, pk_recv, keep_sem,
    om_send, om_recv, op_send, op_recv, oz_send, oz_recv, gs_send, gs_recv, gr_send, gr_recv, pg_sem,
):
    i = pl.program_id(0)
    heads, total, _ = k_ref.shape
    h = jnp.where(i < heads, i, (i - heads) // (n - 1))
    t = jnp.where(i < heads, 0, lax.rem(i - heads, n - 1) + 1)
    rows = total // n
    me = lax.axis_index("tensor")
    place = lax.axis_index("dp")
    core = lax.rem(place, 2)
    bits = chips.bit_length() - 1
    share = og_ref.shape[0]
    mine = pl.ds(pl.multiple_of(me * rows, rows), rows)

    def push(step):
        return remote(
            gc.at[step], do.at[mine], send_sem.at[step], recv_sem.at[step], tensor=ring(n, step + 1)
        )

    def push_out(s):
        return remote(
            parts_ref.at[s], sums_ref.at[s - 1], out_send.at[s - 1], out_recv.at[s - 1],
            dp=same_core(s, chips),
        )

    def columns(slot):
        return pl.ds(pl.multiple_of(slot * 128, 128), 128)

    def push_pack(slot, step):
        owner = ring(n, step + 1)
        return remote(
            pk_ref.at[pl.ds(pl.multiple_of(owner * rows, rows), rows), columns(slot)],
            own_ref.at[me, :, columns(slot)],
            pk_send.at[slot, step], pk_recv.at[slot, step], tensor=owner,
        )

    def keep(slot):
        return pltpu.make_async_copy(
            pk_ref.at[mine, columns(slot)], own_ref.at[me, :, columns(slot)], keep_sem.at[slot]
        )

    @pl.when(i == 0)
    def _():
        greet(n, chips, True)

        def send(step, carry):
            gc[step] = dot(ga_ref[...], wo_ref[ring(n, step + 1)], NT).astype(BF)
            push(step).start()
            return carry

        lax.fori_loop(0, n - 1, send, 0)
        do[mine, :] = dot(ga_ref[...], wo_ref[me], NT).astype(BF)

    def pg_spread(s):
        return remote(pg_ref, pg_all.at[place], gs_send.at[s], gs_recv.at[s], dp=same_core(s, chips))

    def pg_relay(s):
        there = pg_all.at[differ(place // 2, s, bits) * 2 + core]
        return remote(there if s else pg_ref, there, gr_send.at[s], gr_recv.at[s], dp=sibling())

    def pg_keep():
        return pltpu.make_async_copy(pg_ref, pg_all.at[place], pg_sem)

    @pl.when(i == heads * n - 8)
    def _():
        for s in range(1, chips):
            pg_spread(s).start()
        pg_relay(0).start()
        pg_keep().start()

    def og_swap():
        return remote(og_mate, og_sib, om_send, om_recv, dp=sibling())

    def og_push(s):
        return remote(og_sib.at[s], og_land.at[s], op_send.at[s], op_recv.at[s], dp=same_core(s, chips))

    def og_over(step):
        to = ring(n, step + 1)
        return remote(og_piece.at[to], og_z.at[me], oz_send.at[step], oz_recv.at[step], tensor=to)

    @pl.when(i == 1)
    def _():
        def term(part, carry):
            og_full[...] = dot(cown_ref[part], ga_ref[...], TN)
            for s in range(chips):
                start = differ(place // 2, s, bits) * 2
                here = pl.ds(pl.multiple_of((start + core) * share, share), share)
                there = pl.ds(pl.multiple_of((start + 1 - core) * share, share), share)
                og_own[s, part] = og_full[here, :]
                og_mate[s, part] = og_full[there, :].astype(BF)
            return carry

        lax.fori_loop(0, n, term, 0)
        og_swap().start()

    @pl.when(i == 2)
    def _():
        og_swap().wait_recv()
        for s in range(chips):
            og_sib[s] = (og_own[s] + og_sib[s].astype(F32)).astype(BF)
            if s:
                og_push(s).start()

    @pl.when(i == heads * n - 6)
    def _():
        joined = og_sib[0].astype(F32)
        for s in range(1, chips):
            og_push(s).wait_recv()
            joined = joined + og_land[s].astype(F32)
        og_piece[...] = joined.astype(BF)
        for step in range(n - 1):
            og_over(step).start()

    @pl.when(i == heads + 1)
    def _():
        for s in range(1, chips):
            push_out(s).start()

    @pl.when(i == heads * n - 1)
    def _():
        og_z[me] = og_piece[me]
        for step in range(n - 1):
            og_over(step).wait_recv()
        joined = og_z[0].astype(F32)
        for part in range(1, n):
            joined = joined + og_z[part].astype(F32)
        og_ref[...] = joined.astype(BF)

    @pl.when((h == 0) & (t > 0))
    def _():
        push(t - 1).wait_recv()

    source = ring(n, n - t)
    block = pl.ds(pl.multiple_of(source * rows, rows), rows)
    pair = columns(h // 2)
    odd = lax.rem(h, 2) == 1
    lane = lanes((rows, 128))
    off = lane - HD
    logsum = jnp.sum(jnp.where(lane == h, lse_ref[block, :], 0.0), axis=1, keepdims=True)
    a, b, c = split3(-logsum)
    q = q_ref[h, block, :].astype(F32)
    q = jnp.where(off == 0, a, jnp.where(off == 1, b, jnp.where(off == 2, c, q))).astype(BF)
    g = jnp.where((lane >= HD) == odd, do[block, pair].astype(F32), 0.0)
    delta = jnp.sum(g * ctx_ref[block, pair].astype(F32), axis=1, keepdims=True)
    a, b, c = split3(-delta)
    g = jnp.where(odd, pltpu.roll(g, HD, 1), g)
    g = jnp.where(off == 0, a, jnp.where(off == 1, b, jnp.where(off == 2, c, g))).astype(BF)
    acc = jnp.zeros((rows, 128), F32)
    for j in range(total // bk):
        rk = pl.ds(j * bk, bk)
        kt = k_ref[h, rk, :]
        probs = jnp.exp(dot(kt, q, NT))
        grad = (probs * dot(v_ref[h, rk, :], g, NT)).astype(BF)
        for sums, term in ((dva, dot(probs.astype(BF), g)), (dka, dot(grad, q))):
            before = jnp.where(t == 0, jnp.zeros_like(term), sums[h, rk, :])
            sums[h, rk, :] = before + term
        acc = acc + dot(grad, kt, TN)
    acc = acc * SCALE

    @pl.when(jnp.logical_not(odd))
    def _():
        dqs[block, :] = acc

    @pl.when(odd)
    def _():
        grad = jnp.where(lane < HD, dqs[block, :], pltpu.roll(acc, HD, 1))
        grad = grad * cos_ref[block, :] - partner(grad) * sin_ref[block, :]
        pk_ref[block, columns(heads + h // 2)] = grad.astype(BF)

    @pl.when(odd & (t == 0))
    def _():
        keep(heads + h // 2).start()

    @pl.when(odd & (t > 0))
    def _():
        push_pack(heads + h // 2, n - 1 - t).start()

    @pl.when(t == n - 1)
    def _():
        dk = dka[h]
        dk = dk * cos_ref[...] - partner(dk) * sin_ref[...]
        both = jnp.where(lanes((total, 128)) < HD, dk, pltpu.roll(dva[h], HD, 1))
        pk_ref[:, columns(h)] = both.astype(BF)
        for step in range(n - 1):
            push_pack(h, step).start()
        keep(h).start()

    @pl.when(i == heads * n - 1)
    def _():
        for s in range(1, chips):
            pg_spread(s).wait_recv()
            pg_relay(s).start()
        for step in range(n - 1):
            push(step).wait_send()
        for s in range(1, chips):
            push_out(s).wait()
        og_swap().wait_send()
        pg_keep().wait()
        for s in range(chips):
            pg_relay(s).wait()
            if s:
                pg_spread(s).wait_send()
        for s in range(1, chips):
            og_push(s).wait_send()
        for step in range(n - 1):
            og_over(step).wait_send()
        for slot in range(heads + heads // 2):
            keep(slot).wait()
            for step in range(n - 1):
                push_pack(slot, step).wait()


def att_bwd(
    grad_attn, w_out, ctx_own, parts, pair_grads, q, k, v, ctx, lse, cosine, sine, n, bk=512
):
    heads, total, _ = q.shape
    width = heads * HD
    rows, depth = grad_attn.shape
    chips = parts.shape[0]
    share = width // (2 * chips)
    slots = heads + heads // 2
    hbm = pl.BlockSpec(memory_space=pl.ANY)

    def whole(*shape):
        return pl.BlockSpec(shape, lambda *_: (0,) * len(shape), pipeline_mode=pl.Buffered(1))

    return pl.pallas_call(
        functools.partial(att_bwd_kernel, n, bk, chips),
        out_shape=(
            jax.ShapeDtypeStruct((total, slots * 128), BF),
            jax.ShapeDtypeStruct((n, rows, slots * 128), BF),
            jax.ShapeDtypeStruct((chips - 1, rows, depth), BF),
            jax.ShapeDtypeStruct((share, depth), BF),
            jax.ShapeDtypeStruct((2 * chips, *pair_grads.shape), BF),
        ),
        grid_spec=pltpu.PrefetchScalarGridSpec(
            num_scalar_prefetch=0,
            grid=(heads * n,),
            in_specs=[whole(rows, depth), whole(n, width, depth), whole(n, rows, width), hbm, hbm]
            + [whole(heads, total, 128)] * 3
            + [whole(total, width)]
            + [whole(total, 128)] * 3,
            out_specs=[whole(total, slots * 128), hbm, hbm, whole(share, depth), hbm],
            scratch_shapes=[
                pltpu.VMEM((total, width), BF),
                pltpu.VMEM((n - 1, rows, width), BF),
            ]
            + [pltpu.VMEM((heads, total, 128), F32)] * 2
            + [pltpu.VMEM((total, 128), F32)]
            + [
                pltpu.VMEM((width, depth), F32),
                pltpu.VMEM((chips, n, share, depth), F32),
                pltpu.VMEM((chips, n, share, depth), BF),
                pltpu.VMEM((chips, n, share, depth), BF),
                pltpu.VMEM((chips, n, share, depth), BF),
                pltpu.VMEM((n, share, depth), BF),
                pltpu.VMEM((n, share, depth), BF),
            ]
            + [pltpu.SemaphoreType.DMA((n - 1,))] * 2
            + [pltpu.SemaphoreType.DMA((chips - 1,))] * 2
            + [pltpu.SemaphoreType.DMA((slots, n - 1))] * 2
            + [pltpu.SemaphoreType.DMA((slots,))]
            + [pltpu.SemaphoreType.DMA] * 2
            + [pltpu.SemaphoreType.DMA((chips,))] * 2
            + [pltpu.SemaphoreType.DMA((n - 1,))] * 2
            + [pltpu.SemaphoreType.DMA((chips,))] * 4
            + [pltpu.SemaphoreType.DMA],
        ),
        compiler_params=pltpu.CompilerParams(
            vmem_limit_bytes=60 << 20, collective_id=2, has_side_effects=True
        ),
        cost_estimate=pl.CostEstimate(
            flops=10 * total * total * 256 * heads,
            bytes_accessed=20 * total * width,
            transcendentals=total * total * heads,
        ),
        name="att_bwd",
    )(grad_attn, w_out, ctx_own, parts, pair_grads, q, k, v, ctx, lse, cosine, sine)


def finish_kernel(
    chips, n, width, x_ref, pk_ref, own_ref, w_ref, tokens_ref, middle_ref, gain_ref, vec_ref,
    input_ref, q_ref, k_ref, v_ref, sums_ref,
    full, mate, sib, land, fin, every, vec_z, vec_dp, vec_me,
    sx_send, sx_recv, rs_send, rs_recv, ag_send, ag_recv, rl_send, rl_recv,
    vz_send, vz_recv, vd_send, vd_recv, own_sem,
):
    bits = chips.bit_length() - 1
    me = lax.axis_index("dp")
    place = lax.axis_index("tensor")
    core = lax.rem(me, 2)
    chip = me // 2
    other = 1 - core
    heads = width // HD
    piece = fin.shape[0]

    def swap(s):
        return remote(mate.at[s], sib.at[s], sx_send.at[s], sx_recv.at[s], dp=chip * 2 + other)

    def push(s):
        return remote(sib.at[s], land.at[s], rs_send.at[s], rs_recv.at[s], dp=same_core(s, chips))

    def spread(s):
        return remote(
            fin, every.at[chip, core], ag_send.at[s], ag_recv.at[s], dp=same_core(s, chips)
        )

    def relay(s):
        src = every.at[differ(chip, s, bits), core]
        return remote(src, src, rl_send.at[s], rl_recv.at[s], dp=chip * 2 + other)

    def vec_over(step):
        return remote(
            vec_me.at[0], vec_z.at[place], vz_send.at[step], vz_recv.at[step], tensor=ring(n, step + 1)
        )

    def vec_across(step):
        return remote(
            vec_me.at[1], vec_dp.at[me], vd_send.at[step], vd_recv.at[step],
            dp=lax.rem(me + step + 1, 2 * chips),
        )

    barrier = pltpu.get_barrier_semaphore()
    for step in range(n - 1):
        pl.semaphore_signal(barrier, inc=1, device_id={"tensor": ring(n, step + 1)}, device_id_type=MESH)
    for step in range(2 * chips - 1):
        to = lax.rem(me + step + 1, 2 * chips)
        pl.semaphore_signal(barrier, inc=1, device_id={"dp": to}, device_id_type=MESH)

    full[...] = dot(x_ref[...], pk_ref[...], TN)
    pl.semaphore_wait(barrier, n + 2 * chips - 2)

    def part(s, which):
        start = (differ(chip, s, bits) * 2 + which) * piece
        return full[pl.ds(pl.multiple_of(start, piece), piece), :]

    for s in range(chips):
        mate[s] = part(s, other).astype(BF)
        swap(s).start()

    grad = jnp.zeros(input_ref.shape, F32)
    for t in range(n):
        w = w_ref[:, t].reshape(w_ref.shape[0] * w_ref.shape[2], w_ref.shape[3])
        grad = grad + dot(own_ref[t], w, NT).astype(BF).astype(F32)

    for s in range(1, chips):
        swap(s).wait_recv()
        sib[s] = (sib[s].astype(F32) + part(s, core)).astype(BF)
        push(s).start()
    swap(0).wait_recv()
    total = sib[0].astype(F32) + part(0, core)

    values = tokens_ref[...].astype(F32)
    values = values - jnp.mean(values, axis=1, keepdims=True)
    inverse = lax.rsqrt(jnp.mean(values * values, axis=1, keepdims=True) + EPS)
    scaled = values * inverse
    through = grad * gain_ref[...]
    inner = through - jnp.mean(through, axis=1, keepdims=True)
    inner = inner - scaled * jnp.mean(through * scaled, axis=1, keepdims=True)
    input_ref[...] = middle_ref[...] + inverse * inner
    vec_me[0, 0:1] = jnp.sum(grad * scaled, axis=0, keepdims=True)
    vec_me[0, 1:2] = jnp.sum(grad, axis=0, keepdims=True)
    vec_me[0, 2:4] = vec_ref[...]
    vec_me[0, 4:8] = jnp.zeros((4, vec_ref.shape[1]), F32)
    vec_z[place] = vec_me[0]
    for step in range(n - 1):
        vec_over(step).start()

    for s in range(1, chips):
        push(s).wait_recv()
        total = total + land[s].astype(F32)
    fin[...] = total.astype(BF)
    for s in range(1, chips):
        spread(s).start()
    mine = pltpu.make_async_copy(fin, every.at[chip, core], own_sem)
    mine.start()
    mine.wait()
    relay(0).start()

    for step in range(n - 1):
        vec_over(step).wait()
    vec = vec_z[0]
    for t in range(1, n):
        vec = vec + vec_z[t]
    vec_me[1] = vec
    vec_dp[me] = vec
    for step in range(2 * chips - 1):
        vec_across(step).start()
    for s in range(1, chips):
        spread(s).wait_recv()
        relay(s).start()
    for step in range(2 * chips - 1):
        vec_across(step).wait()
    vec = vec_dp[0]
    for t in range(1, 2 * chips):
        vec = vec + vec_dp[t]
    sums_ref[...] = vec
    for s in range(chips):
        relay(s).wait()
        swap(s).wait_send()
        if s > 0:
            spread(s).wait_send()
            push(s).wait_send()
    first = lanes((piece, 128)) < HD
    for d in range(2 * chips):
        rows = slice(d * piece, (d + 1) * piece)
        g = every[d // 2, d % 2].astype(F32)
        for pair in range(heads // 2):
            a = g[:, pair * 256 : pair * 256 + 128]
            b = g[:, pair * 256 + 128 : pair * 256 + 256]
            out = slice(pair * 128, pair * 128 + 128)
            q_ref[rows, out] = g[:, (heads + pair) * 128 : (heads + pair + 1) * 128]
            k_ref[rows, out] = jnp.where(first, a, pltpu.roll(b, HD, 1))
            v_ref[rows, out] = jnp.where(first, pltpu.roll(a, HD, 1), b)


def finish(rows_all, packed, own, w_all, tokens, middle, gain, vec, width, devices):
    n, rows, packs = own.shape
    depth = tokens.shape[1]
    chips = devices // 2
    piece = depth // devices
    vmem = pl.BlockSpec(memory_space=pltpu.VMEM)
    out = jax.ShapeDtypeStruct((depth, width), F32)
    return pl.pallas_call(
        functools.partial(finish_kernel, chips, n, width),
        out_shape=(
            jax.ShapeDtypeStruct((rows, depth), F32), out, out, out,
            jax.ShapeDtypeStruct((8, depth), F32),
        ),
        in_specs=[vmem] * 8,
        out_specs=[vmem] * 5,
        scratch_shapes=[
            pltpu.VMEM((depth, packs), F32),
            pltpu.VMEM((chips, piece, packs), BF),
            pltpu.VMEM((chips, piece, packs), BF),
            pltpu.VMEM((chips, piece, packs), BF),
            pltpu.VMEM((piece, packs), BF),
            pltpu.VMEM((chips, 2, piece, packs), BF),
            pltpu.VMEM((n, 8, depth), F32),
            pltpu.VMEM((devices, 8, depth), F32),
            pltpu.VMEM((2, 8, depth), F32),
        ]
        + [pltpu.SemaphoreType.DMA((chips,))] * 8
        + [pltpu.SemaphoreType.DMA((n - 1,))] * 2
        + [pltpu.SemaphoreType.DMA((devices - 1,))] * 2
        + [pltpu.SemaphoreType.DMA],
        compiler_params=pltpu.CompilerParams(
            vmem_limit_bytes=56 << 20, collective_id=4, has_side_effects=True
        ),
        cost_estimate=pl.CostEstimate(
            flops=4 * n * rows * depth * packs, bytes_accessed=20 << 20, transcendentals=0
        ),
        name="finish",
    )(rows_all, packed, own, w_all, tokens, middle, gain.reshape(1, depth), vec)


def ffn_kernel(
    chips, x_ref, gb_ref, w_ref, wp_ref, dx_ref, out_ref, dw_ref, zs_ref, wp_z,
    rows_all, gb, hid, gate_g, up_g, own, sib, mate, partial, z_left, z_right,
    ag_send, ag_recv, rl_send, rl_recv, sx_send, sx_recv, rs_send, rs_recv, fw_send, fw_recv,
    gb_sem, out_sem, dx_sem, wp_send, wp_recv, wp_sem, zr_send, zr_recv, zl_send, zl_recv,
):
    bits = chips.bit_length() - 1
    me = lax.axis_index("dp")
    core = lax.rem(me, 2)
    chip = me // 2
    other = 1 - core
    rows, depth = x_ref.shape
    n, share, _ = dw_ref.shape

    def spread(s):
        to = differ(chip, s, bits) * 2 + core
        return remote(x_ref, rows_all.at[chip, core], ag_send.at[s], ag_recv.at[s], dp=to)

    square = chips == 4

    def hand_on(s):
        half = pl.ds((s - 1) * (rows // 2), rows // 2)
        part = rows_all.at[differ(chip, s, bits), core, half]
        to = differ(chip, 3 - s, bits) * 2 + core
        return remote(part, part, fw_send.at[s], fw_recv.at[s], dp=to)

    def handed(s):
        half = pl.ds((s - 1) * (rows // 2), rows // 2)
        part = rows_all.at[differ(chip, 3, bits), core, half]
        to = differ(chip, 3 - s, bits) * 2 + core
        return remote(part, part, fw_send.at[s], fw_recv.at[s], dp=to)

    def relay(s):
        src = differ(chip, s, bits)
        return remote(
            rows_all.at[src, core], rows_all.at[src, core], rl_send.at[s], rl_recv.at[s],
            dp=chip * 2 + other,
        )

    def swap(s):
        return remote(
            mate.at[lax.rem(s, 2)], sib.at[s], sx_send.at[s], sx_recv.at[s], dp=chip * 2 + other
        )

    def push(s):
        to = differ(chip, s, bits) * 2 + core
        return remote(sib.at[s, 0], dx_ref.at[s], rs_send.at[s], rs_recv.at[s], dp=to)

    def fetch(s):
        src = differ(chip, s, bits)
        return pltpu.make_async_copy(gb_ref.at[src], gb.at[src], gb_sem.at[s])

    part = lax.axis_index("tensor")

    def over(step):
        return remote(
            wp_ref, wp_z.at[part], wp_send.at[step], wp_recv.at[step], tensor=ring(n, step + 1)
        )

    def keep(s):
        return pltpu.make_async_copy(sib.at[s, 1], out_ref.at[s], out_sem.at[s])

    for s in range(chips):
        fetch(s).start()
    barrier = pltpu.get_barrier_semaphore()
    for step in range(1, n):
        pl.semaphore_signal(barrier, inc=1, device_id={"tensor": ring(n, step)}, device_id_type=MESH)
    pl.semaphore_signal(barrier, inc=1, device_id={"dp": chip * 2 + other}, device_id_type=MESH)
    for s in range(1, chips):
        to = differ(chip, s, bits) * 2 + core
        pl.semaphore_signal(barrier, inc=1, device_id={"dp": to}, device_id_type=MESH)
    pl.semaphore_wait(barrier, chips + n - 1)
    direct = range(1, 3) if square else range(1, chips)
    for s in direct:
        spread(s).start()
    mine = pltpu.make_async_copy(x_ref, rows_all.at[chip, core], ag_send.at[0])
    mine.start()
    mine.wait()
    relay(0).start()
    for step in range(n - 1):
        over(step).start()
    keep_wp = pltpu.make_async_copy(wp_ref, wp_z.at[part], wp_sem)
    keep_wp.start()

    def shard(src, which, put):
        x = rows_all[src, which]
        grad = gb[src, which]
        gate = dot(x, w_ref[0], NT)
        upper = dot(x, w_ref[1], NT)
        grad_hidden = dot(grad, w_ref[2], NT)
        sigma = jax.nn.sigmoid(gate)
        act = gate * sigma
        hidden = (act * upper).astype(BF)
        grad_gate = (grad_hidden * upper * sigma * (1.0 + gate * (1.0 - sigma))).astype(BF)
        grad_upper = (grad_hidden * act).astype(BF)
        hid[src, which] = hidden
        gate_g[src, which] = grad_gate
        up_g[src, which] = grad_upper
        put[0] = (dot(grad_gate, w_ref[0]) + dot(grad_upper, w_ref[1])).astype(BF)
        put[1] = dot(hidden, w_ref[2]).astype(BF)

    def step(s, carry):
        src = differ(chip, s, bits)
        slot = lax.rem(s, 2)
        relay(s).wait_recv()
        fetch(s).wait()

        @pl.when(s >= 2)
        def _():
            swap(s - 2).wait_send()

        shard(src, other, mate.at[slot])
        swap(s).start()
        shard(src, core, own)
        swap(s).wait_recv()
        for k in range(2):
            sib[s, k] = (sib[s, k].astype(F32) + own[k].astype(F32)).astype(BF)

        @pl.when(s > 0)
        def _():
            push(s).start()

        keep(s).start()

        if square:

            @pl.when(s == 0)
            def _():
                for near in (1, 2):
                    spread(near).wait_recv()
                    hand_on(near).start()
                    relay(near).start()

        else:

            @pl.when(s < chips - 1)
            def _():
                spread(s + 1).wait_recv()
                relay(s + 1).start()

        if square:

            @pl.when(s == 1)
            def _():
                handed(1).wait_recv()
                handed(2).wait_recv()
                relay(3).start()

        return carry

    lax.fori_loop(0, chips, step, 0)
    first = pltpu.make_async_copy(sib.at[0, 0], dx_ref.at[0], dx_sem)
    first.start()
    def zr(t, k, to):
        return remote(
            partial.at[t, k], z_left.at[t, k], zr_send.at[t, k], zr_recv.at[t, k], tensor=to
        )

    def zl(t, k, to):
        return remote(
            partial.at[t, k], z_right.at[t, k], zl_send.at[t, k], zl_recv.at[t, k], tensor=to
        )

    def join(t, k, more):
        partial[t, k] = (partial[t, k].astype(F32) + more[t, k].astype(F32)).astype(BF)

    def weight_grad(left, right):
        left = left[...].reshape(-1, n * share)
        return dot(left, right[...].reshape(-1, depth), TN)

    def hand_along(k):
        for j in range(n - 1):
            t = n - 1 - j

            @pl.when((part > 0) & (part < t))
            def _():
                zr(t, k, part + 1).wait_recv()
                join(t, k, z_left)
                zr(t, k, part + 1).start()

            @pl.when((part < n - 1) & (part > j))
            def _():
                zl(j, k, part - 1).wait_recv()
                join(j, k, z_right)
                zl(j, k, part - 1).start()

    for k, left in enumerate((gate_g, up_g)):
        grad = weight_grad(left, rows_all)
        for t in range(n):
            partial[t, k] = grad[t * share : (t + 1) * share, :].astype(BF)

        for j in range(n - 1):

            @pl.when(part == 0)
            def _():
                zr(n - 1 - j, k, 1).start()

            @pl.when(part == n - 1)
            def _():
                zl(j, k, n - 2).start()

    hand_along(0)
    grad = weight_grad(hid, gb)
    for t in range(n):
        dw_ref[t] = grad[t * share : (t + 1) * share, :].astype(BF)
    hand_along(1)
    for k in range(2):
        for t in range(n):

            @pl.when((part == t) & (part > 0))
            def _():
                zr(t, k, part - 1).wait_recv()
                join(t, k, z_left)

            @pl.when((part == t) & (part < n - 1))
            def _():
                zl(t, k, part + 1).wait_recv()
                join(t, k, z_right)

            @pl.when(part == t)
            def _():
                zs_ref[k] = partial[t, k]

            @pl.when(part < t)
            def _():
                zr(t, k, part + 1).wait_send()

            @pl.when(part > t)
            def _():
                zl(t, k, part - 1).wait_send()

    first.wait()
    keep_wp.wait()
    for step in range(n - 1):
        over(step).wait()
    for s in range(chips):
        keep(s).wait()
        relay(s).wait_send()
        if s >= chips - 2:
            swap(s).wait_send()
        if s in direct:
            spread(s).wait_send()
        if s > 0:
            push(s).wait()
    if square:
        hand_on(1).wait_send()
        hand_on(2).wait_send()


def ffn(x, grad_branch, weights, w_packed, n, devices):
    rows, depth = x.shape
    chips = devices // 2
    hidden = weights.shape[1]
    share = hidden // n
    vmem = pl.BlockSpec(memory_space=pltpu.VMEM)
    hbm = pl.BlockSpec(memory_space=pl.ANY)
    return pl.pallas_call(
        functools.partial(ffn_kernel, chips),
        out_shape=(
            jax.ShapeDtypeStruct((chips, rows, depth), BF),
            jax.ShapeDtypeStruct((chips, rows, depth), BF),
            jax.ShapeDtypeStruct((n, share, depth), BF),
            jax.ShapeDtypeStruct((2, share, depth), BF),
            jax.ShapeDtypeStruct((n, *w_packed.shape), BF),
        ),
        in_specs=[vmem, hbm, vmem, hbm],
        out_specs=[hbm, hbm, vmem, vmem, hbm],
        scratch_shapes=[
            pltpu.VMEM((chips, 2, rows, depth), BF),
            pltpu.VMEM((chips, 2, rows, depth), BF),
        ]
        + [pltpu.VMEM((chips, 2, rows, hidden), BF)] * 3
        + [
            pltpu.VMEM((2, rows, depth), BF),
            pltpu.VMEM((chips, 2, rows, depth), BF),
            pltpu.VMEM((2, 2, rows, depth), BF),
        ]
        + [pltpu.VMEM((n, 2, share, depth), BF)] * 3
        + [pltpu.SemaphoreType.DMA((chips,))] * 8
        + [pltpu.SemaphoreType.DMA((3,))] * 2
        + [pltpu.SemaphoreType.DMA((chips,))] * 2
        + [pltpu.SemaphoreType.DMA]
        + [pltpu.SemaphoreType.DMA((n - 1,))] * 2
        + [pltpu.SemaphoreType.DMA]
        + [pltpu.SemaphoreType.DMA((n, 2))] * 4,
        compiler_params=pltpu.CompilerParams(
            vmem_limit_bytes=62 << 20, collective_id=3, has_side_effects=True
        ),
        cost_estimate=pl.CostEstimate(
            flops=2 * 9 * devices * rows * depth * hidden, bytes_accessed=30 << 20, transcendentals=0
        ),
        name="ffn",
    )(x, grad_branch, weights, w_packed)


def unpack_kernel(share, pair_ref, rest_ref, gate_ref, up_ref, down_ref, out_ref):
    gate_ref[...] = pair_ref[0, 0].astype(F32).T
    up_ref[...] = pair_ref[0, 1].astype(F32).T
    rest = rest_ref[0].astype(F32)
    down_ref[...] = rest[:share]
    out_ref[...] = rest[share:]


def unpack(pair, rest):
    devices, _, share, depth = pair.shape
    hidden = devices * share
    height = rest.shape[1]
    width = devices * (height - share)
    if share % 128:
        down = rest[:, :share].reshape(hidden, depth).astype(F32)
        gate, up = (pair[:, k].reshape(hidden, depth).astype(F32).T for k in range(2))
        return gate, up, down, rest[:, share:].reshape(width, depth).astype(F32)
    column = pl.BlockSpec((depth, share), lambda i: (0, i))
    return pl.pallas_call(
        functools.partial(unpack_kernel, share),
        out_shape=(jax.ShapeDtypeStruct((depth, hidden), F32),) * 2
        + (
            jax.ShapeDtypeStruct((hidden, depth), F32),
            jax.ShapeDtypeStruct((width, depth), F32),
        ),
        grid=(devices,),
        in_specs=[
            pl.BlockSpec((1, 2, share, depth), lambda i: (i, 0, 0, 0)),
            pl.BlockSpec((1, height, depth), lambda i: (i, 0, 0)),
        ],
        out_specs=[
            column, column, pl.BlockSpec((share, depth), lambda i: (i, 0)),
            pl.BlockSpec((height - share, depth), lambda i: (i, 0)),
        ],
        compiler_params=pltpu.CompilerParams(vmem_limit_bytes=40 << 20),
        name="unpack",
    )(pair, rest)


def norm_parts(values):
    centre = jnp.mean(values, axis=-1, keepdims=True)
    centred = values - centre
    inverse = lax.rsqrt(jnp.mean(centred * centred, axis=-1, keepdims=True) + EPS)
    return centred * inverse, inverse


def norm_back(upstream, scaled, inverse, gain):
    through = upstream * gain
    inner = (
        through
        - jnp.mean(through, axis=-1, keepdims=True)
        - scaled * jnp.mean(through * scaled, axis=-1, keepdims=True)
    )
    return inverse * inner, jnp.sum(upstream * scaled, axis=0), jnp.sum(upstream, axis=0)


def on_device(
    tokens, lengths, ln1_gain, ln1_bias, w_query, w_key, w_value, w_out,
    ln2_gain, ln2_bias, w_gate, w_up, down_weight, cotangent,
):
    n = lax.axis_size("tensor")
    local_rows, depth = tokens.shape
    length = local_rows * n
    width = w_query.shape[1]
    row_ids = lax.axis_index("tensor") * local_rows + lax.iota(jnp.int32, local_rows)
    valid = (row_ids < lengths[0])[:, None]

    inputs = tokens.astype(F32)
    grad_out = jnp.where(valid, cotangent.astype(F32), 0.0)
    devices = lax.axis_size("dp")
    place = lax.axis_index("dp")
    share = w_gate.shape[1] // devices

    (
        context, logsum, w_packed, q, k, v, cosine, sine, attn_rows, grad_branch, weights, context_own, _,
        w_out_all,
    ) = front(
        tokens, cotangent, ln1_gain, ln1_bias, angle_tables(length), w_query, w_key, w_value,
        w_gate, w_up, down_weight, w_out, lengths, n, devices,
    )
    attn_rows = attn_rows.reshape(length, depth)
    weights = weights.reshape(3, n * share, depth)

    w_out_all = w_out_all.reshape(n, width, depth)
    attn_out = sum(dot(context_own[t], w_out_all[t]).astype(BF).astype(F32) for t in range(n))
    middle = inputs + attn_out
    scaled2, inverse2 = norm_parts(middle)
    ffn_in = (scaled2 * ln2_gain + ln2_bias).astype(BF)
    grad_parts, out_parts, down_grad, pair_grads, w_packed = ffn(
        ffn_in, grad_branch, weights, w_packed, n, devices
    )
    grad_ffn_in = sum(grad_parts[p].astype(F32) for p in range(devices // 2))
    grad_norm2, gain2_grad, shift2_grad = norm_back(
        grad_ffn_in, scaled2, inverse2, ln2_gain
    )
    grad_middle = grad_out + grad_norm2
    grad_attn = grad_middle.astype(BF)
    w_packed = lax.all_gather(w_packed, "dp", axis=0)
    down_grad = lax.psum_scatter(down_grad, "tensor", scatter_dimension=0, tiled=True)[0]
    packed, packed_own, out_sums, out_piece, pair_grads = att_bwd(
        grad_attn, w_out_all, context_own, out_parts, pair_grads, q, k, v, context, logsum, cosine, sine, n
    )
    down_grad, out_piece, w_packed = lax.optimization_barrier((down_grad, out_piece, w_packed))
    grads = lax.all_gather(jnp.concatenate([down_grad, out_piece]), "dp", axis=0)
    ffn_out = sum(x.astype(F32) for x in (out_parts[0], *out_sums))
    output = jnp.where(valid, middle + ffn_out, 0.0).astype(BF)
    input_grad, query_grad, key_grad, value_grad, sums = finish(
        attn_rows, packed, packed_own, w_packed, tokens, grad_middle, ln1_gain,
        jnp.stack([gain2_grad, shift2_grad]), width, devices,
    )
    gate_grad, up_grad, down_grad, out_grad = unpack(pair_grads, grads)
    gain1_grad, shift1_grad, gain2_grad, shift2_grad = (sums[i] for i in range(4))
    return (
        output, input_grad, gain1_grad, shift1_grad, query_grad, key_grad, value_grad, out_grad,
        gain2_grad, shift2_grad, gate_grad, up_grad, down_grad,
    )


def solution(mesh):
    rows = P(("dp", "tensor"), None)
    columns = P(None, "tensor")
    parts = P("tensor", None)
    return jax.shard_map(
        on_device,
        mesh=mesh,
        in_specs=(
            rows, P("dp"), P(), P(), columns, columns, columns, parts,
            P(), P(), columns, columns, parts, rows,
        ),
        out_specs=(
            rows, rows, P(), P(), columns, columns, columns, parts,
            P(), P(), columns, columns, parts,
        ),
        check_vma=False,
    )
```

```python
import functools
import math

import jax
import jax.numpy as jnp
from jax import lax
from jax.experimental import pallas as pl
from jax.experimental.pallas import tpu as pltpu
from jax.sharding import PartitionSpec as P

HD = 64
EPS = 1e-05
SCALE = 1.0 / math.sqrt(HD)
F32 = jnp.float32
BF = jnp.bfloat16
NT = (((1,), (1,)), ((), ()))
NN = (((1,), (0,)), ((), ()))
TN = (((0,), (0,)), ((), ()))
MESH = pl.DeviceIdType.MESH


def dot(a, b, dims=NN):
    return lax.dot_general(a, b, dims, preferred_element_type=F32)


def lanes(shape):
    return lax.broadcasted_iota(jnp.int32, shape, 1)


def split3(x):
    hi = x.astype(BF).astype(F32)
    mid = (x - hi).astype(BF).astype(F32)
    return hi, mid, x - hi - mid


def partner(x):
    width = x.shape[1]
    first = lanes(x.shape) % HD < HD // 2
    return jnp.where(first, pltpu.roll(x, width - HD // 2, 1), pltpu.roll(x, HD // 2, 1))


STEP = 64


def angle_tables(length):
    half = HD // 2
    lane = lax.optimization_barrier(lax.iota(jnp.int32, 2 * HD))
    freqs = 10000.0 ** (-((lane % half).astype(F32) * 2.0 / HD))
    sign = jnp.where(lane % HD < half, -1.0, 1.0)

    def table(positions):
        angles = positions[:, None] * freqs[None, :]
        return jnp.stack([jnp.cos(angles), jnp.sin(angles)])

    return table(lax.iota(F32, length // STEP) * STEP), table(lax.iota(F32, STEP)), sign[None, :]


def differ(a, b, bits):
    return sum(lax.rem(a // (1 << k) + b // (1 << k), 2) * (1 << k) for k in range(bits))


def remote(src, dst, send, recv, **to):
    return pltpu.make_async_remote_copy(
        src_ref=src, dst_ref=dst, send_sem=send, recv_sem=recv, device_id=to, device_id_type=MESH
    )


def ring(n, step):
    return lax.rem(lax.axis_index("tensor") + step, n)


def same_core(s, chips):
    me = lax.axis_index("dp")
    return differ(me // 2, s, chips.bit_length() - 1) * 2 + lax.rem(me, 2)


def sibling():
    me = lax.axis_index("dp")
    return me + 1 - 2 * lax.rem(me, 2)


def greet(n, chips, both_cores=False):
    barrier = pltpu.get_barrier_semaphore()
    if both_cores:
        pl.semaphore_signal(barrier, inc=1, device_id={"dp": sibling()}, device_id_type=MESH)
    for step in range(1, n):
        pl.semaphore_signal(barrier, inc=1, device_id={"tensor": ring(n, step)}, device_id_type=MESH)
    for s in range(1, chips):
        pl.semaphore_signal(
            barrier, inc=1, device_id={"dp": same_core(s, chips)}, device_id_type=MESH
        )
    pl.semaphore_wait(barrier, n + chips - 2 + both_cores)


def front_kernel(
    n, chips, chunks, limit_ref, tokens_ref, ct_ref, gain_ref, shift_ref, coarse_ref, fine_ref, sign_ref,
    wq_ref, wk_ref, wv_ref, gate_ref, up_ref, wo_ref,
    ctx_ref, lse_ref, wp_ref, q_out, k_out, v_out, cos_out, sin_out, rows_ref, gb_all, w_all, out_ref, wo_z, wo_all,
    landed, gb, columns, own_w, wqkv, q_ref, k_ref, v_ref, cos_ref, sin_ref,
    right_send, right_recv, left_send, left_recv, gs_send, gs_recv, gr_send, gr_recv, rows_sem,
    wr_send, wr_recv, wl_send, wl_recv, send_sem, recv_sem, wz_send, wz_recv, ws_send, ws_recv,
    wx_send, wx_recv, cut_sem, load_sem, save_sem, keep_sem,
):
    i = pl.program_id(0)
    steps = pl.num_programs(0)
    me = lax.axis_index("tensor")
    place = lax.axis_index("dp")
    core = lax.rem(place, 2)
    bits = chips.bit_length() - 1
    rows, depth = tokens_ref.shape
    heads = q_ref.shape[0]
    piece = rows // chunks
    limit = limit_ref[0]
    s = i // heads
    h = lax.rem(i, heads)

    def over(shard, d, c, send, recv, to):
        part = landed.at[shard, pl.ds(c * piece, piece)]
        return remote(part, part, send.at[d, c], recv.at[d, c], tensor=to)

    def rightward(d, c):
        return over(me - d, d, c, right_send, right_recv, me + 1)

    def leftward(d, c):
        return over(me + d, d, c, left_send, left_recv, me - 1)

    def from_left(d, c):
        return over(me - d, d - 1, c, right_send, right_recv, me - 1)

    def from_right(d, c):
        return over(me + d, d - 1, c, left_send, left_recv, me + 1)

    def weights(shard, d, k, send, recv, to):
        there = w_all.at[k, shard]
        return remote(there if d else own_w.at[k], there, send.at[d, k], recv.at[d, k], tensor=to)

    def w_right(d, k):
        return weights(me - d, d, k, wr_send, wr_recv, me + 1)

    def w_left(d, k):
        return weights(me + d, d, k, wl_send, wl_recv, me - 1)

    def w_from_left(d, k):
        return weights(me - d, d - 1, k, wr_send, wr_recv, me - 1)

    def w_from_right(d, k):
        return weights(me + d, d - 1, k, wl_send, wl_recv, me + 1)

    def spread_gb(c):
        return remote(
            gb, gb_all.at[place // 2, core], gs_send.at[c], gs_recv.at[c], dp=same_core(c, chips)
        )

    def relay_gb(c):
        there = gb_all.at[differ(place // 2, c, bits), core]
        return remote(there if c else gb, there, gr_send.at[c], gr_recv.at[c], dp=sibling())

    def wo_over(step):
        return remote(
            wo_ref, wo_z.at[me], wz_send.at[step], wz_recv.at[step], tensor=ring(n, step + 1)
        )

    def spread_wo(c):
        return remote(
            wo_z, wo_all.at[:, place], ws_send.at[c], ws_recv.at[c], dp=same_core(c, chips)
        )

    def relay_wo(c):
        there = wo_all.at[:, differ(place // 2, c, bits) * 2 + core]
        return remote(there if c else wo_z, there, wx_send.at[c], wx_recv.at[c], dp=sibling())

    def push(step):
        owner = ring(n, step + 1)
        return remote(
            ctx_ref.at[pl.ds(pl.multiple_of(owner * rows, rows), rows)], out_ref.at[me],
            send_sem.at[step], recv_sem.at[step], tensor=owner,
        )

    def save(shard):
        return pltpu.make_async_copy(landed.at[shard], rows_ref.at[shard], rows_sem.at[shard])

    mine = pl.ds(pl.multiple_of(me * rows, rows), rows)
    keeps = [
        pltpu.make_async_copy(gb, gb_all.at[place // 2, core], keep_sem.at[0]),
        pltpu.make_async_copy(wo_ref, wo_z.at[me], keep_sem.at[1]),
        pltpu.make_async_copy(wo_z, wo_all.at[:, place], keep_sem.at[2]),
        pltpu.make_async_copy(ctx_ref.at[mine], out_ref.at[me], keep_sem.at[3]),
        pltpu.make_async_copy(own_w, w_all.at[:, me], keep_sem.at[4]),
    ]
    saves = [
        pltpu.make_async_copy(a, b, save_sem.at[j])
        for j, (a, b) in enumerate(
            ((q_ref, q_out), (k_ref, k_out), (v_ref, v_out), (cos_ref, cos_out), (sin_ref, sin_out))
        )
    ]

    @pl.when(i == 0)
    def _():
        loads = [
            pltpu.make_async_copy(ref, wqkv.at[j], load_sem.at[j])
            for j, ref in enumerate((wq_ref, wk_ref, wv_ref))
        ]
        share = own_w.shape[1]
        ours = pl.ds(pl.multiple_of(place * share, share), share)
        cuts = []
        for k, ref in enumerate((gate_ref, up_ref)):
            src = ref if share % 128 else ref.at[:, ours]
            cuts.append(pltpu.make_async_copy(src, columns.at[k], cut_sem.at[k]))
        for copy in loads + cuts:
            copy.start()

        barrier = pltpu.get_barrier_semaphore()
        for step in range(1, n):
            to = ring(n, step)
            pl.semaphore_signal(barrier, inc=1, device_id={"tensor": to}, device_id_type=MESH)
        pl.semaphore_signal(barrier, inc=1, device_id={"dp": sibling()}, device_id_type=MESH)
        for c in range(1, chips):
            to = same_core(c, chips)
            pl.semaphore_signal(barrier, inc=1, device_id={"dp": to}, device_id_type=MESH)

        values = tokens_ref[...].astype(F32)
        values = values - jnp.mean(values, axis=1, keepdims=True)
        inverse = lax.rsqrt(jnp.mean(values * values, axis=1, keepdims=True) + EPS)
        landed[me] = (values * inverse * gain_ref[...] + shift_ref[...]).astype(BF)

        pl.semaphore_wait(barrier, n - 1 + chips)

        for c in range(chunks):

            @pl.when(me < n - 1)
            def _():
                rightward(0, c).start()

            @pl.when(me > 0)
            def _():
                leftward(0, c).start()

        row = me * rows + lax.broadcasted_iota(jnp.int32, (rows, depth), 0)
        gb[...] = jnp.where(row < limit, ct_ref[...].astype(F32), 0.0).astype(BF)
        for c in range(1, chips):
            spread_gb(c).start()
        relay_gb(0).start()
        keeps[0].start()
        keeps[1].start()
        for copy in loads:
            copy.wait()

        cut = wp_ref.shape[0]
        here = pl.ds(pl.multiple_of(place * cut, cut), cut)
        first = lanes((cut, 128)) < HD
        for p in range(heads // 2):
            at = slice(p * 128, p * 128 + 128)
            query, key, value = (wqkv[j, here, at].astype(F32) for j in range(3))
            even = jnp.where(first, key, pltpu.roll(value, HD, 1))
            odd = jnp.where(first, pltpu.roll(key, HD, 1), value)
            for slot, values in ((2 * p, even), (2 * p + 1, odd), (heads + p, query)):
                wp_ref[:, slot * 128 : slot * 128 + 128] = values.astype(BF)

        lane = lanes((rows, 128))
        ones = jnp.where(lane < HD + 3, 1.0, 0.0)
        unit = jnp.where(lane == HD + 3, 1.0, 0.0)

        def put(out, here, values, extra):
            for head in range(heads):
                own = values[:, head // 2 * 128 : head // 2 * 128 + 128]
                own = pltpu.roll(own, HD, 1) if head % 2 else own
                out[head, here, :] = jnp.where(lane < HD, own, extra).astype(BF)

        def project(shard):
            here = pl.ds(pl.multiple_of(shard * rows, rows), rows)
            for j in range(rows // STEP):
                part = pl.ds(pl.multiple_of(shard * rows + j * STEP, STEP), STEP)
                coarse = pl.ds(shard * (rows // STEP) + j, 1)
                c0, s0 = coarse_ref[0, coarse, :], coarse_ref[1, coarse, :]
                cos_ref[part, :] = c0 * fine_ref[0] - s0 * fine_ref[1]
                sin_ref[part, :] = (s0 * fine_ref[0] + c0 * fine_ref[1]) * sign_ref[...]
            cosine = jnp.tile(cos_ref[here, :], (1, heads // 2))
            sine = jnp.tile(sin_ref[here, :], (1, heads // 2))
            x = landed[shard]
            row = shard * rows + lax.broadcasted_iota(jnp.int32, (rows, 128), 0)
            bias = jnp.where(lane == HD + 3, jnp.where(row < limit, 0.0, -1e30), ones)
            raw = dot(x, wqkv[0])
            turned = (raw * cosine + partner(raw) * sine).astype(BF).astype(F32)
            put(q_ref, here, turned * SCALE, unit)
            raw = dot(x, wqkv[1])
            put(k_ref, here, raw * cosine + partner(raw) * sine, bias)
            put(v_ref, here, dot(x, wqkv[2]), ones)

        for d in range(1, n + 1):
            for c in range(chunks):
                if d < n:

                    @pl.when(me >= d)
                    def _():
                        from_left(d, c).wait_recv()

                    @pl.when((me >= d) & (me < n - 1))
                    def _():
                        rightward(d, c).start()

                    @pl.when(me + d < n)
                    def _():
                        from_right(d, c).wait_recv()

                    @pl.when((me + d < n) & (me > 0))
                    def _():
                        leftward(d, c).start()

                if c == 0:

                    @pl.when(me >= d - 1)
                    def _():
                        save(me - d + 1).start()
                        project(me - d + 1)

                if c == 1 and d > 1:

                    @pl.when(me + d - 1 < n)
                    def _():
                        save(me + d - 1).start()
                        project(me + d - 1)

                if c == 2 and d == 1:
                    for cut in cuts:
                        cut.wait()
                    for k in range(2):
                        own_w[k] = columns[k].astype(F32).T.astype(BF)
                    keeps[4].start()

                if c == chunks - 1 and d == 2:
                    for near in range(1, chips // 2 + 1):
                        spread_gb(near).wait_recv()
                        relay_gb(near).start()

            if d < n:

                @pl.when((me < n - 1) & (me + 1 == d))
                def _():
                    for k in range(2):
                        w_right(0, k).start()

                @pl.when((me > 0) & (n - me == d))
                def _():
                    for k in range(2):
                        w_left(0, k).start()

        for copy in saves:
            copy.start()
        for step in range(n - 1):
            wo_over(step).start()
        for far in range(chips // 2 + 1, chips):
            spread_gb(far).wait_recv()
            relay_gb(far).start()

    stride = max((heads * n - 2) // max(n - 2, 1), 1)
    for d in range(1, n - 1):

        @pl.when(i == 1 + (d - 1) * stride)
        def _():
            for k in range(2):

                @pl.when((me >= d) & (me < n - 1))
                def _():
                    w_from_left(d, k).wait_recv()
                    w_right(d, k).start()

                @pl.when((me + d < n) & (me > 0))
                def _():
                    w_from_right(d, k).wait_recv()
                    w_left(d, k).start()

    @pl.when(i == heads)
    def _():
        for step in range(n - 1):
            wo_over(step).wait()
        keeps[1].wait()
        for c in range(1, chips):
            spread_wo(c).start()
        relay_wo(0).start()
        keeps[2].start()

    @pl.when(i == (n - 1) * heads)
    def _():
        for c in range(1, chips):
            spread_wo(c).wait_recv()
            relay_wo(c).start()

    owner = ring(n, s + 1)
    block = pl.ds(pl.multiple_of(owner * rows, rows), rows)
    scores = dot(q_ref[h, block, :], k_ref[h], NT)
    peak = jnp.max(scores, axis=1, keepdims=True)
    acc = dot(jnp.exp(scores - peak).astype(BF), v_ref[h])
    lane = lanes((rows, 128))
    total = jnp.sum(jnp.where(lane == HD, acc, 0.0), axis=1, keepdims=True)
    out = acc * (1.0 / total)
    odd = lax.rem(h, 2)
    out = jnp.where(odd == 1, pltpu.roll(out, HD, 1), out).astype(BF)
    pair = pl.ds(pl.multiple_of(h // 2 * 128, 128), 128)
    ctx_ref[block, pair] = jnp.where((lane >= HD) == (odd == 1), out, ctx_ref[block, pair])
    lse_ref[block, :] = jnp.where(lane == h, peak + jnp.log(total), lse_ref[block, :])

    @pl.when((h == heads - 1) & (s < n - 1))
    def _():
        push(s).start()

    @pl.when(i == steps - 1)
    def _():
        keeps[3].start()
        for d in range(n - 1):
            for c in range(chunks):

                @pl.when((me >= d) & (me < n - 1))
                def _():
                    rightward(d, c).wait_send()

                @pl.when((me + d < n) & (me > 0))
                def _():
                    leftward(d, c).wait_send()

            for k in range(2):

                @pl.when((me >= d) & (me < n - 1))
                def _():
                    w_right(d, k).wait_send()

                @pl.when((me + d < n) & (me > 0))
                def _():
                    w_left(d, k).wait_send()

        for k in range(2):
            for d in range(1, n):

                @pl.when((me >= d) & ((me == n - 1) | (d == n - 1)))
                def _():
                    w_from_left(d, k).wait_recv()

                @pl.when((me + d < n) & ((me == 0) | (d == n - 1)))
                def _():
                    w_from_right(d, k).wait_recv()

        for c in range(chips):
            relay_gb(c).wait()
            relay_wo(c).wait()
            if c:
                spread_gb(c).wait_send()
                spread_wo(c).wait_send()
        for shard in range(n):
            save(shard).wait()
        for copy in saves:
            copy.wait()
        for step in range(n - 1):
            push(step).wait()
        for j in (0, 2, 3, 4):
            keeps[j].wait()


def front(
    tokens, cotangent, gain, shift, tables, w_query, w_key, w_value, gate, up, w_out, limit, n, devices
):
    rows, depth = tokens.shape
    total = n * rows
    width = w_query.shape[1]
    heads = width // HD
    chips = devices // 2
    chunks = 4
    place = lax.axis_index("dp")
    share = gate.shape[1] // devices
    part = width // devices
    if share % 128:
        gate, up = (lax.dynamic_slice_in_dim(w, place * share, share, 1) for w in (gate, up))
    hbm = pl.BlockSpec(memory_space=pl.ANY)

    def whole(*shape):
        return pl.BlockSpec(shape, lambda *_: (0,) * len(shape), pipeline_mode=pl.Buffered(1))

    def dma(*shape):
        return pltpu.SemaphoreType.DMA(shape)

    head_array = jax.ShapeDtypeStruct((heads, total, 128), BF)
    table = jax.ShapeDtypeStruct((total, 128), F32)
    coarse, fine, sign = tables
    return pl.pallas_call(
        functools.partial(front_kernel, n, chips, chunks),
        out_shape=(
            jax.ShapeDtypeStruct((total, width), BF),
            table,
            jax.ShapeDtypeStruct((depth // devices, 3 * width), BF),
            head_array, head_array, head_array, table, table,
            jax.ShapeDtypeStruct((n, rows, depth), BF),
            jax.ShapeDtypeStruct((chips, 2, rows, depth), BF),
            jax.ShapeDtypeStruct((2, n, share, depth), BF),
            jax.ShapeDtypeStruct((n, rows, width), BF),
            jax.ShapeDtypeStruct((n, part, depth), BF),
            jax.ShapeDtypeStruct((n, devices, part, depth), BF),
        ),
        grid_spec=pltpu.PrefetchScalarGridSpec(
            num_scalar_prefetch=0,
            grid=(n * heads,),
            in_specs=[pl.BlockSpec(memory_space=pltpu.SMEM)]
            + [whole(rows, depth)] * 2
            + [whole(1, depth)] * 2
            + [whole(*coarse.shape), whole(*fine.shape), whole(*sign.shape)]
            + [hbm] * 6,
            out_specs=[whole(total, width), whole(total, 128), whole(depth // devices, 3 * width)]
            + [hbm] * 11,
            scratch_shapes=[
                pltpu.VMEM((n, rows, depth), BF),
                pltpu.VMEM((rows, depth), BF),
                pltpu.VMEM((2, depth, share), BF),
                pltpu.VMEM((2, share, depth), BF),
                pltpu.VMEM((3, depth, width), BF),
            ]
            + [pltpu.VMEM((heads, total, 128), BF)] * 3
            + [pltpu.VMEM((total, 128), F32)] * 2
            + [dma(n - 1, chunks)] * 4
            + [dma(chips)] * 4
            + [dma(n)]
            + [dma(n - 1, 2)] * 4
            + [dma(n - 1)] * 4
            + [dma(chips)] * 4
            + [dma(3), dma(3), dma(5), dma(5)],
        ),
        compiler_params=pltpu.CompilerParams(
            vmem_limit_bytes=60 << 20, collective_id=1, has_side_effects=True
        ),
        cost_estimate=pl.CostEstimate(
            flops=4 * total * total * 256 * heads * 3, bytes_accessed=40 << 20, transcendentals=0
        ),
        name="front",
    )(
        limit, tokens, cotangent, gain.reshape(1, depth), shift.reshape(1, depth), coarse, fine, sign,
        w_query, w_key, w_value, gate, up,
        lax.dynamic_slice_in_dim(w_out, place * part, part, 0),
    )


def att_bwd_kernel(
    n, bk, chips, ga_ref, wo_ref, cown_ref, parts_ref, pg_ref, q_ref, k_ref, v_ref, ctx_ref, lse_ref,
    cos_ref, sin_ref, pk_ref, own_ref, sums_ref, og_ref, pg_all, do, gc, dka, dva, dqs,
    og_full, og_own, og_mate, og_sib, og_land, og_piece, og_z,
    send_sem, recv_sem, out_send, out_recv, pk_send, pk_recv, keep_sem,
    om_send, om_recv, op_send, op_recv, oz_send, oz_recv, gs_send, gs_recv, gr_send, gr_recv, pg_sem,
):
    i = pl.program_id(0)
    heads, total, _ = k_ref.shape
    h = jnp.where(i < heads, i, (i - heads) // (n - 1))
    t = jnp.where(i < heads, 0, lax.rem(i - heads, n - 1) + 1)
    rows = total // n
    me = lax.axis_index("tensor")
    place = lax.axis_index("dp")
    core = lax.rem(place, 2)
    bits = chips.bit_length() - 1
    share = og_ref.shape[0]
    mine = pl.ds(pl.multiple_of(me * rows, rows), rows)

    def push(step):
        return remote(
            gc.at[step], do.at[mine], send_sem.at[step], recv_sem.at[step], tensor=ring(n, step + 1)
        )

    def push_out(s):
        return remote(
            parts_ref.at[s], sums_ref.at[s - 1], out_send.at[s - 1], out_recv.at[s - 1],
            dp=same_core(s, chips),
        )

    def columns(slot):
        return pl.ds(pl.multiple_of(slot * 128, 128), 128)

    def push_pack(slot, step):
        owner = ring(n, step + 1)
        return remote(
            pk_ref.at[pl.ds(pl.multiple_of(owner * rows, rows), rows), columns(slot)],
            own_ref.at[me, :, columns(slot)],
            pk_send.at[slot, step], pk_recv.at[slot, step], tensor=owner,
        )

    def keep(slot):
        return pltpu.make_async_copy(
            pk_ref.at[mine, columns(slot)], own_ref.at[me, :, columns(slot)], keep_sem.at[slot]
        )

    @pl.when(i == 0)
    def _():
        greet(n, chips, True)

        def send(step, carry):
            gc[step] = dot(ga_ref[...], wo_ref[ring(n, step + 1)], NT).astype(BF)
            push(step).start()
            return carry

        lax.fori_loop(0, n - 1, send, 0)
        do[mine, :] = dot(ga_ref[...], wo_ref[me], NT).astype(BF)

    def pg_spread(s):
        return remote(pg_ref, pg_all.at[place], gs_send.at[s], gs_recv.at[s], dp=same_core(s, chips))

    def pg_relay(s):
        there = pg_all.at[differ(place // 2, s, bits) * 2 + core]
        return remote(there if s else pg_ref, there, gr_send.at[s], gr_recv.at[s], dp=sibling())

    def pg_keep():
        return pltpu.make_async_copy(pg_ref, pg_all.at[place], pg_sem)

    @pl.when(i == heads * n - 8)
    def _():
        for s in range(1, chips):
            pg_spread(s).start()
        pg_relay(0).start()
        pg_keep().start()

    def og_swap():
        return remote(og_mate, og_sib, om_send, om_recv, dp=sibling())

    def og_push(s):
        return remote(og_sib.at[s], og_land.at[s], op_send.at[s], op_recv.at[s], dp=same_core(s, chips))

    def og_over(step):
        to = ring(n, step + 1)
        return remote(og_piece.at[to], og_z.at[me], oz_send.at[step], oz_recv.at[step], tensor=to)

    @pl.when(i == 1)
    def _():
        def term(part, carry):
            og_full[...] = dot(cown_ref[part], ga_ref[...], TN)
            for s in range(chips):
                start = differ(place // 2, s, bits) * 2
                here = pl.ds(pl.multiple_of((start + core) * share, share), share)
                there = pl.ds(pl.multiple_of((start + 1 - core) * share, share), share)
                og_own[s, part] = og_full[here, :]
                og_mate[s, part] = og_full[there, :].astype(BF)
            return carry

        lax.fori_loop(0, n, term, 0)
        og_swap().start()

    @pl.when(i == 2)
    def _():
        og_swap().wait_recv()
        for s in range(chips):
            og_sib[s] = (og_own[s] + og_sib[s].astype(F32)).astype(BF)
            if s:
                og_push(s).start()

    @pl.when(i == heads * n - 6)
    def _():
        joined = og_sib[0].astype(F32)
        for s in range(1, chips):
            og_push(s).wait_recv()
            joined = joined + og_land[s].astype(F32)
        og_piece[...] = joined.astype(BF)
        for step in range(n - 1):
            og_over(step).start()

    @pl.when(i == heads + 1)
    def _():
        for s in range(1, chips):
            push_out(s).start()

    @pl.when(i == heads * n - 1)
    def _():
        og_z[me] = og_piece[me]
        for step in range(n - 1):
            og_over(step).wait_recv()
        joined = og_z[0].astype(F32)
        for part in range(1, n):
            joined = joined + og_z[part].astype(F32)
        og_ref[...] = joined.astype(BF)

    @pl.when((h == 0) & (t > 0))
    def _():
        push(t - 1).wait_recv()

    source = ring(n, n - t)
    block = pl.ds(pl.multiple_of(source * rows, rows), rows)
    pair = columns(h // 2)
    odd = lax.rem(h, 2) == 1
    lane = lanes((rows, 128))
    off = lane - HD
    logsum = jnp.sum(jnp.where(lane == h, lse_ref[block, :], 0.0), axis=1, keepdims=True)
    a, b, c = split3(-logsum)
    q = q_ref[h, block, :].astype(F32)
    q = jnp.where(off == 0, a, jnp.where(off == 1, b, jnp.where(off == 2, c, q))).astype(BF)
    g = jnp.where((lane >= HD) == odd, do[block, pair].astype(F32), 0.0)
    delta = jnp.sum(g * ctx_ref[block, pair].astype(F32), axis=1, keepdims=True)
    a, b, c = split3(-delta)
    g = jnp.where(odd, pltpu.roll(g, HD, 1), g)
    g = jnp.where(off == 0, a, jnp.where(off == 1, b, jnp.where(off == 2, c, g))).astype(BF)
    acc = jnp.zeros((rows, 128), F32)
    for j in range(total // bk):
        rk = pl.ds(j * bk, bk)
        kt = k_ref[h, rk, :]
        probs = jnp.exp(dot(kt, q, NT))
        grad = (probs * dot(v_ref[h, rk, :], g, NT)).astype(BF)
        for sums, term in ((dva, dot(probs.astype(BF), g)), (dka, dot(grad, q))):
            before = jnp.where(t == 0, jnp.zeros_like(term), sums[h, rk, :])
            sums[h, rk, :] = before + term
        acc = acc + dot(grad, kt, TN)
    acc = acc * SCALE

    @pl.when(jnp.logical_not(odd))
    def _():
        dqs[block, :] = acc

    @pl.when(odd)
    def _():
        grad = jnp.where(lane < HD, dqs[block, :], pltpu.roll(acc, HD, 1))
        grad = grad * cos_ref[block, :] - partner(grad) * sin_ref[block, :]
        pk_ref[block, columns(heads + h // 2)] = grad.astype(BF)

    @pl.when(odd & (t == 0))
    def _():
        keep(heads + h // 2).start()

    @pl.when(odd & (t > 0))
    def _():
        push_pack(heads + h // 2, n - 1 - t).start()

    @pl.when(t == n - 1)
    def _():
        dk = dka[h]
        dk = dk * cos_ref[...] - partner(dk) * sin_ref[...]
        both = jnp.where(lanes((total, 128)) < HD, dk, pltpu.roll(dva[h], HD, 1))
        pk_ref[:, columns(h)] = both.astype(BF)
        for step in range(n - 1):
            push_pack(h, step).start()
        keep(h).start()

    @pl.when(i == heads * n - 1)
    def _():
        for s in range(1, chips):
            pg_spread(s).wait_recv()
            pg_relay(s).start()
        for step in range(n - 1):
            push(step).wait_send()
        for s in range(1, chips):
            push_out(s).wait()
        og_swap().wait_send()
        pg_keep().wait()
        for s in range(chips):
            pg_relay(s).wait()
            if s:
                pg_spread(s).wait_send()
        for s in range(1, chips):
            og_push(s).wait_send()
        for step in range(n - 1):
            og_over(step).wait_send()
        for slot in range(heads + heads // 2):
            keep(slot).wait()
            for step in range(n - 1):
                push_pack(slot, step).wait()


def att_bwd(
    grad_attn, w_out, ctx_own, parts, pair_grads, q, k, v, ctx, lse, cosine, sine, n, bk=512
):
    heads, total, _ = q.shape
    width = heads * HD
    rows, depth = grad_attn.shape
    chips = parts.shape[0]
    share = width // (2 * chips)
    slots = heads + heads // 2
    hbm = pl.BlockSpec(memory_space=pl.ANY)

    def whole(*shape):
        return pl.BlockSpec(shape, lambda *_: (0,) * len(shape), pipeline_mode=pl.Buffered(1))

    return pl.pallas_call(
        functools.partial(att_bwd_kernel, n, bk, chips),
        out_shape=(
            jax.ShapeDtypeStruct((total, slots * 128), BF),
            jax.ShapeDtypeStruct((n, rows, slots * 128), BF),
            jax.ShapeDtypeStruct((chips - 1, rows, depth), BF),
            jax.ShapeDtypeStruct((share, depth), BF),
            jax.ShapeDtypeStruct((2 * chips, *pair_grads.shape), BF),
        ),
        grid_spec=pltpu.PrefetchScalarGridSpec(
            num_scalar_prefetch=0,
            grid=(heads * n,),
            in_specs=[whole(rows, depth), whole(n, width, depth), whole(n, rows, width), hbm, hbm]
            + [whole(heads, total, 128)] * 3
            + [whole(total, width)]
            + [whole(total, 128)] * 3,
            out_specs=[whole(total, slots * 128), hbm, hbm, whole(share, depth), hbm],
            scratch_shapes=[
                pltpu.VMEM((total, width), BF),
                pltpu.VMEM((n - 1, rows, width), BF),
            ]
            + [pltpu.VMEM((heads, total, 128), F32)] * 2
            + [pltpu.VMEM((total, 128), F32)]
            + [
                pltpu.VMEM((width, depth), F32),
                pltpu.VMEM((chips, n, share, depth), F32),
                pltpu.VMEM((chips, n, share, depth), BF),
                pltpu.VMEM((chips, n, share, depth), BF),
                pltpu.VMEM((chips, n, share, depth), BF),
                pltpu.VMEM((n, share, depth), BF),
                pltpu.VMEM((n, share, depth), BF),
            ]
            + [pltpu.SemaphoreType.DMA((n - 1,))] * 2
            + [pltpu.SemaphoreType.DMA((chips - 1,))] * 2
            + [pltpu.SemaphoreType.DMA((slots, n - 1))] * 2
            + [pltpu.SemaphoreType.DMA((slots,))]
            + [pltpu.SemaphoreType.DMA] * 2
            + [pltpu.SemaphoreType.DMA((chips,))] * 2
            + [pltpu.SemaphoreType.DMA((n - 1,))] * 2
            + [pltpu.SemaphoreType.DMA((chips,))] * 4
            + [pltpu.SemaphoreType.DMA],
        ),
        compiler_params=pltpu.CompilerParams(
            vmem_limit_bytes=60 << 20, collective_id=2, has_side_effects=True
        ),
        cost_estimate=pl.CostEstimate(
            flops=10 * total * total * 256 * heads,
            bytes_accessed=20 * total * width,
            transcendentals=total * total * heads,
        ),
        name="att_bwd",
    )(grad_attn, w_out, ctx_own, parts, pair_grads, q, k, v, ctx, lse, cosine, sine)


def finish_kernel(
    chips, n, x_ref, pk_ref, own_ref, w_ref, tokens_ref, middle_ref, gain_ref, vec_ref,
    input_ref, sums_ref, every,
    full, mate, sib, land, fin, vec_z, vec_dp, vec_me,
    sx_send, sx_recv, rs_send, rs_recv, ag_send, ag_recv, rl_send, rl_recv,
    vz_send, vz_recv, vd_send, vd_recv, own_sem,
):
    bits = chips.bit_length() - 1
    me = lax.axis_index("dp")
    place = lax.axis_index("tensor")
    core = lax.rem(me, 2)
    chip = me // 2
    other = 1 - core
    piece = fin.shape[0]

    def swap(s):
        return remote(mate.at[s], sib.at[s], sx_send.at[s], sx_recv.at[s], dp=chip * 2 + other)

    def push(s):
        return remote(sib.at[s], land.at[s], rs_send.at[s], rs_recv.at[s], dp=same_core(s, chips))

    def spread(s):
        return remote(
            fin, every.at[chip, core], ag_send.at[s], ag_recv.at[s], dp=same_core(s, chips)
        )

    def relay(s):
        src = every.at[differ(chip, s, bits), core]
        return remote(src, src, rl_send.at[s], rl_recv.at[s], dp=chip * 2 + other)

    def vec_over(step):
        return remote(
            vec_me.at[0], vec_z.at[place], vz_send.at[step], vz_recv.at[step], tensor=ring(n, step + 1)
        )

    def vec_across(step):
        return remote(
            vec_me.at[1], vec_dp.at[me], vd_send.at[step], vd_recv.at[step],
            dp=lax.rem(me + step + 1, 2 * chips),
        )

    barrier = pltpu.get_barrier_semaphore()
    for step in range(n - 1):
        pl.semaphore_signal(barrier, inc=1, device_id={"tensor": ring(n, step + 1)}, device_id_type=MESH)
    for step in range(2 * chips - 1):
        to = lax.rem(me + step + 1, 2 * chips)
        pl.semaphore_signal(barrier, inc=1, device_id={"dp": to}, device_id_type=MESH)

    full[...] = dot(x_ref[...], pk_ref[...], TN)
    pl.semaphore_wait(barrier, n + 2 * chips - 2)

    def part(s, which):
        start = (differ(chip, s, bits) * 2 + which) * piece
        return full[pl.ds(pl.multiple_of(start, piece), piece), :]

    for s in range(chips):
        mate[s] = part(s, other).astype(BF)
        swap(s).start()

    grad = jnp.zeros(input_ref.shape, F32)
    for t in range(n):
        w = w_ref[:, t].reshape(w_ref.shape[0] * w_ref.shape[2], w_ref.shape[3])
        grad = grad + dot(own_ref[t], w, NT).astype(BF).astype(F32)

    for s in range(1, chips):
        swap(s).wait_recv()
        sib[s] = (sib[s].astype(F32) + part(s, core)).astype(BF)
        push(s).start()
    swap(0).wait_recv()
    total = sib[0].astype(F32) + part(0, core)

    values = tokens_ref[...].astype(F32)
    values = values - jnp.mean(values, axis=1, keepdims=True)
    inverse = lax.rsqrt(jnp.mean(values * values, axis=1, keepdims=True) + EPS)
    scaled = values * inverse
    through = grad * gain_ref[...]
    inner = through - jnp.mean(through, axis=1, keepdims=True)
    inner = inner - scaled * jnp.mean(through * scaled, axis=1, keepdims=True)
    input_ref[...] = middle_ref[...] + inverse * inner
    vec_me[0, 0:1] = jnp.sum(grad * scaled, axis=0, keepdims=True)
    vec_me[0, 1:2] = jnp.sum(grad, axis=0, keepdims=True)
    vec_me[0, 2:4] = vec_ref[...]
    vec_me[0, 4:8] = jnp.zeros((4, vec_ref.shape[1]), F32)
    vec_z[place] = vec_me[0]
    for step in range(n - 1):
        vec_over(step).start()

    for s in range(1, chips):
        push(s).wait_recv()
        total = total + land[s].astype(F32)
    fin[...] = total.astype(BF)
    for s in range(1, chips):
        spread(s).start()
    mine = pltpu.make_async_copy(fin, every.at[chip, core], own_sem)
    mine.start()
    mine.wait()
    relay(0).start()

    for step in range(n - 1):
        vec_over(step).wait()
    vec = vec_z[0]
    for t in range(1, n):
        vec = vec + vec_z[t]
    vec_me[1] = vec
    vec_dp[me] = vec
    for step in range(2 * chips - 1):
        vec_across(step).start()
    for s in range(1, chips):
        spread(s).wait_recv()
        relay(s).start()
    for step in range(2 * chips - 1):
        vec_across(step).wait()
    vec = vec_dp[0]
    for t in range(1, 2 * chips):
        vec = vec + vec_dp[t]
    sums_ref[...] = vec
    for s in range(chips):
        relay(s).wait()
        swap(s).wait_send()
        if s > 0:
            spread(s).wait_send()
            push(s).wait_send()


def finish(rows_all, packed, own, w_all, tokens, middle, gain, vec, devices):
    n, rows, packs = own.shape
    depth = tokens.shape[1]
    chips = devices // 2
    piece = depth // devices
    vmem = pl.BlockSpec(memory_space=pltpu.VMEM)
    return pl.pallas_call(
        functools.partial(finish_kernel, chips, n),
        out_shape=(
            jax.ShapeDtypeStruct((rows, depth), F32),
            jax.ShapeDtypeStruct((8, depth), F32),
            jax.ShapeDtypeStruct((chips, 2, piece, packs), BF),
        ),
        in_specs=[vmem] * 8,
        out_specs=[vmem, vmem, pl.BlockSpec(memory_space=pl.ANY)],
        scratch_shapes=[
            pltpu.VMEM((depth, packs), F32),
            pltpu.VMEM((chips, piece, packs), BF),
            pltpu.VMEM((chips, piece, packs), BF),
            pltpu.VMEM((chips, piece, packs), BF),
            pltpu.VMEM((piece, packs), BF),
            pltpu.VMEM((n, 8, depth), F32),
            pltpu.VMEM((devices, 8, depth), F32),
            pltpu.VMEM((2, 8, depth), F32),
        ]
        + [pltpu.SemaphoreType.DMA((chips,))] * 8
        + [pltpu.SemaphoreType.DMA((n - 1,))] * 2
        + [pltpu.SemaphoreType.DMA((devices - 1,))] * 2
        + [pltpu.SemaphoreType.DMA],
        compiler_params=pltpu.CompilerParams(
            vmem_limit_bytes=56 << 20, collective_id=4, has_side_effects=True
        ),
        cost_estimate=pl.CostEstimate(
            flops=4 * n * rows * depth * packs, bytes_accessed=20 << 20, transcendentals=0
        ),
        name="finish",
    )(rows_all, packed, own, w_all, tokens, middle, gain.reshape(1, depth), vec)


def ffn_kernel(
    chips, x_ref, gb_ref, w_ref, down_ref, wp_ref, dx_ref, out_ref, dw_ref, zs_ref, wp_z,
    rows_all, gb, hid, gate_g, up_g, own, sib, mate, partial, z_left, z_right, wd,
    ag_send, ag_recv, rl_send, rl_recv, sx_send, sx_recv, rs_send, rs_recv, fw_send, fw_recv,
    gb_sem, out_sem, dx_sem, wp_send, wp_recv, wp_sem, zr_send, zr_recv, zl_send, zl_recv,
    dr_send, dr_recv, dl_send, dl_recv, wd_sem,
):
    bits = chips.bit_length() - 1
    me = lax.axis_index("dp")
    core = lax.rem(me, 2)
    chip = me // 2
    other = 1 - core
    rows, depth = x_ref.shape
    n, share, _ = dw_ref.shape

    def spread(s):
        to = differ(chip, s, bits) * 2 + core
        return remote(x_ref, rows_all.at[chip, core], ag_send.at[s], ag_recv.at[s], dp=to)

    square = chips == 4

    def hand_on(s):
        half = pl.ds((s - 1) * (rows // 2), rows // 2)
        part = rows_all.at[differ(chip, s, bits), core, half]
        to = differ(chip, 3 - s, bits) * 2 + core
        return remote(part, part, fw_send.at[s], fw_recv.at[s], dp=to)

    def handed(s):
        half = pl.ds((s - 1) * (rows // 2), rows // 2)
        part = rows_all.at[differ(chip, 3, bits), core, half]
        to = differ(chip, 3 - s, bits) * 2 + core
        return remote(part, part, fw_send.at[s], fw_recv.at[s], dp=to)

    def relay(s):
        src = differ(chip, s, bits)
        return remote(
            rows_all.at[src, core], rows_all.at[src, core], rl_send.at[s], rl_recv.at[s],
            dp=chip * 2 + other,
        )

    def swap(s):
        return remote(
            mate.at[lax.rem(s, 2)], sib.at[s], sx_send.at[s], sx_recv.at[s], dp=chip * 2 + other
        )

    def push(s):
        to = differ(chip, s, bits) * 2 + core
        return remote(sib.at[s, 0], dx_ref.at[s], rs_send.at[s], rs_recv.at[s], dp=to)

    def fetch(s):
        src = differ(chip, s, bits)
        return pltpu.make_async_copy(gb_ref.at[src], gb.at[src], gb_sem.at[s])

    part = lax.axis_index("tensor")

    def over(step):
        return remote(
            wp_ref, wp_z.at[part], wp_send.at[step], wp_recv.at[step], tensor=ring(n, step + 1)
        )

    def keep(s):
        return pltpu.make_async_copy(sib.at[s, 1], out_ref.at[s], out_sem.at[s])

    ours = pl.ds(pl.multiple_of(me * share, share), share)
    cut = pltpu.make_async_copy(down_ref.at[ours], wd.at[part], wd_sem)
    cut.start()
    for s in range(chips):
        fetch(s).start()
    barrier = pltpu.get_barrier_semaphore()
    for step in range(1, n):
        pl.semaphore_signal(barrier, inc=1, device_id={"tensor": ring(n, step)}, device_id_type=MESH)
    pl.semaphore_signal(barrier, inc=1, device_id={"dp": chip * 2 + other}, device_id_type=MESH)
    for s in range(1, chips):
        to = differ(chip, s, bits) * 2 + core
        pl.semaphore_signal(barrier, inc=1, device_id={"dp": to}, device_id_type=MESH)
    pl.semaphore_wait(barrier, chips + n - 1)
    direct = range(1, 3) if square else range(1, chips)
    for s in direct:
        spread(s).start()
    mine = pltpu.make_async_copy(x_ref, rows_all.at[chip, core], ag_send.at[0])
    mine.start()
    mine.wait()
    relay(0).start()
    keep_wp = pltpu.make_async_copy(wp_ref, wp_z.at[part], wp_sem)
    keep_wp.start()

    def d_right(d):
        there = wd.at[part - d]
        return remote(there, there, dr_send.at[d], dr_recv.at[d], tensor=part + 1)

    def d_left(d):
        there = wd.at[part + d]
        return remote(there, there, dl_send.at[d], dl_recv.at[d], tensor=part - 1)

    def d_from_left(d):
        there = wd.at[part - d]
        return remote(there, there, dr_send.at[d - 1], dr_recv.at[d - 1], tensor=part - 1)

    def d_from_right(d):
        there = wd.at[part + d]
        return remote(there, there, dl_send.at[d - 1], dl_recv.at[d - 1], tensor=part + 1)

    cut.wait()
    for d in range(n):
        if d:

            @pl.when(part >= d)
            def _():
                d_from_left(d).wait_recv()

        if d < n - 1:

            @pl.when((part >= d) & (part < n - 1))
            def _():
                d_right(d).start()

        if d:

            @pl.when(part + d < n)
            def _():
                d_from_right(d).wait_recv()

        if d < n - 1:

            @pl.when((part + d < n) & (part > 0))
            def _():
                d_left(d).start()

    for step in range(n - 1):
        over(step).start()

    def shard(src, which, put):
        x = rows_all[src, which]
        grad = gb[src, which]
        gate = dot(x, w_ref[0], NT)
        upper = dot(x, w_ref[1], NT)
        w_down = wd[...].reshape(n * share, depth)
        grad_hidden = dot(grad, w_down, NT)
        sigma = jax.nn.sigmoid(gate)
        act = gate * sigma
        hidden = (act * upper).astype(BF)
        grad_gate = (grad_hidden * upper * sigma * (1.0 + gate * (1.0 - sigma))).astype(BF)
        grad_upper = (grad_hidden * act).astype(BF)
        hid[src, which] = hidden
        gate_g[src, which] = grad_gate
        up_g[src, which] = grad_upper
        put[0] = (dot(grad_gate, w_ref[0]) + dot(grad_upper, w_ref[1])).astype(BF)
        put[1] = dot(hidden, w_down).astype(BF)

    def step(s, carry):
        src = differ(chip, s, bits)
        slot = lax.rem(s, 2)
        relay(s).wait_recv()
        fetch(s).wait()

        @pl.when(s >= 2)
        def _():
            swap(s - 2).wait_send()

        shard(src, other, mate.at[slot])
        swap(s).start()
        shard(src, core, own)
        swap(s).wait_recv()
        for k in range(2):
            sib[s, k] = (sib[s, k].astype(F32) + own[k].astype(F32)).astype(BF)

        @pl.when(s > 0)
        def _():
            push(s).start()

        keep(s).start()

        if square:

            @pl.when(s == 0)
            def _():
                for near in (1, 2):
                    spread(near).wait_recv()
                    hand_on(near).start()
                    relay(near).start()

        else:

            @pl.when(s < chips - 1)
            def _():
                spread(s + 1).wait_recv()
                relay(s + 1).start()

        if square:

            @pl.when(s == 1)
            def _():
                handed(1).wait_recv()
                handed(2).wait_recv()
                relay(3).start()

        return carry

    lax.fori_loop(0, chips, step, 0)
    first = pltpu.make_async_copy(sib.at[0, 0], dx_ref.at[0], dx_sem)
    first.start()
    def zr(t, k, to):
        return remote(
            partial.at[t, k], z_left.at[t, k], zr_send.at[t, k], zr_recv.at[t, k], tensor=to
        )

    def zl(t, k, to):
        return remote(
            partial.at[t, k], z_right.at[t, k], zl_send.at[t, k], zl_recv.at[t, k], tensor=to
        )

    def join(t, k, more):
        partial[t, k] = (partial[t, k].astype(F32) + more[t, k].astype(F32)).astype(BF)

    def weight_grad(left, right):
        left = left[...].reshape(-1, n * share)
        return dot(left, right[...].reshape(-1, depth), TN)

    def hand_along(k):
        for j in range(n - 1):
            t = n - 1 - j

            @pl.when((part > 0) & (part < t))
            def _():
                zr(t, k, part + 1).wait_recv()
                join(t, k, z_left)
                zr(t, k, part + 1).start()

            @pl.when((part < n - 1) & (part > j))
            def _():
                zl(j, k, part - 1).wait_recv()
                join(j, k, z_right)
                zl(j, k, part - 1).start()

    for k, left in enumerate((gate_g, up_g)):
        grad = weight_grad(left, rows_all)
        for t in range(n):
            partial[t, k] = grad[t * share : (t + 1) * share, :].astype(BF)

        for j in range(n - 1):

            @pl.when(part == 0)
            def _():
                zr(n - 1 - j, k, 1).start()

            @pl.when(part == n - 1)
            def _():
                zl(j, k, n - 2).start()

    hand_along(0)
    grad = weight_grad(hid, gb)
    for t in range(n):
        dw_ref[t] = grad[t * share : (t + 1) * share, :].astype(BF)
    hand_along(1)
    for k in range(2):
        for t in range(n):

            @pl.when((part == t) & (part > 0))
            def _():
                zr(t, k, part - 1).wait_recv()
                join(t, k, z_left)

            @pl.when((part == t) & (part < n - 1))
            def _():
                zl(t, k, part + 1).wait_recv()
                join(t, k, z_right)

            @pl.when(part == t)
            def _():
                zs_ref[k] = partial[t, k]

            @pl.when(part < t)
            def _():
                zr(t, k, part + 1).wait_send()

            @pl.when(part > t)
            def _():
                zl(t, k, part - 1).wait_send()

    for d in range(n - 1):

        @pl.when((part >= d) & (part < n - 1))
        def _():
            d_right(d).wait_send()

        @pl.when((part + d < n) & (part > 0))
        def _():
            d_left(d).wait_send()

    first.wait()
    keep_wp.wait()
    for step in range(n - 1):
        over(step).wait()
    for s in range(chips):
        keep(s).wait()
        relay(s).wait_send()
        if s >= chips - 2:
            swap(s).wait_send()
        if s in direct:
            spread(s).wait_send()
        if s > 0:
            push(s).wait()
    if square:
        hand_on(1).wait_send()
        hand_on(2).wait_send()


def ffn(x, grad_branch, weights, down, w_packed, n, devices):
    rows, depth = x.shape
    chips = devices // 2
    hidden = weights.shape[1]
    share = hidden // n
    vmem = pl.BlockSpec(memory_space=pltpu.VMEM)
    hbm = pl.BlockSpec(memory_space=pl.ANY)
    return pl.pallas_call(
        functools.partial(ffn_kernel, chips),
        out_shape=(
            jax.ShapeDtypeStruct((chips, rows, depth), BF),
            jax.ShapeDtypeStruct((chips, rows, depth), BF),
            jax.ShapeDtypeStruct((n, share, depth), BF),
            jax.ShapeDtypeStruct((2, share, depth), BF),
            jax.ShapeDtypeStruct((n, *w_packed.shape), BF),
        ),
        in_specs=[vmem, hbm, vmem, hbm, hbm],
        out_specs=[hbm, hbm, vmem, vmem, hbm],
        scratch_shapes=[
            pltpu.VMEM((chips, 2, rows, depth), BF),
            pltpu.VMEM((chips, 2, rows, depth), BF),
        ]
        + [pltpu.VMEM((chips, 2, rows, hidden), BF)] * 3
        + [
            pltpu.VMEM((2, rows, depth), BF),
            pltpu.VMEM((chips, 2, rows, depth), BF),
            pltpu.VMEM((2, 2, rows, depth), BF),
        ]
        + [pltpu.VMEM((n, 2, share, depth), BF)] * 3
        + [pltpu.VMEM((n, share, depth), BF)]
        + [pltpu.SemaphoreType.DMA((chips,))] * 8
        + [pltpu.SemaphoreType.DMA((3,))] * 2
        + [pltpu.SemaphoreType.DMA((chips,))] * 2
        + [pltpu.SemaphoreType.DMA]
        + [pltpu.SemaphoreType.DMA((n - 1,))] * 2
        + [pltpu.SemaphoreType.DMA]
        + [pltpu.SemaphoreType.DMA((n, 2))] * 4
        + [pltpu.SemaphoreType.DMA((n - 1,))] * 4
        + [pltpu.SemaphoreType.DMA],
        compiler_params=pltpu.CompilerParams(
            vmem_limit_bytes=62 << 20, collective_id=3, has_side_effects=True
        ),
        cost_estimate=pl.CostEstimate(
            flops=2 * 9 * devices * rows * depth * hidden, bytes_accessed=30 << 20, transcendentals=0
        ),
        name="ffn",
    )(x, grad_branch, weights, down, w_packed)


def unpack_kernel(
    share, pair_ref, rest_ref, pack_ref, gate_ref, up_ref, down_ref, out_ref, q_ref, k_ref, v_ref
):
    gate_ref[...] = pair_ref[0, 0].astype(F32).T
    up_ref[...] = pair_ref[0, 1].astype(F32).T
    rest = rest_ref[0].astype(F32)
    down_ref[...] = rest[:share]
    out_ref[...] = rest[share:]
    pack = pack_ref[0].astype(F32)
    pairs = q_ref.shape[1] // 128
    first = lanes((pack.shape[0], 128)) < HD
    for p in range(pairs):
        even = pack[:, p * 256 : p * 256 + 128]
        odd = pack[:, p * 256 + 128 : p * 256 + 256]
        out = slice(p * 128, p * 128 + 128)
        q_ref[:, out] = pack[:, (2 * pairs + p) * 128 : (2 * pairs + p + 1) * 128]
        k_ref[:, out] = jnp.where(first, even, pltpu.roll(odd, HD, 1))
        v_ref[:, out] = jnp.where(first, pltpu.roll(even, HD, 1), odd)


def unpack(pair, rest, pack):
    devices, _, share, depth = pair.shape
    hidden = devices * share
    height = rest.shape[1]
    width = devices * (height - share)
    piece = depth // devices
    if share % 128:
        down = rest[:, :share].reshape(hidden, depth).astype(F32)
        gate, up = (pair[:, k].reshape(hidden, depth).astype(F32).T for k in range(2))
        pack = pack.reshape(depth, 3 * width).astype(F32)
        both = pack[:, : 2 * width].reshape(depth, width // HD, 2, HD)
        key, value = (both[:, :, k].reshape(depth, width) for k in range(2))
        out = rest[:, share:].reshape(width, depth).astype(F32)
        return gate, up, down, out, pack[:, 2 * width :], key, value
    column = pl.BlockSpec((depth, share), lambda i: (0, i))
    rows = pl.BlockSpec((piece, width), lambda i: (i, 0))
    return pl.pallas_call(
        functools.partial(unpack_kernel, share),
        out_shape=(jax.ShapeDtypeStruct((depth, hidden), F32),) * 2
        + (
            jax.ShapeDtypeStruct((hidden, depth), F32),
            jax.ShapeDtypeStruct((width, depth), F32),
        )
        + (jax.ShapeDtypeStruct((depth, width), F32),) * 3,
        grid=(devices,),
        in_specs=[
            pl.BlockSpec((1, 2, share, depth), lambda i: (i, 0, 0, 0)),
            pl.BlockSpec((1, height, depth), lambda i: (i, 0, 0)),
            pl.BlockSpec((1, piece, 3 * width), lambda i: (i, 0, 0)),
        ],
        out_specs=[
            column, column, pl.BlockSpec((share, depth), lambda i: (i, 0)),
            pl.BlockSpec((height - share, depth), lambda i: (i, 0)), rows, rows, rows,
        ],
        compiler_params=pltpu.CompilerParams(vmem_limit_bytes=62 << 20),
        name="unpack",
    )(pair, rest, pack)


def norm_parts(values):
    centre = jnp.mean(values, axis=-1, keepdims=True)
    centred = values - centre
    inverse = lax.rsqrt(jnp.mean(centred * centred, axis=-1, keepdims=True) + EPS)
    return centred * inverse, inverse


def norm_back(upstream, scaled, inverse, gain):
    through = upstream * gain
    inner = (
        through
        - jnp.mean(through, axis=-1, keepdims=True)
        - scaled * jnp.mean(through * scaled, axis=-1, keepdims=True)
    )
    return inverse * inner, jnp.sum(upstream * scaled, axis=0), jnp.sum(upstream, axis=0)


def on_device(
    tokens, lengths, ln1_gain, ln1_bias, w_query, w_key, w_value, w_out,
    ln2_gain, ln2_bias, w_gate, w_up, down_weight, cotangent,
):
    n = lax.axis_size("tensor")
    local_rows, depth = tokens.shape
    length = local_rows * n
    width = w_query.shape[1]
    row_ids = lax.axis_index("tensor") * local_rows + lax.iota(jnp.int32, local_rows)
    valid = (row_ids < lengths[0])[:, None]

    inputs = tokens.astype(F32)
    grad_out = jnp.where(valid, cotangent.astype(F32), 0.0)
    devices = lax.axis_size("dp")
    place = lax.axis_index("dp")
    share = w_gate.shape[1] // devices

    (
        context, logsum, w_packed, q, k, v, cosine, sine, attn_rows, grad_branch, weights, context_own, _,
        w_out_all,
    ) = front(
        tokens, cotangent, ln1_gain, ln1_bias, angle_tables(length), w_query, w_key, w_value,
        w_gate, w_up, w_out, lengths, n, devices,
    )
    attn_rows = attn_rows.reshape(length, depth)
    weights = weights.reshape(2, n * share, depth)

    w_out_all = w_out_all.reshape(n, width, depth)
    attn_out = sum(dot(context_own[t], w_out_all[t]).astype(BF).astype(F32) for t in range(n))
    middle = inputs + attn_out
    scaled2, inverse2 = norm_parts(middle)
    ffn_in = (scaled2 * ln2_gain + ln2_bias).astype(BF)
    grad_parts, out_parts, down_grad, pair_grads, w_packed = ffn(
        ffn_in, grad_branch, weights, down_weight, w_packed, n, devices
    )
    grad_ffn_in = sum(grad_parts[p].astype(F32) for p in range(devices // 2))
    grad_norm2, gain2_grad, shift2_grad = norm_back(
        grad_ffn_in, scaled2, inverse2, ln2_gain
    )
    grad_middle = grad_out + grad_norm2
    grad_attn = grad_middle.astype(BF)
    w_packed = lax.all_gather(w_packed, "dp", axis=0)
    down_grad = lax.psum_scatter(down_grad, "tensor", scatter_dimension=0, tiled=True)[0]
    packed, packed_own, out_sums, out_piece, pair_grads = att_bwd(
        grad_attn, w_out_all, context_own, out_parts, pair_grads, q, k, v, context, logsum, cosine, sine, n
    )
    down_grad, out_piece, w_packed = lax.optimization_barrier((down_grad, out_piece, w_packed))
    grads = lax.all_gather(jnp.concatenate([down_grad, out_piece]), "dp", axis=0)
    ffn_out = sum(x.astype(F32) for x in (out_parts[0], *out_sums))
    output = jnp.where(valid, middle + ffn_out, 0.0).astype(BF)
    input_grad, sums, packed_grads = finish(
        attn_rows, packed, packed_own, w_packed, tokens, grad_middle, ln1_gain,
        jnp.stack([gain2_grad, shift2_grad]), devices,
    )
    packed_grads = packed_grads.reshape(devices, depth // devices, 3 * width)
    gate_grad, up_grad, down_grad, out_grad, query_grad, key_grad, value_grad = unpack(
        pair_grads, grads, packed_grads
    )
    gain1_grad, shift1_grad, gain2_grad, shift2_grad = (sums[i] for i in range(4))
    return (
        output, input_grad, gain1_grad, shift1_grad, query_grad, key_grad, value_grad, out_grad,
        gain2_grad, shift2_grad, gate_grad, up_grad, down_grad,
    )


def solution(mesh):
    rows = P(("dp", "tensor"), None)
    columns = P(None, "tensor")
    parts = P("tensor", None)
    return jax.shard_map(
        on_device,
        mesh=mesh,
        in_specs=(
            rows, P("dp"), P(), P(), columns, columns, columns, parts,
            P(), P(), columns, columns, parts, rows,
        ),
        out_specs=(
            rows, rows, P(), P(), columns, columns, columns, parts,
            P(), P(), columns, columns, parts,
        ),
        check_vma=False,
    )
```

```python
import functools
import math

import jax
import jax.numpy as jnp
from jax import lax
from jax.experimental import pallas as pl
from jax.experimental.pallas import tpu as pltpu
from jax.sharding import PartitionSpec as P

HD = 64
EPS = 1e-05
SCALE = 1.0 / math.sqrt(HD)
F32 = jnp.float32
BF = jnp.bfloat16
NT = (((1,), (1,)), ((), ()))
NN = (((1,), (0,)), ((), ()))
TN = (((0,), (0,)), ((), ()))
MESH = pl.DeviceIdType.MESH


def dot(a, b, dims=NN):
    return lax.dot_general(a, b, dims, preferred_element_type=F32)


def lanes(shape):
    return lax.broadcasted_iota(jnp.int32, shape, 1)


def split3(x):
    hi = x.astype(BF).astype(F32)
    mid = (x - hi).astype(BF).astype(F32)
    return hi, mid, x - hi - mid


def partner(x):
    width = x.shape[1]
    first = lanes(x.shape) % HD < HD // 2
    return jnp.where(first, pltpu.roll(x, width - HD // 2, 1), pltpu.roll(x, HD // 2, 1))


STEP = 64


def angle_tables(length):
    half = HD // 2
    lane = lax.optimization_barrier(lax.iota(jnp.int32, 2 * HD))
    freqs = 10000.0 ** (-((lane % half).astype(F32) * 2.0 / HD))
    sign = jnp.where(lane % HD < half, -1.0, 1.0)

    def table(positions):
        angles = positions[:, None] * freqs[None, :]
        return jnp.stack([jnp.cos(angles), jnp.sin(angles)])

    return table(lax.iota(F32, length // STEP) * STEP), table(lax.iota(F32, STEP)), sign[None, :]


def differ(a, b, bits):
    return sum(lax.rem(a // (1 << k) + b // (1 << k), 2) * (1 << k) for k in range(bits))


def remote(src, dst, send, recv, **to):
    return pltpu.make_async_remote_copy(
        src_ref=src, dst_ref=dst, send_sem=send, recv_sem=recv, device_id=to, device_id_type=MESH
    )


def ring(n, step):
    return lax.rem(lax.axis_index("tensor") + step, n)


def same_core(s, chips):
    me = lax.axis_index("dp")
    return differ(me // 2, s, chips.bit_length() - 1) * 2 + lax.rem(me, 2)


def sibling():
    me = lax.axis_index("dp")
    return me + 1 - 2 * lax.rem(me, 2)


def greet(n, chips, both_cores=False):
    barrier = pltpu.get_barrier_semaphore()
    if both_cores:
        pl.semaphore_signal(barrier, inc=1, device_id={"dp": sibling()}, device_id_type=MESH)
    for step in range(1, n):
        pl.semaphore_signal(barrier, inc=1, device_id={"tensor": ring(n, step)}, device_id_type=MESH)
    for s in range(1, chips):
        pl.semaphore_signal(
            barrier, inc=1, device_id={"dp": same_core(s, chips)}, device_id_type=MESH
        )
    pl.semaphore_wait(barrier, n + chips - 2 + both_cores)


def front_kernel(
    n, chips, chunks, limit_ref, tokens_ref, ct_ref, gain_ref, shift_ref, coarse_ref, fine_ref, sign_ref,
    wq_ref, wk_ref, wv_ref, gate_ref, up_ref, wo_ref,
    ctx_ref, lse_ref, wp_ref, q_out, k_out, v_out, cos_out, sin_out, rows_ref, gb_all, w_all, out_ref, wo_z, wo_all,
    landed, gb, columns, own_w, wqkv, q_ref, k_ref, v_ref, cos_ref, sin_ref,
    right_send, right_recv, left_send, left_recv, gs_send, gs_recv, gr_send, gr_recv, rows_sem,
    wr_send, wr_recv, wl_send, wl_recv, send_sem, recv_sem, wz_send, wz_recv, ws_send, ws_recv,
    wx_send, wx_recv, cut_sem, load_sem, save_sem, keep_sem,
):
    i = pl.program_id(0)
    steps = pl.num_programs(0)
    me = lax.axis_index("tensor")
    place = lax.axis_index("dp")
    core = lax.rem(place, 2)
    bits = chips.bit_length() - 1
    rows, depth = tokens_ref.shape
    heads = q_ref.shape[0]
    piece = rows // chunks
    limit = limit_ref[0]
    s = i // heads
    h = lax.rem(i, heads)

    def over(shard, d, c, send, recv, to):
        part = landed.at[shard, pl.ds(c * piece, piece)]
        return remote(part, part, send.at[d, c], recv.at[d, c], tensor=to)

    def rightward(d, c):
        return over(me - d, d, c, right_send, right_recv, me + 1)

    def leftward(d, c):
        return over(me + d, d, c, left_send, left_recv, me - 1)

    def from_left(d, c):
        return over(me - d, d - 1, c, right_send, right_recv, me - 1)

    def from_right(d, c):
        return over(me + d, d - 1, c, left_send, left_recv, me + 1)

    def weights(shard, d, k, send, recv, to):
        there = w_all.at[k, shard]
        return remote(there if d else own_w.at[k], there, send.at[d, k], recv.at[d, k], tensor=to)

    def w_right(d, k):
        return weights(me - d, d, k, wr_send, wr_recv, me + 1)

    def w_left(d, k):
        return weights(me + d, d, k, wl_send, wl_recv, me - 1)

    def w_from_left(d, k):
        return weights(me - d, d - 1, k, wr_send, wr_recv, me - 1)

    def w_from_right(d, k):
        return weights(me + d, d - 1, k, wl_send, wl_recv, me + 1)

    def spread_gb(c):
        return remote(
            gb, gb_all.at[place // 2, core], gs_send.at[c], gs_recv.at[c], dp=same_core(c, chips)
        )

    def relay_gb(c):
        there = gb_all.at[differ(place // 2, c, bits), core]
        return remote(there if c else gb, there, gr_send.at[c], gr_recv.at[c], dp=sibling())

    def wo_over(step):
        return remote(
            wo_ref, wo_z.at[me], wz_send.at[step], wz_recv.at[step], tensor=ring(n, step + 1)
        )

    def spread_wo(c):
        return remote(
            wo_z, wo_all.at[:, place], ws_send.at[c], ws_recv.at[c], dp=same_core(c, chips)
        )

    def relay_wo(c):
        there = wo_all.at[:, differ(place // 2, c, bits) * 2 + core]
        return remote(there if c else wo_z, there, wx_send.at[c], wx_recv.at[c], dp=sibling())

    def push(step):
        owner = ring(n, step + 1)
        return remote(
            ctx_ref.at[pl.ds(pl.multiple_of(owner * rows, rows), rows)], out_ref.at[me],
            send_sem.at[step], recv_sem.at[step], tensor=owner,
        )

    def save(shard):
        return pltpu.make_async_copy(landed.at[shard], rows_ref.at[shard], rows_sem.at[shard])

    mine = pl.ds(pl.multiple_of(me * rows, rows), rows)
    keeps = [
        pltpu.make_async_copy(gb, gb_all.at[place // 2, core], keep_sem.at[0]),
        pltpu.make_async_copy(wo_ref, wo_z.at[me], keep_sem.at[1]),
        pltpu.make_async_copy(wo_z, wo_all.at[:, place], keep_sem.at[2]),
        pltpu.make_async_copy(ctx_ref.at[mine], out_ref.at[me], keep_sem.at[3]),
        pltpu.make_async_copy(own_w, w_all.at[:, me], keep_sem.at[4]),
    ]
    saves = [
        pltpu.make_async_copy(a, b, save_sem.at[j])
        for j, (a, b) in enumerate(
            ((q_ref, q_out), (k_ref, k_out), (v_ref, v_out), (cos_ref, cos_out), (sin_ref, sin_out))
        )
    ]

    @pl.when(i == 0)
    def _():
        loads = [
            pltpu.make_async_copy(ref, wqkv.at[j], load_sem.at[j])
            for j, ref in enumerate((wq_ref, wk_ref, wv_ref))
        ]
        share = own_w.shape[1]
        ours = pl.ds(pl.multiple_of(place * share, share), share)
        cuts = []
        for k, ref in enumerate((gate_ref, up_ref)):
            src = ref if share % 128 else ref.at[:, ours]
            cuts.append(pltpu.make_async_copy(src, columns.at[k], cut_sem.at[k]))
        for copy in loads + cuts:
            copy.start()

        barrier = pltpu.get_barrier_semaphore()
        for step in range(1, n):
            to = ring(n, step)
            pl.semaphore_signal(barrier, inc=1, device_id={"tensor": to}, device_id_type=MESH)
        pl.semaphore_signal(barrier, inc=1, device_id={"dp": sibling()}, device_id_type=MESH)
        for c in range(1, chips):
            to = same_core(c, chips)
            pl.semaphore_signal(barrier, inc=1, device_id={"dp": to}, device_id_type=MESH)

        values = tokens_ref[...].astype(F32)
        values = values - jnp.mean(values, axis=1, keepdims=True)
        inverse = lax.rsqrt(jnp.mean(values * values, axis=1, keepdims=True) + EPS)
        landed[me] = (values * inverse * gain_ref[...] + shift_ref[...]).astype(BF)

        pl.semaphore_wait(barrier, n - 1 + chips)

        for c in range(chunks):

            @pl.when(me < n - 1)
            def _():
                rightward(0, c).start()

            @pl.when(me > 0)
            def _():
                leftward(0, c).start()

        row = me * rows + lax.broadcasted_iota(jnp.int32, (rows, depth), 0)
        gb[...] = jnp.where(row < limit, ct_ref[...].astype(F32), 0.0).astype(BF)
        for c in range(1, chips):
            spread_gb(c).start()
        relay_gb(0).start()
        keeps[0].start()
        keeps[1].start()
        for copy in loads:
            copy.wait()

        cut = wp_ref.shape[0]
        here = pl.ds(pl.multiple_of(place * cut, cut), cut)
        first = lanes((cut, 128)) < HD
        for p in range(heads // 2):
            at = slice(p * 128, p * 128 + 128)
            query, key, value = (wqkv[j, here, at].astype(F32) for j in range(3))
            even = jnp.where(first, key, pltpu.roll(value, HD, 1))
            odd = jnp.where(first, pltpu.roll(key, HD, 1), value)
            for slot, values in ((2 * p, even), (2 * p + 1, odd), (heads + p, query)):
                wp_ref[:, slot * 128 : slot * 128 + 128] = values.astype(BF)

        lane = lanes((rows, 128))
        ones = jnp.where(lane < HD + 3, 1.0, 0.0)
        unit = jnp.where(lane == HD + 3, 1.0, 0.0)

        def put(out, here, values, extra):
            for head in range(heads):
                own = values[:, head // 2 * 128 : head // 2 * 128 + 128]
                own = pltpu.roll(own, HD, 1) if head % 2 else own
                out[head, here, :] = jnp.where(lane < HD, own, extra).astype(BF)

        def project(shard):
            here = pl.ds(pl.multiple_of(shard * rows, rows), rows)
            for j in range(rows // STEP):
                part = pl.ds(pl.multiple_of(shard * rows + j * STEP, STEP), STEP)
                coarse = pl.ds(shard * (rows // STEP) + j, 1)
                c0, s0 = coarse_ref[0, coarse, :], coarse_ref[1, coarse, :]
                cos_ref[part, :] = c0 * fine_ref[0] - s0 * fine_ref[1]
                sin_ref[part, :] = (s0 * fine_ref[0] + c0 * fine_ref[1]) * sign_ref[...]
            cosine = jnp.tile(cos_ref[here, :], (1, heads // 2))
            sine = jnp.tile(sin_ref[here, :], (1, heads // 2))
            x = landed[shard]
            row = shard * rows + lax.broadcasted_iota(jnp.int32, (rows, 128), 0)
            bias = jnp.where(lane == HD + 3, jnp.where(row < limit, 0.0, -1e30), ones)
            raw = dot(x, wqkv[0])
            turned = (raw * cosine + partner(raw) * sine).astype(BF).astype(F32)
            put(q_ref, here, turned * SCALE, unit)
            raw = dot(x, wqkv[1])
            put(k_ref, here, raw * cosine + partner(raw) * sine, bias)
            put(v_ref, here, dot(x, wqkv[2]), ones)

        for d in range(1, n + 1):
            for c in range(chunks):
                if d < n:

                    @pl.when(me >= d)
                    def _():
                        from_left(d, c).wait_recv()

                    @pl.when((me >= d) & (me < n - 1))
                    def _():
                        rightward(d, c).start()

                    @pl.when(me + d < n)
                    def _():
                        from_right(d, c).wait_recv()

                    @pl.when((me + d < n) & (me > 0))
                    def _():
                        leftward(d, c).start()

                if c == 0:

                    @pl.when(me >= d - 1)
                    def _():
                        save(me - d + 1).start()
                        project(me - d + 1)

                if c == 1 and d > 1:

                    @pl.when(me + d - 1 < n)
                    def _():
                        save(me + d - 1).start()
                        project(me + d - 1)

                if c == 2 and d == 1:
                    for cut in cuts:
                        cut.wait()
                    for k in range(2):
                        own_w[k] = columns[k].astype(F32).T.astype(BF)
                    keeps[4].start()

                if c == chunks - 1 and d == 2:
                    for near in range(1, chips // 2 + 1):
                        spread_gb(near).wait_recv()
                        relay_gb(near).start()

            if d < n:

                @pl.when((me < n - 1) & (me + 1 == d))
                def _():
                    for k in range(2):
                        w_right(0, k).start()

                @pl.when((me > 0) & (n - me == d))
                def _():
                    for k in range(2):
                        w_left(0, k).start()

        for copy in saves:
            copy.start()
        for step in range(n - 1):
            wo_over(step).start()
        for far in range(chips // 2 + 1, chips):
            spread_gb(far).wait_recv()
            relay_gb(far).start()

    stride = max((heads * n - 2) // max(n - 2, 1), 1)
    for d in range(1, n - 1):

        @pl.when(i == 1 + (d - 1) * stride)
        def _():
            for k in range(2):

                @pl.when((me >= d) & (me < n - 1))
                def _():
                    w_from_left(d, k).wait_recv()
                    w_right(d, k).start()

                @pl.when((me + d < n) & (me > 0))
                def _():
                    w_from_right(d, k).wait_recv()
                    w_left(d, k).start()

    @pl.when(i == heads)
    def _():
        for step in range(n - 1):
            wo_over(step).wait()
        keeps[1].wait()
        for c in range(1, chips):
            spread_wo(c).start()
        relay_wo(0).start()
        keeps[2].start()

    @pl.when(i == (n - 1) * heads)
    def _():
        for c in range(1, chips):
            spread_wo(c).wait_recv()
            relay_wo(c).start()

    owner = ring(n, s + 1)
    block = pl.ds(pl.multiple_of(owner * rows, rows), rows)
    scores = dot(q_ref[h, block, :], k_ref[h], NT)
    peak = jnp.max(scores, axis=1, keepdims=True)
    acc = dot(jnp.exp(scores - peak).astype(BF), v_ref[h])
    lane = lanes((rows, 128))
    total = jnp.sum(jnp.where(lane == HD, acc, 0.0), axis=1, keepdims=True)
    out = acc * (1.0 / total)
    odd = lax.rem(h, 2)
    out = jnp.where(odd == 1, pltpu.roll(out, HD, 1), out).astype(BF)
    pair = pl.ds(pl.multiple_of(h // 2 * 128, 128), 128)
    ctx_ref[block, pair] = jnp.where((lane >= HD) == (odd == 1), out, ctx_ref[block, pair])
    lse_ref[block, :] = jnp.where(lane == h, peak + jnp.log(total), lse_ref[block, :])

    @pl.when((h == heads - 1) & (s < n - 1))
    def _():
        push(s).start()

    @pl.when(i == steps - 1)
    def _():
        keeps[3].start()
        for d in range(n - 1):
            for c in range(chunks):

                @pl.when((me >= d) & (me < n - 1))
                def _():
                    rightward(d, c).wait_send()

                @pl.when((me + d < n) & (me > 0))
                def _():
                    leftward(d, c).wait_send()

            for k in range(2):

                @pl.when((me >= d) & (me < n - 1))
                def _():
                    w_right(d, k).wait_send()

                @pl.when((me + d < n) & (me > 0))
                def _():
                    w_left(d, k).wait_send()

        for k in range(2):
            for d in range(1, n):

                @pl.when((me >= d) & ((me == n - 1) | (d == n - 1)))
                def _():
                    w_from_left(d, k).wait_recv()

                @pl.when((me + d < n) & ((me == 0) | (d == n - 1)))
                def _():
                    w_from_right(d, k).wait_recv()

        for c in range(chips):
            relay_gb(c).wait()
            relay_wo(c).wait()
            if c:
                spread_gb(c).wait_send()
                spread_wo(c).wait_send()
        for shard in range(n):
            save(shard).wait()
        for copy in saves:
            copy.wait()
        for step in range(n - 1):
            push(step).wait()
        for j in (0, 2, 3, 4):
            keeps[j].wait()


def front(
    tokens, cotangent, gain, shift, tables, w_query, w_key, w_value, gate, up, w_out, limit, n, devices
):
    rows, depth = tokens.shape
    total = n * rows
    width = w_query.shape[1]
    heads = width // HD
    chips = devices // 2
    chunks = 4
    place = lax.axis_index("dp")
    share = gate.shape[1] // devices
    part = width // devices
    if share % 128:
        gate, up = (lax.dynamic_slice_in_dim(w, place * share, share, 1) for w in (gate, up))
    hbm = pl.BlockSpec(memory_space=pl.ANY)

    def whole(*shape):
        return pl.BlockSpec(shape, lambda *_: (0,) * len(shape), pipeline_mode=pl.Buffered(1))

    def dma(*shape):
        return pltpu.SemaphoreType.DMA(shape)

    head_array = jax.ShapeDtypeStruct((heads, total, 128), BF)
    table = jax.ShapeDtypeStruct((total, 128), F32)
    coarse, fine, sign = tables
    return pl.pallas_call(
        functools.partial(front_kernel, n, chips, chunks),
        out_shape=(
            jax.ShapeDtypeStruct((total, width), BF),
            table,
            jax.ShapeDtypeStruct((depth // devices, 3 * width), BF),
            head_array, head_array, head_array, table, table,
            jax.ShapeDtypeStruct((n, rows, depth), BF),
            jax.ShapeDtypeStruct((chips, 2, rows, depth), BF),
            jax.ShapeDtypeStruct((2, n, share, depth), BF),
            jax.ShapeDtypeStruct((n, rows, width), BF),
            jax.ShapeDtypeStruct((n, part, depth), BF),
            jax.ShapeDtypeStruct((n, devices, part, depth), BF),
        ),
        grid_spec=pltpu.PrefetchScalarGridSpec(
            num_scalar_prefetch=0,
            grid=(n * heads,),
            in_specs=[pl.BlockSpec(memory_space=pltpu.SMEM)]
            + [whole(rows, depth)] * 2
            + [whole(1, depth)] * 2
            + [whole(*coarse.shape), whole(*fine.shape), whole(*sign.shape)]
            + [hbm] * 6,
            out_specs=[whole(total, width), whole(total, 128), whole(depth // devices, 3 * width)]
            + [hbm] * 11,
            scratch_shapes=[
                pltpu.VMEM((n, rows, depth), BF),
                pltpu.VMEM((rows, depth), BF),
                pltpu.VMEM((2, depth, share), BF),
                pltpu.VMEM((2, share, depth), BF),
                pltpu.VMEM((3, depth, width), BF),
            ]
            + [pltpu.VMEM((heads, total, 128), BF)] * 3
            + [pltpu.VMEM((total, 128), F32)] * 2
            + [dma(n - 1, chunks)] * 4
            + [dma(chips)] * 4
            + [dma(n)]
            + [dma(n - 1, 2)] * 4
            + [dma(n - 1)] * 4
            + [dma(chips)] * 4
            + [dma(3), dma(3), dma(5), dma(5)],
        ),
        compiler_params=pltpu.CompilerParams(
            vmem_limit_bytes=60 << 20, collective_id=1, has_side_effects=True
        ),
        cost_estimate=pl.CostEstimate(
            flops=4 * total * total * 256 * heads * 3, bytes_accessed=40 << 20, transcendentals=0
        ),
        name="front",
    )(
        limit, tokens, cotangent, gain.reshape(1, depth), shift.reshape(1, depth), coarse, fine, sign,
        w_query, w_key, w_value, gate, up,
        lax.dynamic_slice_in_dim(w_out, place * part, part, 0),
    )


def att_bwd_kernel(
    n, bk, chips, ga_ref, wo_ref, parts_ref, pg_ref, q_hbm, k_hbm, v_hbm, ctx_hbm, lse_hbm,
    cos_hbm, sin_hbm, cown_hbm, pk_ref, own_ref, sums_ref, og_ref, pg_all,
    q_ref, k_ref, v_ref, ctx_ref, lse_ref, cos_ref, sin_ref, cown_ref, do, gc, dka, dva, dqs,
    og_full, og_own, og_mate, og_sib, og_land, og_piece, og_z,
    send_sem, recv_sem, out_send, out_recv, pk_send, pk_recv, keep_sem,
    om_send, om_recv, op_send, op_recv, oz_send, oz_recv, gs_send, gs_recv, gr_send, gr_recv, pg_sem, load_sem,
):
    i = pl.program_id(0)
    heads, total, _ = k_ref.shape
    h = jnp.where(i < heads, i, (i - heads) // (n - 1))
    t = jnp.where(i < heads, 0, lax.rem(i - heads, n - 1) + 1)
    rows = total // n
    me = lax.axis_index("tensor")
    place = lax.axis_index("dp")
    core = lax.rem(place, 2)
    bits = chips.bit_length() - 1
    share = og_ref.shape[0]
    mine = pl.ds(pl.multiple_of(me * rows, rows), rows)

    def push(step):
        return remote(
            gc.at[step], do.at[mine], send_sem.at[step], recv_sem.at[step], tensor=ring(n, step + 1)
        )

    def push_out(s):
        return remote(
            parts_ref.at[s], sums_ref.at[s - 1], out_send.at[s - 1], out_recv.at[s - 1],
            dp=same_core(s, chips),
        )

    def columns(slot):
        return pl.ds(pl.multiple_of(slot * 128, 128), 128)

    def push_pack(slot, step):
        owner = ring(n, step + 1)
        return remote(
            pk_ref.at[pl.ds(pl.multiple_of(owner * rows, rows), rows), columns(slot)],
            own_ref.at[me, :, columns(slot)],
            pk_send.at[slot, step], pk_recv.at[slot, step], tensor=owner,
        )

    def keep(slot):
        return pltpu.make_async_copy(
            pk_ref.at[mine, columns(slot)], own_ref.at[me, :, columns(slot)], keep_sem.at[slot]
        )

    far = (q_hbm, k_hbm, v_hbm, ctx_hbm, lse_hbm, cos_hbm, sin_hbm, cown_hbm)
    near = (q_ref, k_ref, v_ref, ctx_ref, lse_ref, cos_ref, sin_ref, cown_ref)
    loads = [pltpu.make_async_copy(a, b, load_sem.at[j]) for j, (a, b) in enumerate(zip(far, near))]

    @pl.when(i == 0)
    def _():
        for load in loads:
            load.start()
        greet(n, chips, True)

        def send(step, carry):
            gc[step] = dot(ga_ref[...], wo_ref[ring(n, step + 1)], NT).astype(BF)
            push(step).start()
            return carry

        lax.fori_loop(0, n - 1, send, 0)
        do[mine, :] = dot(ga_ref[...], wo_ref[me], NT).astype(BF)
        for load in loads:
            load.wait()

    def pg_spread(s):
        return remote(pg_ref, pg_all.at[place], gs_send.at[s], gs_recv.at[s], dp=same_core(s, chips))

    def pg_relay(s):
        there = pg_all.at[differ(place // 2, s, bits) * 2 + core]
        return remote(there if s else pg_ref, there, gr_send.at[s], gr_recv.at[s], dp=sibling())

    def pg_keep():
        return pltpu.make_async_copy(pg_ref, pg_all.at[place], pg_sem)

    @pl.when(i == heads * n - 8)
    def _():
        for s in range(1, chips):
            pg_spread(s).start()
        pg_relay(0).start()
        pg_keep().start()

    def og_swap():
        return remote(og_mate, og_sib, om_send, om_recv, dp=sibling())

    def og_push(s):
        return remote(og_sib.at[s], og_land.at[s], op_send.at[s], op_recv.at[s], dp=same_core(s, chips))

    def og_over(step):
        to = ring(n, step + 1)
        return remote(og_piece.at[to], og_z.at[me], oz_send.at[step], oz_recv.at[step], tensor=to)

    @pl.when(i == 1)
    def _():
        def term(part, carry):
            og_full[...] = dot(cown_ref[part], ga_ref[...], TN)
            for s in range(chips):
                start = differ(place // 2, s, bits) * 2
                here = pl.ds(pl.multiple_of((start + core) * share, share), share)
                there = pl.ds(pl.multiple_of((start + 1 - core) * share, share), share)
                og_own[s, part] = og_full[here, :]
                og_mate[s, part] = og_full[there, :].astype(BF)
            return carry

        lax.fori_loop(0, n, term, 0)
        og_swap().start()

    @pl.when(i == 2)
    def _():
        og_swap().wait_recv()
        for s in range(chips):
            og_sib[s] = (og_own[s] + og_sib[s].astype(F32)).astype(BF)
            if s:
                og_push(s).start()

    @pl.when(i == heads * n - 6)
    def _():
        joined = og_sib[0].astype(F32)
        for s in range(1, chips):
            og_push(s).wait_recv()
            joined = joined + og_land[s].astype(F32)
        og_piece[...] = joined.astype(BF)
        for step in range(n - 1):
            og_over(step).start()

    @pl.when(i == heads + 1)
    def _():
        for s in range(1, chips):
            push_out(s).start()

    @pl.when(i == heads * n - 1)
    def _():
        og_z[me] = og_piece[me]
        for step in range(n - 1):
            og_over(step).wait_recv()
        joined = og_z[0].astype(F32)
        for part in range(1, n):
            joined = joined + og_z[part].astype(F32)
        og_ref[...] = joined.astype(BF)

    @pl.when((h == 0) & (t > 0))
    def _():
        push(t - 1).wait_recv()

    source = ring(n, n - t)
    block = pl.ds(pl.multiple_of(source * rows, rows), rows)
    pair = columns(h // 2)
    odd = lax.rem(h, 2) == 1
    lane = lanes((rows, 128))
    off = lane - HD
    logsum = jnp.sum(jnp.where(lane == h, lse_ref[block, :], 0.0), axis=1, keepdims=True)
    a, b, c = split3(-logsum)
    q = q_ref[h, block, :].astype(F32)
    q = jnp.where(off == 0, a, jnp.where(off == 1, b, jnp.where(off == 2, c, q))).astype(BF)
    g = jnp.where((lane >= HD) == odd, do[block, pair].astype(F32), 0.0)
    delta = jnp.sum(g * ctx_ref[block, pair].astype(F32), axis=1, keepdims=True)
    a, b, c = split3(-delta)
    g = jnp.where(odd, pltpu.roll(g, HD, 1), g)
    g = jnp.where(off == 0, a, jnp.where(off == 1, b, jnp.where(off == 2, c, g))).astype(BF)
    acc = jnp.zeros((rows, 128), F32)
    for j in range(total // bk):
        rk = pl.ds(j * bk, bk)
        kt = k_ref[h, rk, :]
        probs = jnp.exp(dot(kt, q, NT))
        grad = (probs * dot(v_ref[h, rk, :], g, NT)).astype(BF)
        for sums, term in ((dva, dot(probs.astype(BF), g)), (dka, dot(grad, q))):
            before = jnp.where(t == 0, jnp.zeros_like(term), sums[h, rk, :])
            sums[h, rk, :] = before + term
        acc = acc + dot(grad, kt, TN)
    acc = acc * SCALE

    @pl.when(jnp.logical_not(odd))
    def _():
        dqs[block, :] = acc

    @pl.when(odd)
    def _():
        grad = jnp.where(lane < HD, dqs[block, :], pltpu.roll(acc, HD, 1))
        grad = grad * cos_ref[block, :] - partner(grad) * sin_ref[block, :]
        pk_ref[block, columns(heads + h // 2)] = grad.astype(BF)

    @pl.when(odd & (t == 0))
    def _():
        keep(heads + h // 2).start()

    @pl.when(odd & (t > 0))
    def _():
        push_pack(heads + h // 2, n - 1 - t).start()

    @pl.when(t == n - 1)
    def _():
        dk = dka[h]
        dk = dk * cos_ref[...] - partner(dk) * sin_ref[...]
        both = jnp.where(lanes((total, 128)) < HD, dk, pltpu.roll(dva[h], HD, 1))
        pk_ref[:, columns(h)] = both.astype(BF)
        for step in range(n - 1):
            push_pack(h, step).start()
        keep(h).start()

    @pl.when(i == heads * n - 1)
    def _():
        for s in range(1, chips):
            pg_spread(s).wait_recv()
            pg_relay(s).start()
        for step in range(n - 1):
            push(step).wait_send()
        for s in range(1, chips):
            push_out(s).wait()
        og_swap().wait_send()
        pg_keep().wait()
        for s in range(chips):
            pg_relay(s).wait()
            if s:
                pg_spread(s).wait_send()
        for s in range(1, chips):
            og_push(s).wait_send()
        for step in range(n - 1):
            og_over(step).wait_send()
        for slot in range(heads + heads // 2):
            keep(slot).wait()
            for step in range(n - 1):
                push_pack(slot, step).wait()


def att_bwd(
    grad_attn, w_out, ctx_own, parts, pair_grads, q, k, v, ctx, lse, cosine, sine, n, bk=512
):
    heads, total, _ = q.shape
    width = heads * HD
    rows, depth = grad_attn.shape
    chips = parts.shape[0]
    share = width // (2 * chips)
    slots = heads + heads // 2
    hbm = pl.BlockSpec(memory_space=pl.ANY)

    def whole(*shape):
        return pl.BlockSpec(shape, lambda *_: (0,) * len(shape), pipeline_mode=pl.Buffered(1))

    return pl.pallas_call(
        functools.partial(att_bwd_kernel, n, bk, chips),
        out_shape=(
            jax.ShapeDtypeStruct((total, slots * 128), BF),
            jax.ShapeDtypeStruct((n, rows, slots * 128), BF),
            jax.ShapeDtypeStruct((chips - 1, rows, depth), BF),
            jax.ShapeDtypeStruct((share, depth), BF),
            jax.ShapeDtypeStruct((2 * chips, *pair_grads.shape), BF),
        ),
        grid_spec=pltpu.PrefetchScalarGridSpec(
            num_scalar_prefetch=0,
            grid=(heads * n,),
            in_specs=[whole(rows, depth), whole(n, width, depth)] + [hbm] * 10,
            out_specs=[whole(total, slots * 128), hbm, hbm, whole(share, depth), hbm],
            scratch_shapes=[pltpu.VMEM((heads, total, 128), BF)] * 3
            + [pltpu.VMEM((total, width), BF)]
            + [pltpu.VMEM((total, 128), F32)] * 3
            + [pltpu.VMEM((n, rows, width), BF)]
            + [
                pltpu.VMEM((total, width), BF),
                pltpu.VMEM((n - 1, rows, width), BF),
            ]
            + [pltpu.VMEM((heads, total, 128), F32)] * 2
            + [pltpu.VMEM((total, 128), F32)]
            + [
                pltpu.VMEM((width, depth), F32),
                pltpu.VMEM((chips, n, share, depth), F32),
                pltpu.VMEM((chips, n, share, depth), BF),
                pltpu.VMEM((chips, n, share, depth), BF),
                pltpu.VMEM((chips, n, share, depth), BF),
                pltpu.VMEM((n, share, depth), BF),
                pltpu.VMEM((n, share, depth), BF),
            ]
            + [pltpu.SemaphoreType.DMA((n - 1,))] * 2
            + [pltpu.SemaphoreType.DMA((chips - 1,))] * 2
            + [pltpu.SemaphoreType.DMA((slots, n - 1))] * 2
            + [pltpu.SemaphoreType.DMA((slots,))]
            + [pltpu.SemaphoreType.DMA] * 2
            + [pltpu.SemaphoreType.DMA((chips,))] * 2
            + [pltpu.SemaphoreType.DMA((n - 1,))] * 2
            + [pltpu.SemaphoreType.DMA((chips,))] * 4
            + [pltpu.SemaphoreType.DMA, pltpu.SemaphoreType.DMA((8,))],
        ),
        compiler_params=pltpu.CompilerParams(
            vmem_limit_bytes=60 << 20, collective_id=2, has_side_effects=True
        ),
        cost_estimate=pl.CostEstimate(
            flops=10 * total * total * 256 * heads,
            bytes_accessed=20 * total * width,
            transcendentals=total * total * heads,
        ),
        name="att_bwd",
    )(grad_attn, w_out, parts, pair_grads, q, k, v, ctx, lse, cosine, sine, ctx_own)


def finish_kernel(
    chips, n, x_ref, pk_ref, own_hbm, w_hbm, tokens_hbm, middle_hbm, gain_ref, vec_ref,
    input_ref, sums_ref, every,
    own_ref, w_ref, tokens_ref, middle_ref, full, mate, sib, land, fin, vec_z, vec_dp, vec_me,
    sx_send, sx_recv, rs_send, rs_recv, ag_send, ag_recv, rl_send, rl_recv,
    vz_send, vz_recv, vd_send, vd_recv, own_sem, load_sem,
):
    bits = chips.bit_length() - 1
    me = lax.axis_index("dp")
    place = lax.axis_index("tensor")
    core = lax.rem(me, 2)
    chip = me // 2
    other = 1 - core
    piece = fin.shape[0]

    def swap(s):
        return remote(mate.at[s], sib.at[s], sx_send.at[s], sx_recv.at[s], dp=chip * 2 + other)

    def push(s):
        return remote(sib.at[s], land.at[s], rs_send.at[s], rs_recv.at[s], dp=same_core(s, chips))

    def spread(s):
        return remote(
            fin, every.at[chip, core], ag_send.at[s], ag_recv.at[s], dp=same_core(s, chips)
        )

    def relay(s):
        src = every.at[differ(chip, s, bits), core]
        return remote(src, src, rl_send.at[s], rl_recv.at[s], dp=chip * 2 + other)

    def vec_over(step):
        return remote(
            vec_me.at[0], vec_z.at[place], vz_send.at[step], vz_recv.at[step], tensor=ring(n, step + 1)
        )

    def vec_across(step):
        return remote(
            vec_me.at[1], vec_dp.at[me], vd_send.at[step], vd_recv.at[step],
            dp=lax.rem(me + step + 1, 2 * chips),
        )

    far = (own_hbm, w_hbm, tokens_hbm, middle_hbm)
    near = (own_ref, w_ref, tokens_ref, middle_ref)
    loads = [pltpu.make_async_copy(a, b, load_sem.at[j]) for j, (a, b) in enumerate(zip(far, near))]
    for load in loads:
        load.start()
    barrier = pltpu.get_barrier_semaphore()
    for step in range(n - 1):
        pl.semaphore_signal(barrier, inc=1, device_id={"tensor": ring(n, step + 1)}, device_id_type=MESH)
    for step in range(2 * chips - 1):
        to = lax.rem(me + step + 1, 2 * chips)
        pl.semaphore_signal(barrier, inc=1, device_id={"dp": to}, device_id_type=MESH)

    full[...] = dot(x_ref[...], pk_ref[...], TN)
    pl.semaphore_wait(barrier, n + 2 * chips - 2)

    def part(s, which):
        start = (differ(chip, s, bits) * 2 + which) * piece
        return full[pl.ds(pl.multiple_of(start, piece), piece), :]

    for s in range(chips):
        mate[s] = part(s, other).astype(BF)
        swap(s).start()

    for load in loads:
        load.wait()
    grad = jnp.zeros(input_ref.shape, F32)
    for t in range(n):
        w = w_ref[:, t].reshape(w_ref.shape[0] * w_ref.shape[2], w_ref.shape[3])
        grad = grad + dot(own_ref[t], w, NT).astype(BF).astype(F32)

    for s in range(1, chips):
        swap(s).wait_recv()
        sib[s] = (sib[s].astype(F32) + part(s, core)).astype(BF)
        push(s).start()
    swap(0).wait_recv()
    total = sib[0].astype(F32) + part(0, core)

    values = tokens_ref[...].astype(F32)
    values = values - jnp.mean(values, axis=1, keepdims=True)
    inverse = lax.rsqrt(jnp.mean(values * values, axis=1, keepdims=True) + EPS)
    scaled = values * inverse
    through = grad * gain_ref[...]
    inner = through - jnp.mean(through, axis=1, keepdims=True)
    inner = inner - scaled * jnp.mean(through * scaled, axis=1, keepdims=True)
    input_ref[...] = middle_ref[...] + inverse * inner
    vec_me[0, 0:1] = jnp.sum(grad * scaled, axis=0, keepdims=True)
    vec_me[0, 1:2] = jnp.sum(grad, axis=0, keepdims=True)
    vec_me[0, 2:4] = vec_ref[...]
    vec_me[0, 4:8] = jnp.zeros((4, vec_ref.shape[1]), F32)
    vec_z[place] = vec_me[0]
    for step in range(n - 1):
        vec_over(step).start()

    for s in range(1, chips):
        push(s).wait_recv()
        total = total + land[s].astype(F32)
    fin[...] = total.astype(BF)
    for s in range(1, chips):
        spread(s).start()
    mine = pltpu.make_async_copy(fin, every.at[chip, core], own_sem)
    mine.start()
    mine.wait()
    relay(0).start()

    for step in range(n - 1):
        vec_over(step).wait()
    vec = vec_z[0]
    for t in range(1, n):
        vec = vec + vec_z[t]
    vec_me[1] = vec
    vec_dp[me] = vec
    for step in range(2 * chips - 1):
        vec_across(step).start()
    for s in range(1, chips):
        spread(s).wait_recv()
        relay(s).start()
    for step in range(2 * chips - 1):
        vec_across(step).wait()
    vec = vec_dp[0]
    for t in range(1, 2 * chips):
        vec = vec + vec_dp[t]
    sums_ref[...] = vec
    for s in range(chips):
        relay(s).wait()
        swap(s).wait_send()
        if s > 0:
            spread(s).wait_send()
            push(s).wait_send()


def finish(rows_all, packed, own, w_all, tokens, middle, gain, vec, devices):
    n, rows, packs = own.shape
    depth = tokens.shape[1]
    chips = devices // 2
    piece = depth // devices
    vmem = pl.BlockSpec(memory_space=pltpu.VMEM)
    return pl.pallas_call(
        functools.partial(finish_kernel, chips, n),
        out_shape=(
            jax.ShapeDtypeStruct((rows, depth), F32),
            jax.ShapeDtypeStruct((8, depth), F32),
            jax.ShapeDtypeStruct((chips, 2, piece, packs), BF),
        ),
        in_specs=[vmem] * 2 + [pl.BlockSpec(memory_space=pl.ANY)] * 4 + [vmem] * 2,
        out_specs=[vmem, vmem, pl.BlockSpec(memory_space=pl.ANY)],
        scratch_shapes=[
            pltpu.VMEM(own.shape, BF),
            pltpu.VMEM(w_all.shape, BF),
            pltpu.VMEM((rows, depth), BF),
            pltpu.VMEM((rows, depth), F32),
            pltpu.VMEM((depth, packs), F32),
            pltpu.VMEM((chips, piece, packs), BF),
            pltpu.VMEM((chips, piece, packs), BF),
            pltpu.VMEM((chips, piece, packs), BF),
            pltpu.VMEM((piece, packs), BF),
            pltpu.VMEM((n, 8, depth), F32),
            pltpu.VMEM((devices, 8, depth), F32),
            pltpu.VMEM((2, 8, depth), F32),
        ]
        + [pltpu.SemaphoreType.DMA((chips,))] * 8
        + [pltpu.SemaphoreType.DMA((n - 1,))] * 2
        + [pltpu.SemaphoreType.DMA((devices - 1,))] * 2
        + [pltpu.SemaphoreType.DMA, pltpu.SemaphoreType.DMA((4,))],
        compiler_params=pltpu.CompilerParams(
            vmem_limit_bytes=56 << 20, collective_id=4, has_side_effects=True
        ),
        cost_estimate=pl.CostEstimate(
            flops=4 * n * rows * depth * packs, bytes_accessed=20 << 20, transcendentals=0
        ),
        name="finish",
    )(rows_all, packed, own, w_all, tokens, middle, gain.reshape(1, depth), vec)


def ffn_kernel(
    chips, x_ref, gb_ref, w_ref, down_ref, wp_ref, dx_ref, out_ref, dw_ref, zs_ref, wp_z,
    rows_all, gb, hid, gate_g, up_g, own, sib, mate, partial, z_left, z_right, wd,
    ag_send, ag_recv, rl_send, rl_recv, sx_send, sx_recv, rs_send, rs_recv, fw_send, fw_recv,
    gb_sem, out_sem, dx_sem, wp_send, wp_recv, wp_sem, zr_send, zr_recv, zl_send, zl_recv,
    dr_send, dr_recv, dl_send, dl_recv, wd_sem,
):
    bits = chips.bit_length() - 1
    me = lax.axis_index("dp")
    core = lax.rem(me, 2)
    chip = me // 2
    other = 1 - core
    rows, depth = x_ref.shape
    n, share, _ = dw_ref.shape

    def spread(s):
        to = differ(chip, s, bits) * 2 + core
        return remote(x_ref, rows_all.at[chip, core], ag_send.at[s], ag_recv.at[s], dp=to)

    square = chips == 4

    def hand_on(s):
        half = pl.ds((s - 1) * (rows // 2), rows // 2)
        part = rows_all.at[differ(chip, s, bits), core, half]
        to = differ(chip, 3 - s, bits) * 2 + core
        return remote(part, part, fw_send.at[s], fw_recv.at[s], dp=to)

    def handed(s):
        half = pl.ds((s - 1) * (rows // 2), rows // 2)
        part = rows_all.at[differ(chip, 3, bits), core, half]
        to = differ(chip, 3 - s, bits) * 2 + core
        return remote(part, part, fw_send.at[s], fw_recv.at[s], dp=to)

    def relay(s):
        src = differ(chip, s, bits)
        return remote(
            rows_all.at[src, core], rows_all.at[src, core], rl_send.at[s], rl_recv.at[s],
            dp=chip * 2 + other,
        )

    def swap(s):
        return remote(
            mate.at[lax.rem(s, 2)], sib.at[s], sx_send.at[s], sx_recv.at[s], dp=chip * 2 + other
        )

    def push(s):
        to = differ(chip, s, bits) * 2 + core
        return remote(sib.at[s, 0], dx_ref.at[s], rs_send.at[s], rs_recv.at[s], dp=to)

    def fetch(s):
        src = differ(chip, s, bits)
        return pltpu.make_async_copy(gb_ref.at[src], gb.at[src], gb_sem.at[s])

    part = lax.axis_index("tensor")

    def over(step):
        return remote(
            wp_ref, wp_z.at[part], wp_send.at[step], wp_recv.at[step], tensor=ring(n, step + 1)
        )

    def keep(s):
        return pltpu.make_async_copy(sib.at[s, 1], out_ref.at[s], out_sem.at[s])

    ours = pl.ds(pl.multiple_of(me * share, share), share)
    cut = pltpu.make_async_copy(down_ref.at[ours], wd.at[part], wd_sem)
    cut.start()
    for s in range(chips):
        fetch(s).start()
    barrier = pltpu.get_barrier_semaphore()
    for step in range(1, n):
        pl.semaphore_signal(barrier, inc=1, device_id={"tensor": ring(n, step)}, device_id_type=MESH)
    pl.semaphore_signal(barrier, inc=1, device_id={"dp": chip * 2 + other}, device_id_type=MESH)
    for s in range(1, chips):
        to = differ(chip, s, bits) * 2 + core
        pl.semaphore_signal(barrier, inc=1, device_id={"dp": to}, device_id_type=MESH)
    pl.semaphore_wait(barrier, chips + n - 1)
    direct = range(1, 3) if square else range(1, chips)
    for s in direct:
        spread(s).start()
    mine = pltpu.make_async_copy(x_ref, rows_all.at[chip, core], ag_send.at[0])
    mine.start()
    mine.wait()
    relay(0).start()
    keep_wp = pltpu.make_async_copy(wp_ref, wp_z.at[part], wp_sem)
    keep_wp.start()

    def d_right(d):
        there = wd.at[part - d]
        return remote(there, there, dr_send.at[d], dr_recv.at[d], tensor=part + 1)

    def d_left(d):
        there = wd.at[part + d]
        return remote(there, there, dl_send.at[d], dl_recv.at[d], tensor=part - 1)

    def d_from_left(d):
        there = wd.at[part - d]
        return remote(there, there, dr_send.at[d - 1], dr_recv.at[d - 1], tensor=part - 1)

    def d_from_right(d):
        there = wd.at[part + d]
        return remote(there, there, dl_send.at[d - 1], dl_recv.at[d - 1], tensor=part + 1)

    cut.wait()
    for d in range(n):
        if d:

            @pl.when(part >= d)
            def _():
                d_from_left(d).wait_recv()

        if d < n - 1:

            @pl.when((part >= d) & (part < n - 1))
            def _():
                d_right(d).start()

        if d:

            @pl.when(part + d < n)
            def _():
                d_from_right(d).wait_recv()

        if d < n - 1:

            @pl.when((part + d < n) & (part > 0))
            def _():
                d_left(d).start()

    for step in range(n - 1):
        over(step).start()

    def shard(src, which, put):
        x = rows_all[src, which]
        grad = gb[src, which]
        gate = dot(x, w_ref[0], NT)
        upper = dot(x, w_ref[1], NT)
        w_down = wd[...].reshape(n * share, depth)
        grad_hidden = dot(grad, w_down, NT)
        sigma = jax.nn.sigmoid(gate)
        act = gate * sigma
        hidden = (act * upper).astype(BF)
        grad_gate = (grad_hidden * upper * sigma * (1.0 + gate * (1.0 - sigma))).astype(BF)
        grad_upper = (grad_hidden * act).astype(BF)
        hid[src, which] = hidden
        gate_g[src, which] = grad_gate
        up_g[src, which] = grad_upper
        put[0] = (dot(grad_gate, w_ref[0]) + dot(grad_upper, w_ref[1])).astype(BF)
        put[1] = dot(hidden, w_down).astype(BF)

    def step(s, carry):
        src = differ(chip, s, bits)
        slot = lax.rem(s, 2)
        relay(s).wait_recv()
        fetch(s).wait()

        @pl.when(s >= 2)
        def _():
            swap(s - 2).wait_send()

        shard(src, other, mate.at[slot])
        swap(s).start()
        shard(src, core, own)
        swap(s).wait_recv()
        for k in range(2):
            sib[s, k] = (sib[s, k].astype(F32) + own[k].astype(F32)).astype(BF)

        @pl.when(s > 0)
        def _():
            push(s).start()

        keep(s).start()

        if square:

            @pl.when(s == 0)
            def _():
                for near in (1, 2):
                    spread(near).wait_recv()
                    hand_on(near).start()
                    relay(near).start()

        else:

            @pl.when(s < chips - 1)
            def _():
                spread(s + 1).wait_recv()
                relay(s + 1).start()

        if square:

            @pl.when(s == 1)
            def _():
                handed(1).wait_recv()
                handed(2).wait_recv()
                relay(3).start()

        return carry

    lax.fori_loop(0, chips, step, 0)
    first = pltpu.make_async_copy(sib.at[0, 0], dx_ref.at[0], dx_sem)
    first.start()
    def zr(t, k, to):
        return remote(
            partial.at[t, k], z_left.at[t, k], zr_send.at[t, k], zr_recv.at[t, k], tensor=to
        )

    def zl(t, k, to):
        return remote(
            partial.at[t, k], z_right.at[t, k], zl_send.at[t, k], zl_recv.at[t, k], tensor=to
        )

    def join(t, k, more):
        partial[t, k] = (partial[t, k].astype(F32) + more[t, k].astype(F32)).astype(BF)

    def weight_grad(left, right):
        left = left[...].reshape(-1, n * share)
        return dot(left, right[...].reshape(-1, depth), TN)

    def hand_along(k):
        for j in range(n - 1):
            t = n - 1 - j

            @pl.when((part > 0) & (part < t))
            def _():
                zr(t, k, part + 1).wait_recv()
                join(t, k, z_left)
                zr(t, k, part + 1).start()

            @pl.when((part < n - 1) & (part > j))
            def _():
                zl(j, k, part - 1).wait_recv()
                join(j, k, z_right)
                zl(j, k, part - 1).start()

    for k, left in enumerate((gate_g, up_g)):
        grad = weight_grad(left, rows_all)
        for t in range(n):
            partial[t, k] = grad[t * share : (t + 1) * share, :].astype(BF)

        for j in range(n - 1):

            @pl.when(part == 0)
            def _():
                zr(n - 1 - j, k, 1).start()

            @pl.when(part == n - 1)
            def _():
                zl(j, k, n - 2).start()

    hand_along(0)
    grad = weight_grad(hid, gb)
    for t in range(n):
        dw_ref[t] = grad[t * share : (t + 1) * share, :].astype(BF)
    hand_along(1)
    for k in range(2):
        for t in range(n):

            @pl.when((part == t) & (part > 0))
            def _():
                zr(t, k, part - 1).wait_recv()
                join(t, k, z_left)

            @pl.when((part == t) & (part < n - 1))
            def _():
                zl(t, k, part + 1).wait_recv()
                join(t, k, z_right)

            @pl.when(part == t)
            def _():
                zs_ref[k] = partial[t, k]

            @pl.when(part < t)
            def _():
                zr(t, k, part + 1).wait_send()

            @pl.when(part > t)
            def _():
                zl(t, k, part - 1).wait_send()

    for d in range(n - 1):

        @pl.when((part >= d) & (part < n - 1))
        def _():
            d_right(d).wait_send()

        @pl.when((part + d < n) & (part > 0))
        def _():
            d_left(d).wait_send()

    first.wait()
    keep_wp.wait()
    for step in range(n - 1):
        over(step).wait()
    for s in range(chips):
        keep(s).wait()
        relay(s).wait_send()
        if s >= chips - 2:
            swap(s).wait_send()
        if s in direct:
            spread(s).wait_send()
        if s > 0:
            push(s).wait()
    if square:
        hand_on(1).wait_send()
        hand_on(2).wait_send()


def ffn(x, grad_branch, weights, down, w_packed, n, devices):
    rows, depth = x.shape
    chips = devices // 2
    hidden = weights.shape[1]
    share = hidden // n
    vmem = pl.BlockSpec(memory_space=pltpu.VMEM)
    hbm = pl.BlockSpec(memory_space=pl.ANY)
    return pl.pallas_call(
        functools.partial(ffn_kernel, chips),
        out_shape=(
            jax.ShapeDtypeStruct((chips, rows, depth), BF),
            jax.ShapeDtypeStruct((chips, rows, depth), BF),
            jax.ShapeDtypeStruct((n, share, depth), BF),
            jax.ShapeDtypeStruct((2, share, depth), BF),
            jax.ShapeDtypeStruct((n, *w_packed.shape), BF),
        ),
        in_specs=[vmem, hbm, vmem, hbm, hbm],
        out_specs=[hbm, hbm, vmem, vmem, hbm],
        scratch_shapes=[
            pltpu.VMEM((chips, 2, rows, depth), BF),
            pltpu.VMEM((chips, 2, rows, depth), BF),
        ]
        + [pltpu.VMEM((chips, 2, rows, hidden), BF)] * 3
        + [
            pltpu.VMEM((2, rows, depth), BF),
            pltpu.VMEM((chips, 2, rows, depth), BF),
            pltpu.VMEM((2, 2, rows, depth), BF),
        ]
        + [pltpu.VMEM((n, 2, share, depth), BF)] * 3
        + [pltpu.VMEM((n, share, depth), BF)]
        + [pltpu.SemaphoreType.DMA((chips,))] * 8
        + [pltpu.SemaphoreType.DMA((3,))] * 2
        + [pltpu.SemaphoreType.DMA((chips,))] * 2
        + [pltpu.SemaphoreType.DMA]
        + [pltpu.SemaphoreType.DMA((n - 1,))] * 2
        + [pltpu.SemaphoreType.DMA]
        + [pltpu.SemaphoreType.DMA((n, 2))] * 4
        + [pltpu.SemaphoreType.DMA((n - 1,))] * 4
        + [pltpu.SemaphoreType.DMA],
        compiler_params=pltpu.CompilerParams(
            vmem_limit_bytes=62 << 20, collective_id=3, has_side_effects=True
        ),
        cost_estimate=pl.CostEstimate(
            flops=2 * 9 * devices * rows * depth * hidden, bytes_accessed=30 << 20, transcendentals=0
        ),
        name="ffn",
    )(x, grad_branch, weights, down, w_packed)


def unpack_kernel(
    share, pair_ref, rest_ref, pack_ref, gate_ref, up_ref, down_ref, out_ref, q_ref, k_ref, v_ref
):
    gate_ref[...] = pair_ref[0, 0].astype(F32).T
    up_ref[...] = pair_ref[0, 1].astype(F32).T
    rest = rest_ref[0].astype(F32)
    down_ref[...] = rest[:share]
    out_ref[...] = rest[share:]
    pack = pack_ref[0].astype(F32)
    pairs = q_ref.shape[1] // 128
    first = lanes((pack.shape[0], 128)) < HD
    for p in range(pairs):
        even = pack[:, p * 256 : p * 256 + 128]
        odd = pack[:, p * 256 + 128 : p * 256 + 256]
        out = slice(p * 128, p * 128 + 128)
        q_ref[:, out] = pack[:, (2 * pairs + p) * 128 : (2 * pairs + p + 1) * 128]
        k_ref[:, out] = jnp.where(first, even, pltpu.roll(odd, HD, 1))
        v_ref[:, out] = jnp.where(first, pltpu.roll(even, HD, 1), odd)


def unpack(pair, rest, pack):
    devices, _, share, depth = pair.shape
    hidden = devices * share
    height = rest.shape[1]
    width = devices * (height - share)
    piece = depth // devices
    if share % 128:
        down = rest[:, :share].reshape(hidden, depth).astype(F32)
        gate, up = (pair[:, k].reshape(hidden, depth).astype(F32).T for k in range(2))
        pack = pack.reshape(depth, 3 * width).astype(F32)
        both = pack[:, : 2 * width].reshape(depth, width // HD, 2, HD)
        key, value = (both[:, :, k].reshape(depth, width) for k in range(2))
        out = rest[:, share:].reshape(width, depth).astype(F32)
        return gate, up, down, out, pack[:, 2 * width :], key, value
    column = pl.BlockSpec((depth, share), lambda i: (0, i))
    rows = pl.BlockSpec((piece, width), lambda i: (i, 0))
    return pl.pallas_call(
        functools.partial(unpack_kernel, share),
        out_shape=(jax.ShapeDtypeStruct((depth, hidden), F32),) * 2
        + (
            jax.ShapeDtypeStruct((hidden, depth), F32),
            jax.ShapeDtypeStruct((width, depth), F32),
        )
        + (jax.ShapeDtypeStruct((depth, width), F32),) * 3,
        grid=(devices,),
        in_specs=[
            pl.BlockSpec((1, 2, share, depth), lambda i: (i, 0, 0, 0)),
            pl.BlockSpec((1, height, depth), lambda i: (i, 0, 0)),
            pl.BlockSpec((1, piece, 3 * width), lambda i: (i, 0, 0)),
        ],
        out_specs=[
            column, column, pl.BlockSpec((share, depth), lambda i: (i, 0)),
            pl.BlockSpec((height - share, depth), lambda i: (i, 0)), rows, rows, rows,
        ],
        compiler_params=pltpu.CompilerParams(vmem_limit_bytes=62 << 20),
        name="unpack",
    )(pair, rest, pack)


def norm_parts(values):
    centre = jnp.mean(values, axis=-1, keepdims=True)
    centred = values - centre
    inverse = lax.rsqrt(jnp.mean(centred * centred, axis=-1, keepdims=True) + EPS)
    return centred * inverse, inverse


def norm_back(upstream, scaled, inverse, gain):
    through = upstream * gain
    inner = (
        through
        - jnp.mean(through, axis=-1, keepdims=True)
        - scaled * jnp.mean(through * scaled, axis=-1, keepdims=True)
    )
    return inverse * inner, jnp.sum(upstream * scaled, axis=0), jnp.sum(upstream, axis=0)


def on_device(
    tokens, lengths, ln1_gain, ln1_bias, w_query, w_key, w_value, w_out,
    ln2_gain, ln2_bias, w_gate, w_up, down_weight, cotangent,
):
    n = lax.axis_size("tensor")
    local_rows, depth = tokens.shape
    length = local_rows * n
    width = w_query.shape[1]
    row_ids = lax.axis_index("tensor") * local_rows + lax.iota(jnp.int32, local_rows)
    valid = (row_ids < lengths[0])[:, None]

    inputs = tokens.astype(F32)
    grad_out = jnp.where(valid, cotangent.astype(F32), 0.0)
    devices = lax.axis_size("dp")
    place = lax.axis_index("dp")
    share = w_gate.shape[1] // devices

    (
        context, logsum, w_packed, q, k, v, cosine, sine, attn_rows, grad_branch, weights, context_own, _,
        w_out_all,
    ) = front(
        tokens, cotangent, ln1_gain, ln1_bias, angle_tables(length), w_query, w_key, w_value,
        w_gate, w_up, w_out, lengths, n, devices,
    )
    attn_rows = attn_rows.reshape(length, depth)
    weights = weights.reshape(2, n * share, depth)

    w_out_all = w_out_all.reshape(n, width, depth)
    attn_out = sum(dot(context_own[t], w_out_all[t]).astype(BF).astype(F32) for t in range(n))
    middle = inputs + attn_out
    scaled2, inverse2 = norm_parts(middle)
    ffn_in = (scaled2 * ln2_gain + ln2_bias).astype(BF)
    grad_parts, out_parts, down_grad, pair_grads, w_packed = ffn(
        ffn_in, grad_branch, weights, down_weight, w_packed, n, devices
    )
    grad_ffn_in = sum(grad_parts[p].astype(F32) for p in range(devices // 2))
    grad_norm2, gain2_grad, shift2_grad = norm_back(
        grad_ffn_in, scaled2, inverse2, ln2_gain
    )
    grad_middle = grad_out + grad_norm2
    grad_attn = grad_middle.astype(BF)
    w_packed = lax.all_gather(w_packed, "dp", axis=0)
    down_grad = lax.psum_scatter(down_grad, "tensor", scatter_dimension=0, tiled=True)[0]
    packed, packed_own, out_sums, out_piece, pair_grads = att_bwd(
        grad_attn, w_out_all, context_own, out_parts, pair_grads, q, k, v, context, logsum, cosine, sine, n
    )
    down_grad, out_piece, w_packed = lax.optimization_barrier((down_grad, out_piece, w_packed))
    grads = lax.all_gather(jnp.concatenate([down_grad, out_piece]), "dp", axis=0)
    ffn_out = sum(x.astype(F32) for x in (out_parts[0], *out_sums))
    output = jnp.where(valid, middle + ffn_out, 0.0).astype(BF)
    input_grad, sums, packed_grads = finish(
        attn_rows, packed, packed_own, w_packed, tokens, grad_middle, ln1_gain,
        jnp.stack([gain2_grad, shift2_grad]), devices,
    )
    packed_grads = packed_grads.reshape(devices, depth // devices, 3 * width)
    gate_grad, up_grad, down_grad, out_grad, query_grad, key_grad, value_grad = unpack(
        pair_grads, grads, packed_grads
    )
    gain1_grad, shift1_grad, gain2_grad, shift2_grad = (sums[i] for i in range(4))
    return (
        output, input_grad, gain1_grad, shift1_grad, query_grad, key_grad, value_grad, out_grad,
        gain2_grad, shift2_grad, gate_grad, up_grad, down_grad,
    )


def solution(mesh):
    rows = P(("dp", "tensor"), None)
    columns = P(None, "tensor")
    parts = P("tensor", None)
    return jax.shard_map(
        on_device,
        mesh=mesh,
        in_specs=(
            rows, P("dp"), P(), P(), columns, columns, columns, parts,
            P(), P(), columns, columns, parts, rows,
        ),
        out_specs=(
            rows, rows, P(), P(), columns, columns, columns, parts,
            P(), P(), columns, columns, parts,
        ),
        check_vma=False,
    )
```

```python
import functools
import math

import jax
import jax.numpy as jnp
from jax import lax
from jax.experimental import pallas as pl
from jax.experimental.pallas import tpu as pltpu
from jax.sharding import PartitionSpec as P

HD = 64
EPS = 1e-05
SCALE = 1.0 / math.sqrt(HD)
F32 = jnp.float32
BF = jnp.bfloat16
NT = (((1,), (1,)), ((), ()))
NN = (((1,), (0,)), ((), ()))
TN = (((0,), (0,)), ((), ()))
MESH = pl.DeviceIdType.MESH


def dot(a, b, dims=NN):
    return lax.dot_general(a, b, dims, preferred_element_type=F32)


def lanes(shape):
    return lax.broadcasted_iota(jnp.int32, shape, 1)


def split3(x):
    hi = x.astype(BF).astype(F32)
    mid = (x - hi).astype(BF).astype(F32)
    return hi, mid, x - hi - mid


def partner(x):
    width = x.shape[1]
    first = lanes(x.shape) % HD < HD // 2
    return jnp.where(first, pltpu.roll(x, width - HD // 2, 1), pltpu.roll(x, HD // 2, 1))


STEP = 64


def angle_tables(length):
    half = HD // 2
    lane = lax.optimization_barrier(lax.iota(jnp.int32, 2 * HD))
    freqs = 10000.0 ** (-((lane % half).astype(F32) * 2.0 / HD))
    sign = jnp.where(lane % HD < half, -1.0, 1.0)

    def table(positions):
        angles = positions[:, None] * freqs[None, :]
        return jnp.stack([jnp.cos(angles), jnp.sin(angles)])

    return table(lax.iota(F32, length // STEP) * STEP), table(lax.iota(F32, STEP)), sign[None, :]


def differ(a, b, bits):
    return sum(lax.rem(a // (1 << k) + b // (1 << k), 2) * (1 << k) for k in range(bits))


def remote(src, dst, send, recv, **to):
    return pltpu.make_async_remote_copy(
        src_ref=src, dst_ref=dst, send_sem=send, recv_sem=recv, device_id=to, device_id_type=MESH
    )


def ring(n, step):
    return lax.rem(lax.axis_index("tensor") + step, n)


def same_core(s, chips):
    me = lax.axis_index("dp")
    return differ(me // 2, s, chips.bit_length() - 1) * 2 + lax.rem(me, 2)


def sibling():
    me = lax.axis_index("dp")
    return me + 1 - 2 * lax.rem(me, 2)


def greet(n, chips, both_cores=False):
    barrier = pltpu.get_barrier_semaphore()
    if both_cores:
        pl.semaphore_signal(barrier, inc=1, device_id={"dp": sibling()}, device_id_type=MESH)
    for step in range(1, n):
        pl.semaphore_signal(barrier, inc=1, device_id={"tensor": ring(n, step)}, device_id_type=MESH)
    for s in range(1, chips):
        pl.semaphore_signal(
            barrier, inc=1, device_id={"dp": same_core(s, chips)}, device_id_type=MESH
        )
    pl.semaphore_wait(barrier, n + chips - 2 + both_cores)


def front_kernel(
    n, chips, chunks, limit_ref, tokens_ref, ct_ref, gain_ref, shift_ref, coarse_ref, fine_ref, sign_ref,
    wq_ref, wk_ref, wv_ref, gate_ref, up_ref, wo_ref,
    ctx_ref, lse_ref, wp_ref, q_out, k_out, v_out, cos_out, sin_out, rows_ref, gb_all, w_all, out_ref, wo_z, wo_all,
    landed, gb, columns, own_w, wqkv, q_ref, k_ref, v_ref, cos_ref, sin_ref,
    right_send, right_recv, left_send, left_recv, gs_send, gs_recv, gr_send, gr_recv, rows_sem,
    wr_send, wr_recv, wl_send, wl_recv, send_sem, recv_sem, wz_send, wz_recv, ws_send, ws_recv,
    wx_send, wx_recv, cut_sem, load_sem, save_sem, keep_sem,
):
    i = pl.program_id(0)
    steps = pl.num_programs(0)
    me = lax.axis_index("tensor")
    place = lax.axis_index("dp")
    core = lax.rem(place, 2)
    bits = chips.bit_length() - 1
    rows, depth = tokens_ref.shape
    heads = q_ref.shape[0]
    piece = rows // chunks
    limit = limit_ref[0]
    s = i // heads
    h = lax.rem(i, heads)

    def over(shard, d, c, send, recv, to):
        part = landed.at[shard, pl.ds(c * piece, piece)]
        return remote(part, part, send.at[d, c], recv.at[d, c], tensor=to)

    def rightward(d, c):
        return over(me - d, d, c, right_send, right_recv, me + 1)

    def leftward(d, c):
        return over(me + d, d, c, left_send, left_recv, me - 1)

    def from_left(d, c):
        return over(me - d, d - 1, c, right_send, right_recv, me - 1)

    def from_right(d, c):
        return over(me + d, d - 1, c, left_send, left_recv, me + 1)

    def weights(shard, d, k, send, recv, to):
        there = w_all.at[k, shard]
        return remote(there if d else own_w.at[k], there, send.at[d, k], recv.at[d, k], tensor=to)

    def w_right(d, k):
        return weights(me - d, d, k, wr_send, wr_recv, me + 1)

    def w_left(d, k):
        return weights(me + d, d, k, wl_send, wl_recv, me - 1)

    def w_from_left(d, k):
        return weights(me - d, d - 1, k, wr_send, wr_recv, me - 1)

    def w_from_right(d, k):
        return weights(me + d, d - 1, k, wl_send, wl_recv, me + 1)

    def spread_gb(c):
        return remote(
            gb, gb_all.at[place // 2, core], gs_send.at[c], gs_recv.at[c], dp=same_core(c, chips)
        )

    def relay_gb(c):
        there = gb_all.at[differ(place // 2, c, bits), core]
        return remote(there if c else gb, there, gr_send.at[c], gr_recv.at[c], dp=sibling())

    def wo_over(step):
        return remote(
            wo_ref, wo_z.at[me], wz_send.at[step], wz_recv.at[step], tensor=ring(n, step + 1)
        )

    def spread_wo(c):
        return remote(
            wo_z, wo_all.at[:, place], ws_send.at[c], ws_recv.at[c], dp=same_core(c, chips)
        )

    def relay_wo(c):
        there = wo_all.at[:, differ(place // 2, c, bits) * 2 + core]
        return remote(there if c else wo_z, there, wx_send.at[c], wx_recv.at[c], dp=sibling())

    def push(step):
        owner = ring(n, step + 1)
        return remote(
            ctx_ref.at[pl.ds(pl.multiple_of(owner * rows, rows), rows)], out_ref.at[me],
            send_sem.at[step], recv_sem.at[step], tensor=owner,
        )

    def save(shard):
        return pltpu.make_async_copy(landed.at[shard], rows_ref.at[shard], rows_sem.at[shard])

    mine = pl.ds(pl.multiple_of(me * rows, rows), rows)
    keeps = [
        pltpu.make_async_copy(gb, gb_all.at[place // 2, core], keep_sem.at[0]),
        pltpu.make_async_copy(wo_ref, wo_z.at[me], keep_sem.at[1]),
        pltpu.make_async_copy(wo_z, wo_all.at[:, place], keep_sem.at[2]),
        pltpu.make_async_copy(ctx_ref.at[mine], out_ref.at[me], keep_sem.at[3]),
        pltpu.make_async_copy(own_w, w_all.at[:, me], keep_sem.at[4]),
    ]
    saves = [
        pltpu.make_async_copy(a, b, save_sem.at[j])
        for j, (a, b) in enumerate(
            ((q_ref, q_out), (k_ref, k_out), (v_ref, v_out), (cos_ref, cos_out), (sin_ref, sin_out))
        )
    ]

    @pl.when(i == 0)
    def _():
        loads = [
            pltpu.make_async_copy(ref, wqkv.at[j], load_sem.at[j])
            for j, ref in enumerate((wq_ref, wk_ref, wv_ref))
        ]
        share = own_w.shape[1]
        ours = pl.ds(pl.multiple_of(place * share, share), share)
        cuts = []
        for k, ref in enumerate((gate_ref, up_ref)):
            src = ref if share % 128 else ref.at[:, ours]
            cuts.append(pltpu.make_async_copy(src, columns.at[k], cut_sem.at[k]))
        for copy in loads + cuts:
            copy.start()

        barrier = pltpu.get_barrier_semaphore()
        for step in range(1, n):
            to = ring(n, step)
            pl.semaphore_signal(barrier, inc=1, device_id={"tensor": to}, device_id_type=MESH)
        pl.semaphore_signal(barrier, inc=1, device_id={"dp": sibling()}, device_id_type=MESH)
        for c in range(1, chips):
            to = same_core(c, chips)
            pl.semaphore_signal(barrier, inc=1, device_id={"dp": to}, device_id_type=MESH)

        values = tokens_ref[...].astype(F32)
        values = values - jnp.mean(values, axis=1, keepdims=True)
        inverse = lax.rsqrt(jnp.mean(values * values, axis=1, keepdims=True) + EPS)
        landed[me] = (values * inverse * gain_ref[...] + shift_ref[...]).astype(BF)

        pl.semaphore_wait(barrier, n - 1 + chips)

        for c in range(chunks):

            @pl.when(me < n - 1)
            def _():
                rightward(0, c).start()

            @pl.when(me > 0)
            def _():
                leftward(0, c).start()

        row = me * rows + lax.broadcasted_iota(jnp.int32, (rows, depth), 0)
        gb[...] = jnp.where(row < limit, ct_ref[...].astype(F32), 0.0).astype(BF)
        for c in range(1, chips):
            spread_gb(c).start()
        relay_gb(0).start()
        keeps[0].start()
        keeps[1].start()
        for copy in loads:
            copy.wait()

        cut = wp_ref.shape[0]
        here = pl.ds(pl.multiple_of(place * cut, cut), cut)
        first = lanes((cut, 128)) < HD
        for p in range(heads // 2):
            at = slice(p * 128, p * 128 + 128)
            query, key, value = (wqkv[j, here, at].astype(F32) for j in range(3))
            even = jnp.where(first, key, pltpu.roll(value, HD, 1))
            odd = jnp.where(first, pltpu.roll(key, HD, 1), value)
            for slot, values in ((2 * p, even), (2 * p + 1, odd), (heads + p, query)):
                wp_ref[:, slot * 128 : slot * 128 + 128] = values.astype(BF)

        lane = lanes((rows, 128))
        ones = jnp.where(lane < HD + 3, 1.0, 0.0)
        unit = jnp.where(lane == HD + 3, 1.0, 0.0)

        def put(out, here, values, extra):
            for head in range(heads):
                own = values[:, head // 2 * 128 : head // 2 * 128 + 128]
                own = pltpu.roll(own, HD, 1) if head % 2 else own
                out[head, here, :] = jnp.where(lane < HD, own, extra).astype(BF)

        def project(shard):
            here = pl.ds(pl.multiple_of(shard * rows, rows), rows)
            for j in range(rows // STEP):
                part = pl.ds(pl.multiple_of(shard * rows + j * STEP, STEP), STEP)
                coarse = pl.ds(shard * (rows // STEP) + j, 1)
                c0, s0 = coarse_ref[0, coarse, :], coarse_ref[1, coarse, :]
                cos_ref[part, :] = c0 * fine_ref[0] - s0 * fine_ref[1]
                sin_ref[part, :] = (s0 * fine_ref[0] + c0 * fine_ref[1]) * sign_ref[...]
            cosine = jnp.tile(cos_ref[here, :], (1, heads // 2))
            sine = jnp.tile(sin_ref[here, :], (1, heads // 2))
            x = landed[shard]
            row = shard * rows + lax.broadcasted_iota(jnp.int32, (rows, 128), 0)
            bias = jnp.where(lane == HD + 3, jnp.where(row < limit, 0.0, -1e30), ones)
            raw = dot(x, wqkv[0])
            turned = (raw * cosine + partner(raw) * sine).astype(BF).astype(F32)
            put(q_ref, here, turned * SCALE, unit)
            raw = dot(x, wqkv[1])
            put(k_ref, here, raw * cosine + partner(raw) * sine, bias)
            put(v_ref, here, dot(x, wqkv[2]), ones)

        for d in range(1, n + 1):
            for c in range(chunks):
                if d < n:

                    @pl.when(me >= d)
                    def _():
                        from_left(d, c).wait_recv()

                    @pl.when((me >= d) & (me < n - 1))
                    def _():
                        rightward(d, c).start()

                    @pl.when(me + d < n)
                    def _():
                        from_right(d, c).wait_recv()

                    @pl.when((me + d < n) & (me > 0))
                    def _():
                        leftward(d, c).start()

                if c == 0:

                    @pl.when(me >= d - 1)
                    def _():
                        save(me - d + 1).start()
                        project(me - d + 1)

                if c == 1 and d > 1:

                    @pl.when(me + d - 1 < n)
                    def _():
                        save(me + d - 1).start()
                        project(me + d - 1)

                if c == 2 and d == 1:
                    for cut in cuts:
                        cut.wait()
                    for k in range(2):
                        own_w[k] = columns[k].astype(F32).T.astype(BF)
                    keeps[4].start()

                if c == chunks - 1 and d == 2:
                    for near in range(1, chips // 2 + 1):
                        spread_gb(near).wait_recv()
                        relay_gb(near).start()

            if d < n:

                @pl.when((me < n - 1) & (me + 1 == d))
                def _():
                    for k in range(2):
                        w_right(0, k).start()

                @pl.when((me > 0) & (n - me == d))
                def _():
                    for k in range(2):
                        w_left(0, k).start()

        for copy in saves:
            copy.start()
        for step in range(n - 1):
            wo_over(step).start()
        for far in range(chips // 2 + 1, chips):
            spread_gb(far).wait_recv()
            relay_gb(far).start()

    stride = max((heads * n - 2) // max(n - 2, 1), 1)
    for d in range(1, n - 1):

        @pl.when(i == 1 + (d - 1) * stride)
        def _():
            for k in range(2):

                @pl.when((me >= d) & (me < n - 1))
                def _():
                    w_from_left(d, k).wait_recv()
                    w_right(d, k).start()

                @pl.when((me + d < n) & (me > 0))
                def _():
                    w_from_right(d, k).wait_recv()
                    w_left(d, k).start()

    @pl.when(i == heads)
    def _():
        for step in range(n - 1):
            wo_over(step).wait()
        keeps[1].wait()
        for c in range(1, chips):
            spread_wo(c).start()
        relay_wo(0).start()
        keeps[2].start()

    @pl.when(i == (n - 1) * heads)
    def _():
        for c in range(1, chips):
            spread_wo(c).wait_recv()
            relay_wo(c).start()

    owner = ring(n, s + 1)
    block = pl.ds(pl.multiple_of(owner * rows, rows), rows)
    scores = dot(q_ref[h, block, :], k_ref[h], NT)
    peak = jnp.max(scores, axis=1, keepdims=True)
    acc = dot(jnp.exp(scores - peak).astype(BF), v_ref[h])
    lane = lanes((rows, 128))
    total = jnp.sum(jnp.where(lane == HD, acc, 0.0), axis=1, keepdims=True)
    out = acc * (1.0 / total)
    odd = lax.rem(h, 2)
    out = jnp.where(odd == 1, pltpu.roll(out, HD, 1), out).astype(BF)
    pair = pl.ds(pl.multiple_of(h // 2 * 128, 128), 128)
    ctx_ref[block, pair] = jnp.where((lane >= HD) == (odd == 1), out, ctx_ref[block, pair])
    lse_ref[block, :] = jnp.where(lane == h, peak + jnp.log(total), lse_ref[block, :])

    @pl.when((h == heads - 1) & (s < n - 1))
    def _():
        push(s).start()

    @pl.when(i == steps - 1)
    def _():
        keeps[3].start()
        for d in range(n - 1):
            for c in range(chunks):

                @pl.when((me >= d) & (me < n - 1))
                def _():
                    rightward(d, c).wait_send()

                @pl.when((me + d < n) & (me > 0))
                def _():
                    leftward(d, c).wait_send()

            for k in range(2):

                @pl.when((me >= d) & (me < n - 1))
                def _():
                    w_right(d, k).wait_send()

                @pl.when((me + d < n) & (me > 0))
                def _():
                    w_left(d, k).wait_send()

        for k in range(2):
            for d in range(1, n):

                @pl.when((me >= d) & ((me == n - 1) | (d == n - 1)))
                def _():
                    w_from_left(d, k).wait_recv()

                @pl.when((me + d < n) & ((me == 0) | (d == n - 1)))
                def _():
                    w_from_right(d, k).wait_recv()

        for c in range(chips):
            relay_gb(c).wait()
            relay_wo(c).wait()
            if c:
                spread_gb(c).wait_send()
                spread_wo(c).wait_send()
        for shard in range(n):
            save(shard).wait()
        for copy in saves:
            copy.wait()
        for step in range(n - 1):
            push(step).wait()
        for j in (0, 2, 3, 4):
            keeps[j].wait()


def front(
    tokens, cotangent, gain, shift, tables, w_query, w_key, w_value, gate, up, w_out, limit, n, devices
):
    rows, depth = tokens.shape
    total = n * rows
    width = w_query.shape[1]
    heads = width // HD
    chips = devices // 2
    chunks = 4
    place = lax.axis_index("dp")
    share = gate.shape[1] // devices
    part = width // devices
    if share % 128:
        gate, up = (lax.dynamic_slice_in_dim(w, place * share, share, 1) for w in (gate, up))
    hbm = pl.BlockSpec(memory_space=pl.ANY)

    def whole(*shape):
        return pl.BlockSpec(shape, lambda *_: (0,) * len(shape), pipeline_mode=pl.Buffered(1))

    def dma(*shape):
        return pltpu.SemaphoreType.DMA(shape)

    head_array = jax.ShapeDtypeStruct((heads, total, 128), BF)
    table = jax.ShapeDtypeStruct((total, 128), F32)
    coarse, fine, sign = tables
    return pl.pallas_call(
        functools.partial(front_kernel, n, chips, chunks),
        out_shape=(
            jax.ShapeDtypeStruct((total, width), BF),
            table,
            jax.ShapeDtypeStruct((depth // devices, 3 * width), BF),
            head_array, head_array, head_array, table, table,
            jax.ShapeDtypeStruct((n, rows, depth), BF),
            jax.ShapeDtypeStruct((chips, 2, rows, depth), BF),
            jax.ShapeDtypeStruct((2, n, share, depth), BF),
            jax.ShapeDtypeStruct((n, rows, width), BF),
            jax.ShapeDtypeStruct((n, part, depth), BF),
            jax.ShapeDtypeStruct((n, devices, part, depth), BF),
        ),
        grid_spec=pltpu.PrefetchScalarGridSpec(
            num_scalar_prefetch=0,
            grid=(n * heads,),
            in_specs=[pl.BlockSpec(memory_space=pltpu.SMEM)]
            + [whole(rows, depth)] * 2
            + [whole(1, depth)] * 2
            + [whole(*coarse.shape), whole(*fine.shape), whole(*sign.shape)]
            + [hbm] * 6,
            out_specs=[whole(total, width), whole(total, 128), whole(depth // devices, 3 * width)]
            + [hbm] * 11,
            scratch_shapes=[
                pltpu.VMEM((n, rows, depth), BF),
                pltpu.VMEM((rows, depth), BF),
                pltpu.VMEM((2, depth, share), BF),
                pltpu.VMEM((2, share, depth), BF),
                pltpu.VMEM((3, depth, width), BF),
            ]
            + [pltpu.VMEM((heads, total, 128), BF)] * 3
            + [pltpu.VMEM((total, 128), F32)] * 2
            + [dma(n - 1, chunks)] * 4
            + [dma(chips)] * 4
            + [dma(n)]
            + [dma(n - 1, 2)] * 4
            + [dma(n - 1)] * 4
            + [dma(chips)] * 4
            + [dma(3), dma(3), dma(5), dma(5)],
        ),
        compiler_params=pltpu.CompilerParams(
            vmem_limit_bytes=60 << 20, collective_id=1, has_side_effects=True
        ),
        cost_estimate=pl.CostEstimate(
            flops=4 * total * total * 256 * heads * 3, bytes_accessed=40 << 20, transcendentals=0
        ),
        name="front",
    )(
        limit, tokens, cotangent, gain.reshape(1, depth), shift.reshape(1, depth), coarse, fine, sign,
        w_query, w_key, w_value, gate, up,
        lax.dynamic_slice_in_dim(w_out, place * part, part, 0),
    )


def att_bwd_kernel(
    n, bk, chips, ga_ref, wo_ref, parts_ref, pg_ref, q_hbm, k_hbm, v_hbm, ctx_hbm, lse_hbm,
    cos_hbm, sin_hbm, cown_hbm, pk_ref, own_ref, sums_ref, og_ref, pg_all,
    q_ref, k_ref, v_ref, ctx_ref, lse_ref, cos_ref, sin_ref, cown_ref, do, gc, dka, dva, dqs,
    og_full, og_own, og_mate, og_sib, og_land, og_piece, og_z,
    send_sem, recv_sem, out_send, out_recv, pk_send, pk_recv, keep_sem,
    om_send, om_recv, op_send, op_recv, oz_send, oz_recv, gs_send, gs_recv, gr_send, gr_recv, pg_sem, load_sem,
):
    i = pl.program_id(0)
    heads, total, _ = k_ref.shape
    h = jnp.where(i < heads, i, (i - heads) // (n - 1))
    t = jnp.where(i < heads, 0, lax.rem(i - heads, n - 1) + 1)
    rows = total // n
    me = lax.axis_index("tensor")
    place = lax.axis_index("dp")
    core = lax.rem(place, 2)
    bits = chips.bit_length() - 1
    share = og_ref.shape[0]
    mine = pl.ds(pl.multiple_of(me * rows, rows), rows)

    def push(step):
        return remote(
            gc.at[step], do.at[mine], send_sem.at[step], recv_sem.at[step], tensor=ring(n, step + 1)
        )

    def push_out(s):
        return remote(
            parts_ref.at[s], sums_ref.at[s - 1], out_send.at[s - 1], out_recv.at[s - 1],
            dp=same_core(s, chips),
        )

    def columns(slot):
        return pl.ds(pl.multiple_of(slot * 128, 128), 128)

    def push_pack(slot, step):
        owner = ring(n, step + 1)
        return remote(
            pk_ref.at[pl.ds(pl.multiple_of(owner * rows, rows), rows), columns(slot)],
            own_ref.at[me, :, columns(slot)],
            pk_send.at[slot, step], pk_recv.at[slot, step], tensor=owner,
        )

    def keep(slot):
        return pltpu.make_async_copy(
            pk_ref.at[mine, columns(slot)], own_ref.at[me, :, columns(slot)], keep_sem.at[slot]
        )

    far = (q_hbm, k_hbm, v_hbm, ctx_hbm, lse_hbm, cos_hbm, sin_hbm, cown_hbm)
    near = (q_ref, k_ref, v_ref, ctx_ref, lse_ref, cos_ref, sin_ref, cown_ref)
    loads = [pltpu.make_async_copy(a, b, load_sem.at[j]) for j, (a, b) in enumerate(zip(far, near))]

    @pl.when(i == 0)
    def _():
        for load in loads:
            load.start()
        greet(n, chips, True)

        def send(step, carry):
            gc[step] = dot(ga_ref[...], wo_ref[ring(n, step + 1)], NT).astype(BF)
            push(step).start()
            return carry

        lax.fori_loop(0, n - 1, send, 0)
        do[mine, :] = dot(ga_ref[...], wo_ref[me], NT).astype(BF)
        for load in loads:
            load.wait()

    def pg_spread(s):
        return remote(pg_ref, pg_all.at[place], gs_send.at[s], gs_recv.at[s], dp=same_core(s, chips))

    def pg_relay(s):
        there = pg_all.at[differ(place // 2, s, bits) * 2 + core]
        return remote(there if s else pg_ref, there, gr_send.at[s], gr_recv.at[s], dp=sibling())

    def pg_keep():
        return pltpu.make_async_copy(pg_ref, pg_all.at[place], pg_sem)

    @pl.when(i == heads * n - 8)
    def _():
        for s in range(1, chips):
            pg_spread(s).start()
        pg_relay(0).start()
        pg_keep().start()

    def og_swap():
        return remote(og_mate, og_sib, om_send, om_recv, dp=sibling())

    def og_push(s):
        return remote(og_sib.at[s], og_land.at[s], op_send.at[s], op_recv.at[s], dp=same_core(s, chips))

    def og_over(step):
        to = ring(n, step + 1)
        return remote(og_piece.at[to], og_z.at[me], oz_send.at[step], oz_recv.at[step], tensor=to)

    @pl.when(i == 1)
    def _():
        def term(part, carry):
            og_full[...] = dot(cown_ref[part], ga_ref[...], TN)
            for s in range(chips):
                start = differ(place // 2, s, bits) * 2
                here = pl.ds(pl.multiple_of((start + core) * share, share), share)
                there = pl.ds(pl.multiple_of((start + 1 - core) * share, share), share)
                og_own[s, part] = og_full[here, :]
                og_mate[s, part] = og_full[there, :].astype(BF)
            return carry

        lax.fori_loop(0, n, term, 0)
        og_swap().start()

    @pl.when(i == 2)
    def _():
        og_swap().wait_recv()
        for s in range(chips):
            og_sib[s] = (og_own[s] + og_sib[s].astype(F32)).astype(BF)
            if s:
                og_push(s).start()

    @pl.when(i == heads * n - 6)
    def _():
        joined = og_sib[0].astype(F32)
        for s in range(1, chips):
            og_push(s).wait_recv()
            joined = joined + og_land[s].astype(F32)
        og_piece[...] = joined.astype(BF)
        for step in range(n - 1):
            og_over(step).start()

    @pl.when(i == heads + 1)
    def _():
        for s in range(1, chips):
            push_out(s).start()

    @pl.when(i == heads * n - 1)
    def _():
        og_z[me] = og_piece[me]
        for step in range(n - 1):
            og_over(step).wait_recv()
        joined = og_z[0].astype(F32)
        for part in range(1, n):
            joined = joined + og_z[part].astype(F32)
        og_ref[...] = joined.astype(BF)

    @pl.when((h == 0) & (t > 0))
    def _():
        push(t - 1).wait_recv()

    source = ring(n, n - t)
    block = pl.ds(pl.multiple_of(source * rows, rows), rows)
    pair = columns(h // 2)
    odd = lax.rem(h, 2) == 1
    lane = lanes((rows, 128))
    off = lane - HD
    logsum = jnp.sum(jnp.where(lane == h, lse_ref[block, :], 0.0), axis=1, keepdims=True)
    a, b, c = split3(-logsum)
    q = q_ref[h, block, :].astype(F32)
    q = jnp.where(off == 0, a, jnp.where(off == 1, b, jnp.where(off == 2, c, q))).astype(BF)
    g = jnp.where((lane >= HD) == odd, do[block, pair].astype(F32), 0.0)
    delta = jnp.sum(g * ctx_ref[block, pair].astype(F32), axis=1, keepdims=True)
    a, b, c = split3(-delta)
    g = jnp.where(odd, pltpu.roll(g, HD, 1), g)
    g = jnp.where(off == 0, a, jnp.where(off == 1, b, jnp.where(off == 2, c, g))).astype(BF)
    acc = jnp.zeros((rows, 128), F32)
    for j in range(total // bk):
        rk = pl.ds(j * bk, bk)
        kt = k_ref[h, rk, :]
        probs = jnp.exp(dot(kt, q, NT))
        grad = (probs * dot(v_ref[h, rk, :], g, NT)).astype(BF)
        for sums, term in ((dva, dot(probs.astype(BF), g)), (dka, dot(grad, q))):
            before = jnp.where(t == 0, jnp.zeros_like(term), sums[h, rk, :])
            sums[h, rk, :] = before + term
        acc = acc + dot(grad, kt, TN)
    acc = acc * SCALE

    @pl.when(jnp.logical_not(odd))
    def _():
        dqs[block, :] = acc

    @pl.when(odd)
    def _():
        grad = jnp.where(lane < HD, dqs[block, :], pltpu.roll(acc, HD, 1))
        grad = grad * cos_ref[block, :] - partner(grad) * sin_ref[block, :]
        pk_ref[block, columns(heads + h // 2)] = grad.astype(BF)

    @pl.when(odd & (t == 0))
    def _():
        keep(heads + h // 2).start()

    @pl.when(odd & (t > 0))
    def _():
        push_pack(heads + h // 2, n - 1 - t).start()

    @pl.when(t == n - 1)
    def _():
        dk = dka[h]
        dk = dk * cos_ref[...] - partner(dk) * sin_ref[...]
        both = jnp.where(lanes((total, 128)) < HD, dk, pltpu.roll(dva[h], HD, 1))
        pk_ref[:, columns(h)] = both.astype(BF)
        for step in range(n - 1):
            push_pack(h, step).start()
        keep(h).start()

    @pl.when(i == heads * n - 1)
    def _():
        for s in range(1, chips):
            pg_spread(s).wait_recv()
            pg_relay(s).start()
        for step in range(n - 1):
            push(step).wait_send()
        for s in range(1, chips):
            push_out(s).wait()
        og_swap().wait_send()
        pg_keep().wait()
        for s in range(chips):
            pg_relay(s).wait()
            if s:
                pg_spread(s).wait_send()
        for s in range(1, chips):
            og_push(s).wait_send()
        for step in range(n - 1):
            og_over(step).wait_send()
        for slot in range(heads + heads // 2):
            keep(slot).wait()
            for step in range(n - 1):
                push_pack(slot, step).wait()


def att_bwd(
    grad_attn, w_out, ctx_own, parts, pair_grads, q, k, v, ctx, lse, cosine, sine, n, bk=512
):
    heads, total, _ = q.shape
    width = heads * HD
    rows, depth = grad_attn.shape
    chips = parts.shape[0]
    share = width // (2 * chips)
    slots = heads + heads // 2
    hbm = pl.BlockSpec(memory_space=pl.ANY)

    def whole(*shape):
        return pl.BlockSpec(shape, lambda *_: (0,) * len(shape), pipeline_mode=pl.Buffered(1))

    return pl.pallas_call(
        functools.partial(att_bwd_kernel, n, bk, chips),
        out_shape=(
            jax.ShapeDtypeStruct((total, slots * 128), BF),
            jax.ShapeDtypeStruct((n, rows, slots * 128), BF),
            jax.ShapeDtypeStruct((chips - 1, rows, depth), BF),
            jax.ShapeDtypeStruct((share, depth), BF),
            jax.ShapeDtypeStruct((2 * chips, *pair_grads.shape), BF),
        ),
        grid_spec=pltpu.PrefetchScalarGridSpec(
            num_scalar_prefetch=0,
            grid=(heads * n,),
            in_specs=[whole(rows, depth), whole(n, width, depth)] + [hbm] * 10,
            out_specs=[whole(total, slots * 128), hbm, hbm, whole(share, depth), hbm],
            scratch_shapes=[pltpu.VMEM((heads, total, 128), BF)] * 3
            + [pltpu.VMEM((total, width), BF)]
            + [pltpu.VMEM((total, 128), F32)] * 3
            + [pltpu.VMEM((n, rows, width), BF)]
            + [
                pltpu.VMEM((total, width), BF),
                pltpu.VMEM((n - 1, rows, width), BF),
            ]
            + [pltpu.VMEM((heads, total, 128), F32)] * 2
            + [pltpu.VMEM((total, 128), F32)]
            + [
                pltpu.VMEM((width, depth), F32),
                pltpu.VMEM((chips, n, share, depth), F32),
                pltpu.VMEM((chips, n, share, depth), BF),
                pltpu.VMEM((chips, n, share, depth), BF),
                pltpu.VMEM((chips, n, share, depth), BF),
                pltpu.VMEM((n, share, depth), BF),
                pltpu.VMEM((n, share, depth), BF),
            ]
            + [pltpu.SemaphoreType.DMA((n - 1,))] * 2
            + [pltpu.SemaphoreType.DMA((chips - 1,))] * 2
            + [pltpu.SemaphoreType.DMA((slots, n - 1))] * 2
            + [pltpu.SemaphoreType.DMA((slots,))]
            + [pltpu.SemaphoreType.DMA] * 2
            + [pltpu.SemaphoreType.DMA((chips,))] * 2
            + [pltpu.SemaphoreType.DMA((n - 1,))] * 2
            + [pltpu.SemaphoreType.DMA((chips,))] * 4
            + [pltpu.SemaphoreType.DMA, pltpu.SemaphoreType.DMA((8,))],
        ),
        compiler_params=pltpu.CompilerParams(
            vmem_limit_bytes=60 << 20, collective_id=2, has_side_effects=True
        ),
        cost_estimate=pl.CostEstimate(
            flops=10 * total * total * 256 * heads,
            bytes_accessed=20 * total * width,
            transcendentals=total * total * heads,
        ),
        name="att_bwd",
    )(grad_attn, w_out, parts, pair_grads, q, k, v, ctx, lse, cosine, sine, ctx_own)


def finish_kernel(
    chips, n, x_ref, pk_ref, own_hbm, w_hbm, tokens_hbm, middle_hbm, gain_ref, vec_ref,
    input_ref, sums_ref, every,
    own_ref, w_ref, tokens_ref, middle_ref, full, mate, sib, land, fin, vec_z, vec_dp, vec_me,
    sx_send, sx_recv, rs_send, rs_recv, ag_send, ag_recv, rl_send, rl_recv,
    vz_send, vz_recv, vd_send, vd_recv, own_sem, load_sem,
):
    bits = chips.bit_length() - 1
    me = lax.axis_index("dp")
    place = lax.axis_index("tensor")
    core = lax.rem(me, 2)
    chip = me // 2
    other = 1 - core
    piece = fin.shape[0]

    def swap(s):
        return remote(mate.at[s], sib.at[s], sx_send.at[s], sx_recv.at[s], dp=chip * 2 + other)

    def push(s):
        return remote(sib.at[s], land.at[s], rs_send.at[s], rs_recv.at[s], dp=same_core(s, chips))

    def spread(s):
        return remote(
            fin, every.at[chip, core], ag_send.at[s], ag_recv.at[s], dp=same_core(s, chips)
        )

    def relay(s):
        src = every.at[differ(chip, s, bits), core]
        return remote(src, src, rl_send.at[s], rl_recv.at[s], dp=chip * 2 + other)

    def vec_over(step):
        return remote(
            vec_me.at[0], vec_z.at[place], vz_send.at[step], vz_recv.at[step], tensor=ring(n, step + 1)
        )

    def vec_across(step):
        return remote(
            vec_me.at[1], vec_dp.at[me], vd_send.at[step], vd_recv.at[step],
            dp=lax.rem(me + step + 1, 2 * chips),
        )

    far = (own_hbm, w_hbm, tokens_hbm, middle_hbm)
    near = (own_ref, w_ref, tokens_ref, middle_ref)
    loads = [pltpu.make_async_copy(a, b, load_sem.at[j]) for j, (a, b) in enumerate(zip(far, near))]
    for load in loads:
        load.start()
    barrier = pltpu.get_barrier_semaphore()
    for step in range(n - 1):
        pl.semaphore_signal(barrier, inc=1, device_id={"tensor": ring(n, step + 1)}, device_id_type=MESH)
    for step in range(2 * chips - 1):
        to = lax.rem(me + step + 1, 2 * chips)
        pl.semaphore_signal(barrier, inc=1, device_id={"dp": to}, device_id_type=MESH)

    full[...] = dot(x_ref[...], pk_ref[...], TN)
    pl.semaphore_wait(barrier, n + 2 * chips - 2)

    def part(s, which):
        start = (differ(chip, s, bits) * 2 + which) * piece
        return full[pl.ds(pl.multiple_of(start, piece), piece), :]

    for s in range(chips):
        mate[s] = part(s, other).astype(BF)
        swap(s).start()

    for load in loads:
        load.wait()
    grad = jnp.zeros(input_ref.shape, F32)
    for t in range(n):
        w = w_ref[:, t].reshape(w_ref.shape[0] * w_ref.shape[2], w_ref.shape[3])
        grad = grad + dot(own_ref[t], w, NT).astype(BF).astype(F32)

    for s in range(1, chips):
        swap(s).wait_recv()
        sib[s] = (sib[s].astype(F32) + part(s, core)).astype(BF)
        push(s).start()
    swap(0).wait_recv()
    total = sib[0].astype(F32) + part(0, core)

    values = tokens_ref[...].astype(F32)
    values = values - jnp.mean(values, axis=1, keepdims=True)
    inverse = lax.rsqrt(jnp.mean(values * values, axis=1, keepdims=True) + EPS)
    scaled = values * inverse
    through = grad * gain_ref[...]
    inner = through - jnp.mean(through, axis=1, keepdims=True)
    inner = inner - scaled * jnp.mean(through * scaled, axis=1, keepdims=True)
    input_ref[...] = middle_ref[...] + inverse * inner
    vec_me[0, 0:1] = jnp.sum(grad * scaled, axis=0, keepdims=True)
    vec_me[0, 1:2] = jnp.sum(grad, axis=0, keepdims=True)
    vec_me[0, 2:4] = vec_ref[...]
    vec_me[0, 4:8] = jnp.zeros((4, vec_ref.shape[1]), F32)
    vec_z[place] = vec_me[0]
    for step in range(n - 1):
        vec_over(step).start()

    for s in range(1, chips):
        push(s).wait_recv()
        total = total + land[s].astype(F32)
    fin[...] = total.astype(BF)
    for s in range(1, chips):
        spread(s).start()
    mine = pltpu.make_async_copy(fin, every.at[chip, core], own_sem)
    mine.start()
    mine.wait()
    relay(0).start()

    for step in range(n - 1):
        vec_over(step).wait()
    vec = vec_z[0]
    for t in range(1, n):
        vec = vec + vec_z[t]
    vec_me[1] = vec
    vec_dp[me] = vec
    for step in range(2 * chips - 1):
        vec_across(step).start()
    for s in range(1, chips):
        spread(s).wait_recv()
        relay(s).start()
    for step in range(2 * chips - 1):
        vec_across(step).wait()
    vec = vec_dp[0]
    for t in range(1, 2 * chips):
        vec = vec + vec_dp[t]
    sums_ref[...] = vec
    for s in range(chips):
        relay(s).wait()
        swap(s).wait_send()
        if s > 0:
            spread(s).wait_send()
            push(s).wait_send()


def finish(rows_all, packed, own, w_all, tokens, middle, gain, vec, devices):
    n, rows, packs = own.shape
    depth = tokens.shape[1]
    chips = devices // 2
    piece = depth // devices
    vmem = pl.BlockSpec(memory_space=pltpu.VMEM)
    return pl.pallas_call(
        functools.partial(finish_kernel, chips, n),
        out_shape=(
            jax.ShapeDtypeStruct((rows, depth), F32),
            jax.ShapeDtypeStruct((8, depth), F32),
            jax.ShapeDtypeStruct((chips, 2, piece, packs), BF),
        ),
        in_specs=[vmem] * 2 + [pl.BlockSpec(memory_space=pl.ANY)] * 4 + [vmem] * 2,
        out_specs=[vmem, vmem, pl.BlockSpec(memory_space=pl.ANY)],
        scratch_shapes=[
            pltpu.VMEM(own.shape, BF),
            pltpu.VMEM(w_all.shape, BF),
            pltpu.VMEM((rows, depth), BF),
            pltpu.VMEM((rows, depth), F32),
            pltpu.VMEM((depth, packs), F32),
            pltpu.VMEM((chips, piece, packs), BF),
            pltpu.VMEM((chips, piece, packs), BF),
            pltpu.VMEM((chips, piece, packs), BF),
            pltpu.VMEM((piece, packs), BF),
            pltpu.VMEM((n, 8, depth), F32),
            pltpu.VMEM((devices, 8, depth), F32),
            pltpu.VMEM((2, 8, depth), F32),
        ]
        + [pltpu.SemaphoreType.DMA((chips,))] * 8
        + [pltpu.SemaphoreType.DMA((n - 1,))] * 2
        + [pltpu.SemaphoreType.DMA((devices - 1,))] * 2
        + [pltpu.SemaphoreType.DMA, pltpu.SemaphoreType.DMA((4,))],
        compiler_params=pltpu.CompilerParams(
            vmem_limit_bytes=56 << 20, collective_id=4, has_side_effects=True
        ),
        cost_estimate=pl.CostEstimate(
            flops=4 * n * rows * depth * packs, bytes_accessed=20 << 20, transcendentals=0
        ),
        name="finish",
    )(rows_all, packed, own, w_all, tokens, middle, gain.reshape(1, depth), vec)


def ffn_kernel(
    chips, x_ref, gb_ref, w_ref, down_ref, wp_ref, dx_ref, out_ref, dw_ref, zs_ref, wp_z,
    rows_all, gb, hid, gate_g, up_g, own, sib, mate, partial, z_left, z_right, wd,
    ag_send, ag_recv, rl_send, rl_recv, sx_send, sx_recv, rs_send, rs_recv, fw_send, fw_recv,
    gb_sem, out_sem, dx_sem, wp_send, wp_recv, wp_sem, zr_send, zr_recv, zl_send, zl_recv,
    dr_send, dr_recv, dl_send, dl_recv, wd_sem,
):
    bits = chips.bit_length() - 1
    me = lax.axis_index("dp")
    core = lax.rem(me, 2)
    chip = me // 2
    other = 1 - core
    rows, depth = x_ref.shape
    n, share, _ = dw_ref.shape

    def spread(s):
        to = differ(chip, s, bits) * 2 + core
        return remote(x_ref, rows_all.at[chip, core], ag_send.at[s], ag_recv.at[s], dp=to)

    square = chips == 4

    def hand_on(s):
        half = pl.ds((s - 1) * (rows // 2), rows // 2)
        part = rows_all.at[differ(chip, s, bits), core, half]
        to = differ(chip, 3 - s, bits) * 2 + core
        return remote(part, part, fw_send.at[s], fw_recv.at[s], dp=to)

    def handed(s):
        half = pl.ds((s - 1) * (rows // 2), rows // 2)
        part = rows_all.at[differ(chip, 3, bits), core, half]
        to = differ(chip, 3 - s, bits) * 2 + core
        return remote(part, part, fw_send.at[s], fw_recv.at[s], dp=to)

    def relay(s):
        src = differ(chip, s, bits)
        return remote(
            rows_all.at[src, core], rows_all.at[src, core], rl_send.at[s], rl_recv.at[s],
            dp=chip * 2 + other,
        )

    def swap(s):
        return remote(
            mate.at[lax.rem(s, 2)], sib.at[s], sx_send.at[s], sx_recv.at[s], dp=chip * 2 + other
        )

    def push(s):
        to = differ(chip, s, bits) * 2 + core
        return remote(sib.at[s, 0], dx_ref.at[s], rs_send.at[s], rs_recv.at[s], dp=to)

    def fetch(s):
        src = differ(chip, s, bits)
        return pltpu.make_async_copy(gb_ref.at[src], gb.at[src], gb_sem.at[s])

    part = lax.axis_index("tensor")

    def over(step):
        return remote(
            wp_ref, wp_z.at[part], wp_send.at[step], wp_recv.at[step], tensor=ring(n, step + 1)
        )

    def keep(s):
        return pltpu.make_async_copy(sib.at[s, 1], out_ref.at[s], out_sem.at[s])

    ours = pl.ds(pl.multiple_of(me * share, share), share)
    cut = pltpu.make_async_copy(down_ref.at[ours], wd.at[part], wd_sem)
    cut.start()
    for s in range(chips):
        fetch(s).start()
    barrier = pltpu.get_barrier_semaphore()
    for step in range(1, n):
        pl.semaphore_signal(barrier, inc=1, device_id={"tensor": ring(n, step)}, device_id_type=MESH)
    pl.semaphore_signal(barrier, inc=1, device_id={"dp": chip * 2 + other}, device_id_type=MESH)
    for s in range(1, chips):
        to = differ(chip, s, bits) * 2 + core
        pl.semaphore_signal(barrier, inc=1, device_id={"dp": to}, device_id_type=MESH)
    pl.semaphore_wait(barrier, chips + n - 1)
    direct = range(1, 3) if square else range(1, chips)
    for s in direct:
        spread(s).start()
    mine = pltpu.make_async_copy(x_ref, rows_all.at[chip, core], ag_send.at[0])
    mine.start()
    mine.wait()
    relay(0).start()
    keep_wp = pltpu.make_async_copy(wp_ref, wp_z.at[part], wp_sem)
    keep_wp.start()

    def d_right(d):
        there = wd.at[part - d]
        return remote(there, there, dr_send.at[d], dr_recv.at[d], tensor=part + 1)

    def d_left(d):
        there = wd.at[part + d]
        return remote(there, there, dl_send.at[d], dl_recv.at[d], tensor=part - 1)

    def d_from_left(d):
        there = wd.at[part - d]
        return remote(there, there, dr_send.at[d - 1], dr_recv.at[d - 1], tensor=part - 1)

    def d_from_right(d):
        there = wd.at[part + d]
        return remote(there, there, dl_send.at[d - 1], dl_recv.at[d - 1], tensor=part + 1)

    cut.wait()
    for d in range(n):
        if d:

            @pl.when(part >= d)
            def _():
                d_from_left(d).wait_recv()

        if d < n - 1:

            @pl.when((part >= d) & (part < n - 1))
            def _():
                d_right(d).start()

        if d:

            @pl.when(part + d < n)
            def _():
                d_from_right(d).wait_recv()

        if d < n - 1:

            @pl.when((part + d < n) & (part > 0))
            def _():
                d_left(d).start()

    for step in range(n - 1):
        over(step).start()

    def shard(src, which, put):
        x = rows_all[src, which]
        grad = gb[src, which]
        gate = dot(x, w_ref[0], NT)
        upper = dot(x, w_ref[1], NT)
        w_down = wd[...].reshape(n * share, depth)
        grad_hidden = dot(grad, w_down, NT)
        sigma = jax.nn.sigmoid(gate)
        act = gate * sigma
        hidden = (act * upper).astype(BF)
        grad_gate = (grad_hidden * upper * sigma * (1.0 + gate * (1.0 - sigma))).astype(BF)
        grad_upper = (grad_hidden * act).astype(BF)
        hid[src, which] = hidden
        gate_g[src, which] = grad_gate
        up_g[src, which] = grad_upper
        put[0] = (dot(grad_gate, w_ref[0]) + dot(grad_upper, w_ref[1])).astype(BF)
        put[1] = dot(hidden, w_down).astype(BF)

    def step(s, carry):
        src = differ(chip, s, bits)
        slot = lax.rem(s, 2)
        relay(s).wait_recv()
        fetch(s).wait()

        @pl.when(s >= 2)
        def _():
            swap(s - 2).wait_send()

        shard(src, other, mate.at[slot])
        swap(s).start()
        shard(src, core, own)
        swap(s).wait_recv()
        for k in range(2):
            sib[s, k] = (sib[s, k].astype(F32) + own[k].astype(F32)).astype(BF)

        @pl.when(s > 0)
        def _():
            push(s).start()

        keep(s).start()

        if square:

            @pl.when(s == 0)
            def _():
                for near in (1, 2):
                    spread(near).wait_recv()
                    hand_on(near).start()
                    relay(near).start()

        else:

            @pl.when(s < chips - 1)
            def _():
                spread(s + 1).wait_recv()
                relay(s + 1).start()

        if square:

            @pl.when(s == 1)
            def _():
                handed(1).wait_recv()
                handed(2).wait_recv()
                relay(3).start()

        return carry

    lax.fori_loop(0, chips, step, 0)
    first = pltpu.make_async_copy(sib.at[0, 0], dx_ref.at[0], dx_sem)
    first.start()
    def zr(t, k, to):
        return remote(
            partial.at[t, k], z_left.at[t, k], zr_send.at[t, k], zr_recv.at[t, k], tensor=to
        )

    def zl(t, k, to):
        return remote(
            partial.at[t, k], z_right.at[t, k], zl_send.at[t, k], zl_recv.at[t, k], tensor=to
        )

    def join(t, k, more):
        partial[t, k] = (partial[t, k].astype(F32) + more[t, k].astype(F32)).astype(BF)

    def weight_grad(left, right):
        left = left[...].reshape(-1, n * share)
        return dot(left, right[...].reshape(-1, depth), TN)

    def hand_along(k):
        for j in range(n - 1):
            t = n - 1 - j

            @pl.when((part > 0) & (part < t))
            def _():
                zr(t, k, part + 1).wait_recv()
                join(t, k, z_left)
                zr(t, k, part + 1).start()

            @pl.when((part < n - 1) & (part > j))
            def _():
                zl(j, k, part - 1).wait_recv()
                join(j, k, z_right)
                zl(j, k, part - 1).start()

    for k, left in enumerate((gate_g, up_g)):
        grad = weight_grad(left, rows_all)
        for t in range(n):
            partial[t, k] = grad[t * share : (t + 1) * share, :].astype(BF)

        for j in range(n - 1):

            @pl.when(part == 0)
            def _():
                zr(n - 1 - j, k, 1).start()

            @pl.when(part == n - 1)
            def _():
                zl(j, k, n - 2).start()

    hand_along(0)
    grad = weight_grad(hid, gb)
    for t in range(n):
        dw_ref[t] = grad[t * share : (t + 1) * share, :].astype(BF)
    hand_along(1)
    for k in range(2):
        for t in range(n):

            @pl.when((part == t) & (part > 0))
            def _():
                zr(t, k, part - 1).wait_recv()
                join(t, k, z_left)

            @pl.when((part == t) & (part < n - 1))
            def _():
                zl(t, k, part + 1).wait_recv()
                join(t, k, z_right)

            @pl.when(part == t)
            def _():
                zs_ref[k] = partial[t, k]

            @pl.when(part < t)
            def _():
                zr(t, k, part + 1).wait_send()

            @pl.when(part > t)
            def _():
                zl(t, k, part - 1).wait_send()

    for d in range(n - 1):

        @pl.when((part >= d) & (part < n - 1))
        def _():
            d_right(d).wait_send()

        @pl.when((part + d < n) & (part > 0))
        def _():
            d_left(d).wait_send()

    first.wait()
    keep_wp.wait()
    for step in range(n - 1):
        over(step).wait()
    for s in range(chips):
        keep(s).wait()
        relay(s).wait_send()
        if s >= chips - 2:
            swap(s).wait_send()
        if s in direct:
            spread(s).wait_send()
        if s > 0:
            push(s).wait()
    if square:
        hand_on(1).wait_send()
        hand_on(2).wait_send()


def ffn(x, grad_branch, weights, down, w_packed, n, devices):
    rows, depth = x.shape
    chips = devices // 2
    hidden = weights.shape[1]
    share = hidden // n
    vmem = pl.BlockSpec(memory_space=pltpu.VMEM)
    hbm = pl.BlockSpec(memory_space=pl.ANY)
    return pl.pallas_call(
        functools.partial(ffn_kernel, chips),
        out_shape=(
            jax.ShapeDtypeStruct((chips, rows, depth), BF),
            jax.ShapeDtypeStruct((chips, rows, depth), BF),
            jax.ShapeDtypeStruct((n, share, depth), BF),
            jax.ShapeDtypeStruct((2, share, depth), BF),
            jax.ShapeDtypeStruct((n, *w_packed.shape), BF),
        ),
        in_specs=[vmem, hbm, vmem, hbm, hbm],
        out_specs=[hbm, hbm, vmem, vmem, hbm],
        scratch_shapes=[
            pltpu.VMEM((chips, 2, rows, depth), BF),
            pltpu.VMEM((chips, 2, rows, depth), BF),
        ]
        + [pltpu.VMEM((chips, 2, rows, hidden), BF)] * 3
        + [
            pltpu.VMEM((2, rows, depth), BF),
            pltpu.VMEM((chips, 2, rows, depth), BF),
            pltpu.VMEM((2, 2, rows, depth), BF),
        ]
        + [pltpu.VMEM((n, 2, share, depth), BF)] * 3
        + [pltpu.VMEM((n, share, depth), BF)]
        + [pltpu.SemaphoreType.DMA((chips,))] * 8
        + [pltpu.SemaphoreType.DMA((3,))] * 2
        + [pltpu.SemaphoreType.DMA((chips,))] * 2
        + [pltpu.SemaphoreType.DMA]
        + [pltpu.SemaphoreType.DMA((n - 1,))] * 2
        + [pltpu.SemaphoreType.DMA]
        + [pltpu.SemaphoreType.DMA((n, 2))] * 4
        + [pltpu.SemaphoreType.DMA((n - 1,))] * 4
        + [pltpu.SemaphoreType.DMA],
        compiler_params=pltpu.CompilerParams(
            vmem_limit_bytes=62 << 20, collective_id=3, has_side_effects=True
        ),
        cost_estimate=pl.CostEstimate(
            flops=2 * 9 * devices * rows * depth * hidden, bytes_accessed=30 << 20, transcendentals=0
        ),
        name="ffn",
    )(x, grad_branch, weights, down, w_packed)


def unpack_kernel(
    share, pair_ref, rest_ref, pack_ref, input_ref, sums_ref, gate_ref, up_ref, down_ref, out_ref,
    q_ref, k_ref, v_ref, grad_ref, *vector_refs,
):
    grad_ref[...] = input_ref[...]
    for i, vector_ref in enumerate(vector_refs):
        vector_ref[...] = sums_ref[i]
    gate_ref[...] = pair_ref[0, 0].astype(F32).T
    up_ref[...] = pair_ref[0, 1].astype(F32).T
    rest = rest_ref[0].astype(F32)
    down_ref[...] = rest[:share]
    out_ref[...] = rest[share:]
    pack = pack_ref[0].astype(F32)
    pairs = q_ref.shape[1] // 128
    first = lanes((pack.shape[0], 128)) < HD
    for p in range(pairs):
        even = pack[:, p * 256 : p * 256 + 128]
        odd = pack[:, p * 256 + 128 : p * 256 + 256]
        out = slice(p * 128, p * 128 + 128)
        q_ref[:, out] = pack[:, (2 * pairs + p) * 128 : (2 * pairs + p + 1) * 128]
        k_ref[:, out] = jnp.where(first, even, pltpu.roll(odd, HD, 1))
        v_ref[:, out] = jnp.where(first, pltpu.roll(even, HD, 1), odd)


def unpack(pair, rest, pack, input_grad, sums):
    devices, _, share, depth = pair.shape
    hidden = devices * share
    height = rest.shape[1]
    width = devices * (height - share)
    piece = depth // devices
    if share % 128:
        down = rest[:, :share].reshape(hidden, depth).astype(F32)
        gate, up = (pair[:, k].reshape(hidden, depth).astype(F32).T for k in range(2))
        pack = pack.reshape(depth, 3 * width).astype(F32)
        both = pack[:, : 2 * width].reshape(depth, width // HD, 2, HD)
        key, value = (both[:, :, k].reshape(depth, width) for k in range(2))
        out = rest[:, share:].reshape(width, depth).astype(F32)
        vectors = (sums[i] for i in range(4))
        return gate, up, down, out, pack[:, 2 * width :], key, value, input_grad, *vectors
    column = pl.BlockSpec((depth, share), lambda i: (0, i))
    rows = pl.BlockSpec((piece, width), lambda i: (i, 0))
    part = pl.BlockSpec((input_grad.shape[0] // devices, depth), lambda i: (i, 0))
    vector = pl.BlockSpec((depth,), lambda i: (0,))
    return pl.pallas_call(
        functools.partial(unpack_kernel, share),
        out_shape=(jax.ShapeDtypeStruct((depth, hidden), F32),) * 2
        + (
            jax.ShapeDtypeStruct((hidden, depth), F32),
            jax.ShapeDtypeStruct((width, depth), F32),
        )
        + (jax.ShapeDtypeStruct((depth, width), F32),) * 3
        + (jax.ShapeDtypeStruct(input_grad.shape, F32),)
        + (jax.ShapeDtypeStruct((depth,), F32),) * 4,
        grid=(devices,),
        in_specs=[
            pl.BlockSpec((1, 2, share, depth), lambda i: (i, 0, 0, 0)),
            pl.BlockSpec((1, height, depth), lambda i: (i, 0, 0)),
            pl.BlockSpec((1, piece, 3 * width), lambda i: (i, 0, 0)),
            part,
            pl.BlockSpec(sums.shape, lambda i: (0, 0)),
        ],
        out_specs=[
            column, column, pl.BlockSpec((share, depth), lambda i: (i, 0)),
            pl.BlockSpec((height - share, depth), lambda i: (i, 0)), rows, rows, rows,
            part, vector, vector, vector, vector,
        ],
        compiler_params=pltpu.CompilerParams(vmem_limit_bytes=62 << 20),
        name="unpack",
    )(pair, rest, pack, input_grad, sums)


def norm_parts(values):
    centre = jnp.mean(values, axis=-1, keepdims=True)
    centred = values - centre
    inverse = lax.rsqrt(jnp.mean(centred * centred, axis=-1, keepdims=True) + EPS)
    return centred * inverse, inverse


def norm_back(upstream, scaled, inverse, gain):
    through = upstream * gain
    inner = (
        through
        - jnp.mean(through, axis=-1, keepdims=True)
        - scaled * jnp.mean(through * scaled, axis=-1, keepdims=True)
    )
    return inverse * inner, jnp.sum(upstream * scaled, axis=0), jnp.sum(upstream, axis=0)


def on_device(
    tokens, lengths, ln1_gain, ln1_bias, w_query, w_key, w_value, w_out,
    ln2_gain, ln2_bias, w_gate, w_up, down_weight, cotangent,
):
    n = lax.axis_size("tensor")
    local_rows, depth = tokens.shape
    length = local_rows * n
    width = w_query.shape[1]
    row_ids = lax.axis_index("tensor") * local_rows + lax.iota(jnp.int32, local_rows)
    valid = (row_ids < lengths[0])[:, None]

    inputs = tokens.astype(F32)
    grad_out = jnp.where(valid, cotangent.astype(F32), 0.0)
    devices = lax.axis_size("dp")
    place = lax.axis_index("dp")
    share = w_gate.shape[1] // devices

    (
        context, logsum, w_packed, q, k, v, cosine, sine, attn_rows, grad_branch, weights, context_own, _,
        w_out_all,
    ) = front(
        tokens, cotangent, ln1_gain, ln1_bias, angle_tables(length), w_query, w_key, w_value,
        w_gate, w_up, w_out, lengths, n, devices,
    )
    attn_rows = attn_rows.reshape(length, depth)
    weights = weights.reshape(2, n * share, depth)

    w_out_all = w_out_all.reshape(n, width, depth)
    attn_out = sum(dot(context_own[t], w_out_all[t]).astype(BF).astype(F32) for t in range(n))
    middle = inputs + attn_out
    scaled2, inverse2 = norm_parts(middle)
    ffn_in = (scaled2 * ln2_gain + ln2_bias).astype(BF)
    grad_parts, out_parts, down_grad, pair_grads, w_packed = ffn(
        ffn_in, grad_branch, weights, down_weight, w_packed, n, devices
    )
    grad_ffn_in = sum(grad_parts[p].astype(F32) for p in range(devices // 2))
    grad_norm2, gain2_grad, shift2_grad = norm_back(
        grad_ffn_in, scaled2, inverse2, ln2_gain
    )
    grad_middle = grad_out + grad_norm2
    grad_attn = grad_middle.astype(BF)
    w_packed = lax.all_gather(w_packed, "dp", axis=0)
    down_grad = lax.psum_scatter(down_grad, "tensor", scatter_dimension=0, tiled=True)[0]
    packed, packed_own, out_sums, out_piece, pair_grads = att_bwd(
        grad_attn, w_out_all, context_own, out_parts, pair_grads, q, k, v, context, logsum, cosine, sine, n
    )
    down_grad, out_piece, w_packed = lax.optimization_barrier((down_grad, out_piece, w_packed))
    grads = lax.all_gather(jnp.concatenate([down_grad, out_piece]), "dp", axis=0)
    ffn_out = sum(x.astype(F32) for x in (out_parts[0], *out_sums))
    output = jnp.where(valid, middle + ffn_out, 0.0).astype(BF)
    input_grad, sums, packed_grads = finish(
        attn_rows, packed, packed_own, w_packed, tokens, grad_middle, ln1_gain,
        jnp.stack([gain2_grad, shift2_grad]), devices,
    )
    packed_grads = packed_grads.reshape(devices, depth // devices, 3 * width)
    (
        gate_grad, up_grad, down_grad, out_grad, query_grad, key_grad, value_grad, input_grad,
        gain1_grad, shift1_grad, gain2_grad, shift2_grad,
    ) = unpack(pair_grads, grads, packed_grads, input_grad, sums)
    return (
        output, input_grad, gain1_grad, shift1_grad, query_grad, key_grad, value_grad, out_grad,
        gain2_grad, shift2_grad, gate_grad, up_grad, down_grad,
    )


def solution(mesh):
    rows = P(("dp", "tensor"), None)
    columns = P(None, "tensor")
    parts = P("tensor", None)
    return jax.shard_map(
        on_device,
        mesh=mesh,
        in_specs=(
            rows, P("dp"), P(), P(), columns, columns, columns, parts,
            P(), P(), columns, columns, parts, rows,
        ),
        out_specs=(
            rows, rows, P(), P(), columns, columns, columns, parts,
            P(), P(), columns, columns, parts,
        ),
        check_vma=False,
    )
```

```python
import functools
import math

import jax
import jax.numpy as jnp
from jax import lax
from jax.experimental import pallas as pl
from jax.experimental.pallas import tpu as pltpu
from jax.sharding import PartitionSpec as P

HD = 64
EPS = 1e-05
SCALE = 1.0 / math.sqrt(HD)
F32 = jnp.float32
BF = jnp.bfloat16
NT = (((1,), (1,)), ((), ()))
NN = (((1,), (0,)), ((), ()))
TN = (((0,), (0,)), ((), ()))
MESH = pl.DeviceIdType.MESH


def dot(a, b, dims=NN):
    return lax.dot_general(a, b, dims, preferred_element_type=F32)


def lanes(shape):
    return lax.broadcasted_iota(jnp.int32, shape, 1)


def split3(x):
    hi = x.astype(BF).astype(F32)
    mid = (x - hi).astype(BF).astype(F32)
    return hi, mid, x - hi - mid


def partner(x):
    width = x.shape[1]
    first = lanes(x.shape) % HD < HD // 2
    return jnp.where(first, pltpu.roll(x, width - HD // 2, 1), pltpu.roll(x, HD // 2, 1))


STEP = 64


def angle_tables(length):
    half = HD // 2
    lane = lax.optimization_barrier(lax.iota(jnp.int32, 2 * HD))
    freqs = 10000.0 ** (-((lane % half).astype(F32) * 2.0 / HD))
    sign = jnp.where(lane % HD < half, -1.0, 1.0)

    def table(positions):
        angles = positions[:, None] * freqs[None, :]
        return jnp.stack([jnp.cos(angles), jnp.sin(angles)])

    return table(lax.iota(F32, length // STEP) * STEP), table(lax.iota(F32, STEP)), sign[None, :]


def differ(a, b, bits):
    return sum(lax.rem(a // (1 << k) + b // (1 << k), 2) * (1 << k) for k in range(bits))


def remote(src, dst, send, recv, **to):
    return pltpu.make_async_remote_copy(
        src_ref=src, dst_ref=dst, send_sem=send, recv_sem=recv, device_id=to, device_id_type=MESH
    )


def ring(n, step):
    return lax.rem(lax.axis_index("tensor") + step, n)


def same_core(s, chips):
    me = lax.axis_index("dp")
    return differ(me // 2, s, chips.bit_length() - 1) * 2 + lax.rem(me, 2)


def sibling():
    me = lax.axis_index("dp")
    return me + 1 - 2 * lax.rem(me, 2)


def greet(n, chips, both_cores=False):
    barrier = pltpu.get_barrier_semaphore()
    if both_cores:
        pl.semaphore_signal(barrier, inc=1, device_id={"dp": sibling()}, device_id_type=MESH)
    for step in range(1, n):
        pl.semaphore_signal(barrier, inc=1, device_id={"tensor": ring(n, step)}, device_id_type=MESH)
    for s in range(1, chips):
        pl.semaphore_signal(
            barrier, inc=1, device_id={"dp": same_core(s, chips)}, device_id_type=MESH
        )
    pl.semaphore_wait(barrier, n + chips - 2 + both_cores)


def front_kernel(
    n, chips, chunks, limit_ref, tokens_ref, ct_ref, gain_ref, shift_ref, coarse_ref, fine_ref, sign_ref,
    wq_ref, wk_ref, wv_ref, gate_ref, up_ref, wo_ref,
    ctx_ref, lse_ref, wp_ref, q_out, k_out, v_out, cos_out, sin_out, rows_ref, gb_all, w_all, out_ref, wo_z, wo_all,
    landed, gb, columns, own_w, wqkv, q_ref, k_ref, v_ref, cos_ref, sin_ref,
    right_send, right_recv, left_send, left_recv, gs_send, gs_recv, gr_send, gr_recv, rows_sem,
    wr_send, wr_recv, wl_send, wl_recv, send_sem, recv_sem, wz_send, wz_recv, ws_send, ws_recv,
    wx_send, wx_recv, cut_sem, load_sem, save_sem, keep_sem,
):
    i = pl.program_id(0)
    steps = pl.num_programs(0)
    me = lax.axis_index("tensor")
    place = lax.axis_index("dp")
    core = lax.rem(place, 2)
    bits = chips.bit_length() - 1
    rows, depth = tokens_ref.shape
    heads = q_ref.shape[0]
    piece = rows // chunks
    limit = limit_ref[0]
    s = i // heads
    h = lax.rem(i, heads)

    def over(shard, d, c, send, recv, to):
        part = landed.at[shard, pl.ds(c * piece, piece)]
        return remote(part, part, send.at[d, c], recv.at[d, c], tensor=to)

    def rightward(d, c):
        return over(me - d, d, c, right_send, right_recv, me + 1)

    def leftward(d, c):
        return over(me + d, d, c, left_send, left_recv, me - 1)

    def from_left(d, c):
        return over(me - d, d - 1, c, right_send, right_recv, me - 1)

    def from_right(d, c):
        return over(me + d, d - 1, c, left_send, left_recv, me + 1)

    def weights(shard, d, k, send, recv, to):
        there = w_all.at[k, shard]
        return remote(there if d else own_w.at[k], there, send.at[d, k], recv.at[d, k], tensor=to)

    def w_right(d, k):
        return weights(me - d, d, k, wr_send, wr_recv, me + 1)

    def w_left(d, k):
        return weights(me + d, d, k, wl_send, wl_recv, me - 1)

    def w_from_left(d, k):
        return weights(me - d, d - 1, k, wr_send, wr_recv, me - 1)

    def w_from_right(d, k):
        return weights(me + d, d - 1, k, wl_send, wl_recv, me + 1)

    def spread_gb(c):
        return remote(
            gb, gb_all.at[place // 2, core], gs_send.at[c], gs_recv.at[c], dp=same_core(c, chips)
        )

    def relay_gb(c):
        there = gb_all.at[differ(place // 2, c, bits), core]
        return remote(there if c else gb, there, gr_send.at[c], gr_recv.at[c], dp=sibling())

    def wo_over(step):
        return remote(
            wo_ref, wo_z.at[me], wz_send.at[step], wz_recv.at[step], tensor=ring(n, step + 1)
        )

    def spread_wo(c):
        return remote(
            wo_z, wo_all.at[:, place], ws_send.at[c], ws_recv.at[c], dp=same_core(c, chips)
        )

    def relay_wo(c):
        there = wo_all.at[:, differ(place // 2, c, bits) * 2 + core]
        return remote(there if c else wo_z, there, wx_send.at[c], wx_recv.at[c], dp=sibling())

    def push(step):
        owner = ring(n, step + 1)
        return remote(
            ctx_ref.at[pl.ds(pl.multiple_of(owner * rows, rows), rows)], out_ref.at[me],
            send_sem.at[step], recv_sem.at[step], tensor=owner,
        )

    def save(shard):
        return pltpu.make_async_copy(landed.at[shard], rows_ref.at[shard], rows_sem.at[shard])

    mine = pl.ds(pl.multiple_of(me * rows, rows), rows)
    keeps = [
        pltpu.make_async_copy(gb, gb_all.at[place // 2, core], keep_sem.at[0]),
        pltpu.make_async_copy(wo_ref, wo_z.at[me], keep_sem.at[1]),
        pltpu.make_async_copy(wo_z, wo_all.at[:, place], keep_sem.at[2]),
        pltpu.make_async_copy(ctx_ref.at[mine], out_ref.at[me], keep_sem.at[3]),
        pltpu.make_async_copy(own_w, w_all.at[:, me], keep_sem.at[4]),
    ]
    saves = [
        pltpu.make_async_copy(a, b, save_sem.at[j])
        for j, (a, b) in enumerate(
            ((q_ref, q_out), (k_ref, k_out), (v_ref, v_out), (cos_ref, cos_out), (sin_ref, sin_out))
        )
    ]

    @pl.when(i == 0)
    def _():
        loads = [
            pltpu.make_async_copy(ref, wqkv.at[j], load_sem.at[j])
            for j, ref in enumerate((wq_ref, wk_ref, wv_ref))
        ]
        share = own_w.shape[1]
        ours = pl.ds(pl.multiple_of(place * share, share), share)
        cuts = []
        for k, ref in enumerate((gate_ref, up_ref)):
            src = ref if share % 128 else ref.at[:, ours]
            cuts.append(pltpu.make_async_copy(src, columns.at[k], cut_sem.at[k]))
        for copy in loads + cuts:
            copy.start()

        barrier = pltpu.get_barrier_semaphore()
        for step in range(1, n):
            to = ring(n, step)
            pl.semaphore_signal(barrier, inc=1, device_id={"tensor": to}, device_id_type=MESH)
        pl.semaphore_signal(barrier, inc=1, device_id={"dp": sibling()}, device_id_type=MESH)
        for c in range(1, chips):
            to = same_core(c, chips)
            pl.semaphore_signal(barrier, inc=1, device_id={"dp": to}, device_id_type=MESH)

        values = tokens_ref[...].astype(F32)
        values = values - jnp.mean(values, axis=1, keepdims=True)
        inverse = lax.rsqrt(jnp.mean(values * values, axis=1, keepdims=True) + EPS)
        landed[me] = (values * inverse * gain_ref[...] + shift_ref[...]).astype(BF)

        pl.semaphore_wait(barrier, n - 1 + chips)

        for c in range(chunks):

            @pl.when(me < n - 1)
            def _():
                rightward(0, c).start()

            @pl.when(me > 0)
            def _():
                leftward(0, c).start()

        row = me * rows + lax.broadcasted_iota(jnp.int32, (rows, depth), 0)
        gb[...] = jnp.where(row < limit, ct_ref[...].astype(F32), 0.0).astype(BF)
        for c in range(1, chips):
            spread_gb(c).start()
        relay_gb(0).start()
        keeps[0].start()
        keeps[1].start()
        for copy in loads:
            copy.wait()

        cut = wp_ref.shape[0]
        here = pl.ds(pl.multiple_of(place * cut, cut), cut)
        first = lanes((cut, 128)) < HD
        for p in range(heads // 2):
            at = slice(p * 128, p * 128 + 128)
            query, key, value = (wqkv[j, here, at].astype(F32) for j in range(3))
            even = jnp.where(first, key, pltpu.roll(value, HD, 1))
            odd = jnp.where(first, pltpu.roll(key, HD, 1), value)
            for slot, values in ((2 * p, even), (2 * p + 1, odd), (heads + p, query)):
                wp_ref[:, slot * 128 : slot * 128 + 128] = values.astype(BF)

        lane = lanes((rows, 128))
        ones = jnp.where(lane < HD + 3, 1.0, 0.0)
        unit = jnp.where(lane == HD + 3, 1.0, 0.0)

        def put(out, here, values, extra):
            for head in range(heads):
                own = values[:, head // 2 * 128 : head // 2 * 128 + 128]
                own = pltpu.roll(own, HD, 1) if head % 2 else own
                out[head, here, :] = jnp.where(lane < HD, own, extra).astype(BF)

        def project(shard):
            here = pl.ds(pl.multiple_of(shard * rows, rows), rows)
            for j in range(rows // STEP):
                part = pl.ds(pl.multiple_of(shard * rows + j * STEP, STEP), STEP)
                coarse = pl.ds(shard * (rows // STEP) + j, 1)
                c0, s0 = coarse_ref[0, coarse, :], coarse_ref[1, coarse, :]
                cos_ref[part, :] = c0 * fine_ref[0] - s0 * fine_ref[1]
                sin_ref[part, :] = (s0 * fine_ref[0] + c0 * fine_ref[1]) * sign_ref[...]
            cosine = jnp.tile(cos_ref[here, :], (1, heads // 2))
            sine = jnp.tile(sin_ref[here, :], (1, heads // 2))
            x = landed[shard]
            row = shard * rows + lax.broadcasted_iota(jnp.int32, (rows, 128), 0)
            bias = jnp.where(lane == HD + 3, jnp.where(row < limit, 0.0, -1e30), ones)
            raw = dot(x, wqkv[0])
            turned = (raw * cosine + partner(raw) * sine).astype(BF).astype(F32)
            put(q_ref, here, turned * SCALE, unit)
            raw = dot(x, wqkv[1])
            put(k_ref, here, raw * cosine + partner(raw) * sine, bias)
            put(v_ref, here, dot(x, wqkv[2]), ones)

        for d in range(1, n + 1):
            for c in range(chunks):
                if d < n:

                    @pl.when(me >= d)
                    def _():
                        from_left(d, c).wait_recv()

                    @pl.when((me >= d) & (me < n - 1))
                    def _():
                        rightward(d, c).start()

                    @pl.when(me + d < n)
                    def _():
                        from_right(d, c).wait_recv()

                    @pl.when((me + d < n) & (me > 0))
                    def _():
                        leftward(d, c).start()

                if c == 0:

                    @pl.when(me >= d - 1)
                    def _():
                        save(me - d + 1).start()
                        project(me - d + 1)

                if c == 1 and d > 1:

                    @pl.when(me + d - 1 < n)
                    def _():
                        save(me + d - 1).start()
                        project(me + d - 1)

                if c == 2 and d == 1:
                    for cut in cuts:
                        cut.wait()
                    for k in range(2):
                        own_w[k] = columns[k].astype(F32).T.astype(BF)
                    keeps[4].start()

                if c == chunks - 1 and d == 2:
                    for near in range(1, chips // 2 + 1):
                        spread_gb(near).wait_recv()
                        relay_gb(near).start()

            if d < n:

                @pl.when((me < n - 1) & (me + 1 == d))
                def _():
                    for k in range(2):
                        w_right(0, k).start()

                @pl.when((me > 0) & (n - me == d))
                def _():
                    for k in range(2):
                        w_left(0, k).start()

        for copy in saves:
            copy.start()
        for step in range(n - 1):
            wo_over(step).start()
        for far in range(chips // 2 + 1, chips):
            spread_gb(far).wait_recv()
            relay_gb(far).start()

    stride = max((heads * n - 2) // max(n - 2, 1), 1)
    for d in range(1, n - 1):

        @pl.when(i == 1 + (d - 1) * stride)
        def _():
            for k in range(2):

                @pl.when((me >= d) & (me < n - 1))
                def _():
                    w_from_left(d, k).wait_recv()
                    w_right(d, k).start()

                @pl.when((me + d < n) & (me > 0))
                def _():
                    w_from_right(d, k).wait_recv()
                    w_left(d, k).start()

    @pl.when(i == heads)
    def _():
        for step in range(n - 1):
            wo_over(step).wait()
        keeps[1].wait()
        for c in range(1, chips):
            spread_wo(c).start()
        relay_wo(0).start()
        keeps[2].start()

    @pl.when(i == (n - 1) * heads)
    def _():
        for c in range(1, chips):
            spread_wo(c).wait_recv()
            relay_wo(c).start()

    owner = ring(n, s + 1)
    block = pl.ds(pl.multiple_of(owner * rows, rows), rows)
    scores = dot(q_ref[h, block, :], k_ref[h], NT)
    peak = jnp.max(scores, axis=1, keepdims=True)
    acc = dot(jnp.exp(scores - peak).astype(BF), v_ref[h])
    lane = lanes((rows, 128))
    total = jnp.sum(jnp.where(lane == HD, acc, 0.0), axis=1, keepdims=True)
    out = acc * (1.0 / total)
    odd = lax.rem(h, 2)
    out = jnp.where(odd == 1, pltpu.roll(out, HD, 1), out).astype(BF)
    pair = pl.ds(pl.multiple_of(h // 2 * 128, 128), 128)
    ctx_ref[block, pair] = jnp.where((lane >= HD) == (odd == 1), out, ctx_ref[block, pair])
    lse_ref[block, :] = jnp.where(lane == h, peak + jnp.log(total), lse_ref[block, :])

    @pl.when((h == heads - 1) & (s < n - 1))
    def _():
        push(s).start()

    @pl.when(i == steps - 1)
    def _():
        keeps[3].start()
        for d in range(n - 1):
            for c in range(chunks):

                @pl.when((me >= d) & (me < n - 1))
                def _():
                    rightward(d, c).wait_send()

                @pl.when((me + d < n) & (me > 0))
                def _():
                    leftward(d, c).wait_send()

            for k in range(2):

                @pl.when((me >= d) & (me < n - 1))
                def _():
                    w_right(d, k).wait_send()

                @pl.when((me + d < n) & (me > 0))
                def _():
                    w_left(d, k).wait_send()

        for k in range(2):
            for d in range(1, n):

                @pl.when((me >= d) & ((me == n - 1) | (d == n - 1)))
                def _():
                    w_from_left(d, k).wait_recv()

                @pl.when((me + d < n) & ((me == 0) | (d == n - 1)))
                def _():
                    w_from_right(d, k).wait_recv()

        for c in range(chips):
            relay_gb(c).wait()
            relay_wo(c).wait()
            if c:
                spread_gb(c).wait_send()
                spread_wo(c).wait_send()
        for shard in range(n):
            save(shard).wait()
        for copy in saves:
            copy.wait()
        for step in range(n - 1):
            push(step).wait()
        for j in (0, 2, 3, 4):
            keeps[j].wait()


def front(
    tokens, cotangent, gain, shift, tables, w_query, w_key, w_value, gate, up, w_out, limit, n, devices
):
    rows, depth = tokens.shape
    total = n * rows
    width = w_query.shape[1]
    heads = width // HD
    chips = devices // 2
    chunks = 4
    place = lax.axis_index("dp")
    share = gate.shape[1] // devices
    part = width // devices
    if share % 128:
        gate, up = (lax.dynamic_slice_in_dim(w, place * share, share, 1) for w in (gate, up))
    hbm = pl.BlockSpec(memory_space=pl.ANY)

    def whole(*shape):
        return pl.BlockSpec(shape, lambda *_: (0,) * len(shape), pipeline_mode=pl.Buffered(1))

    def dma(*shape):
        return pltpu.SemaphoreType.DMA(shape)

    head_array = jax.ShapeDtypeStruct((heads, total, 128), BF)
    table = jax.ShapeDtypeStruct((total, 128), F32)
    coarse, fine, sign = tables
    return pl.pallas_call(
        functools.partial(front_kernel, n, chips, chunks),
        out_shape=(
            jax.ShapeDtypeStruct((total, width), BF),
            table,
            jax.ShapeDtypeStruct((depth // devices, 3 * width), BF),
            head_array, head_array, head_array, table, table,
            jax.ShapeDtypeStruct((n, rows, depth), BF),
            jax.ShapeDtypeStruct((chips, 2, rows, depth), BF),
            jax.ShapeDtypeStruct((2, n, share, depth), BF),
            jax.ShapeDtypeStruct((n, rows, width), BF),
            jax.ShapeDtypeStruct((n, part, depth), BF),
            jax.ShapeDtypeStruct((n, devices, part, depth), BF),
        ),
        grid_spec=pltpu.PrefetchScalarGridSpec(
            num_scalar_prefetch=0,
            grid=(n * heads,),
            in_specs=[pl.BlockSpec(memory_space=pltpu.SMEM)]
            + [whole(rows, depth)] * 2
            + [whole(1, depth)] * 2
            + [whole(*coarse.shape), whole(*fine.shape), whole(*sign.shape)]
            + [hbm] * 6,
            out_specs=[whole(total, width), whole(total, 128), whole(depth // devices, 3 * width)]
            + [hbm] * 11,
            scratch_shapes=[
                pltpu.VMEM((n, rows, depth), BF),
                pltpu.VMEM((rows, depth), BF),
                pltpu.VMEM((2, depth, share), BF),
                pltpu.VMEM((2, share, depth), BF),
                pltpu.VMEM((3, depth, width), BF),
            ]
            + [pltpu.VMEM((heads, total, 128), BF)] * 3
            + [pltpu.VMEM((total, 128), F32)] * 2
            + [dma(n - 1, chunks)] * 4
            + [dma(chips)] * 4
            + [dma(n)]
            + [dma(n - 1, 2)] * 4
            + [dma(n - 1)] * 4
            + [dma(chips)] * 4
            + [dma(3), dma(3), dma(5), dma(5)],
        ),
        compiler_params=pltpu.CompilerParams(
            vmem_limit_bytes=60 << 20, collective_id=1, has_side_effects=True
        ),
        cost_estimate=pl.CostEstimate(
            flops=4 * total * total * 256 * heads * 3, bytes_accessed=40 << 20, transcendentals=0
        ),
        name="front",
    )(
        limit, tokens, cotangent, gain.reshape(1, depth), shift.reshape(1, depth), coarse, fine, sign,
        w_query, w_key, w_value, gate, up,
        lax.dynamic_slice_in_dim(w_out, place * part, part, 0),
    )


def att_bwd_kernel(
    n, bk, chips, ga_ref, wo_ref, parts_ref, pg_ref, q_hbm, k_hbm, v_hbm, ctx_hbm, lse_hbm,
    cos_hbm, sin_hbm, cown_hbm, pk_ref, own_ref, sums_ref, og_ref, pg_all,
    q_ref, k_ref, v_ref, ctx_ref, lse_ref, cos_ref, sin_ref, cown_ref, do, gc, dka, dva, dqs,
    og_full, og_own, og_mate, og_sib, og_land, og_piece, og_z,
    send_sem, recv_sem, out_send, out_recv, pk_send, pk_recv, keep_sem,
    om_send, om_recv, op_send, op_recv, oz_send, oz_recv, gs_send, gs_recv, gr_send, gr_recv, pg_sem, load_sem,
):
    i = pl.program_id(0)
    heads, total, _ = k_ref.shape
    h = jnp.where(i < heads, i, (i - heads) // (n - 1))
    t = jnp.where(i < heads, 0, lax.rem(i - heads, n - 1) + 1)
    rows = total // n
    me = lax.axis_index("tensor")
    place = lax.axis_index("dp")
    core = lax.rem(place, 2)
    bits = chips.bit_length() - 1
    share = og_ref.shape[0]
    mine = pl.ds(pl.multiple_of(me * rows, rows), rows)

    def push(step):
        return remote(
            gc.at[step], do.at[mine], send_sem.at[step], recv_sem.at[step], tensor=ring(n, step + 1)
        )

    def push_out(s):
        return remote(
            parts_ref.at[s], sums_ref.at[s - 1], out_send.at[s - 1], out_recv.at[s - 1],
            dp=same_core(s, chips),
        )

    def columns(slot):
        return pl.ds(pl.multiple_of(slot * 128, 128), 128)

    def push_pack(slot, step):
        owner = ring(n, step + 1)
        return remote(
            pk_ref.at[pl.ds(pl.multiple_of(owner * rows, rows), rows), columns(slot)],
            own_ref.at[me, :, columns(slot)],
            pk_send.at[slot, step], pk_recv.at[slot, step], tensor=owner,
        )

    def keep(slot):
        return pltpu.make_async_copy(
            pk_ref.at[mine, columns(slot)], own_ref.at[me, :, columns(slot)], keep_sem.at[slot]
        )

    far = (q_hbm, k_hbm, v_hbm, ctx_hbm, lse_hbm, cos_hbm, sin_hbm, cown_hbm)
    near = (q_ref, k_ref, v_ref, ctx_ref, lse_ref, cos_ref, sin_ref, cown_ref)
    loads = [pltpu.make_async_copy(a, b, load_sem.at[j]) for j, (a, b) in enumerate(zip(far, near))]

    @pl.when(i == 0)
    def _():
        for load in loads:
            load.start()
        greet(n, chips, True)

        def send(step, carry):
            gc[step] = dot(ga_ref[...], wo_ref[ring(n, step + 1)], NT).astype(BF)
            push(step).start()
            return carry

        lax.fori_loop(0, n - 1, send, 0)
        do[mine, :] = dot(ga_ref[...], wo_ref[me], NT).astype(BF)
        for load in loads:
            load.wait()

    def pg_spread(s):
        return remote(pg_ref, pg_all.at[place], gs_send.at[s], gs_recv.at[s], dp=same_core(s, chips))

    def pg_relay(s):
        there = pg_all.at[differ(place // 2, s, bits) * 2 + core]
        return remote(there if s else pg_ref, there, gr_send.at[s], gr_recv.at[s], dp=sibling())

    def pg_keep():
        return pltpu.make_async_copy(pg_ref, pg_all.at[place], pg_sem)

    @pl.when(i == heads * n - 8)
    def _():
        for s in range(1, chips):
            pg_spread(s).start()
        pg_relay(0).start()
        pg_keep().start()

    def og_swap():
        return remote(og_mate, og_sib, om_send, om_recv, dp=sibling())

    def og_push(s):
        return remote(og_sib.at[s], og_land.at[s], op_send.at[s], op_recv.at[s], dp=same_core(s, chips))

    def og_over(step):
        to = ring(n, step + 1)
        return remote(og_piece.at[to], og_z.at[me], oz_send.at[step], oz_recv.at[step], tensor=to)

    @pl.when(i == 1)
    def _():
        def term(part, carry):
            og_full[...] = dot(cown_ref[part], ga_ref[...], TN)
            for s in range(chips):
                start = differ(place // 2, s, bits) * 2
                here = pl.ds(pl.multiple_of((start + core) * share, share), share)
                there = pl.ds(pl.multiple_of((start + 1 - core) * share, share), share)
                og_own[s, part] = og_full[here, :]
                og_mate[s, part] = og_full[there, :].astype(BF)
            return carry

        lax.fori_loop(0, n, term, 0)
        og_swap().start()

    @pl.when(i == 2)
    def _():
        og_swap().wait_recv()
        for s in range(chips):
            og_sib[s] = (og_own[s] + og_sib[s].astype(F32)).astype(BF)
            if s:
                og_push(s).start()

    @pl.when(i == heads * n - 6)
    def _():
        joined = og_sib[0].astype(F32)
        for s in range(1, chips):
            og_push(s).wait_recv()
            joined = joined + og_land[s].astype(F32)
        og_piece[...] = joined.astype(BF)
        for step in range(n - 1):
            og_over(step).start()

    @pl.when(i == heads + 1)
    def _():
        for s in range(1, chips):
            push_out(s).start()

    @pl.when(i == heads * n - 1)
    def _():
        og_z[me] = og_piece[me]
        for step in range(n - 1):
            og_over(step).wait_recv()
        joined = og_z[0].astype(F32)
        for part in range(1, n):
            joined = joined + og_z[part].astype(F32)
        og_ref[...] = joined.astype(BF)

    @pl.when((h == 0) & (t > 0))
    def _():
        push(t - 1).wait_recv()

    source = ring(n, n - t)
    block = pl.ds(pl.multiple_of(source * rows, rows), rows)
    pair = columns(h // 2)
    odd = lax.rem(h, 2) == 1
    lane = lanes((rows, 128))
    off = lane - HD
    logsum = jnp.sum(jnp.where(lane == h, lse_ref[block, :], 0.0), axis=1, keepdims=True)
    a, b, c = split3(-logsum)
    q = q_ref[h, block, :].astype(F32)
    q = jnp.where(off == 0, a, jnp.where(off == 1, b, jnp.where(off == 2, c, q))).astype(BF)
    g = jnp.where((lane >= HD) == odd, do[block, pair].astype(F32), 0.0)
    delta = jnp.sum(g * ctx_ref[block, pair].astype(F32), axis=1, keepdims=True)
    a, b, c = split3(-delta)
    g = jnp.where(odd, pltpu.roll(g, HD, 1), g)
    g = jnp.where(off == 0, a, jnp.where(off == 1, b, jnp.where(off == 2, c, g))).astype(BF)
    acc = jnp.zeros((rows, 128), F32)
    for j in range(total // bk):
        rk = pl.ds(j * bk, bk)
        kt = k_ref[h, rk, :]
        probs = jnp.exp(dot(kt, q, NT))
        grad = (probs * dot(v_ref[h, rk, :], g, NT)).astype(BF)
        for sums, term in ((dva, dot(probs.astype(BF), g)), (dka, dot(grad, q))):
            before = jnp.where(t == 0, jnp.zeros_like(term), sums[h, rk, :])
            sums[h, rk, :] = before + term
        acc = acc + dot(grad, kt, TN)
    acc = acc * SCALE

    @pl.when(jnp.logical_not(odd))
    def _():
        dqs[block, :] = acc

    @pl.when(odd)
    def _():
        grad = jnp.where(lane < HD, dqs[block, :], pltpu.roll(acc, HD, 1))
        grad = grad * cos_ref[block, :] - partner(grad) * sin_ref[block, :]
        pk_ref[block, columns(heads + h // 2)] = grad.astype(BF)

    @pl.when(odd & (t == 0))
    def _():
        keep(heads + h // 2).start()

    @pl.when(odd & (t > 0))
    def _():
        push_pack(heads + h // 2, n - 1 - t).start()

    @pl.when(t == n - 1)
    def _():
        dk = dka[h]
        dk = dk * cos_ref[...] - partner(dk) * sin_ref[...]
        both = jnp.where(lanes((total, 128)) < HD, dk, pltpu.roll(dva[h], HD, 1))
        pk_ref[:, columns(h)] = both.astype(BF)
        for step in range(n - 1):
            push_pack(h, step).start()
        keep(h).start()

    @pl.when(i == heads * n - 1)
    def _():
        for s in range(1, chips):
            pg_spread(s).wait_recv()
            pg_relay(s).start()
        for step in range(n - 1):
            push(step).wait_send()
        for s in range(1, chips):
            push_out(s).wait()
        og_swap().wait_send()
        pg_keep().wait()
        for s in range(chips):
            pg_relay(s).wait()
            if s:
                pg_spread(s).wait_send()
        for s in range(1, chips):
            og_push(s).wait_send()
        for step in range(n - 1):
            og_over(step).wait_send()
        for slot in range(heads + heads // 2):
            keep(slot).wait()
            for step in range(n - 1):
                push_pack(slot, step).wait()


def att_bwd(
    grad_attn, w_out, ctx_own, parts, pair_grads, q, k, v, ctx, lse, cosine, sine, n, bk=512
):
    heads, total, _ = q.shape
    width = heads * HD
    rows, depth = grad_attn.shape
    chips = parts.shape[0]
    share = width // (2 * chips)
    slots = heads + heads // 2
    hbm = pl.BlockSpec(memory_space=pl.ANY)

    def whole(*shape):
        return pl.BlockSpec(shape, lambda *_: (0,) * len(shape), pipeline_mode=pl.Buffered(1))

    return pl.pallas_call(
        functools.partial(att_bwd_kernel, n, bk, chips),
        out_shape=(
            jax.ShapeDtypeStruct((total, slots * 128), BF),
            jax.ShapeDtypeStruct((n, rows, slots * 128), BF),
            jax.ShapeDtypeStruct((chips - 1, rows, depth), BF),
            jax.ShapeDtypeStruct((share, depth), BF),
            jax.ShapeDtypeStruct((2 * chips, *pair_grads.shape), BF),
        ),
        grid_spec=pltpu.PrefetchScalarGridSpec(
            num_scalar_prefetch=0,
            grid=(heads * n,),
            in_specs=[whole(rows, depth), whole(n, width, depth)] + [hbm] * 10,
            out_specs=[whole(total, slots * 128), hbm, hbm, whole(share, depth), hbm],
            scratch_shapes=[pltpu.VMEM((heads, total, 128), BF)] * 3
            + [pltpu.VMEM((total, width), BF)]
            + [pltpu.VMEM((total, 128), F32)] * 3
            + [pltpu.VMEM((n, rows, width), BF)]
            + [
                pltpu.VMEM((total, width), BF),
                pltpu.VMEM((n - 1, rows, width), BF),
            ]
            + [pltpu.VMEM((heads, total, 128), F32)] * 2
            + [pltpu.VMEM((total, 128), F32)]
            + [
                pltpu.VMEM((width, depth), F32),
                pltpu.VMEM((chips, n, share, depth), F32),
                pltpu.VMEM((chips, n, share, depth), BF),
                pltpu.VMEM((chips, n, share, depth), BF),
                pltpu.VMEM((chips, n, share, depth), BF),
                pltpu.VMEM((n, share, depth), BF),
                pltpu.VMEM((n, share, depth), BF),
            ]
            + [pltpu.SemaphoreType.DMA((n - 1,))] * 2
            + [pltpu.SemaphoreType.DMA((chips - 1,))] * 2
            + [pltpu.SemaphoreType.DMA((slots, n - 1))] * 2
            + [pltpu.SemaphoreType.DMA((slots,))]
            + [pltpu.SemaphoreType.DMA] * 2
            + [pltpu.SemaphoreType.DMA((chips,))] * 2
            + [pltpu.SemaphoreType.DMA((n - 1,))] * 2
            + [pltpu.SemaphoreType.DMA((chips,))] * 4
            + [pltpu.SemaphoreType.DMA, pltpu.SemaphoreType.DMA((8,))],
        ),
        compiler_params=pltpu.CompilerParams(
            vmem_limit_bytes=60 << 20, collective_id=2, has_side_effects=True
        ),
        cost_estimate=pl.CostEstimate(
            flops=10 * total * total * 256 * heads,
            bytes_accessed=20 * total * width,
            transcendentals=total * total * heads,
        ),
        name="att_bwd",
    )(grad_attn, w_out, parts, pair_grads, q, k, v, ctx, lse, cosine, sine, ctx_own)


def finish_kernel(
    chips, n, x_ref, pk_ref, own_hbm, w_hbm, tokens_hbm, middle_hbm, gain_ref, vec_ref,
    input_ref, sums_ref, every,
    own_ref, w_ref, tokens_ref, middle_ref, full, mate, sib, land, fin, vec_z, vec_dp, vec_me,
    sx_send, sx_recv, rs_send, rs_recv, ag_send, ag_recv, rl_send, rl_recv,
    vz_send, vz_recv, vd_send, vd_recv, own_sem, load_sem,
):
    bits = chips.bit_length() - 1
    me = lax.axis_index("dp")
    place = lax.axis_index("tensor")
    core = lax.rem(me, 2)
    chip = me // 2
    other = 1 - core
    piece = fin.shape[0]

    def swap(s):
        return remote(mate.at[s], sib.at[s], sx_send.at[s], sx_recv.at[s], dp=chip * 2 + other)

    def push(s):
        return remote(sib.at[s], land.at[s], rs_send.at[s], rs_recv.at[s], dp=same_core(s, chips))

    def spread(s):
        return remote(
            fin, every.at[chip, core], ag_send.at[s], ag_recv.at[s], dp=same_core(s, chips)
        )

    def relay(s):
        src = every.at[differ(chip, s, bits), core]
        return remote(src, src, rl_send.at[s], rl_recv.at[s], dp=chip * 2 + other)

    def vec_over(step):
        return remote(
            vec_me.at[0], vec_z.at[place], vz_send.at[step], vz_recv.at[step], tensor=ring(n, step + 1)
        )

    def vec_across(step):
        return remote(
            vec_me.at[1], vec_dp.at[me], vd_send.at[step], vd_recv.at[step],
            dp=lax.rem(me + step + 1, 2 * chips),
        )

    far = (own_hbm, w_hbm, tokens_hbm, middle_hbm)
    near = (own_ref, w_ref, tokens_ref, middle_ref)
    loads = [pltpu.make_async_copy(a, b, load_sem.at[j]) for j, (a, b) in enumerate(zip(far, near))]
    for load in loads:
        load.start()
    barrier = pltpu.get_barrier_semaphore()
    for step in range(n - 1):
        pl.semaphore_signal(barrier, inc=1, device_id={"tensor": ring(n, step + 1)}, device_id_type=MESH)
    for step in range(2 * chips - 1):
        to = lax.rem(me + step + 1, 2 * chips)
        pl.semaphore_signal(barrier, inc=1, device_id={"dp": to}, device_id_type=MESH)

    full[...] = dot(x_ref[...], pk_ref[...], TN)
    pl.semaphore_wait(barrier, n + 2 * chips - 2)

    def part(s, which):
        start = (differ(chip, s, bits) * 2 + which) * piece
        return full[pl.ds(pl.multiple_of(start, piece), piece), :]

    for s in range(chips):
        mate[s] = part(s, other).astype(BF)
        swap(s).start()

    for load in loads:
        load.wait()
    grad = jnp.zeros(input_ref.shape, F32)
    for t in range(n):
        w = w_ref[:, t].reshape(w_ref.shape[0] * w_ref.shape[2], w_ref.shape[3])
        grad = grad + dot(own_ref[t], w, NT).astype(BF).astype(F32)

    for s in range(1, chips):
        swap(s).wait_recv()
        sib[s] = (sib[s].astype(F32) + part(s, core)).astype(BF)
        push(s).start()
    swap(0).wait_recv()
    total = sib[0].astype(F32) + part(0, core)

    values = tokens_ref[...].astype(F32)
    values = values - jnp.mean(values, axis=1, keepdims=True)
    inverse = lax.rsqrt(jnp.mean(values * values, axis=1, keepdims=True) + EPS)
    scaled = values * inverse
    through = grad * gain_ref[...]
    inner = through - jnp.mean(through, axis=1, keepdims=True)
    inner = inner - scaled * jnp.mean(through * scaled, axis=1, keepdims=True)
    input_ref[...] = middle_ref[...] + inverse * inner
    vec_me[0, 0:1] = jnp.sum(grad * scaled, axis=0, keepdims=True)
    vec_me[0, 1:2] = jnp.sum(grad, axis=0, keepdims=True)
    vec_me[0, 2:4] = vec_ref[...]
    vec_me[0, 4:8] = jnp.zeros((4, vec_ref.shape[1]), F32)
    vec_z[place] = vec_me[0]
    for step in range(n - 1):
        vec_over(step).start()

    for s in range(1, chips):
        push(s).wait_recv()
        total = total + land[s].astype(F32)
    fin[...] = total.astype(BF)
    for s in range(1, chips):
        spread(s).start()
    mine = pltpu.make_async_copy(fin, every.at[chip, core], own_sem)
    mine.start()
    mine.wait()
    relay(0).start()

    for step in range(n - 1):
        vec_over(step).wait()
    vec = vec_z[0]
    for t in range(1, n):
        vec = vec + vec_z[t]
    vec_me[1] = vec
    vec_dp[me] = vec
    for step in range(2 * chips - 1):
        vec_across(step).start()
    for s in range(1, chips):
        spread(s).wait_recv()
        relay(s).start()
    for step in range(2 * chips - 1):
        vec_across(step).wait()
    vec = vec_dp[0]
    for t in range(1, 2 * chips):
        vec = vec + vec_dp[t]
    sums_ref[...] = vec
    for s in range(chips):
        relay(s).wait()
        swap(s).wait_send()
        if s > 0:
            spread(s).wait_send()
            push(s).wait_send()


def finish(rows_all, packed, own, w_all, tokens, middle, gain, vec, devices):
    n, rows, packs = own.shape
    depth = tokens.shape[1]
    chips = devices // 2
    piece = depth // devices
    vmem = pl.BlockSpec(memory_space=pltpu.VMEM)
    return pl.pallas_call(
        functools.partial(finish_kernel, chips, n),
        out_shape=(
            jax.ShapeDtypeStruct((rows, depth), F32),
            jax.ShapeDtypeStruct((8, depth), F32),
            jax.ShapeDtypeStruct((chips, 2, piece, packs), BF),
        ),
        in_specs=[vmem] * 2 + [pl.BlockSpec(memory_space=pl.ANY)] * 4 + [vmem] * 2,
        out_specs=[vmem, vmem, pl.BlockSpec(memory_space=pl.ANY)],
        scratch_shapes=[
            pltpu.VMEM(own.shape, BF),
            pltpu.VMEM(w_all.shape, BF),
            pltpu.VMEM((rows, depth), BF),
            pltpu.VMEM((rows, depth), F32),
            pltpu.VMEM((depth, packs), F32),
            pltpu.VMEM((chips, piece, packs), BF),
            pltpu.VMEM((chips, piece, packs), BF),
            pltpu.VMEM((chips, piece, packs), BF),
            pltpu.VMEM((piece, packs), BF),
            pltpu.VMEM((n, 8, depth), F32),
            pltpu.VMEM((devices, 8, depth), F32),
            pltpu.VMEM((2, 8, depth), F32),
        ]
        + [pltpu.SemaphoreType.DMA((chips,))] * 8
        + [pltpu.SemaphoreType.DMA((n - 1,))] * 2
        + [pltpu.SemaphoreType.DMA((devices - 1,))] * 2
        + [pltpu.SemaphoreType.DMA, pltpu.SemaphoreType.DMA((4,))],
        compiler_params=pltpu.CompilerParams(
            vmem_limit_bytes=56 << 20, collective_id=4, has_side_effects=True
        ),
        cost_estimate=pl.CostEstimate(
            flops=4 * n * rows * depth * packs, bytes_accessed=20 << 20, transcendentals=0
        ),
        name="finish",
    )(rows_all, packed, own, w_all, tokens, middle, gain.reshape(1, depth), vec)


def ffn_kernel(
    chips, x_ref, gb_ref, w_ref, down_ref, wp_ref, dx_ref, out_ref, dw_ref, zs_ref, wp_z,
    rows_all, gb, hid, gate_g, up_g, own, sib, mate, partial, z_left, z_right, wd,
    ag_send, ag_recv, rl_send, rl_recv, sx_send, sx_recv, rs_send, rs_recv, fw_send, fw_recv,
    gb_sem, out_sem, dx_sem, wp_send, wp_recv, wp_sem, zr_send, zr_recv, zl_send, zl_recv,
    dr_send, dr_recv, dl_send, dl_recv, wd_sem,
):
    bits = chips.bit_length() - 1
    me = lax.axis_index("dp")
    core = lax.rem(me, 2)
    chip = me // 2
    other = 1 - core
    rows, depth = x_ref.shape
    n, share, _ = dw_ref.shape

    def spread(s):
        to = differ(chip, s, bits) * 2 + core
        return remote(x_ref, rows_all.at[chip, core], ag_send.at[s], ag_recv.at[s], dp=to)

    square = chips == 4

    def hand_on(s):
        half = pl.ds((s - 1) * (rows // 2), rows // 2)
        part = rows_all.at[differ(chip, s, bits), core, half]
        to = differ(chip, 3 - s, bits) * 2 + core
        return remote(part, part, fw_send.at[s], fw_recv.at[s], dp=to)

    def handed(s):
        half = pl.ds((s - 1) * (rows // 2), rows // 2)
        part = rows_all.at[differ(chip, 3, bits), core, half]
        to = differ(chip, 3 - s, bits) * 2 + core
        return remote(part, part, fw_send.at[s], fw_recv.at[s], dp=to)

    def relay(s):
        src = differ(chip, s, bits)
        return remote(
            rows_all.at[src, core], rows_all.at[src, core], rl_send.at[s], rl_recv.at[s],
            dp=chip * 2 + other,
        )

    def swap(s):
        return remote(
            mate.at[lax.rem(s, 2)], sib.at[s], sx_send.at[s], sx_recv.at[s], dp=chip * 2 + other
        )

    def push(s):
        to = differ(chip, s, bits) * 2 + core
        return remote(sib.at[s, 0], dx_ref.at[s], rs_send.at[s], rs_recv.at[s], dp=to)

    def fetch(s):
        src = differ(chip, s, bits)
        return pltpu.make_async_copy(gb_ref.at[src], gb.at[src], gb_sem.at[s])

    part = lax.axis_index("tensor")

    def over(step):
        return remote(
            wp_ref, wp_z.at[part], wp_send.at[step], wp_recv.at[step], tensor=ring(n, step + 1)
        )

    def keep(s):
        return pltpu.make_async_copy(sib.at[s, 1], out_ref.at[s], out_sem.at[s])

    ours = pl.ds(pl.multiple_of(me * share, share), share)
    cut = pltpu.make_async_copy(down_ref.at[ours], wd.at[part], wd_sem)
    cut.start()
    for s in range(chips):
        fetch(s).start()
    barrier = pltpu.get_barrier_semaphore()
    for step in range(1, n):
        pl.semaphore_signal(barrier, inc=1, device_id={"tensor": ring(n, step)}, device_id_type=MESH)
    pl.semaphore_signal(barrier, inc=1, device_id={"dp": chip * 2 + other}, device_id_type=MESH)
    for s in range(1, chips):
        to = differ(chip, s, bits) * 2 + core
        pl.semaphore_signal(barrier, inc=1, device_id={"dp": to}, device_id_type=MESH)
    pl.semaphore_wait(barrier, chips + n - 1)
    direct = range(1, 3) if square else range(1, chips)
    for s in direct:
        spread(s).start()
    mine = pltpu.make_async_copy(x_ref, rows_all.at[chip, core], ag_send.at[0])
    mine.start()
    mine.wait()
    relay(0).start()
    keep_wp = pltpu.make_async_copy(wp_ref, wp_z.at[part], wp_sem)
    keep_wp.start()

    def d_right(d):
        there = wd.at[part - d]
        return remote(there, there, dr_send.at[d], dr_recv.at[d], tensor=part + 1)

    def d_left(d):
        there = wd.at[part + d]
        return remote(there, there, dl_send.at[d], dl_recv.at[d], tensor=part - 1)

    def d_from_left(d):
        there = wd.at[part - d]
        return remote(there, there, dr_send.at[d - 1], dr_recv.at[d - 1], tensor=part - 1)

    def d_from_right(d):
        there = wd.at[part + d]
        return remote(there, there, dl_send.at[d - 1], dl_recv.at[d - 1], tensor=part + 1)

    cut.wait()
    for d in range(n):
        if d:

            @pl.when(part >= d)
            def _():
                d_from_left(d).wait_recv()

        if d < n - 1:

            @pl.when((part >= d) & (part < n - 1))
            def _():
                d_right(d).start()

        if d:

            @pl.when(part + d < n)
            def _():
                d_from_right(d).wait_recv()

        if d < n - 1:

            @pl.when((part + d < n) & (part > 0))
            def _():
                d_left(d).start()

    for step in range(n - 1):
        over(step).start()

    def shard(src, which, put):
        x = rows_all[src, which]
        grad = gb[src, which]
        gate = dot(x, w_ref[0], NT)
        upper = dot(x, w_ref[1], NT)
        w_down = wd[...].reshape(n * share, depth)
        grad_hidden = dot(grad, w_down, NT)
        sigma = jax.nn.sigmoid(gate)
        act = gate * sigma
        hidden = (act * upper).astype(BF)
        grad_gate = (grad_hidden * upper * sigma * (1.0 + gate * (1.0 - sigma))).astype(BF)
        grad_upper = (grad_hidden * act).astype(BF)
        hid[src, which] = hidden
        gate_g[src, which] = grad_gate
        up_g[src, which] = grad_upper
        put[0] = (dot(grad_gate, w_ref[0]) + dot(grad_upper, w_ref[1])).astype(BF)
        put[1] = dot(hidden, w_down).astype(BF)

    def step(s, carry):
        src = differ(chip, s, bits)
        slot = lax.rem(s, 2)
        relay(s).wait_recv()
        fetch(s).wait()

        @pl.when(s >= 2)
        def _():
            swap(s - 2).wait_send()

        shard(src, other, mate.at[slot])
        swap(s).start()
        shard(src, core, own)
        swap(s).wait_recv()
        for k in range(2):
            sib[s, k] = (sib[s, k].astype(F32) + own[k].astype(F32)).astype(BF)

        @pl.when(s > 0)
        def _():
            push(s).start()

        keep(s).start()

        if not square:

            @pl.when(s < chips - 1)
            def _():
                spread(s + 1).wait_recv()
                relay(s + 1).start()

        if square:

            @pl.when(s == 1)
            def _():
                handed(1).wait_recv()
                handed(2).wait_recv()
                relay(3).start()

        return carry

    if square:
        for near in (1, 2):
            spread(near).wait_recv()
            hand_on(near).start()
            relay(near).start()
    lax.fori_loop(0, chips, step, 0)
    first = pltpu.make_async_copy(sib.at[0, 0], dx_ref.at[0], dx_sem)
    first.start()
    def zr(t, k, to):
        return remote(
            partial.at[t, k], z_left.at[t, k], zr_send.at[t, k], zr_recv.at[t, k], tensor=to
        )

    def zl(t, k, to):
        return remote(
            partial.at[t, k], z_right.at[t, k], zl_send.at[t, k], zl_recv.at[t, k], tensor=to
        )

    def join(t, k, more):
        partial[t, k] = (partial[t, k].astype(F32) + more[t, k].astype(F32)).astype(BF)

    def weight_grad(left, right):
        left = left[...].reshape(-1, n * share)
        return dot(left, right[...].reshape(-1, depth), TN)

    def hand_along(k):
        for j in range(n - 1):
            t = n - 1 - j

            @pl.when((part > 0) & (part < t))
            def _():
                zr(t, k, part + 1).wait_recv()
                join(t, k, z_left)
                zr(t, k, part + 1).start()

            @pl.when((part < n - 1) & (part > j))
            def _():
                zl(j, k, part - 1).wait_recv()
                join(j, k, z_right)
                zl(j, k, part - 1).start()

    for k, left in enumerate((gate_g, up_g)):
        grad = weight_grad(left, rows_all)
        for t in range(n):
            partial[t, k] = grad[t * share : (t + 1) * share, :].astype(BF)

        for j in range(n - 1):

            @pl.when(part == 0)
            def _():
                zr(n - 1 - j, k, 1).start()

            @pl.when(part == n - 1)
            def _():
                zl(j, k, n - 2).start()

    hand_along(0)
    grad = weight_grad(hid, gb)
    for t in range(n):
        dw_ref[t] = grad[t * share : (t + 1) * share, :].astype(BF)
    hand_along(1)
    for k in range(2):
        for t in range(n):

            @pl.when((part == t) & (part > 0))
            def _():
                zr(t, k, part - 1).wait_recv()
                join(t, k, z_left)

            @pl.when((part == t) & (part < n - 1))
            def _():
                zl(t, k, part + 1).wait_recv()
                join(t, k, z_right)

            @pl.when(part == t)
            def _():
                zs_ref[k] = partial[t, k]

            @pl.when(part < t)
            def _():
                zr(t, k, part + 1).wait_send()

            @pl.when(part > t)
            def _():
                zl(t, k, part - 1).wait_send()

    for d in range(n - 1):

        @pl.when((part >= d) & (part < n - 1))
        def _():
            d_right(d).wait_send()

        @pl.when((part + d < n) & (part > 0))
        def _():
            d_left(d).wait_send()

    first.wait()
    keep_wp.wait()
    for step in range(n - 1):
        over(step).wait()
    for s in range(chips):
        keep(s).wait()
        relay(s).wait_send()
        if s >= chips - 2:
            swap(s).wait_send()
        if s in direct:
            spread(s).wait_send()
        if s > 0:
            push(s).wait()
    if square:
        hand_on(1).wait_send()
        hand_on(2).wait_send()


def ffn(x, grad_branch, weights, down, w_packed, n, devices):
    rows, depth = x.shape
    chips = devices // 2
    hidden = weights.shape[1]
    share = hidden // n
    vmem = pl.BlockSpec(memory_space=pltpu.VMEM)
    hbm = pl.BlockSpec(memory_space=pl.ANY)
    return pl.pallas_call(
        functools.partial(ffn_kernel, chips),
        out_shape=(
            jax.ShapeDtypeStruct((chips, rows, depth), BF),
            jax.ShapeDtypeStruct((chips, rows, depth), BF),
            jax.ShapeDtypeStruct((n, share, depth), BF),
            jax.ShapeDtypeStruct((2, share, depth), BF),
            jax.ShapeDtypeStruct((n, *w_packed.shape), BF),
        ),
        in_specs=[vmem, hbm, vmem, hbm, hbm],
        out_specs=[hbm, hbm, vmem, vmem, hbm],
        scratch_shapes=[
            pltpu.VMEM((chips, 2, rows, depth), BF),
            pltpu.VMEM((chips, 2, rows, depth), BF),
        ]
        + [pltpu.VMEM((chips, 2, rows, hidden), BF)] * 3
        + [
            pltpu.VMEM((2, rows, depth), BF),
            pltpu.VMEM((chips, 2, rows, depth), BF),
            pltpu.VMEM((2, 2, rows, depth), BF),
        ]
        + [pltpu.VMEM((n, 2, share, depth), BF)] * 3
        + [pltpu.VMEM((n, share, depth), BF)]
        + [pltpu.SemaphoreType.DMA((chips,))] * 8
        + [pltpu.SemaphoreType.DMA((3,))] * 2
        + [pltpu.SemaphoreType.DMA((chips,))] * 2
        + [pltpu.SemaphoreType.DMA]
        + [pltpu.SemaphoreType.DMA((n - 1,))] * 2
        + [pltpu.SemaphoreType.DMA]
        + [pltpu.SemaphoreType.DMA((n, 2))] * 4
        + [pltpu.SemaphoreType.DMA((n - 1,))] * 4
        + [pltpu.SemaphoreType.DMA],
        compiler_params=pltpu.CompilerParams(
            vmem_limit_bytes=62 << 20, collective_id=3, has_side_effects=True
        ),
        cost_estimate=pl.CostEstimate(
            flops=2 * 9 * devices * rows * depth * hidden, bytes_accessed=30 << 20, transcendentals=0
        ),
        name="ffn",
    )(x, grad_branch, weights, down, w_packed)


def unpack_kernel(
    share, pair_ref, rest_ref, pack_ref, input_ref, sums_ref, gate_ref, up_ref, down_ref, out_ref,
    q_ref, k_ref, v_ref, grad_ref, *vector_refs,
):
    grad_ref[...] = input_ref[...]
    for i, vector_ref in enumerate(vector_refs):
        vector_ref[...] = sums_ref[i]
    gate_ref[...] = pair_ref[0, 0].astype(F32).T
    up_ref[...] = pair_ref[0, 1].astype(F32).T
    rest = rest_ref[0].astype(F32)
    down_ref[...] = rest[:share]
    out_ref[...] = rest[share:]
    pack = pack_ref[0].astype(F32)
    pairs = q_ref.shape[1] // 128
    first = lanes((pack.shape[0], 128)) < HD
    for p in range(pairs):
        even = pack[:, p * 256 : p * 256 + 128]
        odd = pack[:, p * 256 + 128 : p * 256 + 256]
        out = slice(p * 128, p * 128 + 128)
        q_ref[:, out] = pack[:, (2 * pairs + p) * 128 : (2 * pairs + p + 1) * 128]
        k_ref[:, out] = jnp.where(first, even, pltpu.roll(odd, HD, 1))
        v_ref[:, out] = jnp.where(first, pltpu.roll(even, HD, 1), odd)


def unpack(pair, rest, pack, input_grad, sums):
    devices, _, share, depth = pair.shape
    hidden = devices * share
    height = rest.shape[1]
    width = devices * (height - share)
    piece = depth // devices
    if share % 128:
        down = rest[:, :share].reshape(hidden, depth).astype(F32)
        gate, up = (pair[:, k].reshape(hidden, depth).astype(F32).T for k in range(2))
        pack = pack.reshape(depth, 3 * width).astype(F32)
        both = pack[:, : 2 * width].reshape(depth, width // HD, 2, HD)
        key, value = (both[:, :, k].reshape(depth, width) for k in range(2))
        out = rest[:, share:].reshape(width, depth).astype(F32)
        vectors = (sums[i] for i in range(4))
        return gate, up, down, out, pack[:, 2 * width :], key, value, input_grad, *vectors
    column = pl.BlockSpec((depth, share), lambda i: (0, i))
    rows = pl.BlockSpec((piece, width), lambda i: (i, 0))
    part = pl.BlockSpec((input_grad.shape[0] // devices, depth), lambda i: (i, 0))
    vector = pl.BlockSpec((depth,), lambda i: (0,))
    return pl.pallas_call(
        functools.partial(unpack_kernel, share),
        out_shape=(jax.ShapeDtypeStruct((depth, hidden), F32),) * 2
        + (
            jax.ShapeDtypeStruct((hidden, depth), F32),
            jax.ShapeDtypeStruct((width, depth), F32),
        )
        + (jax.ShapeDtypeStruct((depth, width), F32),) * 3
        + (jax.ShapeDtypeStruct(input_grad.shape, F32),)
        + (jax.ShapeDtypeStruct((depth,), F32),) * 4,
        grid=(devices,),
        in_specs=[
            pl.BlockSpec((1, 2, share, depth), lambda i: (i, 0, 0, 0)),
            pl.BlockSpec((1, height, depth), lambda i: (i, 0, 0)),
            pl.BlockSpec((1, piece, 3 * width), lambda i: (i, 0, 0)),
            part,
            pl.BlockSpec(sums.shape, lambda i: (0, 0)),
        ],
        out_specs=[
            column, column, pl.BlockSpec((share, depth), lambda i: (i, 0)),
            pl.BlockSpec((height - share, depth), lambda i: (i, 0)), rows, rows, rows,
            part, vector, vector, vector, vector,
        ],
        compiler_params=pltpu.CompilerParams(vmem_limit_bytes=62 << 20),
        name="unpack",
    )(pair, rest, pack, input_grad, sums)


def norm_parts(values):
    centre = jnp.mean(values, axis=-1, keepdims=True)
    centred = values - centre
    inverse = lax.rsqrt(jnp.mean(centred * centred, axis=-1, keepdims=True) + EPS)
    return centred * inverse, inverse


def norm_back(upstream, scaled, inverse, gain):
    through = upstream * gain
    inner = (
        through
        - jnp.mean(through, axis=-1, keepdims=True)
        - scaled * jnp.mean(through * scaled, axis=-1, keepdims=True)
    )
    return inverse * inner, jnp.sum(upstream * scaled, axis=0), jnp.sum(upstream, axis=0)


def on_device(
    tokens, lengths, ln1_gain, ln1_bias, w_query, w_key, w_value, w_out,
    ln2_gain, ln2_bias, w_gate, w_up, down_weight, cotangent,
):
    n = lax.axis_size("tensor")
    local_rows, depth = tokens.shape
    length = local_rows * n
    width = w_query.shape[1]
    row_ids = lax.axis_index("tensor") * local_rows + lax.iota(jnp.int32, local_rows)
    valid = (row_ids < lengths[0])[:, None]

    inputs = tokens.astype(F32)
    grad_out = jnp.where(valid, cotangent.astype(F32), 0.0)
    devices = lax.axis_size("dp")
    place = lax.axis_index("dp")
    share = w_gate.shape[1] // devices

    (
        context, logsum, w_packed, q, k, v, cosine, sine, attn_rows, grad_branch, weights, context_own, _,
        w_out_all,
    ) = front(
        tokens, cotangent, ln1_gain, ln1_bias, angle_tables(length), w_query, w_key, w_value,
        w_gate, w_up, w_out, lengths, n, devices,
    )
    attn_rows = attn_rows.reshape(length, depth)
    weights = weights.reshape(2, n * share, depth)

    w_out_all = w_out_all.reshape(n, width, depth)
    attn_out = sum(dot(context_own[t], w_out_all[t]).astype(BF).astype(F32) for t in range(n))
    middle = inputs + attn_out
    scaled2, inverse2 = norm_parts(middle)
    ffn_in = (scaled2 * ln2_gain + ln2_bias).astype(BF)
    grad_parts, out_parts, down_grad, pair_grads, w_packed = ffn(
        ffn_in, grad_branch, weights, down_weight, w_packed, n, devices
    )
    grad_ffn_in = sum(grad_parts[p].astype(F32) for p in range(devices // 2))
    grad_norm2, gain2_grad, shift2_grad = norm_back(
        grad_ffn_in, scaled2, inverse2, ln2_gain
    )
    grad_middle = grad_out + grad_norm2
    grad_attn = grad_middle.astype(BF)
    w_packed = lax.all_gather(w_packed, "dp", axis=0)
    down_grad = lax.psum_scatter(down_grad, "tensor", scatter_dimension=0, tiled=True)[0]
    packed, packed_own, out_sums, out_piece, pair_grads = att_bwd(
        grad_attn, w_out_all, context_own, out_parts, pair_grads, q, k, v, context, logsum, cosine, sine, n
    )
    down_grad, out_piece, w_packed = lax.optimization_barrier((down_grad, out_piece, w_packed))
    grads = lax.all_gather(jnp.concatenate([down_grad, out_piece]), "dp", axis=0)
    ffn_out = sum(x.astype(F32) for x in (out_parts[0], *out_sums))
    output = jnp.where(valid, middle + ffn_out, 0.0).astype(BF)
    input_grad, sums, packed_grads = finish(
        attn_rows, packed, packed_own, w_packed, tokens, grad_middle, ln1_gain,
        jnp.stack([gain2_grad, shift2_grad]), devices,
    )
    packed_grads = packed_grads.reshape(devices, depth // devices, 3 * width)
    (
        gate_grad, up_grad, down_grad, out_grad, query_grad, key_grad, value_grad, input_grad,
        gain1_grad, shift1_grad, gain2_grad, shift2_grad,
    ) = unpack(pair_grads, grads, packed_grads, input_grad, sums)
    return (
        output, input_grad, gain1_grad, shift1_grad, query_grad, key_grad, value_grad, out_grad,
        gain2_grad, shift2_grad, gate_grad, up_grad, down_grad,
    )


def solution(mesh):
    rows = P(("dp", "tensor"), None)
    columns = P(None, "tensor")
    parts = P("tensor", None)
    return jax.shard_map(
        on_device,
        mesh=mesh,
        in_specs=(
            rows, P("dp"), P(), P(), columns, columns, columns, parts,
            P(), P(), columns, columns, parts, rows,
        ),
        out_specs=(
            rows, rows, P(), P(), columns, columns, columns, parts,
            P(), P(), columns, columns, parts,
        ),
        check_vma=False,
    )
```
